32 devices in a mesh: dp: 4 (over x, y), tp: 8 (over z, core).
Axes of the slice: x: 2, y: 2, z: 4, core: 2. Of those that a mesh axis runs over, the one named last changes fastest.
Arguments:
- hidden: bfloat16 [4, 6144, 1024], P('dp'), parts along dimension 0
- norm_w: bfloat16 [2, 1024], replicated
- w_z: bfloat16 [2, 1024, 2048], P(None, None, 'tp')
- w_x: bfloat16 [2, 1024, 2048], P(None, None, 'tp')
- w_bc: bfloat16 [2, 1024, 256], replicated
- w_dt: bfloat16 [2, 1024, 32], P(None, None, 'tp')
- conv_x: bfloat16 [2, 4, 2048], P(None, None, 'tp')
- conv_bc: bfloat16 [2, 4, 256], replicated
- bias_x: bfloat16 [2, 2048], P(None, 'tp')
- bias_bc: bfloat16 [2, 256], replicated
- dt_bias: float32 [2, 32], P(None, 'tp')
- a_log: float32 [2, 32], P(None, 'tp')
- d_skip: float32 [2, 32], P(None, 'tp')
- gate_w: bfloat16 [2, 2048], P(None, 'tp')
- w_out: bfloat16 [2, 2048, 1024], P(None, 'tp')
Outputs:
- output: bfloat16 [4, 6144, 1024], P('dp'), parts along dimension 0
There are 4 independent parts. The reference program is written for one: setup_inputs(seed, part) draws one part's arguments, and reference() takes and returns one part's arrays. A program takes and returns all parts, laid end to end along the dimension named above; an argument that names none is the same for every part.
All inputs are finite; a program needn't handle non-finite values.
Results may differ from the reference program's by a relative error of at most 0.013727.
Values sent between devices are 32-bit elements.
A program may use at most 1 GiB of HBM per device.

```python
import math
import jax
import jax.numpy as jnp
from jax import lax

BATCH_ROWS = 1
SEQ_LEN = 6144
D_MODEL = 1024
HEADS = 32
HEAD_DIM = 64
STATE_DIM = 128
LAYERS = 2
CONV_WIDTH = 4
BLOCK_LEN = 256

INNER_WIDTH = HEADS * HEAD_DIM
EPSILON = 1e-5


def setup_inputs(seed: int = 0, part: int = 0) -> dict:
    key_list = jax.random.split(jax.random.key(seed), 16)
    part_key = jax.random.fold_in(jax.random.key(seed + 1), part)
    in_scale = D_MODEL ** -0.5
    hidden = jax.random.normal(part_key, (BATCH_ROWS, SEQ_LEN, D_MODEL), jnp.float32)
    head_scale = jnp.exp(jax.random.uniform(key_list[0], (LAYERS, HEADS), jnp.float32, -1.2, 1.2))
    col_scale = jnp.repeat(head_scale, HEAD_DIM, axis=1)[:, None, :]
    dt_init = jnp.exp(jax.random.uniform(key_list[1], (LAYERS, HEADS), jnp.float32, math.log(0.001), math.log(0.1)))
    return {
        'hidden': hidden.astype(jnp.bfloat16),
        'norm_w': (1.0 + 0.2 * jax.random.normal(key_list[2], (LAYERS, D_MODEL), jnp.float32)).astype(jnp.bfloat16),
        'w_z': (in_scale * jax.random.normal(key_list[3], (LAYERS, D_MODEL, INNER_WIDTH), jnp.float32)).astype(jnp.bfloat16),
        'w_x': (in_scale * col_scale * jax.random.normal(key_list[4], (LAYERS, D_MODEL, INNER_WIDTH), jnp.float32)).astype(jnp.bfloat16),
        'w_bc': (in_scale * jax.random.normal(key_list[5], (LAYERS, D_MODEL, 2 * STATE_DIM), jnp.float32)).astype(jnp.bfloat16),
        'w_dt': (0.5 * in_scale * jax.random.normal(key_list[6], (LAYERS, D_MODEL, HEADS), jnp.float32)).astype(jnp.bfloat16),
        'conv_x': (0.5 * jax.random.normal(key_list[7], (LAYERS, CONV_WIDTH, INNER_WIDTH), jnp.float32)).astype(jnp.bfloat16),
        'conv_bc': (0.5 * jax.random.normal(key_list[8], (LAYERS, CONV_WIDTH, 2 * STATE_DIM), jnp.float32)).astype(jnp.bfloat16),
        'bias_x': (0.3 * jax.random.normal(key_list[9], (LAYERS, INNER_WIDTH), jnp.float32)).astype(jnp.bfloat16),
        'bias_bc': (0.3 * jax.random.normal(key_list[10], (LAYERS, 2 * STATE_DIM), jnp.float32)).astype(jnp.bfloat16),
        'dt_bias': dt_init + jnp.log(-jnp.expm1(-dt_init)),
        'a_log': jnp.log(jax.random.uniform(key_list[11], (LAYERS, HEADS), jnp.float32, 1.0, 16.0)),
        'd_skip': jax.random.uniform(key_list[12], (LAYERS, HEADS), jnp.float32, 0.5, 2.0),
        'gate_w': (1.0 + 0.2 * jax.random.normal(key_list[13], (LAYERS, INNER_WIDTH), jnp.float32)).astype(jnp.bfloat16),
        'w_out': (INNER_WIDTH ** -0.5 * jax.random.normal(key_list[14], (LAYERS, INNER_WIDTH, D_MODEL), jnp.float32)).astype(jnp.bfloat16),
    }


def causal_conv(seq_in, kernel, conv_bias):
    n_steps = seq_in.shape[1]
    padded = jnp.pad(seq_in, ((0, 0), (CONV_WIDTH - 1, 0), (0, 0)))
    conv_sum = conv_bias.astype(jnp.float32)
    for tap_index in range(CONV_WIDTH):
        conv_sum = conv_sum + padded[:, tap_index:tap_index + n_steps, :].astype(jnp.float32) * kernel[tap_index].astype(jnp.float32)
    return conv_sum


def ssd_sequence(seq_in):
    x_heads, dt_val, a_vals, b_in, c_in = seq_in
    n_blocks = SEQ_LEN // BLOCK_LEN
    step_ids = jnp.arange(BLOCK_LEN)
    lower_tri = step_ids[:, None] >= step_ids[None, :]

    def block_step(state, block):
        x_block, dt_block, a_block, b_block, c_block = block
        a_cum = jnp.cumsum(a_block, axis=0)
        seg_sum = a_cum[:, None, :] - a_cum[None, :, :]
        decay_mat = jnp.where(lower_tri[:, :, None], jnp.exp(jnp.minimum(seg_sum, 0.0)), 0.0)
        c_dot_b = jnp.einsum('in,jn->ij', c_block, b_block)
        x_dt = x_block * dt_block[:, :, None]
        y_in = jnp.einsum('ijh,jhp->ihp', decay_mat * c_dot_b[:, :, None], x_dt)
        y_st = jnp.einsum('in,hpn->ihp', c_block, state) * jnp.exp(a_cum)[:, :, None]
        tail_decay = jnp.exp(a_cum[-1][None, :] - a_cum)
        new_state = state * jnp.exp(a_cum[-1])[:, None, None] + jnp.einsum('jn,jhp->hpn', b_block, x_dt * tail_decay[:, :, None])
        return new_state, y_in + y_st

    blocks_in = (
        x_heads.reshape(n_blocks, BLOCK_LEN, HEADS, HEAD_DIM),
        dt_val.reshape(n_blocks, BLOCK_LEN, HEADS),
        a_vals.reshape(n_blocks, BLOCK_LEN, HEADS),
        b_in.reshape(n_blocks, BLOCK_LEN, STATE_DIM),
        c_in.reshape(n_blocks, BLOCK_LEN, STATE_DIM),
    )
    init_state = jnp.zeros((HEADS, HEAD_DIM, STATE_DIM), jnp.float32)
    last_state, y_blocks = lax.scan(block_step, init_state, blocks_in)
    return y_blocks.reshape(SEQ_LEN, HEADS, HEAD_DIM)


def mixer_layer(current, layer_params):
    norm_w, w_z, w_x, w_bc, w_dt, conv_x, conv_bc, bias_x, bias_bc, dt_bias, a_log, d_skip, gate_w, w_out = layer_params
    tokens = BATCH_ROWS * SEQ_LEN
    residual = current.astype(jnp.float32)
    normed = (residual * lax.rsqrt(jnp.mean(residual * residual, axis=-1, keepdims=True) + EPSILON) * norm_w.astype(jnp.float32)).astype(jnp.bfloat16)
    flat_in = normed.reshape(tokens, D_MODEL)
    gate_z = jnp.dot(flat_in, w_z, preferred_element_type=jnp.float32).astype(jnp.bfloat16)
    x_pre = jnp.dot(flat_in, w_x, preferred_element_type=jnp.float32).astype(jnp.bfloat16)
    bc_pre = jnp.dot(flat_in, w_bc, preferred_element_type=jnp.float32).astype(jnp.bfloat16)
    dt_pre = jnp.dot(flat_in, w_dt, preferred_element_type=jnp.float32).astype(jnp.bfloat16)
    x_act = jax.nn.silu(causal_conv(x_pre.reshape(BATCH_ROWS, SEQ_LEN, INNER_WIDTH), conv_x, bias_x))
    bc_act = jax.nn.silu(causal_conv(bc_pre.reshape(BATCH_ROWS, SEQ_LEN, 2 * STATE_DIM), conv_bc, bias_bc))
    dt_val = jax.nn.softplus(dt_pre.astype(jnp.float32).reshape(BATCH_ROWS, SEQ_LEN, HEADS) + dt_bias)
    a_vals = -dt_val * jnp.exp(a_log)
    x_heads = x_act.reshape(BATCH_ROWS, SEQ_LEN, HEADS, HEAD_DIM)
    y_heads = lax.map(ssd_sequence, (x_heads, dt_val, a_vals, bc_act[..., :STATE_DIM], bc_act[..., STATE_DIM:]))
    y_heads = y_heads + d_skip[:, None] * x_heads
    gated_v = y_heads.reshape(BATCH_ROWS, SEQ_LEN, INNER_WIDTH) * jax.nn.silu(gate_z.astype(jnp.float32).reshape(BATCH_ROWS, SEQ_LEN, INNER_WIDTH))
    normed_y = (gated_v * lax.rsqrt(jnp.mean(gated_v * gated_v, axis=-1, keepdims=True) + EPSILON) * gate_w.astype(jnp.float32)).astype(jnp.bfloat16)
    mixed_out = jnp.dot(normed_y.reshape(tokens, INNER_WIDTH), w_out, preferred_element_type=jnp.float32)
    return (residual + mixed_out.reshape(BATCH_ROWS, SEQ_LEN, D_MODEL)).astype(jnp.bfloat16)


def reference(hidden, norm_w, w_z, w_x, w_bc, w_dt, conv_x, conv_bc, bias_x, bias_bc, dt_bias, a_log, d_skip, gate_w, w_out):
    params = (norm_w, w_z, w_x, w_bc, w_dt, conv_x, conv_bc, bias_x, bias_bc, dt_bias, a_log, d_skip, gate_w, w_out)

    def layer_step(current, layer_params):
        return mixer_layer(current, layer_params), None

    final_hidden, unused = lax.scan(layer_step, hidden, params)
    return final_hidden
```

```python
import functools
import jax
import jax.numpy as jnp
from jax import lax
from jax.experimental import pallas as pl
from jax.experimental.pallas import tpu as pltpu

EPS = 1e-5
LOG2E = 1.4426950408889634
HI = lax.Precision.HIGHEST
F32 = jnp.float32
BF16 = jnp.bfloat16
BLK = 128


def silu(v):
    half = 0.5 * v
    return half + half * jnp.tanh(half)


def split3(v):
    a = v.astype(BF16)
    r = v - a.astype(F32)
    b = r.astype(BF16)
    c = (r - b.astype(F32)).astype(BF16)
    return a, b, c


def rms(u, nw):
    return (u * lax.rsqrt(jnp.mean(u * u, axis=-1, keepdims=True) + EPS) * nw).astype(BF16)


def dot(a, b, prec=None):
    return jnp.dot(a, b, preferred_element_type=F32, precision=prec)


def dott(a, b, prec=None):
    return lax.dot_general(a, b, (((1,), (1,)), ((), ())), preferred_element_type=F32, precision=prec)


def load_cols(wf_ref, wb_ref, n_dp, n_tp, rows, cols):
    for d in range(n_dp):
        for t in range(n_tp):
            wb_ref[d * rows:(d + 1) * rows, t * cols:(t + 1) * cols] = wf_ref[d * n_tp + t].astype(BF16)


def p1_body(off_ref, u_ref, halo_ref, nw_ref, wf_ref, sm_ref, wbc_ref, cbc_ref, bbc_ref, e3_ref,
            y_ref, c_ref, ac_ref, send_ref, wxb, wdt, cst, st, xpad, qpad, aoff, *, geom):
    n_dp, n_tp, hd, width, heads = geom
    i = pl.program_id(0)
    nst = 128
    pc = width // n_tp
    hp = heads // n_tp

    @pl.when(i == 0)
    def _():
        load_cols(wf_ref, wxb, n_dp, n_tp, wxb.shape[0] // n_dp, pc)
        kc = wxb.shape[0] // pc
        for t in range(n_tp):
            for k in range(hp):
                for c in range(kc):
                    wdt[hp * t + k:hp * t + k + 1, c * pc:(c + 1) * pc] = sm_ref[t, 16 + kc * k + c:17 + kc * k + c, :].astype(BF16)
            cst[hp * t:hp * (t + 1), :] = sm_ref[t, 8:8 + hp, :]
            cst[heads + hp * t:heads + hp * (t + 1), :] = sm_ref[t, 12:12 + hp, :]
        st[...] = jnp.zeros_like(st)
        aoff[...] = jnp.zeros_like(aoff)
        hh = rms(halo_ref[...], nw_ref[...])
        xpad[0:8, :] = dot(hh, wxb[...]).astype(BF16).astype(F32)
        qpad[0:8, :] = dot(hh, wbc_ref[...]).astype(BF16).astype(F32)

    @pl.when(i > 0)
    def _():
        xpad[0:8, :] = xpad[BLK:BLK + 8, :]
        qpad[0:8, :] = qpad[BLK:BLK + 8, :]

    h = rms(u_ref[...].astype(F32), nw_ref[...])
    xpad[8:8 + BLK, :] = dot(h, wxb[...]).astype(BF16).astype(F32)
    qpad[8:8 + BLK, :] = dot(h, wbc_ref[...]).astype(BF16).astype(F32)
    rT = dott(wdt[...], h).astype(BF16).astype(F32)

    acc = bbc_ref[...]
    for j in range(4):
        acc = acc + qpad[5 + j:5 + j + BLK, :] * cbc_ref[j:j + 1, :]
    bc = silu(acc)
    bmat, cmat = bc[:, :nst], bc[:, nst:]
    c_ref[...] = cmat

    pre = rT + cst[0:heads, 0:BLK]
    dtT = jnp.maximum(pre, 0.0) + jnp.log1p(jnp.exp(-jnp.abs(pre)))
    aT = dtT * cst[heads:2 * heads, 0:BLK]
    ri = lax.broadcasted_iota(jnp.int32, (BLK, BLK), 0)
    ci = lax.broadcasted_iota(jnp.int32, (BLK, BLK), 1)
    upper = jnp.where(ri <= ci, 1.0, 0.0).astype(F32)
    acT = dot(aT, upper, HI)
    alast = acT[:, BLK - 1:BLK]
    ac = acT.T
    wT = dtT * jnp.exp2(alast - acT)
    w3 = jnp.concatenate(split3(wT), axis=0)
    e3 = jnp.concatenate(split3(jnp.exp2(acT)), axis=0)
    d3 = jnp.concatenate(split3(jnp.broadcast_to(jnp.exp2(alast), (heads, BLK))), axis=0)
    ac_ref[...] = acT + aoff[:, 0:1]
    aoff[...] = aoff[...] + alast

    cbm = jnp.where(ri >= ci, dott(cmat, bmat, HI), 0.0)
    bT = bmat.T

    lane = lax.broadcasted_iota(jnp.int32, (BLK, 128), 1)
    low = lane < hd
    w3t, e3t, d3t = w3.T, e3.T, d3.T
    for t in range(n_tp):
        for pp in range(pc // 128):
            lo = t * pc + pp * 128
            sl = slice(lo, lo + 128)
            csl = slice(pp * 128, (pp + 1) * 128)
            acc = sm_ref[t, 4:5, csl]
            for j in range(4):
                acc = acc + xpad[5 + j:5 + j + BLK, sl] * sm_ref[t, j:j + 1, csl]
            x = silu(acc)
            ms = []
            for hh in range(2):
                h_id = lo // hd + hh
                col = jnp.broadcast_to(ac[:, h_id:h_id + 1], (BLK, BLK))
                dec = jnp.exp2(jnp.minimum(col - acT[h_id:h_id + 1, :], 0.0))
                ms.append(dec * cbm * dtT[h_id:h_id + 1, :])
            m = jnp.concatenate(ms, axis=1)
            xx = jnp.concatenate([jnp.where(low, x, 0.0), jnp.where(low, 0.0, x)], axis=0)
            y = dot(m, xx, HI)
            eexp = dot(e3t, e3_ref[:, sl])
            wexp = dot(w3t, e3_ref[:, sl])
            dexp = dot(d3t, e3_ref[:, sl])
            s = st[:, sl]
            y = y + dot(cmat, s, HI) * eexp
            st[:, sl] = s * dexp + dot(bT, x * wexp, HI)
            y_ref[:, sl] = y + sm_ref[t, 6:7, csl] * x

    @pl.when(i == pl.num_programs(0) - 1)
    def _():
        send_ref[...] = st[...]


def p1(u, off, halo, nw, wf, wbc, cbc, bbc, e3, n, n_dp, n_tp, interpret=False):
    d_model = u.shape[1]
    width = 256 * n_tp
    heads = width // 64
    rows = d_model // n_dp
    geom = (n_dp, n_tp, 64, width, heads)
    nb = n // BLK
    full = lambda shp: pl.BlockSpec(shp, lambda i, o: (0,) * len(shp), pipeline_mode=pl.Buffered(1))
    gs = pltpu.PrefetchScalarGridSpec(
        num_scalar_prefetch=1, grid=(nb,),
        in_specs=[
            pl.BlockSpec((BLK, d_model), lambda i, o: (o[0] + i, 0)),
            full((8, d_model)), full((1, d_model)),
            full((n_dp * n_tp, rows, 256)),
            pl.BlockSpec((n_tp, 32, 256), lambda i, o: (0, rows // 32, 0), pipeline_mode=pl.Buffered(1)),
            full((d_model, 256)), full((4, 256)), full((1, 256)), full((3 * heads, width)),
        ],
        out_specs=[
            pl.BlockSpec((BLK, width), lambda i, o: (i, 0)),
            pl.BlockSpec((BLK, 128), lambda i, o: (i, 0)),
            pl.BlockSpec((heads, BLK), lambda i, o: (0, i)),
            pl.BlockSpec((128, width), lambda i, o: (0, 0)),
        ],
        scratch_shapes=[
            pltpu.VMEM((d_model, width), BF16), pltpu.VMEM((heads, d_model), BF16), pltpu.VMEM((2 * heads, 256), F32),
            pltpu.VMEM((128, width), F32), pltpu.VMEM((BLK + 8, width), F32), pltpu.VMEM((BLK + 8, 256), F32),
            pltpu.VMEM((heads, 128), F32),
        ])
    return pl.pallas_call(
        functools.partial(p1_body, geom=geom), grid_spec=gs, name="p1",
        out_shape=[jax.ShapeDtypeStruct((n, width), F32), jax.ShapeDtypeStruct((n, 128), F32),
                   jax.ShapeDtypeStruct((heads, n), F32), jax.ShapeDtypeStruct((128, width), F32)],
        compiler_params=pltpu.CompilerParams(dimension_semantics=("arbitrary",), vmem_limit_bytes=60 << 20),
        cost_estimate=pl.CostEstimate(flops=n * 70_000_000, bytes_accessed=n * 12000, transcendentals=0),
        interpret=interpret,
    )(off, u, halo, nw, wf, wf, wbc, cbc, bbc, e3)


def p2_body(off_ref, u_ref, nw_ref, wz_ref, wo_ref, sm_ref, y_ref, c_ref, ac_ref, s_ref, e3_ref,
            o_ref, f_ref, wzb, wob, s3, *, geom):
    n_dp, n_tp, hd, width, heads = geom
    pc = width // n_tp
    rows_z = wzb.shape[0] // n_dp

    @pl.when(pl.program_id(0) == 0)
    def _():
        load_cols(wz_ref, wzb, n_dp, n_tp, rows_z, pc)
        load_wo(wo_ref, wob, n_dp, n_tp)
        a, b, c = split3(s_ref[...])
        s3[0, 0:128, :] = a
        s3[0, 128:256, :] = a
        s3[1, 0:128, :] = b
        s3[1, 128:256, :] = b
        s3[2, 0:128, :] = c
        s3[2, 128:256, :] = a

    u = u_ref[...].astype(F32)
    h = rms(u, nw_ref[...])
    c1, c2, c3 = split3(c_ref[...])
    cc12 = jnp.concatenate([c1, c2], axis=1)
    cc13 = jnp.concatenate([c1, c3], axis=1)
    eT = jnp.concatenate(split3(jnp.exp2(ac_ref[...])), axis=0).T
    vs, ss = [], 0.0
    for t in range(n_tp):
        sl = slice(t * pc, (t + 1) * pc)
        z = dot(h, wzb[:, sl]).astype(BF16).astype(F32)
        cor = dot(cc12, s3[0, :, sl]) + dot(cc12, s3[1, :, sl]) + dot(cc13, s3[2, :, sl])
        v = (y_ref[:, sl] + cor * dot(eT, e3_ref[:, sl])) * silu(z)
        ss = ss + jnp.sum(v * v, axis=-1, keepdims=True)
        vs.append(v)
    sc = lax.rsqrt(ss / width + EPS)
    acc = u
    g = jnp.concatenate([(vs[t] * sc * sm_ref[t, 5:6, :]).astype(BF16) for t in range(n_tp)], axis=1)
    un = (u + dot(g, wob[...])).astype(BF16)
    o_ref[...] = un
    f_ref[...] = un.astype(F32)


def load_wo(wf_ref, wb_ref, n_dp, n_tp):
    rows = wb_ref.shape[0] // n_tp
    cols = wb_ref.shape[1] // n_dp
    for d in range(n_dp):
        for t in range(n_tp):
            wb_ref[t * rows:(t + 1) * rows, d * cols:(d + 1) * cols] = wf_ref[d * n_tp + t].astype(BF16)


def p2(u, off, nw, wz, wo, wsm, y, c, ac, s, e3, n, n_dp, n_tp, out_rows=None, interpret=False):
    d_model = u.shape[1]
    width = 256 * n_tp
    heads = width // 64
    rows = d_model // n_dp
    geom = (n_dp, n_tp, 64, width, heads)
    nb = n // BLK
    full = lambda shp: pl.BlockSpec(shp, lambda i, o: (0,) * len(shp), pipeline_mode=pl.Buffered(1))
    gs = pltpu.PrefetchScalarGridSpec(
        num_scalar_prefetch=1, grid=(nb,),
        in_specs=[
            pl.BlockSpec((BLK, d_model), lambda i, o: (o[0] + i, 0)),
            full((1, d_model)),
            full((n_dp * n_tp, rows, 256)), full((n_dp * n_tp, 256, d_model // n_dp)),
            pl.BlockSpec((n_tp, 32, 256), lambda i, o: (0, rows // 32, 0), pipeline_mode=pl.Buffered(1)),
            pl.BlockSpec((BLK, width), lambda i, o: (i, 0)),
            pl.BlockSpec((BLK, 128), lambda i, o: (i, 0)),
            pl.BlockSpec((heads, BLK), lambda i, o: (0, i)),
            full((128, width)), full((3 * heads, width)),
        ],
        out_specs=[pl.BlockSpec((BLK, d_model), lambda i, o: (o[1] + i, 0)), pl.BlockSpec((BLK, d_model), lambda i, o: (i, 0))],
        scratch_shapes=[pltpu.VMEM((d_model, width), BF16), pltpu.VMEM((width, d_model), BF16),
                        pltpu.VMEM((3, 256, width), BF16)])
    return pl.pallas_call(
        functools.partial(p2_body, geom=geom), grid_spec=gs, name="p2",
        out_shape=[jax.ShapeDtypeStruct((out_rows or n, d_model), BF16), jax.ShapeDtypeStruct((n, d_model), F32)],
        compiler_params=pltpu.CompilerParams(dimension_semantics=("arbitrary",), vmem_limit_bytes=60 << 20),
        cost_estimate=pl.CostEstimate(flops=n * 30_000_000, bytes_accessed=n * 12000, transcendentals=0),
        interpret=interpret,
    )(off, u, nw, wz, wo, wsm, y, c, ac, s, e3)


def fin_body(off_ref, buf_ref, f_ref, o_ref):
    o_ref[...] = f_ref[...].astype(BF16)


def finish(buf, f, off):
    n, d_model = f.shape
    rows = 512
    gs = pltpu.PrefetchScalarGridSpec(
        num_scalar_prefetch=1, grid=(n // rows,),
        in_specs=[pl.BlockSpec(memory_space=pl.ANY), pl.BlockSpec((rows, d_model), lambda i, o: (i, 0))],
        out_specs=pl.BlockSpec((rows, d_model), lambda i, o: (o[0] + i, 0)))
    return pl.pallas_call(
        fin_body, grid_spec=gs, name="finish", out_shape=jax.ShapeDtypeStruct(buf.shape, BF16),
        input_output_aliases={1: 0},
        compiler_params=pltpu.CompilerParams(dimension_semantics=("arbitrary",)),
        cost_estimate=pl.CostEstimate(flops=n * d_model, bytes_accessed=n * d_model * 6, transcendentals=0),
    )(off, buf, f)


from jax.sharding import PartitionSpec as P


def small_rows(conv, bias, gate, skip, dtb, al, wdt):
    f = lambda v: v.astype(F32)
    hp = skip.shape[0]
    return jnp.concatenate([
        f(conv), f(bias)[None], f(gate)[None], jnp.repeat(skip, 256 // hp)[None], jnp.zeros((1, 256), F32),
        jnp.broadcast_to(dtb[:, None], (hp, 256)), jnp.broadcast_to((-jnp.exp(al) * LOG2E)[:, None], (hp, 256)),
        f(wdt).T.reshape(-1, 256)], axis=0)


def solution(mesh):
    n_tp, n_dp = mesh.shape['tp'], mesh.shape['dp']
    rep, col, vec = P(), P(None, None, 'tp'), P(None, 'tp')
    in_specs = (P('dp'), rep, col, col, rep, col, col, rep, vec, rep, vec, vec, vec, vec, P(None, 'tp', None))

    def device_forward(hidden, norm_w, w_z, w_x, w_bc, w_dt, conv_x, conv_bc, bias_x, bias_bc, dt_bias, a_log, d_skip, gate_w, w_out):
        u = hidden[0]
        steps, d_model = u.shape
        heads = dt_bias.shape[1] * n_tp
        n = steps // 2
        dp, tp = lax.axis_index('dp'), lax.axis_index('tp')
        core = tp % 2
        rows, ocols = d_model // n_dp, d_model // n_dp
        gather = lambda v: lax.all_gather(v, ('dp', 'tp'))
        one = jnp.repeat(jnp.eye(heads, dtype=BF16), 64, axis=1)
        e3 = jnp.concatenate([one, one, one], axis=0)
        up = [(2 * k, 2 * k + 1) for k in range(n_tp // 2)]
        swap = [(k, k ^ 1) for k in range(n_tp)]
        wxs, wzs, wos = [], [], []
        for l in range(2):
            sm = small_rows(conv_x[l], bias_x[l], gate_w[l], d_skip[l], dt_bias[l], a_log[l], w_dt[l])
            qx = lax.dynamic_slice(w_x[l], (dp * rows, 0), (rows, 256)).astype(F32)
            wxs.append(gather(jnp.concatenate([qx, sm], axis=0)))
            wzs.append(gather(lax.dynamic_slice(w_z[l], (dp * rows, 0), (rows, 256)).astype(F32)))
            wos.append(gather(lax.dynamic_slice(w_out[l], (0, dp * ocols), (256, ocols)).astype(F32)))
        cur, nb = u, n // BLK
        off = jnp.stack([core * nb, 0 * core])
        zero = jnp.zeros((2,), jnp.int32)
        start = lax.dynamic_slice(u, (core * (n - 8), 0), (8, d_model)).astype(F32)
        halo = jnp.where(core == 1, start, 0.0)
        for l in range(2):
            nw = norm_w[l].astype(F32)[None]
            y, c, ac, s_end = p1(cur, off, halo, nw, wxs[l], w_bc[l], conv_bc[l].astype(F32), bias_bc[l].astype(F32)[None], e3, n, n_dp, n_tp)
            s = lax.ppermute(s_end, 'tp', up)
            off2 = off if l == 0 else jnp.stack([0 * core, core * nb])
            o, f = p2(cur, off2, nw, wzs[l], wos[l], wxs[l], y, c, ac, s, e3, n, n_dp, n_tp, out_rows=n if l == 0 else steps)
            cur, off = o, zero
            if l == 0:
                halo = lax.ppermute(f[n - 8:], 'tp', up)
        other = lax.ppermute(f, 'tp', swap)
        return finish(o, other, jnp.reshape((1 - core) * (n // 512), (1,)))[None]

    return jax.shard_map(device_forward, mesh=mesh, in_specs=in_specs, out_specs=P('dp'), check_vma=False)
```

```python
import functools
import jax
import jax.numpy as jnp
from jax import lax
from jax.experimental import pallas as pl
from jax.experimental.pallas import tpu as pltpu

EPS = 1e-5
LOG2E = 1.4426950408889634
HI = lax.Precision.HIGHEST
F32 = jnp.float32
BF16 = jnp.bfloat16
BLK = 128
BLK2 = 256


def silu(v):
    half = 0.5 * v
    return half + half * jnp.tanh(half)


def split3(v):
    a = v.astype(BF16)
    r = v - a.astype(F32)
    b = r.astype(BF16)
    c = (r - b.astype(F32)).astype(BF16)
    return a, b, c


def rms(u, nw):
    return (u * lax.rsqrt(jnp.mean(u * u, axis=-1, keepdims=True) + EPS) * nw).astype(BF16)


def dot(a, b, prec=None):
    return jnp.dot(a, b, preferred_element_type=F32, precision=prec)


def dott(a, b, prec=None):
    return lax.dot_general(a, b, (((1,), (1,)), ((), ())), preferred_element_type=F32, precision=prec)


def load_cols(wf_ref, wb_ref, n_dp, n_tp, rows, cols):
    for d in range(n_dp):
        for t in range(n_tp):
            wb_ref[d * rows:(d + 1) * rows, t * cols:(t + 1) * cols] = wf_ref[d * n_tp + t].astype(BF16)


def time_of(r):
    return 8 * (r % 8) + r // 8


def roll8(v):
    c = v.shape[1]
    return pltpu.roll(v.reshape(3, 8, c), 1, 1).reshape(24, c)


def conv_block(cur, prev, taps, bias, first):
    now = roll8(cur[40:])
    sh = jnp.where(first, prev, now)
    out = bias + cur * taps[3]
    for k in range(1, 4):
        out = out + jnp.concatenate([sh[8 * (3 - k):], cur[:64 - 8 * k]], axis=0) * taps[3 - k]
    return out, now


def unmix(v, buf):
    n, c = v.shape
    for j in range(c // 128):
        buf[n * j:n * (j + 1), :] = v[:, 128 * j:128 * (j + 1)]
    cols = [jnp.concatenate([buf[pl.ds(n * j + b + k, 8, stride=8), :] for b in range(0, n, 64) for k in range(8)], axis=0)
            for j in range(c // 128)]
    return jnp.concatenate(cols, axis=1)


EARLY = (2, 4, 6)


def head_row(h, heads):
    return (h % 2) * (heads // 2) + h // 2


def expand_mat(heads):
    order = sorted(range(heads), key=lambda h: head_row(h, heads))
    one = jnp.repeat(jnp.eye(heads, dtype=BF16)[jnp.array(order)], 64, axis=1)
    return jnp.concatenate([one, one, one], axis=0)


def kcat6(parts):
    a, b, c = parts
    return jnp.concatenate([a, b, c, a], axis=1), jnp.concatenate([b, a], axis=1)


def kcat6r(parts):
    a, b, c = parts
    return jnp.concatenate([a, a, a, b], axis=0), jnp.concatenate([b, c], axis=0)


def block_diag(x, lo, hi):
    z = jnp.zeros((x.shape[0], 128), BF16)
    l, r = x[:, :128], x[:, 128:]
    return jnp.concatenate([
        jnp.concatenate([l * lo, z], axis=1), jnp.concatenate([l * hi, z], axis=1),
        jnp.concatenate([z, r * lo], axis=1), jnp.concatenate([z, r * hi], axis=1)], axis=0)


def p1_body(off_ref, u_ref, halo_ref, nw_ref, wf_ref, sm_ref, wbc_ref, cbc_ref, bbc_ref, e3_ref,
            y_ref, c_ref, ac_ref, send_ref, wxb, wdt, cst, st, xcar, qcar, aoff, ubuf, *, geom, mixed):
    n_dp, n_tp, hd, width, heads = geom
    i = pl.program_id(0)
    nst = 128
    pc = width // n_tp
    hp = heads // n_tp
    sub = BLK // 2

    @pl.when(i == 0)
    def _():
        load_cols(wf_ref, wxb, n_dp, n_tp, wxb.shape[0] // n_dp, pc)
        kc = wxb.shape[0] // pc
        for t in range(n_tp):
            for k in range(hp):
                r = head_row(hp * t + k, heads)
                for c in range(kc):
                    wdt[r:r + 1, c * pc:(c + 1) * pc] = sm_ref[t, 16 + kc * k + c:17 + kc * k + c, :].astype(BF16)
                cst[r:r + 1, :] = sm_ref[t, 8 + k:9 + k, :]
                cst[heads + r:heads + r + 1, :] = sm_ref[t, 12 + k:13 + k, :]
        st[...] = jnp.zeros_like(st)
        aoff[...] = jnp.zeros_like(aoff)
        hh = rms(halo_ref[...], nw_ref[...])
        xcar[...] = roll8(dot(hh, wxb[...]).astype(BF16).astype(F32))
        qcar[...] = roll8(dot(hh, wbc_ref[...]).astype(BF16).astype(F32))

    if mixed:
        u = u_ref[...].astype(F32)
    else:
        u = unmix(u_ref[...].astype(F32), ubuf)
    h = rms(u, nw_ref[...])
    first = lax.broadcasted_iota(jnp.int32, (24, 256), 0) % 8 == 0

    def conv(cur, prev, taps, bias):
        a, now = conv_block(cur[:sub], prev, taps, bias, first)
        b, now = conv_block(cur[sub:], now, taps, bias, first)
        return silu(jnp.concatenate([a, b], axis=0)), now

    q0 = dot(h, wbc_ref[...])
    rT = dott(wdt[...], h).astype(BF16).astype(F32)
    x0s = {}

    def proj(t):
        if t < n_tp:
            x0s[t] = dot(h, wxb[:, t * pc:(t + 1) * pc])

    for t in range(EARLY[0]):
        proj(t)

    bc, qcar[...] = conv(q0.astype(BF16).astype(F32), qcar[...],
                         [cbc_ref[j:j + 1, :] for j in range(4)], bbc_ref[...])
    bmat, cmat = bc[:, :nst], bc[:, nst:]
    c_ref[...] = cmat

    pre = rT + cst[0:heads, 0:BLK]
    dtT = jnp.maximum(pre, 0.0) + jnp.log1p(jnp.exp(-jnp.abs(pre)))
    aT = dtT * cst[heads:2 * heads, 0:BLK]
    ri = lax.broadcasted_iota(jnp.int32, (BLK, BLK), 0)
    ci = lax.broadcasted_iota(jnp.int32, (BLK, BLK), 1)
    tr, tc = ri // sub * sub + time_of(ri % sub), ci // sub * sub + time_of(ci % sub)
    upper = jnp.where(tr <= tc, 1.0, 0.0).astype(F32)
    acT = dot(aT, upper, HI)
    mid, alast = acT[:, sub - 1:sub], acT[:, BLK - 1:BLK]
    lowh = lax.broadcasted_iota(jnp.int32, (heads, BLK), 1) < sub
    wT = dtT * jnp.exp2(jnp.where(lowh, mid, alast) - acT)
    w3t = jnp.concatenate(split3(wT), axis=0).T
    a3t = jnp.concatenate(split3(acT), axis=0).T
    ac_ref[...] = acT + aoff[:, 0:1]
    aoff[...] = aoff[...] + alast
    low16 = lax.broadcasted_iota(jnp.int32, (heads // 2, BLK), 1) < sub

    def pair_rows(v):
        ev, od = v[:heads // 2], v[heads // 2:]
        return (jnp.where(low16, ev, pltpu.roll(od, sub, 1)), jnp.where(low16, pltpu.roll(ev, sub, 1), od))

    ac_rows, dt_rows = pair_rows(acT), pair_rows(dtT)

    for t in range(EARLY[0], EARLY[1]):
        proj(t)
    cb = dott(cmat, bmat, HI)
    for t in range(EARLY[1], EARLY[2]):
        proj(t)
    rs = lax.broadcasted_iota(jnp.int32, (sub, BLK), 0)
    cs = lax.broadcasted_iota(jnp.int32, (sub, BLK), 1)
    tri = time_of(rs) >= time_of(cs % sub)
    ca, cb_ = cb[:sub], cb[sub:]
    cbd = (jnp.where(tri, jnp.where(cs < sub, ca, pltpu.roll(ca, sub, 1)), 0.0),
           jnp.where(tri, jnp.where(cs < sub, pltpu.roll(cb_, sub, 1), cb_), 0.0))
    bT = bmat.T
    la = jnp.concatenate([bT[:, :sub], cb_[:, :sub]], axis=0)
    la1, la2 = kcat6(split3(la))
    lb1, lb2 = kcat6(split3(pltpu.roll(bT, sub, 1)[:, :sub]))
    c1, c2, c3 = split3(cmat)
    cc12 = jnp.concatenate([c1, c2], axis=1)
    cc13 = jnp.concatenate([c1, c3], axis=1)

    lane = lax.broadcasted_iota(jnp.int32, (sub, 128), 1)
    lo = jnp.where(lane < hd, 1.0, 0.0).astype(BF16)
    hi = jnp.where(lane < hd, 0.0, 1.0).astype(BF16)
    def pre(t):
        sl = slice(t * pc, (t + 1) * pc)
        s1, s2, s3 = split3(st[:, sl])
        inter = (dot(cc12, jnp.concatenate([s1, s1], axis=0)) + dot(cc12, jnp.concatenate([s2, s2], axis=0))
                 + dot(cc13, jnp.concatenate([s3, s1], axis=0)))
        proj(t + EARLY[2])
        return x0s.pop(t), dot(a3t, e3_ref[:, sl]), dot(w3t, e3_ref[:, sl]), inter

    def mid_(t, x0, acx, wx, inter):
        sl = slice(t * pc, (t + 1) * pc)
        x, xcar[:, sl] = conv(x0.astype(BF16).astype(F32), xcar[:, sl],
                              [sm_ref[t, j:j + 1, :] for j in range(4)], sm_ref[t, 4:5, :])
        xw = split3(x * wx)
        r = kcat6r([v[:sub] for v in xw]) + kcat6r([v[sub:] for v in xw])
        ms, xs = [], []
        for k in range(2):
            rows = slice(k * sub, (k + 1) * sub)
            m = []
            for p in range(pc // 128):
                g = t * (pc // 128) + p
                seg = acx[rows, p * 128:(p + 1) * 128] - ac_rows[k][g:g + 1, :]
                m.append(jnp.exp2(jnp.minimum(seg, 0.0)) * cbd[k] * dt_rows[k][g:g + 1, :])
            ms.append(split3(jnp.concatenate(m, axis=1)))
            xs.append([block_diag(v, lo, hi) for v in split3(x[rows])])
        return x, acx, inter, r, ms, xs

    def fin(t, x, acx, inter, r, ms, xs):
        sl = slice(t * pc, (t + 1) * pc)
        ra1, ra2, rb1, rb2 = r
        ra = dot(la1, ra1) + dot(la2, ra2)
        rb = dot(lb1, rb1) + dot(lb2, rb2)
        am, al = acx[sub - 1:sub], acx[BLK - 1:BLK]
        skip = sm_ref[t, 6:7, :]
        for k in range(2):
            rows = slice(k * sub, (k + 1) * sub)
            (m1, m2, m3), (x1, x2, x3) = ms[k], xs[k]
            r1 = dot(jnp.concatenate([m1, m2, m3], axis=0), x1)
            r2 = dot(jnp.concatenate([m1, m2], axis=0), x2)
            y = r1[:sub] + r1[sub:2 * sub] + r1[2 * sub:] + r2[:sub] + r2[sub:] + dot(m1, x3)
            y = y + inter[rows] * jnp.exp2(acx[rows])
            if k == 1:
                y = y + ra[nst:] * jnp.exp2(acx[rows] - am)
            y_ref[rows, sl] = y + skip * x[rows]
        st[:, sl] = st[:, sl] * jnp.exp2(al) + ra[:nst] * jnp.exp2(al - am) + rb

    m = mid_(0, *pre(0))
    for t in range(n_tp):
        if t + 1 < n_tp:
            p = pre(t + 1)
        fin(t, *m)
        if t + 1 < n_tp:
            m = mid_(t + 1, *p)

    @pl.when(i == pl.num_programs(0) - 1)
    def _():
        send_ref[...] = st[...]


def p1(u, off, halo, nw, wf, wbc, cbc, bbc, e3, n, n_dp, n_tp, mixed, interpret=False):
    d_model = u.shape[1]
    width = 256 * n_tp
    heads = width // 64
    rows = d_model // n_dp
    geom = (n_dp, n_tp, 64, width, heads)
    nb = n // BLK
    full = lambda shp: pl.BlockSpec(shp, lambda i, o: (0,) * len(shp), pipeline_mode=pl.Buffered(1))
    gs = pltpu.PrefetchScalarGridSpec(
        num_scalar_prefetch=1, grid=(nb,),
        in_specs=[
            pl.BlockSpec((BLK, d_model), lambda i, o: (o[0] + i, 0)),
            full((24, d_model)), full((1, d_model)),
            full((n_dp * n_tp, rows, 256)),
            pl.BlockSpec((n_tp, 32, 256), lambda i, o: (0, rows // 32, 0), pipeline_mode=pl.Buffered(1)),
            full((d_model, 256)), full((4, 256)), full((1, 256)), full((3 * heads, width)),
        ],
        out_specs=[
            pl.BlockSpec((BLK, width), lambda i, o: (i, 0)),
            pl.BlockSpec((BLK, 128), lambda i, o: (i, 0)),
            pl.BlockSpec((heads, BLK), lambda i, o: (0, i)),
            pl.BlockSpec((128, width), lambda i, o: (0, 0)),
        ],
        scratch_shapes=[
            pltpu.VMEM((d_model, width), BF16), pltpu.VMEM((heads, d_model), BF16), pltpu.VMEM((2 * heads, 256), F32),
            pltpu.VMEM((128, width), F32), pltpu.VMEM((24, width), F32), pltpu.VMEM((24, 256), F32),
            pltpu.VMEM((heads, 128), F32), pltpu.VMEM((d_model // 128 * BLK, 128), F32),
        ])
    return pl.pallas_call(
        functools.partial(p1_body, geom=geom, mixed=mixed), grid_spec=gs, name="p1",
        out_shape=[jax.ShapeDtypeStruct((n, width), F32), jax.ShapeDtypeStruct((n, 128), F32),
                   jax.ShapeDtypeStruct((heads, n), F32), jax.ShapeDtypeStruct((128, width), F32)],
        compiler_params=pltpu.CompilerParams(dimension_semantics=("arbitrary",), vmem_limit_bytes=60 << 20),
        cost_estimate=pl.CostEstimate(flops=n * 70_000_000, bytes_accessed=n * 12000, transcendentals=0),
        interpret=interpret,
    )(off, u, halo, nw, wf, wf, wbc, cbc, bbc, e3)


def p2_body(off_ref, u_ref, nw_ref, wz_ref, wo_ref, sm_ref, y_ref, c_ref, ac_ref, s_ref, e3_ref,
            o_ref, f_ref, wzb, wob, s3, ubuf, *, geom, mix_in, mix_out):
    n_dp, n_tp, hd, width, heads = geom
    pc = width // n_tp
    rows_z = wzb.shape[0] // n_dp

    @pl.when(pl.program_id(0) == 0)
    def _():
        load_cols(wz_ref, wzb, n_dp, n_tp, rows_z, pc)
        load_wo(wo_ref, wob, n_dp, n_tp)
        a, b, c = split3(s_ref[...])
        s3[0, 0:128, :] = a
        s3[0, 128:256, :] = a
        s3[1, 0:128, :] = b
        s3[1, 128:256, :] = b
        s3[2, 0:128, :] = c
        s3[2, 128:256, :] = a

    if mix_in:
        u = u_ref[...].astype(F32)
    else:
        u = unmix(u_ref[...].astype(F32), ubuf)
    h = rms(u, nw_ref[...])
    c1, c2, c3 = split3(c_ref[...])
    cc12 = jnp.concatenate([c1, c2], axis=1)
    cc13 = jnp.concatenate([c1, c3], axis=1)
    eT = jnp.concatenate(split3(jnp.exp2(ac_ref[...])), axis=0).T
    vs, ss = [], 0.0
    for t in range(n_tp):
        sl = slice(t * pc, (t + 1) * pc)
        z = dot(h, wzb[:, sl]).astype(BF16).astype(F32)
        cor = dot(cc12, s3[0, :, sl]) + dot(cc12, s3[1, :, sl]) + dot(cc13, s3[2, :, sl])
        v = (y_ref[:, sl] + cor * dot(eT, e3_ref[:, sl])) * silu(z)
        ss = ss + jnp.sum(v * v, axis=-1, keepdims=True)
        vs.append(v)
    sc = lax.rsqrt(ss / width + EPS)
    acc = u
    g = jnp.concatenate([(vs[t] * sc * sm_ref[t, 5:6, :]).astype(BF16) for t in range(n_tp)], axis=1)
    un = (u + dot(g, wob[...])).astype(BF16)
    f_ref[...] = un.astype(F32)
    if mix_out:
        o_ref[...] = un
    else:
        o_ref[...] = unmix(un.astype(F32), ubuf).astype(BF16)


def load_wo(wf_ref, wb_ref, n_dp, n_tp):
    rows = wb_ref.shape[0] // n_tp
    cols = wb_ref.shape[1] // n_dp
    for d in range(n_dp):
        for t in range(n_tp):
            wb_ref[t * rows:(t + 1) * rows, d * cols:(d + 1) * cols] = wf_ref[d * n_tp + t].astype(BF16)


def p2(u, off, nw, wz, wo, wsm, y, c, ac, s, e3, n, n_dp, n_tp, mix_in, mix_out, out_rows=None, interpret=False):
    d_model = u.shape[1]
    width = 256 * n_tp
    heads = width // 64
    rows = d_model // n_dp
    geom = (n_dp, n_tp, 64, width, heads)
    nb = n // BLK2
    full = lambda shp: pl.BlockSpec(shp, lambda i, o: (0,) * len(shp), pipeline_mode=pl.Buffered(1))
    gs = pltpu.PrefetchScalarGridSpec(
        num_scalar_prefetch=1, grid=(nb,),
        in_specs=[
            pl.BlockSpec((BLK2, d_model), lambda i, o: (o[0] + i, 0)),
            full((1, d_model)),
            full((n_dp * n_tp, rows, 256)), full((n_dp * n_tp, 256, d_model // n_dp)),
            pl.BlockSpec((n_tp, 32, 256), lambda i, o: (0, rows // 32, 0), pipeline_mode=pl.Buffered(1)),
            pl.BlockSpec((BLK2, width), lambda i, o: (i, 0)),
            pl.BlockSpec((BLK2, 128), lambda i, o: (i, 0)),
            pl.BlockSpec((heads, BLK2), lambda i, o: (0, i)),
            full((128, width)), full((3 * heads, width)),
        ],
        out_specs=[pl.BlockSpec((BLK2, d_model), lambda i, o: (o[1] + i, 0)), pl.BlockSpec((BLK2, d_model), lambda i, o: (i, 0))],
        scratch_shapes=[pltpu.VMEM((d_model, width), BF16), pltpu.VMEM((width, d_model), BF16),
                        pltpu.VMEM((3, 256, width), BF16), pltpu.VMEM((d_model // 128 * BLK2, 128), F32)])
    return pl.pallas_call(
        functools.partial(p2_body, geom=geom, mix_in=mix_in, mix_out=mix_out), grid_spec=gs, name="p2",
        out_shape=[jax.ShapeDtypeStruct((out_rows or n, d_model), BF16), jax.ShapeDtypeStruct((n, d_model), F32)],
        compiler_params=pltpu.CompilerParams(dimension_semantics=("arbitrary",), vmem_limit_bytes=60 << 20),
        cost_estimate=pl.CostEstimate(flops=n * 30_000_000, bytes_accessed=n * 12000, transcendentals=0),
        interpret=interpret,
    )(off, u, nw, wz, wo, wsm, y, c, ac, s, e3)


def fin_body(off_ref, buf_ref, f_ref, o_ref, ubuf):
    o_ref[...] = unmix(f_ref[...], ubuf).astype(BF16)


def finish(buf, f, off):
    n, d_model = f.shape
    rows = 512
    gs = pltpu.PrefetchScalarGridSpec(
        num_scalar_prefetch=1, grid=(n // rows,),
        in_specs=[pl.BlockSpec(memory_space=pl.ANY), pl.BlockSpec((rows, d_model), lambda i, o: (i, 0))],
        out_specs=pl.BlockSpec((rows, d_model), lambda i, o: (o[0] + i, 0)),
        scratch_shapes=[pltpu.VMEM((d_model // 128 * rows, 128), F32)])
    return pl.pallas_call(
        fin_body, grid_spec=gs, name="finish", out_shape=jax.ShapeDtypeStruct(buf.shape, BF16),
        input_output_aliases={1: 0},
        compiler_params=pltpu.CompilerParams(dimension_semantics=("arbitrary",)),
        cost_estimate=pl.CostEstimate(flops=n * d_model, bytes_accessed=n * d_model * 6, transcendentals=0),
    )(off, buf, f)


from jax.sharding import PartitionSpec as P


def small_rows(conv, bias, gate, skip, dtb, al, wdt):
    f = lambda v: v.astype(F32)
    hp = skip.shape[0]
    return jnp.concatenate([
        f(conv), f(bias)[None], f(gate)[None], jnp.repeat(skip, 256 // hp)[None], jnp.zeros((1, 256), F32),
        jnp.broadcast_to(dtb[:, None], (hp, 256)), jnp.broadcast_to((-jnp.exp(al) * LOG2E)[:, None], (hp, 256)),
        f(wdt).T.reshape(-1, 256)], axis=0)


def solution(mesh):
    n_tp, n_dp = mesh.shape['tp'], mesh.shape['dp']
    rep, col, vec = P(), P(None, None, 'tp'), P(None, 'tp')
    in_specs = (P('dp'), rep, col, col, rep, col, col, rep, vec, rep, vec, vec, vec, vec, P(None, 'tp', None))

    def device_forward(hidden, norm_w, w_z, w_x, w_bc, w_dt, conv_x, conv_bc, bias_x, bias_bc, dt_bias, a_log, d_skip, gate_w, w_out):
        u = hidden[0]
        steps, d_model = u.shape
        heads = dt_bias.shape[1] * n_tp
        n = steps // 2
        dp, tp = lax.axis_index('dp'), lax.axis_index('tp')
        core = tp % 2
        rows, ocols = d_model // n_dp, d_model // n_dp
        gather = lambda v: lax.all_gather(v, ('dp', 'tp'))
        e3 = expand_mat(heads)
        up = [(2 * k, 2 * k + 1) for k in range(n_tp // 2)]
        swap = [(k, k ^ 1) for k in range(n_tp)]
        wxs, wzs, wos = [], [], []
        for l in range(2):
            sm = small_rows(conv_x[l], bias_x[l], gate_w[l], d_skip[l], dt_bias[l], a_log[l], w_dt[l])
            qx = lax.dynamic_slice(w_x[l], (dp * rows, 0), (rows, 256)).astype(F32)
            wxs.append(gather(jnp.concatenate([qx, sm], axis=0)))
            wzs.append(gather(lax.dynamic_slice(w_z[l], (dp * rows, 0), (rows, 256)).astype(F32)))
            wos.append(gather(lax.dynamic_slice(w_out[l], (0, dp * ocols), (256, ocols)).astype(F32)))
        cur = u
        off = jnp.stack([core * (n // BLK), 0 * core])
        zero = jnp.zeros((2,), jnp.int32)
        tail = u[n - 64:n].astype(F32).reshape(8, 8, d_model).transpose(1, 0, 2).reshape(64, d_model)[40:]
        halo = jnp.where(core == 1, tail, 0.0)
        for l in range(2):
            nw = norm_w[l].astype(F32)[None]
            y, c, ac, s_end = p1(cur, off, halo, nw, wxs[l], w_bc[l], conv_bc[l].astype(F32), bias_bc[l].astype(F32)[None], e3, n, n_dp, n_tp, l > 0)
            s = lax.ppermute(s_end, 'tp', up)
            off2 = jnp.stack([core, 0 * core] if l == 0 else [0 * core, core]) * (n // BLK2)
            o, f = p2(cur, off2, nw, wzs[l], wos[l], wxs[l], y, c, ac, s, e3, n, n_dp, n_tp, l > 0, l == 0, out_rows=n if l == 0 else steps)
            cur, off = o, zero
            if l == 0:
                halo = lax.ppermute(f[n - 24:], 'tp', up)
        other = lax.ppermute(f, 'tp', swap)
        return finish(o, other, jnp.reshape((1 - core) * (n // 512), (1,)))[None]

    return jax.shard_map(device_forward, mesh=mesh, in_specs=in_specs, out_specs=P('dp'), check_vma=False)
```

```python
import functools
import jax
import jax.numpy as jnp
from jax import lax
from jax.experimental import pallas as pl
from jax.experimental.pallas import tpu as pltpu

EPS = 1e-5
LOG2E = 1.4426950408889634
HI = lax.Precision.HIGHEST
F32 = jnp.float32
BF16 = jnp.bfloat16
BLK = 128
BLK2 = 256


def silu(v):
    half = 0.5 * v
    return half + half * jnp.tanh(half)


def split3(v):
    a = v.astype(BF16)
    r = v - a.astype(F32)
    b = r.astype(BF16)
    c = (r - b.astype(F32)).astype(BF16)
    return a, b, c


def rms(u, nw):
    return (u * lax.rsqrt(jnp.mean(u * u, axis=-1, keepdims=True) + EPS) * nw).astype(BF16)


def dot(a, b, prec=None):
    return jnp.dot(a, b, preferred_element_type=F32, precision=prec)


def dott(a, b, prec=None):
    return lax.dot_general(a, b, (((1,), (1,)), ((), ())), preferred_element_type=F32, precision=prec)


def load_cols(wf_ref, wb_ref, n_dp, n_tp, rows, cols):
    for d in range(n_dp):
        for t in range(n_tp):
            wb_ref[d * rows:(d + 1) * rows, t * cols:(t + 1) * cols] = wf_ref[d * n_tp + t].astype(BF16)


def time_of(r):
    return 8 * (r % 8) + r // 8


def roll8(v):
    c = v.shape[1]
    return pltpu.roll(v.reshape(3, 8, c), 1, 1).reshape(24, c)


def conv_block(cur, prev, taps, bias, first):
    now = roll8(cur[40:])
    sh = jnp.where(first, prev, now)
    out = bias + cur * taps[3]
    for k in range(1, 4):
        out = out + jnp.concatenate([sh[8 * (3 - k):], cur[:64 - 8 * k]], axis=0) * taps[3 - k]
    return out, now


def unmix(v, buf):
    n, c = v.shape
    for j in range(c // 128):
        buf[n * j:n * (j + 1), :] = v[:, 128 * j:128 * (j + 1)]
    cols = [jnp.concatenate([buf[pl.ds(n * j + b + k, 8, stride=8), :] for b in range(0, n, 64) for k in range(8)], axis=0)
            for j in range(c // 128)]
    return jnp.concatenate(cols, axis=1)


EARLY = (2, 4, 6)


def head_row(h, heads):
    return (h % 2) * (heads // 2) + h // 2


def expand_mat(heads):
    order = sorted(range(heads), key=lambda h: head_row(h, heads))
    one = jnp.repeat(jnp.eye(heads, dtype=BF16)[jnp.array(order)], 64, axis=1)
    return jnp.concatenate([one, one, one], axis=0)


def kcat6(parts):
    a, b, c = parts
    return jnp.concatenate([a, b, c, a], axis=1), jnp.concatenate([b, a], axis=1)


def kcat6r(parts):
    a, b, c = parts
    return jnp.concatenate([a, a, a, b], axis=0), jnp.concatenate([b, c], axis=0)


def block_diag(x, lo, hi):
    z = jnp.zeros((x.shape[0], 128), BF16)
    l, r = x[:, :128], x[:, 128:]
    return jnp.concatenate([
        jnp.concatenate([l * lo, z], axis=1), jnp.concatenate([l * hi, z], axis=1),
        jnp.concatenate([z, r * lo], axis=1), jnp.concatenate([z, r * hi], axis=1)], axis=0)


def p1_body(off_ref, u_ref, halo_ref, nw_ref, wf_ref, sm_ref, wbc_ref, cbc_ref, bbc_ref, e3_ref,
            y_ref, c_ref, ac_ref, send_ref, wxb, wdt, cst, st, xcar, qcar, aoff, ubuf, *, geom, mixed):
    n_dp, n_tp, hd, width, heads = geom
    i = pl.program_id(0)
    nst = 128
    pc = width // n_tp
    hp = heads // n_tp
    sub = BLK // 2

    @pl.when(i == 0)
    def _():
        load_cols(wf_ref, wxb, n_dp, n_tp, wxb.shape[0] // n_dp, pc)
        kc = wxb.shape[0] // pc
        for t in range(n_tp):
            for k in range(hp):
                r = head_row(hp * t + k, heads)
                for c in range(kc):
                    wdt[r:r + 1, c * pc:(c + 1) * pc] = sm_ref[t, 16 + kc * k + c:17 + kc * k + c, :].astype(BF16)
                cst[r:r + 1, :] = sm_ref[t, 8 + k:9 + k, :]
                cst[heads + r:heads + r + 1, :] = sm_ref[t, 12 + k:13 + k, :]
        st[...] = jnp.zeros_like(st)
        aoff[...] = jnp.zeros_like(aoff)
        hh = rms(halo_ref[...], nw_ref[...])
        xcar[...] = roll8(dot(hh, wxb[...]).astype(BF16).astype(F32))
        qcar[...] = roll8(dot(hh, wbc_ref[...]).astype(BF16).astype(F32))

    if mixed:
        u = u_ref[...].astype(F32)
    else:
        u = unmix(u_ref[...].astype(F32), ubuf)
    h = rms(u, nw_ref[...])
    first = lax.broadcasted_iota(jnp.int32, (24, 256), 0) % 8 == 0

    def conv(cur, prev, taps, bias):
        a, now = conv_block(cur[:sub], prev, taps, bias, first)
        b, now = conv_block(cur[sub:], now, taps, bias, first)
        return silu(jnp.concatenate([a, b], axis=0)), now

    q0 = dot(h, wbc_ref[...])
    rT = dott(wdt[...], h).astype(BF16).astype(F32)
    x0s = {}

    def proj(t):
        if t < n_tp:
            x0s[t] = dot(h, wxb[:, t * pc:(t + 1) * pc])

    for t in range(EARLY[0]):
        proj(t)

    bc, qcar[...] = conv(q0.astype(BF16).astype(F32), qcar[...],
                         [cbc_ref[j:j + 1, :] for j in range(4)], bbc_ref[...])
    bmat, cmat = bc[:, :nst], bc[:, nst:]
    c_ref[...] = cmat

    pre = rT + cst[0:heads, 0:BLK]
    dtT = jnp.maximum(pre, 0.0) + jnp.log1p(jnp.exp(-jnp.abs(pre)))
    aT = dtT * cst[heads:2 * heads, 0:BLK]
    ri = lax.broadcasted_iota(jnp.int32, (BLK, BLK), 0)
    ci = lax.broadcasted_iota(jnp.int32, (BLK, BLK), 1)
    tr, tc = ri // sub * sub + time_of(ri % sub), ci // sub * sub + time_of(ci % sub)
    upper = jnp.where(tr <= tc, 1.0, 0.0).astype(F32)
    acT = dot(aT, upper, HI)
    mid, alast = acT[:, sub - 1:sub], acT[:, BLK - 1:BLK]
    lowh = lax.broadcasted_iota(jnp.int32, (heads, BLK), 1) < sub
    wT = dtT * jnp.exp2(jnp.where(lowh, mid, alast) - acT)
    w3t = jnp.concatenate(split3(wT), axis=0).T
    a3t = jnp.concatenate(split3(acT), axis=0).T
    ac_ref[...] = acT + aoff[:, 0:1]
    aoff[...] = aoff[...] + alast
    low16 = lax.broadcasted_iota(jnp.int32, (heads // 2, BLK), 1) < sub

    def pair_rows(v):
        ev, od = v[:heads // 2], v[heads // 2:]
        return (jnp.where(low16, ev, pltpu.roll(od, sub, 1)), jnp.where(low16, pltpu.roll(ev, sub, 1), od))

    ac_rows, dt_rows = pair_rows(acT), pair_rows(dtT)

    for t in range(EARLY[0], EARLY[1]):
        proj(t)
    cb = dott(cmat, bmat, HI)
    for t in range(EARLY[1], EARLY[2]):
        proj(t)
    rs = lax.broadcasted_iota(jnp.int32, (sub, BLK), 0)
    cs = lax.broadcasted_iota(jnp.int32, (sub, BLK), 1)
    tri = time_of(rs) >= time_of(cs % sub)
    ca, cb_ = cb[:sub], cb[sub:]
    cbd = (jnp.where(tri, jnp.where(cs < sub, ca, pltpu.roll(ca, sub, 1)), 0.0),
           jnp.where(tri, jnp.where(cs < sub, pltpu.roll(cb_, sub, 1), cb_), 0.0))
    bT = bmat.T
    la = jnp.concatenate([bT[:, :sub], cb_[:, :sub]], axis=0)
    la1, la2 = kcat6(split3(la))
    lb1, lb2 = kcat6(split3(pltpu.roll(bT, sub, 1)[:, :sub]))
    c1, c2, c3 = split3(cmat)
    cc12 = jnp.concatenate([c1, c2], axis=1)
    cc13 = jnp.concatenate([c1, c3], axis=1)

    lane = lax.broadcasted_iota(jnp.int32, (sub, 128), 1)
    lo = jnp.where(lane < hd, 1.0, 0.0).astype(BF16)
    hi = jnp.where(lane < hd, 0.0, 1.0).astype(BF16)
    def pre(t):
        sl = slice(t * pc, (t + 1) * pc)
        s1, s2, s3 = split3(st[:, sl])
        inter = (dot(cc12, jnp.concatenate([s1, s1], axis=0)) + dot(cc12, jnp.concatenate([s2, s2], axis=0))
                 + dot(cc13, jnp.concatenate([s3, s1], axis=0)))
        proj(t + EARLY[2])
        return x0s.pop(t), dot(a3t, e3_ref[:, sl]), dot(w3t, e3_ref[:, sl]), inter

    def mid_(t, x0, acx, wx, inter):
        sl = slice(t * pc, (t + 1) * pc)
        x, xcar[:, sl] = conv(x0.astype(BF16).astype(F32), xcar[:, sl],
                              [sm_ref[t, j:j + 1, :] for j in range(4)], sm_ref[t, 4:5, :])
        xw = split3(x * wx)
        r = kcat6r([v[:sub] for v in xw]) + kcat6r([v[sub:] for v in xw])
        ms, xs = [], []
        for k in range(2):
            rows = slice(k * sub, (k + 1) * sub)
            m = []
            for p in range(pc // 128):
                g = t * (pc // 128) + p
                seg = acx[rows, p * 128:(p + 1) * 128] - ac_rows[k][g:g + 1, :]
                m.append(jnp.exp2(jnp.minimum(seg, 0.0)) * cbd[k] * dt_rows[k][g:g + 1, :])
            ms.append(split3(jnp.concatenate(m, axis=1)))
            xs.append([block_diag(v, lo, hi) for v in split3(x[rows])])
        return x, acx, inter, r, ms, xs

    def fin(t, x, acx, inter, r, ms, xs):
        sl = slice(t * pc, (t + 1) * pc)
        ra1, ra2, rb1, rb2 = r
        ra = dot(la1, ra1) + dot(la2, ra2)
        rb = dot(lb1, rb1) + dot(lb2, rb2)
        am, al = acx[sub - 1:sub], acx[BLK - 1:BLK]
        skip = sm_ref[t, 6:7, :]
        for k in range(2):
            rows = slice(k * sub, (k + 1) * sub)
            (m1, m2, m3), (x1, x2, x3) = ms[k], xs[k]
            r1 = dot(jnp.concatenate([m1, m2, m3], axis=0), x1)
            r2 = dot(jnp.concatenate([m1, m2], axis=0), x2)
            y = r1[:sub] + r1[sub:2 * sub] + r1[2 * sub:] + r2[:sub] + r2[sub:] + dot(m1, x3)
            y = y + inter[rows] * jnp.exp2(acx[rows])
            if k == 1:
                y = y + ra[nst:] * jnp.exp2(acx[rows] - am)
            y_ref[rows, sl] = y + skip * x[rows]
        st[:, sl] = st[:, sl] * jnp.exp2(al) + ra[:nst] * jnp.exp2(al - am) + rb

    m = mid_(0, *pre(0))
    for t in range(n_tp):
        if t + 1 < n_tp:
            p = pre(t + 1)
        fin(t, *m)
        if t + 1 < n_tp:
            m = mid_(t + 1, *p)

    @pl.when(i == pl.num_programs(0) - 1)
    def _():
        send_ref[...] = st[...]


def p1(u, off, halo, nw, wf, wbc, cbc, bbc, e3, n, n_dp, n_tp, mixed, interpret=False):
    d_model = u.shape[1]
    width = 256 * n_tp
    heads = width // 64
    rows = d_model // n_dp
    geom = (n_dp, n_tp, 64, width, heads)
    nb = n // BLK
    full = lambda shp: pl.BlockSpec(shp, lambda i, o: (0,) * len(shp), pipeline_mode=pl.Buffered(1))
    gs = pltpu.PrefetchScalarGridSpec(
        num_scalar_prefetch=1, grid=(nb,),
        in_specs=[
            pl.BlockSpec((BLK, d_model), lambda i, o: (o[0] + i, 0)),
            full((24, d_model)), full((1, d_model)),
            full((n_dp * n_tp, rows, 256)),
            pl.BlockSpec((n_tp, 32, 256), lambda i, o: (0, rows // 32, 0), pipeline_mode=pl.Buffered(1)),
            full((d_model, 256)), full((4, 256)), full((1, 256)), full((3 * heads, width)),
        ],
        out_specs=[
            pl.BlockSpec((BLK, width), lambda i, o: (i, 0)),
            pl.BlockSpec((BLK, 128), lambda i, o: (i, 0)),
            pl.BlockSpec((heads, BLK), lambda i, o: (0, i)),
            pl.BlockSpec((128, width), lambda i, o: (0, 0)),
        ],
        scratch_shapes=[
            pltpu.VMEM((d_model, width), BF16), pltpu.VMEM((heads, d_model), BF16), pltpu.VMEM((2 * heads, 256), F32),
            pltpu.VMEM((128, width), F32), pltpu.VMEM((24, width), F32), pltpu.VMEM((24, 256), F32),
            pltpu.VMEM((heads, 128), F32), pltpu.VMEM((d_model // 128 * BLK, 128), F32),
        ])
    return pl.pallas_call(
        functools.partial(p1_body, geom=geom, mixed=mixed), grid_spec=gs, name="p1",
        out_shape=[jax.ShapeDtypeStruct((n, width), F32), jax.ShapeDtypeStruct((n, 128), F32),
                   jax.ShapeDtypeStruct((heads, n), F32), jax.ShapeDtypeStruct((128, width), F32)],
        compiler_params=pltpu.CompilerParams(dimension_semantics=("arbitrary",), vmem_limit_bytes=60 << 20),
        cost_estimate=pl.CostEstimate(flops=n * 70_000_000, bytes_accessed=n * 12000, transcendentals=0),
        interpret=interpret,
    )(off, u, halo, nw, wf, wf, wbc, cbc, bbc, e3)


def p2_body(off_ref, u_ref, nw_ref, wz_ref, wo_ref, sm_ref, y_ref, c_ref, ac_ref, s_ref, e3_ref,
            o_ref, f_ref, wzb, wob, s3, ubuf, *, geom, mix_in, mix_out):
    n_dp, n_tp, hd, width, heads = geom
    pc = width // n_tp
    rows_z = wzb.shape[0] // n_dp

    @pl.when(pl.program_id(0) == 0)
    def _():
        load_cols(wz_ref, wzb, n_dp, n_tp, rows_z, pc)
        load_wo(wo_ref, wob, n_dp, n_tp)
        a, b, c = split3(s_ref[...])
        s3[0, 0:128, :] = a
        s3[0, 128:256, :] = a
        s3[1, 0:128, :] = b
        s3[1, 128:256, :] = b
        s3[2, 0:128, :] = c
        s3[2, 128:256, :] = a

    if mix_in:
        u = u_ref[...].astype(F32)
    else:
        u = unmix(u_ref[...].astype(F32), ubuf)
    h = rms(u, nw_ref[...])
    c1, c2, c3 = split3(c_ref[...])
    cc12 = jnp.concatenate([c1, c2], axis=1)
    cc13 = jnp.concatenate([c1, c3], axis=1)
    eT = jnp.concatenate(split3(jnp.exp2(ac_ref[...])), axis=0).T
    vs, ss = [], 0.0
    for t in range(n_tp):
        sl = slice(t * pc, (t + 1) * pc)
        z = dot(h, wzb[:, sl]).astype(BF16).astype(F32)
        cor = dot(cc12, s3[0, :, sl]) + dot(cc12, s3[1, :, sl]) + dot(cc13, s3[2, :, sl])
        v = (y_ref[:, sl] + cor * dot(eT, e3_ref[:, sl])) * silu(z)
        ss = ss + jnp.sum(v * v, axis=-1, keepdims=True)
        vs.append(v)
    sc = lax.rsqrt(ss / width + EPS)
    acc = u
    g = jnp.concatenate([(vs[t] * sc * sm_ref[t, 5:6, :]).astype(BF16) for t in range(n_tp)], axis=1)
    un = (u + dot(g, wob[...])).astype(BF16)
    f_ref[...] = un.astype(F32)
    if mix_out:
        o_ref[...] = un
    else:
        o_ref[...] = unmix(un.astype(F32), ubuf).astype(BF16)


def load_wo(wf_ref, wb_ref, n_dp, n_tp):
    rows = wb_ref.shape[0] // n_tp
    cols = wb_ref.shape[1] // n_dp
    for d in range(n_dp):
        for t in range(n_tp):
            wb_ref[t * rows:(t + 1) * rows, d * cols:(d + 1) * cols] = wf_ref[d * n_tp + t].astype(BF16)


def p2(u, off, nw, wz, wo, wsm, y, c, ac, s, e3, n, n_dp, n_tp, mix_in, mix_out, out_rows=None, interpret=False):
    d_model = u.shape[1]
    width = 256 * n_tp
    heads = width // 64
    rows = d_model // n_dp
    geom = (n_dp, n_tp, 64, width, heads)
    nb = n // BLK2
    full = lambda shp: pl.BlockSpec(shp, lambda i, o: (0,) * len(shp), pipeline_mode=pl.Buffered(1))
    gs = pltpu.PrefetchScalarGridSpec(
        num_scalar_prefetch=1, grid=(nb,),
        in_specs=[
            pl.BlockSpec((BLK2, d_model), lambda i, o: (o[0] + i, 0)),
            full((1, d_model)),
            full((n_dp * n_tp, rows, 256)), full((n_dp * n_tp, 256, d_model // n_dp)),
            pl.BlockSpec((n_tp, 32, 256), lambda i, o: (0, rows // 32, 0), pipeline_mode=pl.Buffered(1)),
            pl.BlockSpec((BLK2, width), lambda i, o: (i, 0)),
            pl.BlockSpec((BLK2, 128), lambda i, o: (i, 0)),
            pl.BlockSpec((heads, BLK2), lambda i, o: (0, i)),
            full((128, width)), full((3 * heads, width)),
        ],
        out_specs=[pl.BlockSpec((BLK2, d_model), lambda i, o: (o[1] + i, 0)), pl.BlockSpec((BLK2, d_model), lambda i, o: (i, 0))],
        scratch_shapes=[pltpu.VMEM((d_model, width), BF16), pltpu.VMEM((width, d_model), BF16),
                        pltpu.VMEM((3, 256, width), BF16), pltpu.VMEM((d_model // 128 * BLK2, 128), F32)])
    return pl.pallas_call(
        functools.partial(p2_body, geom=geom, mix_in=mix_in, mix_out=mix_out), grid_spec=gs, name="p2",
        out_shape=[jax.ShapeDtypeStruct((out_rows or n, d_model), BF16), jax.ShapeDtypeStruct((n, d_model), F32)],
        compiler_params=pltpu.CompilerParams(dimension_semantics=("arbitrary",), vmem_limit_bytes=60 << 20),
        cost_estimate=pl.CostEstimate(flops=n * 30_000_000, bytes_accessed=n * 12000, transcendentals=0),
        interpret=interpret,
    )(off, u, nw, wz, wo, wsm, y, c, ac, s, e3)


def fin_body(off_ref, buf_ref, f_ref, o_ref, ubuf):
    o_ref[...] = unmix(f_ref[...], ubuf).astype(BF16)


def finish(buf, f, off):
    n, d_model = f.shape
    rows = 512
    gs = pltpu.PrefetchScalarGridSpec(
        num_scalar_prefetch=1, grid=(n // rows,),
        in_specs=[pl.BlockSpec(memory_space=pl.ANY), pl.BlockSpec((rows, d_model), lambda i, o: (i, 0))],
        out_specs=pl.BlockSpec((rows, d_model), lambda i, o: (o[0] + i, 0)),
        scratch_shapes=[pltpu.VMEM((d_model // 128 * rows, 128), F32)])
    return pl.pallas_call(
        fin_body, grid_spec=gs, name="finish", out_shape=jax.ShapeDtypeStruct(buf.shape, BF16),
        input_output_aliases={1: 0},
        compiler_params=pltpu.CompilerParams(dimension_semantics=("arbitrary",)),
        cost_estimate=pl.CostEstimate(flops=n * d_model, bytes_accessed=n * d_model * 6, transcendentals=0),
    )(off, buf, f)


class Gather:
    N_SEM = 17

    def __init__(self, a, g, send, recv, base):
        self.a, self.g, self.send, self.recv, self.base = a, g, send, recv, base
        dp, tp = lax.axis_index('dp'), lax.axis_index('tp')
        x, y, z, c = dp // 2, dp % 2, tp // 2, tp % 2
        self.dp, self.tp, self.z, self.c = dp, tp, z, c
        self.plane = [(1 - x) * 2 + y, x * 2 + 1 - y, (1 - x) * 2 + 1 - y]
        self.partner = (dp, 2 * z + 1 - c)

    def slot(self, dz):
        return 2 * ((self.z + 4 - dz) % 4) + self.c

    def rdma(self, k, src, dst, dev):
        return pltpu.make_async_remote_copy(src_ref=src, dst_ref=dst, send_sem=self.send.at[self.base + k],
                                            recv_sem=self.recv.at[self.base + k], device_id=dev,
                                            device_id_type=pl.DeviceIdType.MESH)

    def local(self):
        return pltpu.make_async_copy(self.a, self.g.at[:, self.tp], self.send.at[self.base])

    def own(self):
        return self.rdma(1, self.a, self.g.at[:, self.tp], self.partner)

    def line(self, dz):
        return self.rdma(1 + dz, self.a.at[self.dp], self.g.at[self.dp, self.tp], (self.dp, 2 * ((self.z + dz) % 4) + self.c))

    def cross(self, dz, n):
        s = self.slot(dz)
        return self.rdma(2 + 3 * dz + n, self.g.at[self.dp, s], self.g.at[self.dp, s], (self.plane[n], self.tp))

    def over(self, dz):
        s = self.slot(dz)
        return self.rdma(13 + dz, self.g.at[:, s], self.g.at[:, s], self.partner)

    def peers(self):
        return [(self.dp, 2 * ((self.z + dz) % 4) + self.c) for dz in (1, 2, 3)] + [(p, self.tp) for p in self.plane] + [self.partner]

    def step0(self):
        for dz in (1, 3, 2):
            self.line(dz).start()
        self.own().start()
        self.local().start()

    def step1(self, dz):
        self.line(dz).wait_recv()
        for n in range(3):
            self.cross(dz, n).start()

    def step2(self, dz):
        for n in range(3):
            self.cross(dz, n).wait_recv()
        self.over(dz).start()

    def step3(self):
        self.local().wait()
        self.own().wait()
        for dz in (1, 2, 3):
            self.line(dz).wait_send()
            for n in range(3):
                self.cross(dz, n).wait_send()
            self.over(dz).wait()


def entry_barrier(peers):
    sem = pltpu.get_barrier_semaphore()
    for p in peers:
        pl.semaphore_signal(sem, inc=1, device_id=p, device_id_type=pl.DeviceIdType.MESH)
    pl.semaphore_wait(sem, len(peers))


def gather_body(*refs, n):
    ins, outs, (send, recv) = refs[:n], refs[n:2 * n], refs[2 * n:]
    gs = [Gather(a, g, send, recv, Gather.N_SEM * k) for k, (a, g) in enumerate(zip(ins, outs))]
    entry_barrier(gs[0].peers())
    for g in gs:
        g.step0()
    for g in gs:
        for dz in (1, 3, 2):
            g.step1(dz)
    for g in gs:
        for dz in (1, 3, 2):
            g.step2(dz)
    for g in gs:
        g.step3()


def gather_all(shards, n_tp, cid):
    n = len(shards)
    return pl.pallas_call(
        functools.partial(gather_body, n=n), name="gather",
        out_shape=[jax.ShapeDtypeStruct((s.shape[0], n_tp) + s.shape[1:], F32) for s in shards],
        in_specs=[pl.BlockSpec(memory_space=pl.ANY)] * n, out_specs=[pl.BlockSpec(memory_space=pl.ANY)] * n,
        scratch_shapes=[pltpu.SemaphoreType.DMA((Gather.N_SEM * n,)), pltpu.SemaphoreType.DMA((Gather.N_SEM * n,))],
        compiler_params=pltpu.CompilerParams(collective_id=cid, has_side_effects=True),
        cost_estimate=pl.CostEstimate(flops=10 ** 10, bytes_accessed=n * 16 * 10 ** 6, transcendentals=0),
    )(*shards)


from jax.sharding import PartitionSpec as P


def small_rows(conv, bias, gate, skip, dtb, al, wdt):
    f = lambda v: v.astype(F32)
    hp = skip.shape[0]
    return jnp.concatenate([
        f(conv), f(bias)[None], f(gate)[None], jnp.repeat(skip, 256 // hp)[None], jnp.zeros((1, 256), F32),
        jnp.broadcast_to(dtb[:, None], (hp, 256)), jnp.broadcast_to((-jnp.exp(al) * LOG2E)[:, None], (hp, 256)),
        f(wdt).T.reshape(-1, 256)], axis=0)


def solution(mesh):
    n_tp, n_dp = mesh.shape['tp'], mesh.shape['dp']
    rep, col, vec = P(), P(None, None, 'tp'), P(None, 'tp')
    in_specs = (P('dp'), rep, col, col, rep, col, col, rep, vec, rep, vec, vec, vec, vec, P(None, 'tp', None))

    def device_forward(hidden, norm_w, w_z, w_x, w_bc, w_dt, conv_x, conv_bc, bias_x, bias_bc, dt_bias, a_log, d_skip, gate_w, w_out):
        u = hidden[0]
        steps, d_model = u.shape
        heads = dt_bias.shape[1] * n_tp
        n = steps // 2
        dp, tp = lax.axis_index('dp'), lax.axis_index('tp')
        core = tp % 2
        rows, ocols = d_model // n_dp, d_model // n_dp
        gather = lambda v: lax.all_gather(v, ('dp', 'tp'))
        e3 = expand_mat(heads)
        up = [(2 * k, 2 * k + 1) for k in range(n_tp // 2)]
        swap = [(k, k ^ 1) for k in range(n_tp)]
        def cut(w):
            return w.reshape(n_dp, rows, 256).astype(F32)

        def cut_o(w):
            return w.reshape(256, n_dp, ocols).transpose(1, 0, 2).astype(F32)

        sm = [small_rows(conv_x[l], bias_x[l], gate_w[l], d_skip[l], dt_bias[l], a_log[l], w_dt[l]) for l in range(2)]
        sx = [jnp.concatenate([cut(w_x[l]), jnp.broadcast_to(sm[l], (n_dp,) + sm[l].shape)], axis=1) for l in range(2)]
        wxs, wzs, wos = [None, None], [None, None], [None, None]
        wxs[0], wzs[0], wos[0] = gather_all([sx[0], cut(w_z[0]), cut_o(w_out[0])], n_tp, 1)
        part = lambda v: lax.dynamic_index_in_dim(v, dp, 0, keepdims=False)
        wxs[1] = gather(part(sx[1]))
        wzs[1] = gather(part(cut(w_z[1])))
        wos[1] = gather(part(cut_o(w_out[1])))
        flat = lambda v: v.reshape((n_dp * n_tp,) + v.shape[2:])
        wxs[0], wzs[0], wos[0] = flat(wxs[0]), flat(wzs[0]), flat(wos[0])
        cur = u
        off = jnp.stack([core * (n // BLK), 0 * core])
        zero = jnp.zeros((2,), jnp.int32)
        tail = u[n - 64:n].astype(F32).reshape(8, 8, d_model).transpose(1, 0, 2).reshape(64, d_model)[40:]
        halo = jnp.where(core == 1, tail, 0.0)
        for l in range(2):
            nw = norm_w[l].astype(F32)[None]
            y, c, ac, s_end = p1(cur, off, halo, nw, wxs[l], w_bc[l], conv_bc[l].astype(F32), bias_bc[l].astype(F32)[None], e3, n, n_dp, n_tp, l > 0)
            s = lax.ppermute(s_end, 'tp', up)
            off2 = jnp.stack([core, 0 * core] if l == 0 else [0 * core, core]) * (n // BLK2)
            o, f = p2(cur, off2, nw, wzs[l], wos[l], wxs[l], y, c, ac, s, e3, n, n_dp, n_tp, l > 0, l == 0, out_rows=n if l == 0 else steps)
            cur, off = o, zero
            if l == 0:
                halo = lax.ppermute(f[n - 24:], 'tp', up)
        other = lax.ppermute(f, 'tp', swap)
        return finish(o, other, jnp.reshape((1 - core) * (n // 512), (1,)))[None]

    return jax.shard_map(device_forward, mesh=mesh, in_specs=in_specs, out_specs=P('dp'), check_vma=False)
```

```python
import functools
import jax
import jax.numpy as jnp
from jax import lax
from jax.experimental import pallas as pl
from jax.experimental.pallas import tpu as pltpu

EPS = 1e-5
LOG2E = 1.4426950408889634
HI = lax.Precision.HIGHEST
F32 = jnp.float32
BF16 = jnp.bfloat16
BLK = 128
BLK2 = 256


def silu(v):
    return v / (1.0 + jnp.exp2(v * -LOG2E))


def split3(v):
    a = v.astype(BF16)
    r = v - a.astype(F32)
    b = r.astype(BF16)
    c = (r - b.astype(F32)).astype(BF16)
    return a, b, c


def rms(u, nw):
    return (u * lax.rsqrt(jnp.mean(u * u, axis=-1, keepdims=True) + EPS) * nw).astype(BF16)


def dot(a, b, prec=None):
    return jnp.dot(a, b, preferred_element_type=F32, precision=prec)


def dott(a, b, prec=None):
    return lax.dot_general(a, b, (((1,), (1,)), ((), ())), preferred_element_type=F32, precision=prec)


def load_cols(wf_ref, wb_ref, n_dp, n_tp, rows, cols):
    for d in range(n_dp):
        for t in range(n_tp):
            wb_ref[d * rows:(d + 1) * rows, t * cols:(t + 1) * cols] = wf_ref[d * n_tp + t].astype(BF16)


def time_of(r):
    return 8 * (r % 8) + r // 8


def roll8(v):
    c = v.shape[1]
    return pltpu.roll(v.reshape(3, 8, c), 1, 1).reshape(24, c)


def conv_block(cur, prev, taps, bias, first):
    now = roll8(cur[40:])
    sh = jnp.where(first, prev, now)
    out = bias + cur * taps[3]
    for k in range(1, 4):
        out = out + jnp.concatenate([sh[8 * (3 - k):], cur[:64 - 8 * k]], axis=0) * taps[3 - k]
    return out, now


def unmix(v, buf):
    n, c = v.shape
    for j in range(c // 128):
        buf[n * j:n * (j + 1), :] = v[:, 128 * j:128 * (j + 1)]
    cols = [jnp.concatenate([buf[pl.ds(n * j + b + k, 8, stride=8), :] for b in range(0, n, 64) for k in range(8)], axis=0)
            for j in range(c // 128)]
    return jnp.concatenate(cols, axis=1)


EARLY = (2, 4, 6)


def comm_sems(shards):
    return [pltpu.SemaphoreType.DMA((Gather.N_SEM * len(shards),)) for _ in range(2)] if shards else []


def comm_outs(shards, n_tp):
    return [jax.ShapeDtypeStruct((v.shape[0], n_tp) + v.shape[1:], F32) for v in shards]


def head_row(h, heads):
    return (h % 2) * (heads // 2) + h // 2


def expand_mat(heads):
    order = sorted(range(heads), key=lambda h: head_row(h, heads))
    one = jnp.repeat(jnp.eye(heads, dtype=BF16)[jnp.array(order)], 64, axis=1)
    return jnp.concatenate([one, one, one], axis=0)


def kcat6(parts):
    a, b, c = parts
    return jnp.concatenate([a, b, c, a], axis=1), jnp.concatenate([b, a], axis=1)


def kcat6r(parts):
    a, b, c = parts
    return jnp.concatenate([a, a, a, b], axis=0), jnp.concatenate([b, c], axis=0)


def block_diag(x, lo, hi):
    z = jnp.zeros((x.shape[0], 128), BF16)
    l, r = x[:, :128], x[:, 128:]
    return jnp.concatenate([
        jnp.concatenate([l * lo, z], axis=1), jnp.concatenate([l * hi, z], axis=1),
        jnp.concatenate([z, r * lo], axis=1), jnp.concatenate([z, r * hi], axis=1)], axis=0)


def p1_body(u_ref, halo_ref, nw_ref, wf_ref, sm_ref, wbc_ref, cbc_ref, bbc_ref, e3_ref, *refs, geom, mixed, plan):
    nc = len(plan)
    ins, (y_ref, c_ref, ac_ref, send_ref), outs = refs[:nc], refs[nc:nc + 4], refs[nc + 4:2 * nc + 4]
    wxb, wdt, cst, st, xcar, qcar, aoff, ubuf, *sems = refs[2 * nc + 4:]
    n_dp, n_tp, hd, width, heads = geom
    i = pl.program_id(0)
    nst = 128
    pc = width // n_tp
    hp = heads // n_tp
    sub = BLK // 2
    if nc:
        background(i, ins, outs, *sems, plan)

    @pl.when(i == 0)
    def _():
        load_cols(wf_ref, wxb, n_dp, n_tp, wxb.shape[0] // n_dp, pc)
        kc = wxb.shape[0] // pc
        for t in range(n_tp):
            for k in range(hp):
                r = head_row(hp * t + k, heads)
                for c in range(kc):
                    wdt[r:r + 1, c * pc:(c + 1) * pc] = sm_ref[t, 16 + kc * k + c:17 + kc * k + c, :].astype(BF16)
                cst[r:r + 1, :] = sm_ref[t, 8 + k:9 + k, :]
                cst[heads + r:heads + r + 1, :] = sm_ref[t, 12 + k:13 + k, :]
        st[...] = jnp.zeros_like(st)
        aoff[...] = jnp.zeros_like(aoff)
        hh = rms(halo_ref[...], nw_ref[...])
        xcar[...] = roll8(dot(hh, wxb[...]).astype(BF16).astype(F32))
        qcar[...] = roll8(dot(hh, wbc_ref[...]).astype(BF16).astype(F32))

    if mixed:
        u = u_ref[...].astype(F32)
    else:
        u = unmix(u_ref[...].astype(F32), ubuf)
    h = rms(u, nw_ref[...])
    first = lax.broadcasted_iota(jnp.int32, (24, 256), 0) % 8 == 0

    def conv(cur, prev, taps, bias):
        a, now = conv_block(cur[:sub], prev, taps, bias, first)
        b, now = conv_block(cur[sub:], now, taps, bias, first)
        return silu(jnp.concatenate([a, b], axis=0)), now

    q0 = dot(h, wbc_ref[...])
    rT = dott(wdt[...], h).astype(BF16).astype(F32)
    x0s = {}

    def proj(t):
        if t < n_tp:
            x0s[t] = dot(h, wxb[:, t * pc:(t + 1) * pc])

    for t in range(EARLY[0]):
        proj(t)

    bc, qcar[...] = conv(q0.astype(BF16).astype(F32), qcar[...],
                         [cbc_ref[j:j + 1, :] for j in range(4)], bbc_ref[...])
    bmat, cmat = bc[:, :nst], bc[:, nst:]
    c_ref[...] = cmat

    pre = rT + cst[0:heads, 0:BLK]
    dtT = jnp.maximum(pre, 0.0) + jnp.log1p(jnp.exp(-jnp.abs(pre)))
    aT = dtT * cst[heads:2 * heads, 0:BLK]
    ri = lax.broadcasted_iota(jnp.int32, (BLK, BLK), 0)
    ci = lax.broadcasted_iota(jnp.int32, (BLK, BLK), 1)
    tr, tc = ri // sub * sub + time_of(ri % sub), ci // sub * sub + time_of(ci % sub)
    upper = jnp.where(tr <= tc, 1.0, 0.0).astype(F32)
    acT = dot(aT, upper, HI)
    mid, alast = acT[:, sub - 1:sub], acT[:, BLK - 1:BLK]
    lowh = lax.broadcasted_iota(jnp.int32, (heads, BLK), 1) < sub
    wT = dtT * jnp.exp2(jnp.where(lowh, mid, alast) - acT)
    w3t = jnp.concatenate(split3(wT), axis=0).T
    a3t = jnp.concatenate(split3(acT), axis=0).T
    ac_ref[...] = acT + aoff[:, 0:1]
    aoff[...] = aoff[...] + alast
    low16 = lax.broadcasted_iota(jnp.int32, (heads // 2, BLK), 1) < sub

    def pair_rows(v):
        ev, od = v[:heads // 2], v[heads // 2:]
        return (jnp.where(low16, ev, pltpu.roll(od, sub, 1)), jnp.where(low16, pltpu.roll(ev, sub, 1), od))

    ac_rows, dt_rows = pair_rows(acT), pair_rows(dtT)

    for t in range(EARLY[0], EARLY[1]):
        proj(t)
    cb = dott(cmat, bmat, HI)
    for t in range(EARLY[1], EARLY[2]):
        proj(t)
    rs = lax.broadcasted_iota(jnp.int32, (sub, BLK), 0)
    cs = lax.broadcasted_iota(jnp.int32, (sub, BLK), 1)
    tri = time_of(rs) >= time_of(cs % sub)
    ca, cb_ = cb[:sub], cb[sub:]
    cbd = (jnp.where(tri, jnp.where(cs < sub, ca, pltpu.roll(ca, sub, 1)), 0.0),
           jnp.where(tri, jnp.where(cs < sub, pltpu.roll(cb_, sub, 1), cb_), 0.0))
    bT = bmat.T
    la = jnp.concatenate([bT[:, :sub], cb_[:, :sub]], axis=0)
    la1, la2 = kcat6(split3(la))
    lb1, lb2 = kcat6(split3(pltpu.roll(bT, sub, 1)[:, :sub]))
    c1, c2, c3 = split3(cmat)
    cc12 = jnp.concatenate([c1, c2], axis=1)
    cc13 = jnp.concatenate([c1, c3], axis=1)

    lane = lax.broadcasted_iota(jnp.int32, (sub, 128), 1)
    lo = jnp.where(lane < hd, 1.0, 0.0).astype(BF16)
    hi = jnp.where(lane < hd, 0.0, 1.0).astype(BF16)
    def pre(t):
        sl = slice(t * pc, (t + 1) * pc)
        s1, s2, s3 = split3(st[:, sl])
        inter = (dot(cc12, jnp.concatenate([s1, s1], axis=0)) + dot(cc12, jnp.concatenate([s2, s2], axis=0))
                 + dot(cc13, jnp.concatenate([s3, s1], axis=0)))
        proj(t + EARLY[2])
        return x0s.pop(t), dot(a3t, e3_ref[:, sl]), dot(w3t, e3_ref[:, sl]), inter

    def mid_(t, x0, acx, wx, inter):
        sl = slice(t * pc, (t + 1) * pc)
        x, xcar[:, sl] = conv(x0.astype(BF16).astype(F32), xcar[:, sl],
                              [sm_ref[t, j:j + 1, :] for j in range(4)], sm_ref[t, 4:5, :])
        xw = split3(x * wx)
        r = kcat6r([v[:sub] for v in xw]) + kcat6r([v[sub:] for v in xw])
        ms, xs = [], []
        for k in range(2):
            rows = slice(k * sub, (k + 1) * sub)
            m = []
            for p in range(pc // 128):
                g = t * (pc // 128) + p
                seg = acx[rows, p * 128:(p + 1) * 128] - ac_rows[k][g:g + 1, :]
                m.append(jnp.exp2(jnp.minimum(seg, 0.0)) * cbd[k] * dt_rows[k][g:g + 1, :])
            ms.append(split3(jnp.concatenate(m, axis=1)))
            xs.append([block_diag(v, lo, hi) for v in split3(x[rows])])
        return x, acx, inter, r, ms, xs

    def fin(t, x, acx, inter, r, ms, xs):
        sl = slice(t * pc, (t + 1) * pc)
        ra1, ra2, rb1, rb2 = r
        ra = dot(la1, ra1) + dot(la2, ra2)
        rb = dot(lb1, rb1) + dot(lb2, rb2)
        am, al = acx[sub - 1:sub], acx[BLK - 1:BLK]
        skip = sm_ref[t, 6:7, :]
        for k in range(2):
            rows = slice(k * sub, (k + 1) * sub)
            (m1, m2, m3), (x1, x2, x3) = ms[k], xs[k]
            r1 = dot(jnp.concatenate([m1, m2, m3], axis=0), x1)
            r2 = dot(jnp.concatenate([m1, m2], axis=0), x2)
            y = r1[:sub] + r1[sub:2 * sub] + r1[2 * sub:] + r2[:sub] + r2[sub:] + dot(m1, x3)
            y = y + inter[rows] * jnp.exp2(acx[rows])
            if k == 1:
                y = y + ra[nst:] * jnp.exp2(acx[rows] - am)
            y_ref[rows, sl] = y + skip * x[rows]
        st[:, sl] = st[:, sl] * jnp.exp2(al) + ra[:nst] * jnp.exp2(al - am) + rb

    m = mid_(0, *pre(0))
    for t in range(n_tp):
        if t + 1 < n_tp:
            p = pre(t + 1)
        fin(t, *m)
        if t + 1 < n_tp:
            m = mid_(t + 1, *p)

    @pl.when(i == pl.num_programs(0) - 1)
    def _():
        send_ref[...] = st[...]


def p1(u, base, halo, nw, wf, wbc, cbc, bbc, e3, n, n_dp, n_tp, mixed, shards=(), plan=(), cid=None, interpret=False):
    d_model = u.shape[1]
    width = 256 * n_tp
    heads = width // 64
    rows = d_model // n_dp
    geom = (n_dp, n_tp, 64, width, heads)
    nb = n // BLK
    full = lambda shp: pl.BlockSpec(shp, lambda i: (0,) * len(shp), pipeline_mode=pl.Buffered(1))
    gs = dict(
        grid=(nb,),
        in_specs=[
            pl.BlockSpec((BLK, d_model), lambda i: (base() + i, 0)),
            full((24, d_model)), full((1, d_model)),
            full((n_dp * n_tp, rows, 256)),
            pl.BlockSpec((n_tp, 32, 256), lambda i: (0, rows // 32, 0), pipeline_mode=pl.Buffered(1)),
            full((d_model, 256)), full((4, 256)), full((1, 256)), full((3 * heads, width)),
        ] + [pl.BlockSpec(memory_space=pl.ANY)] * len(shards),
        out_specs=[
            pl.BlockSpec((BLK, width), lambda i: (i, 0)),
            pl.BlockSpec((BLK, 128), lambda i: (i, 0)),
            pl.BlockSpec((heads, BLK), lambda i: (0, i)),
            pl.BlockSpec((128, width), lambda i: (0, 0)),
        ] + [pl.BlockSpec(memory_space=pl.ANY)] * len(shards),
        scratch_shapes=[
            pltpu.VMEM((d_model, width), BF16), pltpu.VMEM((heads, d_model), BF16), pltpu.VMEM((2 * heads, 256), F32),
            pltpu.VMEM((128, width), F32), pltpu.VMEM((24, width), F32), pltpu.VMEM((24, 256), F32),
            pltpu.VMEM((heads, 128), F32), pltpu.VMEM((d_model // 128 * BLK, 128), F32),
        ] + comm_sems(shards))
    return pl.pallas_call(
        functools.partial(p1_body, geom=geom, mixed=mixed, plan=plan), name="p1",
        out_shape=[jax.ShapeDtypeStruct((n, width), F32), jax.ShapeDtypeStruct((n, 128), F32),
                   jax.ShapeDtypeStruct((heads, n), F32), jax.ShapeDtypeStruct((128, width), F32)] + comm_outs(shards, n_tp),
        compiler_params=pltpu.CompilerParams(dimension_semantics=("arbitrary",), vmem_limit_bytes=60 << 20, collective_id=cid, has_side_effects=bool(shards)),
        cost_estimate=pl.CostEstimate(flops=n * 70_000_000, bytes_accessed=n * 12000, transcendentals=0),
        interpret=interpret, **gs,
    )(u, halo, nw, wf, wf, wbc, cbc, bbc, e3, *shards)


def p2_body(u_ref, nw_ref, wz_ref, wo_ref, sm_ref, y_ref, c_ref, ac_ref, s_ref, e3_ref, *refs,
            geom, mix_in, mix_out, plan):
    nc = len(plan)
    ins, (o_ref, f_ref), outs = refs[:nc], refs[nc:nc + 2], refs[nc + 2:2 * nc + 2]
    wzb, wob, s3, ubuf, *sems = refs[2 * nc + 2:]
    if nc:
        background(pl.program_id(0), ins, outs, *sems, plan)
    n_dp, n_tp, hd, width, heads = geom
    pc = width // n_tp
    rows_z = wzb.shape[0] // n_dp

    @pl.when(pl.program_id(0) == 0)
    def _():
        load_cols(wz_ref, wzb, n_dp, n_tp, rows_z, pc)
        load_wo(wo_ref, wob, n_dp, n_tp)
        a, b, c = split3(s_ref[...])
        s3[0, 0:128, :] = a
        s3[0, 128:256, :] = a
        s3[1, 0:128, :] = b
        s3[1, 128:256, :] = b
        s3[2, 0:128, :] = c
        s3[2, 128:256, :] = a

    if mix_in:
        u = u_ref[...].astype(F32)
    else:
        u = unmix(u_ref[...].astype(F32), ubuf)
    h = rms(u, nw_ref[...])
    c1, c2, c3 = split3(c_ref[...])
    cc12 = jnp.concatenate([c1, c2], axis=1)
    cc13 = jnp.concatenate([c1, c3], axis=1)
    eT = jnp.concatenate(split3(jnp.exp2(ac_ref[...])), axis=0).T
    vs, ss = [], 0.0
    for t in range(n_tp):
        sl = slice(t * pc, (t + 1) * pc)
        z = dot(h, wzb[:, sl]).astype(BF16).astype(F32)
        cor = dot(cc12, s3[0, :, sl]) + dot(cc12, s3[1, :, sl]) + dot(cc13, s3[2, :, sl])
        v = (y_ref[:, sl] + cor * dot(eT, e3_ref[:, sl])) * silu(z)
        ss = ss + jnp.sum(v * v, axis=-1, keepdims=True)
        vs.append(v)
    sc = lax.rsqrt(ss / width + EPS)
    acc = u
    g = jnp.concatenate([(vs[t] * sc * sm_ref[t, 5:6, :]).astype(BF16) for t in range(n_tp)], axis=1)
    un = (u + dot(g, wob[...])).astype(BF16)
    f_ref[...] = un.astype(F32)
    if mix_out:
        o_ref[...] = un
    else:
        o_ref[...] = unmix(un.astype(F32), ubuf).astype(BF16)


def load_wo(wf_ref, wb_ref, n_dp, n_tp):
    rows = wb_ref.shape[0] // n_tp
    cols = wb_ref.shape[1] // n_dp
    for d in range(n_dp):
        for t in range(n_tp):
            wb_ref[t * rows:(t + 1) * rows, d * cols:(d + 1) * cols] = wf_ref[d * n_tp + t].astype(BF16)


def p2(u, base, obase, nw, wz, wo, wsm, y, c, ac, s, e3, n, n_dp, n_tp, mix_in, mix_out, out_rows=None, shards=(), plan=(), cid=None, interpret=False):
    d_model = u.shape[1]
    width = 256 * n_tp
    heads = width // 64
    rows = d_model // n_dp
    geom = (n_dp, n_tp, 64, width, heads)
    nb = n // BLK2
    full = lambda shp: pl.BlockSpec(shp, lambda i: (0,) * len(shp), pipeline_mode=pl.Buffered(1))
    gs = dict(
        grid=(nb,),
        in_specs=[
            pl.BlockSpec((BLK2, d_model), lambda i: (base() + i, 0)),
            full((1, d_model)),
            full((n_dp * n_tp, rows, 256)), full((n_dp * n_tp, 256, d_model // n_dp)),
            pl.BlockSpec((n_tp, 32, 256), lambda i: (0, rows // 32, 0), pipeline_mode=pl.Buffered(1)),
            pl.BlockSpec((BLK2, width), lambda i: (i, 0)),
            pl.BlockSpec((BLK2, 128), lambda i: (i, 0)),
            pl.BlockSpec((heads, BLK2), lambda i: (0, i)),
            full((128, width)), full((3 * heads, width)),
        ] + [pl.BlockSpec(memory_space=pl.ANY)] * len(shards),
        out_specs=[pl.BlockSpec((BLK2, d_model), lambda i: (obase() + i, 0)), pl.BlockSpec((BLK2, d_model), lambda i: (i, 0))]
        + [pl.BlockSpec(memory_space=pl.ANY)] * len(shards),
        scratch_shapes=[pltpu.VMEM((d_model, width), BF16), pltpu.VMEM((width, d_model), BF16),
                        pltpu.VMEM((3, 256, width), BF16), pltpu.VMEM((d_model // 128 * BLK2, 128), F32)] + comm_sems(shards))
    return pl.pallas_call(
        functools.partial(p2_body, geom=geom, mix_in=mix_in, mix_out=mix_out, plan=plan), name="p2",
        out_shape=[jax.ShapeDtypeStruct((out_rows or n, d_model), BF16), jax.ShapeDtypeStruct((n, d_model), F32)] + comm_outs(shards, n_tp),
        compiler_params=pltpu.CompilerParams(dimension_semantics=("arbitrary",), vmem_limit_bytes=60 << 20, collective_id=cid, has_side_effects=bool(shards)),
        cost_estimate=pl.CostEstimate(flops=n * 30_000_000, bytes_accessed=n * 12000, transcendentals=0),
        interpret=interpret, **gs,
    )(u, nw, wz, wo, wsm, y, c, ac, s, e3, *shards)


def fin_body(off_ref, buf_ref, f_ref, o_ref, ubuf):
    o_ref[...] = unmix(f_ref[...], ubuf).astype(BF16)


def finish(buf, f, off):
    n, d_model = f.shape
    rows = 512
    gs = pltpu.PrefetchScalarGridSpec(
        num_scalar_prefetch=1, grid=(n // rows,),
        in_specs=[pl.BlockSpec(memory_space=pl.ANY), pl.BlockSpec((rows, d_model), lambda i, o: (i, 0))],
        out_specs=pl.BlockSpec((rows, d_model), lambda i, o: (o[0] + i, 0)),
        scratch_shapes=[pltpu.VMEM((d_model // 128 * rows, 128), F32)])
    return pl.pallas_call(
        fin_body, grid_spec=gs, name="finish", out_shape=jax.ShapeDtypeStruct(buf.shape, BF16),
        input_output_aliases={1: 0},
        compiler_params=pltpu.CompilerParams(dimension_semantics=("arbitrary",)),
        cost_estimate=pl.CostEstimate(flops=n * d_model, bytes_accessed=n * d_model * 6, transcendentals=0),
    )(off, buf, f)


class Gather:
    N_SEM = 17

    def __init__(self, a, g, send, recv, base):
        self.a, self.g, self.send, self.recv, self.base = a, g, send, recv, base
        dp, tp = lax.axis_index('dp'), lax.axis_index('tp')
        x, y, z, c = dp // 2, dp % 2, tp // 2, tp % 2
        self.dp, self.tp, self.z, self.c = dp, tp, z, c
        self.plane = [(1 - x) * 2 + y, x * 2 + 1 - y, (1 - x) * 2 + 1 - y]
        self.partner = (dp, 2 * z + 1 - c)

    def slot(self, dz):
        return 2 * ((self.z + 4 - dz) % 4) + self.c

    def rdma(self, k, src, dst, dev):
        return pltpu.make_async_remote_copy(src_ref=src, dst_ref=dst, send_sem=self.send.at[self.base + k],
                                            recv_sem=self.recv.at[self.base + k], device_id=dev,
                                            device_id_type=pl.DeviceIdType.MESH)

    def local(self):
        return pltpu.make_async_copy(self.a, self.g.at[:, self.tp], self.send.at[self.base])

    def own(self):
        return self.rdma(1, self.a, self.g.at[:, self.tp], self.partner)

    def line(self, dz):
        return self.rdma(1 + dz, self.a.at[self.dp], self.g.at[self.dp, self.tp], (self.dp, 2 * ((self.z + dz) % 4) + self.c))

    def cross(self, dz, n):
        s = self.slot(dz)
        return self.rdma(2 + 3 * dz + n, self.g.at[self.dp, s], self.g.at[self.dp, s], (self.plane[n], self.tp))

    def over(self, dz):
        s = self.slot(dz)
        return self.rdma(13 + dz, self.g.at[:, s], self.g.at[:, s], self.partner)

    def peers(self):
        return [(self.dp, 2 * ((self.z + dz) % 4) + self.c) for dz in (1, 2, 3)] + [(p, self.tp) for p in self.plane] + [self.partner]

    def step0(self):
        for dz in (1, 3, 2):
            self.line(dz).start()
        self.own().start()
        self.local().start()

    def step1(self, dz):
        self.line(dz).wait_recv()
        for n in range(3):
            self.cross(dz, n).start()

    def step2(self, dz):
        for n in range(3):
            self.cross(dz, n).wait_recv()
        self.over(dz).start()

    def step3(self):
        self.local().wait()
        self.own().wait()
        for dz in (1, 2, 3):
            self.line(dz).wait_send()
            for n in range(3):
                self.cross(dz, n).wait_send()
            self.over(dz).wait()


def entry_barrier(peers):
    sem = pltpu.get_barrier_semaphore()
    for p in peers:
        pl.semaphore_signal(sem, inc=1, device_id=p, device_id_type=pl.DeviceIdType.MESH)
    pl.semaphore_wait(sem, len(peers))


def gather_body(*refs, n):
    ins, outs, (send, recv) = refs[:n], refs[n:2 * n], refs[2 * n:]
    gs = [Gather(a, g, send, recv, Gather.N_SEM * k) for k, (a, g) in enumerate(zip(ins, outs))]
    entry_barrier(gs[0].peers())
    for g in gs:
        g.step0()
    for g in gs:
        for dz in (1, 3, 2):
            g.step1(dz)
    for g in gs:
        for dz in (1, 3, 2):
            g.step2(dz)
    for g in gs:
        g.step3()


def background(i, ins, outs, send, recv, plan):
    gs = [Gather(a, g, send, recv, Gather.N_SEM * k) for k, (a, g) in enumerate(zip(ins, outs))]

    @pl.when(i == 0)
    def _():
        entry_barrier(gs[0].peers())
        for g in gs:
            g.step0()

    for g, at in zip(gs, plan):
        for j, dz in enumerate((1, 3, 2)):
            pl.when(i == at[j])(functools.partial(g.step1, dz))
            pl.when(i == at[3 + j])(functools.partial(g.step2, dz))

    @pl.when(i == pl.num_programs(0) - 1)
    def _():
        for g in gs:
            g.step3()


def gather_all(shards, n_tp, cid):
    n = len(shards)
    return pl.pallas_call(
        functools.partial(gather_body, n=n), name="gather",
        out_shape=[jax.ShapeDtypeStruct((s.shape[0], n_tp) + s.shape[1:], F32) for s in shards],
        in_specs=[pl.BlockSpec(memory_space=pl.ANY)] * n, out_specs=[pl.BlockSpec(memory_space=pl.ANY)] * n,
        scratch_shapes=[pltpu.SemaphoreType.DMA((Gather.N_SEM * n,)), pltpu.SemaphoreType.DMA((Gather.N_SEM * n,))],
        compiler_params=pltpu.CompilerParams(collective_id=cid, has_side_effects=True),
        cost_estimate=pl.CostEstimate(flops=10 ** 10, bytes_accessed=n * 16 * 10 ** 6, transcendentals=0),
    )(*shards)


from jax.sharding import PartitionSpec as P


def small_rows(conv, bias, gate, skip, dtb, al, wdt):
    f = lambda v: v.astype(F32)
    hp = skip.shape[0]
    return jnp.concatenate([
        f(conv), f(bias)[None], f(gate)[None], jnp.repeat(skip, 256 // hp)[None], jnp.zeros((1, 256), F32),
        jnp.broadcast_to(dtb[:, None], (hp, 256)), jnp.broadcast_to((-jnp.exp(al) * LOG2E)[:, None], (hp, 256)),
        f(wdt).T.reshape(-1, 256)], axis=0)


def solution(mesh):
    n_tp, n_dp = mesh.shape['tp'], mesh.shape['dp']
    rep, col, vec = P(), P(None, None, 'tp'), P(None, 'tp')
    in_specs = (P('dp'), rep, col, col, rep, col, col, rep, vec, rep, vec, vec, vec, vec, P(None, 'tp', None))

    def device_forward(hidden, norm_w, w_z, w_x, w_bc, w_dt, conv_x, conv_bc, bias_x, bias_bc, dt_bias, a_log, d_skip, gate_w, w_out):
        u = hidden[0]
        steps, d_model = u.shape
        heads = dt_bias.shape[1] * n_tp
        n = steps // 2
        dp, tp = lax.axis_index('dp'), lax.axis_index('tp')
        core = tp % 2
        rows, ocols = d_model // n_dp, d_model // n_dp
        e3 = expand_mat(heads)
        up = [(2 * k, 2 * k + 1) for k in range(n_tp // 2)]
        swap = [(k, k ^ 1) for k in range(n_tp)]
        def cut(w):
            return w.reshape(n_dp, rows, 256).astype(F32)

        def cut_o(w):
            return w.reshape(256, n_dp, ocols).transpose(1, 0, 2).astype(F32)

        sm = [small_rows(conv_x[l], bias_x[l], gate_w[l], d_skip[l], dt_bias[l], a_log[l], w_dt[l]) for l in range(2)]
        sx = [jnp.concatenate([cut(w_x[l]), jnp.broadcast_to(sm[l], (n_dp,) + sm[l].shape)], axis=1) for l in range(2)]
        flat = lambda v: v.reshape((n_dp * n_tp,) + v.shape[2:])
        sz, so = [cut(w_z[l]) for l in range(2)], [cut_o(w_out[l]) for l in range(2)]
        wx, = gather_all([sx[0]], n_tp, 1)
        wx = flat(wx)
        cur = u
        mine = lambda blk: (lambda: lax.axis_index('tp') % 2 * (n // blk))
        none = lambda: 0
        tail = u[n - 64:n].astype(F32).reshape(8, 8, d_model).transpose(1, 0, 2).reshape(64, d_model)[40:]
        halo = jnp.where(core == 1, tail, 0.0)
        for l in range(2):
            nw = norm_w[l].astype(F32)[None]
            y, c, ac, s_end, wz, wo = p1(cur, mine(BLK) if l == 0 else none, halo, nw, wx, w_bc[l], conv_bc[l].astype(F32), bias_bc[l].astype(F32)[None], e3, n, n_dp, n_tp, l > 0,
                                         shards=(sz[l], so[l]), plan=((4, 6, 8, 12, 14, 16), (9, 11, 13, 18, 20, 22)), cid=2 + l)
            s = lax.ppermute(s_end, 'tp', up)
            more = dict(shards=(sx[1],), plan=((3, 4, 5, 8, 9, 10),), cid=4) if l == 0 else {}
            o, f, *nxt = p2(cur, mine(BLK2) if l == 0 else none, none if l == 0 else mine(BLK2), nw, flat(wz), flat(wo), wx, y, c, ac, s, e3, n, n_dp, n_tp, l > 0, l == 0, out_rows=n if l == 0 else steps, **more)
            cur = o
            if l == 0:
                halo = lax.ppermute(f[n - 24:], 'tp', up)
                wx = flat(nxt[0])
        other = lax.ppermute(f, 'tp', swap)
        return finish(o, other, jnp.reshape((1 - core) * (n // 512), (1,)))[None]

    return jax.shard_map(device_forward, mesh=mesh, in_specs=in_specs, out_specs=P('dp'), check_vma=False)
```

```python
import functools
import jax
import jax.numpy as jnp
from jax import lax
from jax.experimental import pallas as pl
from jax.experimental.pallas import tpu as pltpu
from jax.sharding import PartitionSpec as P

EPS = 1e-5
LOG2E = 1.4426950408889634
HI = lax.Precision.HIGHEST
F32 = jnp.float32
BF16 = jnp.bfloat16
MESH = pl.DeviceIdType.MESH
LANES = 128
BLK = 128
SUB = 64
BLK2 = 256
NBS = 4
PC = 256
HD = 64
NST = 128
CAR = 24
SMALL = 32
SEMS = 26
VMEM_CAP = 60 << 20


def silu(v):
    return v / (1.0 + jnp.exp2(v * -LOG2E))


def split3(v):
    a = v.astype(BF16)
    r = v - a.astype(F32)
    b = r.astype(BF16)
    return a, b, (r - b.astype(F32)).astype(BF16)


def round_bf16(v):
    return v.astype(BF16).astype(F32)


def rms(u, nw):
    return (u * lax.rsqrt(jnp.mean(u * u, axis=-1, keepdims=True) + EPS) * nw).astype(BF16)


def dot(a, b, prec=None):
    return jnp.dot(a, b, preferred_element_type=F32, precision=prec)


def dott(a, b, prec=None):
    return lax.dot_general(a, b, (((1,), (1,)), ((), ())), preferred_element_type=F32, precision=prec)


def rows_cat(*v):
    return jnp.concatenate(v, axis=0)


def lanes_cat(*v):
    return jnp.concatenate(v, axis=1)


def time_of(r):
    return 8 * (r % 8) + r // 8


def roll8(v):
    c = v.shape[-1]
    return pltpu.roll(v.reshape(CAR // 8, 8, c), 1, 1).reshape(CAR, c)


def conv_block(cur, prev, taps, bias, first):
    now = roll8(cur[SUB - CAR:])
    sh = jnp.where(first, prev, now)
    out = bias + cur * taps[-1]
    for k in range(1, 4):
        out = out + rows_cat(sh[CAR - 8 * k:], cur[:SUB - 8 * k]) * taps[3 - k]
    return out, now


def unmix(v, buf):
    n, c = v.shape
    for j in range(c // LANES):
        buf[n * j:n * (j + 1), :] = v[:, LANES * j:LANES * (j + 1)]
    cols = [rows_cat(*[buf[pl.ds(n * j + b + k, 8, stride=8), :] for b in range(0, n, SUB) for k in range(8)])
            for j in range(c // LANES)]
    return lanes_cat(*cols)


def head_row(h, heads):
    return (h % 2) * (heads // 2) + h // 2


def expand_mat(heads):
    order = sorted(range(heads), key=lambda h: head_row(h, heads))
    one = jnp.repeat(jnp.eye(heads, dtype=BF16)[jnp.array(order)], HD, axis=1)
    return rows_cat(one, one, one)


def kcat6(parts):
    a, b, c = parts
    return lanes_cat(a, b, c, a), lanes_cat(b, a)


def kcat6r(parts):
    a, b, c = parts
    return rows_cat(a, a, a, b), rows_cat(b, c)


def block_diag(x, lo, hi):
    z = jnp.zeros((x.shape[0], LANES), BF16)
    l, r = x[:, :LANES], x[:, LANES:]
    return rows_cat(lanes_cat(l * lo, z), lanes_cat(l * hi, z), lanes_cat(z, r * lo), lanes_cat(z, r * hi))


def here():
    dp, tp = lax.axis_index('dp'), lax.axis_index('tp')
    return dp, tp, tp // 2, tp % 2


def source(dz):
    return (here()[2] + 4 - dz) % 4


class Gather:
    def __init__(self, piece, g, send, recv, base):
        self.piece, self.g, self.send, self.recv, self.base = piece, g, send, recv, base
        self.dp, self.tp, self.z, self.c = here()
        x, y = self.dp // 2, self.dp % 2
        self.side = ((1 - x) * 2 + y, x * 2 + 1 - y)
        self.partner = (self.dp, 2 * self.z + 1 - self.c)
        self.quarters = g.shape[0]

    def rdma(self, k, src, dst, dev):
        return pltpu.make_async_remote_copy(src_ref=src, dst_ref=dst, send_sem=self.send.at[self.base + k],
                                            recv_sem=self.recv.at[self.base + k], device_id=dev, device_id_type=MESH)

    def local(self, q):
        return pltpu.make_async_copy(self.piece(q), self.g.at[q, self.tp], self.send.at[self.base + q])

    def own(self, q):
        return self.rdma(4 + q, self.piece(q), self.g.at[q, self.tp], self.partner)

    def line(self, dz):
        return self.rdma(7 + dz, self.piece(self.dp), self.g.at[self.dp, self.tp],
                         (self.dp, 2 * ((self.z + dz) % 4) + self.c))

    def cross(self, dz, n):
        ref = self.g.at[self.dp, 2 * source(dz) + self.c]
        return self.rdma(9 + 2 * dz + n, ref, ref, (self.side[n], self.tp))

    def relay(self, dz, n):
        half = self.g.shape[2] // 2
        ref = self.g.at[self.side[n], 2 * source(dz) + self.c, pl.ds(n * half, half)]
        return self.rdma(15 + 2 * dz + n, ref, ref, (self.side[1 - n], self.tp))

    def over(self, dz):
        ref = self.g.at[:, 2 * source(dz) + self.c]
        return self.rdma(22 + dz, ref, ref, self.partner)

    def peers(self):
        return ([(self.dp, 2 * ((self.z + dz) % 4) + self.c) for dz in (1, 2, 3)]
                + [(p, self.tp) for p in self.side] + [self.partner])

    def start(self):
        for dz in (1, 3, 2):
            self.line(dz).start()
        for q in range(self.quarters):
            self.own(q).start()
            self.local(q).start()

    def spread(self, dz):
        self.line(dz).wait_recv()
        for n in range(2):
            self.cross(dz, n).start()

    def pass_on(self, dz):
        for n in range(2):
            self.cross(dz, n).wait_recv()
            self.relay(dz, n).start()

    def hand(self, dz):
        for n in range(2):
            self.relay(dz, n).wait_recv()
        self.over(dz).start()

    def settle_own(self):
        for q in range(self.quarters):
            self.local(q).wait()
            self.own(q).wait_recv()

    def settle(self, dz):
        self.over(dz).wait_recv()

    def drain(self):
        for q in range(self.quarters):
            self.own(q).wait_send()
        for dz in (1, 2, 3):
            self.line(dz).wait_send()
            self.over(dz).wait_send()
            for n in range(2):
                self.cross(dz, n).wait_send()
                self.relay(dz, n).wait_send()

    def plan(self, s):
        s = bytes.fromhex(s)
        acts = [(s[0], self.start)]
        for k, f in enumerate((self.spread, self.pass_on, self.hand)):
            acts += [(s[1 + 3 * k + j], functools.partial(f, dz)) for j, dz in enumerate((1, 3, 2))]
        return acts

    def finish(self):
        self.settle_own()
        for dz in (1, 2, 3):
            self.settle(dz)
        self.drain()


class Small:
    def __init__(self, a, g, send, recv):
        self.a, self.g, self.send, self.recv = a, g, send, recv
        self.dp, self.tp, _, _ = here()

    def copy(self, k):
        return pltpu.make_async_remote_copy(src_ref=self.a, dst_ref=self.g.at[self.tp], send_sem=self.send.at[k],
                                            recv_sem=self.recv.at[k], device_id=(self.dp, (self.tp + k) % 8),
                                            device_id_type=MESH)

    def local(self):
        return pltpu.make_async_copy(self.a, self.g.at[self.tp], self.send.at[0])

    def peers(self):
        return [(self.dp, (self.tp + k) % 8) for k in range(1, 8)]

    def start(self):
        self.local().start()
        for k in range(1, 8):
            self.copy(k).start()

    def finish(self):
        self.local().wait()
        for k in range(1, 8):
            self.copy(k).wait()


def entry_barrier(peers):
    sem = pltpu.get_barrier_semaphore()
    for p in peers:
        pl.semaphore_signal(sem, inc=1, device_id=p, device_id_type=MESH)
    pl.semaphore_wait(sem, len(peers))


def at_steps(step, acts):
    for k in sorted({k for k, _ in acts}):
        @pl.when(step == k)
        def _():
            for j, f in acts:
                if j == k:
                    f()


def piece_rows(ref, layer):
    return lambda q: ref.at[layer, pl.ds(q * PC, PC)]


def piece_cols(ref, layer):
    return lambda q: ref.at[layer, :, pl.ds(pl.multiple_of(q * PC, PC) if not isinstance(q, int) else q * PC, PC)]


def p1_body(*refs, geom, mixed, layer, fetch_x, plans):
    n_dp, n_tp, heads, nb = geom
    (u_ref, halo_ref, nw_ref, wbc_ref, cbc_ref, bbc_ref, e3_ref), refs = refs[:7], refs[7:]
    if fetch_x:
        (ax, asm, az, ao), (y_ref, c_ref, ac_ref, send_ref), (gx, gs, gz, go), refs = refs[:4], refs[4:8], refs[8:12], refs[12:]
    else:
        (gx, gs, az, ao), (y_ref, c_ref, ac_ref, send_ref), (gz, go), refs = refs[:4], refs[4:8], refs[8:10], refs[10:]
    (wf, wb, wsem, sm, wdt, cst, st, hcar, xcar, qcar, aoff, ubuf, h_s, la1_s, la2_s, lb1_s, lb2_s, cc_s, cbd_s, row_s, aw_s,
     send, recv), sems = refs[:23], refs[23:]
    p, i = pl.program_id(0), pl.program_id(1)
    np_, ni = pl.num_programs(0), pl.num_programs(1)
    step = p * ni + i
    d_model = u_ref.shape[-1]
    quad = 2 * PC
    dz = p + p // 2 * (1 - 2 * (p % 2))
    zs = source(dz)

    zg = Gather(piece_rows(az, layer), gz, send, recv, 0)
    og = Gather(piece_cols(ao, layer), go, send, recv, SEMS)
    acts = zg.plan(plans[0]) + og.plan(plans[1])
    if fetch_x:
        xg = Gather(piece_rows(ax, layer), gx, send, recv, 2 * SEMS)
        small = Small(asm, gs, *sems)
        acts += xg.plan(plans[2])

    def load_w(slot, zsrc):
        return pltpu.make_async_copy(gx.at[:, pl.ds(2 * zsrc, 2)], wf.at[slot], wsem.at[slot])

    @pl.when(step == 0)
    def _():
        entry_barrier((small.peers() + [(s, here()[1]) for s in zg.side]) if fetch_x else zg.peers())
        if fetch_x:
            small.start()
    at_steps(step, acts)

    @pl.when(step == 0)
    def _():
        if fetch_x:
            small.finish()
            xg.settle_own()
        load_w(0, zs).start()
        cp = pltpu.make_async_copy(gs.at[:, pl.ds(layer * SMALL, SMALL)], sm, wsem.at[2])
        cp.start()
        cp.wait()
        kc = d_model // PC
        hp = heads // n_tp
        for t in range(n_tp):
            for k in range(hp):
                r = head_row(hp * t + k, heads)
                for c in range(kc):
                    wdt[r:r + 1, c * PC:(c + 1) * PC] = sm[t, 16 + kc * k + c:17 + kc * k + c, :].astype(BF16)
                cst[r:r + 1, :] = sm[t, 8 + k:9 + k, :]
                cst[heads + r:heads + r + 1, :] = sm[t, 12 + k:13 + k, :]
        aoff[...] = jnp.zeros_like(aoff)
        hh = rms(halo_ref[...], nw_ref[...])
        hcar[...] = hh
        qcar[...] = roll8(round_bf16(dot(hh, wbc_ref[...])))

    first = lax.broadcasted_iota(jnp.int32, (CAR, PC), 0) % 8 == 0

    def conv(cur, prev, taps, bias):
        a, now = conv_block(cur[:SUB], prev, taps, bias, first)
        b, now = conv_block(cur[SUB:], now, taps, bias, first)
        return silu(rows_cat(a, b)), now

    ri = lax.broadcasted_iota(jnp.int32, (BLK, BLK), 0)
    ci = lax.broadcasted_iota(jnp.int32, (BLK, BLK), 1)

    def prologue(b, h):
        j = i * NBS + b
        blk = pl.ds(pl.multiple_of(j * BLK, BLK), BLK)
        h_s[blk, :] = h
        rT = round_bf16(dott(wdt[...], h))
        bc, qcar[...] = conv(round_bf16(dot(h, wbc_ref[...])), qcar[...],
                             [cbc_ref[k:k + 1, :] for k in range(4)], bbc_ref[...])
        bmat, cmat = bc[:, :NST], bc[:, NST:]
        here_rows = slice(b * BLK, (b + 1) * BLK)
        c_ref[here_rows, :] = cmat
        pre = rT + cst[:heads, :BLK]
        dtT = jnp.maximum(pre, 0.0) + jnp.log1p(jnp.exp(-jnp.abs(pre)))
        aT = dtT * cst[heads:, :BLK]
        tr, tc = ri // SUB * SUB + time_of(ri % SUB), ci // SUB * SUB + time_of(ci % SUB)
        acT = dot(aT, jnp.where(tr <= tc, 1.0, 0.0), HI)
        mid, alast = acT[:, SUB - 1:SUB], acT[:, BLK - 1:BLK]
        low = ci[:heads] < SUB
        wT = dtT * jnp.exp2(jnp.where(low, mid, alast) - acT)
        pad = jnp.zeros((BLK - 3 * heads, BLK), BF16)
        aw_s[blk, :] = lanes_cat(rows_cat(*split3(acT), pad).T, rows_cat(*split3(wT), pad).T)
        ac_ref[:, here_rows] = acT + aoff[:, :1]
        aoff[...] = aoff[...] + alast

        def pair_rows(v):
            ev, od = v[:heads // 2], v[heads // 2:]
            l = low[:heads // 2]
            return jnp.where(l, ev, pltpu.roll(od, SUB, 1)), jnp.where(l, pltpu.roll(ev, SUB, 1), od)

        for half, (a, d) in enumerate(zip(pair_rows(acT), pair_rows(dtT))):
            row_s[2 * j + half] = rows_cat(*[v[4 * z:4 * z + 4] for z in range(heads // 8) for v in (a, d)])
        cb = dott(cmat, bmat, HI)
        lowr, tri = ci[:SUB] < SUB, time_of(ri[:SUB]) >= time_of(ci[:SUB] % SUB)
        ca, cd = cb[:SUB], cb[SUB:]
        cbd_s[blk, :] = rows_cat(jnp.where(tri, jnp.where(lowr, ca, pltpu.roll(ca, SUB, 1)), 0.0),
                                 jnp.where(tri, jnp.where(lowr, pltpu.roll(cd, SUB, 1), cd), 0.0))
        bT = bmat.T
        big = pl.ds(pl.multiple_of(j * (NST + SUB), SUB), NST + SUB)
        la1_s[big, :], la2_s[big, :] = kcat6(split3(rows_cat(bT[:, :SUB], cd[:, :SUB])))
        lb1_s[blk, :], lb2_s[blk, :] = kcat6(split3(pltpu.roll(bT, SUB, 1)[:, :SUB]))
        c1, c2, c3 = split3(cmat)
        cc_s[blk, :] = lanes_cat(c1, c2, c1, c3)

    @pl.when(p == 0)
    def _():
        u = u_ref[...].astype(F32)
        h = rms(u if mixed else unmix(u, ubuf), nw_ref[...])
        for b in range(NBS):
            prologue(b, h[b * BLK:(b + 1) * BLK])

    @pl.when(i == 0)
    def _():
        slot = p % 2
        load_w(slot, zs).wait()
        for q in range(n_dp):
            for k in range(2):
                wb[q * PC:(q + 1) * PC, k * PC:(k + 1) * PC] = wf[slot, q, k].astype(BF16)
        xcar[...] = roll8(round_bf16(dot(hcar[...], wb[...])))
        st[...] = jnp.zeros_like(st)

    @pl.when((i == ni - 1) & (p < np_ - 1))
    def _():
        nd = p + 1
        nd = nd + nd // 2 * (1 - 2 * (nd % 2))
        if fetch_x:
            for d in (1, 2, 3):
                pl.when(nd == d)(functools.partial(xg.settle, d))
        load_w((p + 1) % 2, source(nd)).start()

    lane = lax.broadcasted_iota(jnp.int32, (SUB, LANES), 1)
    lo = jnp.where(lane < HD, 1.0, 0.0).astype(BF16)
    hi = jnp.where(lane < HD, 0.0, 1.0).astype(BF16)
    x0 = [dot(h_s[pl.ds(pl.multiple_of(i * NBS * BLK, BLK), NBS * BLK), :], wb[:, k * PC:(k + 1) * PC]) for k in range(2)]

    def place(b):
        j = i * NBS + b
        return j, pl.ds(pl.multiple_of(j * BLK, BLK), BLK), pl.ds(pl.multiple_of(j * (NST + SUB), SUB), NST + SUB)

    def lanes_of(k):
        return slice(k * PC, (k + 1) * PC), pl.ds(pl.multiple_of((2 * zs + k) * PC, PC), PC)

    def pre(b, k):
        (_, blk, _), (sl, gl) = place(b), lanes_of(k)
        s1, s2, s3 = split3(st[:, sl])
        c12, c13 = cc_s[blk, :2 * NST], cc_s[blk, 2 * NST:]
        inter = dot(c12, rows_cat(s1, s1)) + dot(c12, rows_cat(s2, s2)) + dot(c13, rows_cat(s3, s1))
        n3 = e3_ref.shape[0]
        acx = dot(aw_s[blk, :n3], e3_ref[:, gl])
        wx = dot(aw_s[blk, BLK:BLK + n3], e3_ref[:, gl])
        return x0[k][b * BLK:(b + 1) * BLK], acx, wx, inter

    def mid_(b, k, x0, acx, wx, inter):
        (j, blk, _), (sl, _) = place(b), lanes_of(k)
        t = 2 * zs + k
        x, xcar[:, sl] = conv(round_bf16(x0), xcar[:, sl], [sm[t, r:r + 1, :] for r in range(4)], sm[t, 4:5, :])
        xw = split3(x * wx)
        r = kcat6r([v[:SUB] for v in xw]) + kcat6r([v[SUB:] for v in xw])
        ms, xs = [], []
        for half in range(2):
            rows = slice(half * SUB, (half + 1) * SUB)
            row = row_s[2 * j + half, pl.ds(pl.multiple_of(8 * zs, 8), 8), :]
            cbd = cbd_s[pl.ds(pl.multiple_of(j * BLK + half * SUB, SUB), SUB), :]
            m = []
            for g in range(2):
                seg = acx[rows, g * LANES:(g + 1) * LANES] - row[2 * k + g:2 * k + g + 1]
                m.append(jnp.exp2(jnp.minimum(seg, 0.0)) * cbd * row[4 + 2 * k + g:5 + 2 * k + g])
            ms.append(split3(lanes_cat(*m)))
            xs.append([block_diag(v, lo, hi) for v in split3(x[rows])])
        return x, acx, inter, r, ms, xs

    def fin(b, k, x, acx, inter, r, ms, xs):
        (j, blk, big), (sl, _) = place(b), lanes_of(k)
        ra = dot(la1_s[big, :], r[0]) + dot(la2_s[big, :], r[1])
        rb = dot(lb1_s[blk, :], r[2]) + dot(lb2_s[blk, :], r[3])
        am, al = acx[SUB - 1:SUB], acx[BLK - 1:BLK]
        st[:, sl] = st[:, sl] * jnp.exp2(al) + ra[:NST] * jnp.exp2(al - am) + rb
        skip = sm[2 * zs + k, 6:7, :]
        for half in range(2):
            rows = slice(half * SUB, (half + 1) * SUB)
            (m1, m2, m3), (x1, x2, x3) = ms[half], xs[half]
            r1 = dot(rows_cat(m1, m2, m3), x1)
            r2 = dot(rows_cat(m1, m2), x2)
            y = r1[:SUB] + r1[SUB:2 * SUB] + r1[2 * SUB:] + r2[:SUB] + r2[SUB:] + dot(m1, x3)
            y = y + inter[rows] * jnp.exp2(acx[rows])
            if half:
                y = y + ra[NST:] * jnp.exp2(acx[rows] - am)
            y_ref[b * BLK + half * SUB:b * BLK + (half + 1) * SUB, sl] = y + skip * x[rows]

    units = [(b, k) for b in range(NBS) for k in range(2)]
    m = mid_(*units[0], *pre(*units[0]))
    for a, nxt in zip(units, units[1:] + [None]):
        if nxt:
            v = pre(*nxt)
        fin(*a, *m)
        if nxt:
            m = mid_(*nxt, *v)

    @pl.when(i == ni - 1)
    def _():
        send_ref[...] = st[...]

    @pl.when(step == np_ * ni - 1)
    def _():
        zg.finish()
        og.finish()
        if fetch_x:
            xg.drain()


def p1(u, base, halo, nw, wbc, cbc, bbc, e3, comm, n, n_dp, n_tp, mixed, layer, fetch_x, plans, cid):
    d_model, heads = u.shape[1], PC // HD * n_tp
    width, nb, rows = PC * n_tp, n // BLK, BLK * NBS
    ni = nb // NBS
    fixed = lambda shp: pl.BlockSpec(shp, lambda p, i: (0,) * len(shp), pipeline_mode=pl.Buffered(1))
    once = lambda p, i: jnp.where(p == 0, i, ni - 1)
    col = lambda p: source(p + p // 2 * (1 - 2 * (p % 2)))
    hbm = pl.BlockSpec(memory_space=pl.ANY)
    gathered = lambda r: jax.ShapeDtypeStruct((n_dp, n_tp, r, PC), F32)
    outs = [jax.ShapeDtypeStruct((n, width), F32), jax.ShapeDtypeStruct((n, NST), F32),
            jax.ShapeDtypeStruct((heads, n), F32), jax.ShapeDtypeStruct((NST, width), F32)]
    more = ([gathered(PC), jax.ShapeDtypeStruct((n_tp,) + comm[1].shape, F32)] if fetch_x else []) + [gathered(PC)] * 2
    vm = pltpu.VMEM
    dma = lambda k: [pltpu.SemaphoreType.DMA((k,))] * 2
    return pl.pallas_call(
        functools.partial(p1_body, geom=(n_dp, n_tp, heads, nb), mixed=mixed, layer=layer, fetch_x=fetch_x, plans=plans),
        name="p1", grid=(4, ni),
        in_specs=[pl.BlockSpec((rows, d_model), lambda p, i: (base() + once(p, i), 0)),
                  fixed((CAR, d_model)), fixed((1, d_model)), fixed((d_model, PC)), fixed((4, PC)), fixed((1, PC)),
                  fixed((3 * heads, width))] + [hbm] * 4,
        out_specs=[pl.BlockSpec((rows, 2 * PC), lambda p, i: (i, col(p))),
                   pl.BlockSpec((rows, NST), lambda p, i: (once(p, i), 0)),
                   pl.BlockSpec((heads, rows), lambda p, i: (0, once(p, i))),
                   pl.BlockSpec((NST, 2 * PC), lambda p, i: (0, col(p)))] + [hbm] * len(more),
        out_shape=outs + more,
        scratch_shapes=[
            vm((2, n_dp, 2, PC, PC), F32), vm((d_model, 2 * PC), BF16), pltpu.SemaphoreType.DMA((3,)),
            vm((n_tp, SMALL, PC), F32), vm((heads, d_model), BF16), vm((2 * heads, PC), F32), vm((NST, 2 * PC), F32),
            vm((CAR, d_model), BF16), vm((CAR, 2 * PC), F32), vm((CAR, PC), F32), vm((heads, LANES), F32),
            vm((d_model // LANES * rows, LANES), F32), vm((n, d_model), BF16),
            vm((nb * (NST + SUB), 4 * SUB), BF16), vm((nb * (NST + SUB), 2 * SUB), BF16),
            vm((n, 4 * SUB), BF16), vm((n, 2 * SUB), BF16), vm((n, 4 * NST), BF16), vm((n, LANES), F32),
            vm((2 * nb, 2 * heads // 2, LANES), F32), vm((n, 2 * BLK), BF16)]
        + dma(3 * SEMS) + (dma(8) if fetch_x else []),
        compiler_params=pltpu.CompilerParams(dimension_semantics=("arbitrary", "arbitrary"), vmem_limit_bytes=VMEM_CAP,
                                             collective_id=cid, has_side_effects=True),
        cost_estimate=pl.CostEstimate(flops=n * 70 * 10 ** 6, bytes_accessed=n * 12000, transcendentals=0),
    )(u, halo, nw, wbc, cbc, bbc, e3, *comm)


def p2_body(*refs, geom, mix_in, layer, fetch_x, plans):
    n_dp, n_tp, heads = geom
    (u_ref, nw_ref, wz_ref, wo_ref, sm_ref, y_ref, c_ref, ac_ref, s_ref, e3_ref), refs = refs[:10], refs[10:]
    if fetch_x:
        (ax, o_ref, f_ref, gx), refs = refs[:4], refs[4:]
    else:
        (o_ref, r_ref), refs = refs[:2], refs[2:]
    (wzb, wob, s3, ubuf, send, recv), refs = refs[:6], refs[6:]
    i = pl.program_id(0)
    width = PC * n_tp
    if fetch_x:
        xg = Gather(piece_rows(ax, layer + 1), gx, send, recv, 0)

        @pl.when(i == 0)
        def _():
            entry_barrier(xg.peers())
        at_steps(i, xg.plan(plans))
    else:
        fbuf, = refs
        dp, tp, z, c = here()

        def swap(k):
            return pltpu.make_async_remote_copy(
                src_ref=fbuf.at[k % 2], dst_ref=r_ref.at[pl.ds(pl.multiple_of(k * BLK2, BLK2), BLK2)],
                send_sem=send.at[k % 2], recv_sem=recv.at[0], device_id=(dp, 2 * z + 1 - c), device_id_type=MESH)

        @pl.when(i == 0)
        def _():
            entry_barrier([(dp, 2 * z + 1 - c)])

        @pl.when(i > 1)
        def _():
            swap(i - 2).wait_send()

        @pl.when(i > 0)
        def _():
            swap(i - 1).start()

    @pl.when(i == 0)
    def _():
        for d in range(n_dp):
            for t in range(n_tp):
                a, b = slice(d * PC, (d + 1) * PC), slice(t * PC, (t + 1) * PC)
                wzb[a, b] = wz_ref[d, t].astype(BF16)
                wob[b, a] = wo_ref[d, t].astype(BF16)
        a, b, c_ = split3(s_ref[...])
        for k, (v, w) in enumerate(((a, a), (b, b), (c_, a))):
            s3[k] = rows_cat(v, w)

    u = u_ref[...].astype(F32)
    u = u if mix_in else unmix(u, ubuf)
    h = rms(u, nw_ref[...])
    c1, c2, c3 = split3(c_ref[...])
    c12, c13 = lanes_cat(c1, c2), lanes_cat(c1, c3)
    eT = rows_cat(*split3(jnp.exp2(ac_ref[...]))).T
    vs, ss = [], 0.0
    for t in range(n_tp):
        sl = slice(t * PC, (t + 1) * PC)
        z_ = round_bf16(dot(h, wzb[:, sl]))
        cor = dot(c12, s3[0, :, sl]) + dot(c12, s3[1, :, sl]) + dot(c13, s3[2, :, sl])
        v = (y_ref[:, sl] + cor * dot(eT, e3_ref[:, sl])) * silu(z_)
        ss = ss + jnp.sum(v * v, axis=-1, keepdims=True)
        vs.append(v)
    sc = lax.rsqrt(ss / width + EPS)
    g = lanes_cat(*[(v * sc * sm_ref[t, 5:6, :]).astype(BF16) for t, v in enumerate(vs)])
    un = round_bf16(u + dot(g, wob[...]))
    if fetch_x:
        o_ref[...] = un.astype(BF16)
        f_ref[...] = un[BLK2 - CAR:]
    else:
        fbuf[i % 2] = un
        o_ref[...] = unmix(un, ubuf).astype(BF16)

    @pl.when(i == pl.num_programs(0) - 1)
    def _():
        if fetch_x:
            xg.finish()
        else:
            swap(i).start()
            for k in range(2):
                swap(i - 1 + k).wait_send()
            whole = pltpu.make_async_copy(r_ref, r_ref, recv.at[0])
            whole.wait()


def p2(u, base, nw, wz, wo, sm, y, c, ac, s, e3, comm, n, n_dp, n_tp, mix_in, layer, fetch_x, plans, cid):
    d_model, heads = u.shape[1], PC // HD * n_tp
    width = PC * n_tp
    fixed = lambda shp: pl.BlockSpec(shp, lambda i: (0,) * len(shp), pipeline_mode=pl.Buffered(1))
    hbm = pl.BlockSpec(memory_space=pl.ANY)
    rows = lambda w: pl.BlockSpec((BLK2, w), lambda i: (i, 0))
    shape = lambda *s: jax.ShapeDtypeStruct(s, F32)
    vm = pltpu.VMEM
    outs = [jax.ShapeDtypeStruct((n, d_model), BF16)]
    specs = [rows(d_model)]
    if fetch_x:
        outs += [shape(CAR, d_model), shape(n_dp, n_tp, PC, PC)]
        specs += [pl.BlockSpec((CAR, d_model), lambda i: (0, 0)), hbm]
    else:
        outs += [shape(n, d_model)]
        specs += [hbm]
    return pl.pallas_call(
        functools.partial(p2_body, geom=(n_dp, n_tp, heads), mix_in=mix_in, layer=layer, fetch_x=fetch_x, plans=plans),
        name="p2", grid=(n // BLK2,),
        in_specs=[pl.BlockSpec((BLK2, d_model), lambda i: (base() + i, 0)), fixed((1, d_model)),
                  fixed((n_dp, n_tp, PC, PC)), fixed((n_dp, n_tp, PC, PC)),
                  pl.BlockSpec((n_tp, SMALL, PC), lambda i: (0, layer, 0), pipeline_mode=pl.Buffered(1)),
                  rows(width), rows(NST), pl.BlockSpec((heads, BLK2), lambda i: (0, i)),
                  fixed((NST, width)), fixed((3 * heads, width))] + [hbm] * len(comm),
        out_specs=specs, out_shape=outs,
        scratch_shapes=[vm((d_model, width), BF16), vm((width, d_model), BF16), vm((3, 2 * NST, width), BF16),
                        vm((d_model // LANES * BLK2, LANES), F32)]
        + [pltpu.SemaphoreType.DMA((SEMS,))] * 2 + ([] if fetch_x else [vm((2, BLK2, d_model), F32)]),
        compiler_params=pltpu.CompilerParams(dimension_semantics=("arbitrary",), vmem_limit_bytes=VMEM_CAP,
                                             collective_id=cid, has_side_effects=True),
        cost_estimate=pl.CostEstimate(flops=n * 30 * 10 ** 6, bytes_accessed=n * 12000, transcendentals=0),
    )(u, nw, wz, wo, sm, y, c, ac, s, e3, *comm)


def finish_body(own_ref, other_ref, o_ref, ubuf):
    mine = pl.program_id(0) == here()[3]

    @pl.when(mine)
    def _():
        o_ref[...] = own_ref[...]

    @pl.when(jnp.logical_not(mine))
    def _():
        o_ref[...] = unmix(other_ref[...], ubuf).astype(BF16)


def finish(own, other):
    n, d_model = own.shape
    rows = 512
    ni = n // rows
    pick = lambda w: (lambda j, i: (jnp.where((j == here()[3]) == w, i, ni - 1), 0))
    return pl.pallas_call(
        finish_body, name="finish", grid=(2, ni),
        in_specs=[pl.BlockSpec((rows, d_model), pick(True)), pl.BlockSpec((rows, d_model), pick(False))],
        out_specs=pl.BlockSpec((rows, d_model), lambda j, i: (j * ni + i, 0)),
        out_shape=jax.ShapeDtypeStruct((2 * n, d_model), BF16),
        scratch_shapes=[pltpu.VMEM((d_model // LANES * rows, LANES), F32)],
        compiler_params=pltpu.CompilerParams(dimension_semantics=("arbitrary", "arbitrary")),
        cost_estimate=pl.CostEstimate(flops=n * d_model, bytes_accessed=n * d_model * 8, transcendentals=0),
    )(own, other)


def small_rows(conv, bias, gate, skip, dtb, al, wdt):
    f = lambda v: v.astype(F32)
    hp = skip.shape[0]
    wide = lambda v: jnp.broadcast_to(v[:, None], (hp, PC))
    return rows_cat(f(conv), f(bias)[None], f(gate)[None], jnp.repeat(skip, HD)[None], jnp.zeros((1, PC), F32),
                    wide(dtb), wide(-jnp.exp(al) * LOG2E), f(wdt).T.reshape(-1, PC))


PLAN_X = "00020305030506040608"
PLAN_Z0 = "04090a0c0b0c0e0c0e10"
PLAN_O0 = "0a0e1012101214121416"
PLAN_Z1 = "00020305030507050709"
PLAN_O1 = "0407090b090b0d0b0d10"
PLAN_X1 = "00020305030506040608"


def solution(mesh):
    n_tp, n_dp = mesh.shape['tp'], mesh.shape['dp']
    rep, col, vec = P(), P(None, None, 'tp'), P(None, 'tp')
    in_specs = (P('dp'), rep, col, col, rep, col, col, rep, vec, rep, vec, vec, vec, vec, P(None, 'tp', None))

    def device_forward(hidden, norm_w, w_z, w_x, w_bc, w_dt, conv_x, conv_bc, bias_x, bias_bc, dt_bias, a_log, d_skip, gate_w, w_out):
        u = hidden[0]
        steps, d_model = u.shape
        n = steps // 2
        core = lax.axis_index('tp') % 2
        e3 = expand_mat(dt_bias.shape[1] * n_tp)
        up = [(2 * k, 2 * k + 1) for k in range(n_tp // 2)]
        ax, az, ao = w_x.astype(F32), w_z.astype(F32), w_out.astype(F32)
        small = rows_cat(*[small_rows(conv_x[l], bias_x[l], gate_w[l], d_skip[l], dt_bias[l], a_log[l], w_dt[l]) for l in range(2)])
        tail = u[n - SUB:n].astype(F32).reshape(8, 8, d_model).transpose(1, 0, 2).reshape(SUB, d_model)[SUB - CAR:]
        halo = jnp.where(core == 1, tail, 0.0)
        half = lambda blk: (lambda: lax.axis_index('tp') % 2 * (n // blk))
        none = lambda: 0
        row = lambda v: v.astype(F32)[None]
        common = (n, n_dp, n_tp)
        bc = lambda l: (row(norm_w[l]), w_bc[l], conv_bc[l].astype(F32), row(bias_bc[l]), e3)

        y, c, ac, s, gx, gs, gz, go = p1(u, half(BLK * NBS), halo, *bc(0), (ax, small, az, ao), *common, False, 0, True,
                                         (PLAN_Z0, PLAN_O0, PLAN_X), 1)
        s = lax.ppermute(s, 'tp', up)
        u, f, gx = p2(u, half(BLK2), row(norm_w[0]), gz, go, gs, y, c, ac, s, e3, (ax,), *common, False, 0, True, PLAN_X1, 2)
        halo = lax.ppermute(f, 'tp', up)
        y, c, ac, s, gz, go = p1(u, none, halo, *bc(1), (gx, gs, az, ao), *common, True, 1, False, (PLAN_Z1, PLAN_O1), 3)
        s = lax.ppermute(s, 'tp', up)
        own, other = p2(u, none, row(norm_w[1]), gz, go, gs, y, c, ac, s, e3, (), *common, True, 1, False, None, 4)
        return finish(own, other)[None]

    return jax.shard_map(device_forward, mesh=mesh, in_specs=in_specs, out_specs=P('dp'), check_vma=False)
```

```python
import functools
import jax
import jax.numpy as jnp
from jax import lax
from jax.experimental import pallas as pl
from jax.experimental.pallas import tpu as pltpu
from jax.sharding import PartitionSpec as P

EPS = 1e-5
LOG2E = 1.4426950408889634
HI = lax.Precision.HIGHEST
F32 = jnp.float32
BF16 = jnp.bfloat16
MESH = pl.DeviceIdType.MESH
LANES = 128
BLK = 128
SUB = 64
BLK2 = 256
NBS = 4
PC = 256
HD = 64
NST = 128
CAR = 24
SMALL = 32
SEMS = 26
VMEM_CAP = 60 << 20


def silu(v):
    return v / (1.0 + jnp.exp2(v * -LOG2E))


def split3(v):
    a = v.astype(BF16)
    r = v - a.astype(F32)
    b = r.astype(BF16)
    return a, b, (r - b.astype(F32)).astype(BF16)


def round_bf16(v):
    return v.astype(BF16).astype(F32)


def rms(u, nw):
    return (u * lax.rsqrt(jnp.mean(u * u, axis=-1, keepdims=True) + EPS) * nw).astype(BF16)


def dot(a, b, prec=None):
    return jnp.dot(a, b, preferred_element_type=F32, precision=prec)


def dott(a, b, prec=None):
    return lax.dot_general(a, b, (((1,), (1,)), ((), ())), preferred_element_type=F32, precision=prec)


def rows_cat(*v):
    return jnp.concatenate(v, axis=0)


def lanes_cat(*v):
    return jnp.concatenate(v, axis=1)


def time_of(r):
    return 8 * (r % 8) + r // 8


def roll8(v):
    c = v.shape[-1]
    return pltpu.roll(v.reshape(CAR // 8, 8, c), 1, 1).reshape(CAR, c)


def conv_block(cur, prev, taps, bias, first):
    now = roll8(cur[SUB - CAR:])
    sh = jnp.where(first, prev, now)
    out = bias + cur * taps[-1]
    for k in range(1, 4):
        out = out + rows_cat(sh[CAR - 8 * k:], cur[:SUB - 8 * k]) * taps[3 - k]
    return out, now


def unmix(v, buf):
    n, c = v.shape
    for j in range(c // LANES):
        buf[n * j:n * (j + 1), :] = v[:, LANES * j:LANES * (j + 1)]
    cols = [rows_cat(*[buf[pl.ds(n * j + b + k, 8, stride=8), :] for b in range(0, n, SUB) for k in range(8)])
            for j in range(c // LANES)]
    return lanes_cat(*cols)


def head_row(h, heads):
    return (h % 2) * (heads // 2) + h // 2


def expand_mat(heads):
    order = sorted(range(heads), key=lambda h: head_row(h, heads))
    one = jnp.repeat(jnp.eye(heads, dtype=BF16)[jnp.array(order)], HD, axis=1)
    return rows_cat(one, one, one)


def kcat6(parts):
    a, b, c = parts
    return lanes_cat(a, b, c, a), lanes_cat(b, a)


def kcat6r(parts):
    a, b, c = parts
    return rows_cat(a, a, a, b), rows_cat(b, c)


def block_diag(x, lo, hi):
    z = jnp.zeros((x.shape[0], LANES), BF16)
    l, r = x[:, :LANES], x[:, LANES:]
    return rows_cat(lanes_cat(l * lo, z), lanes_cat(l * hi, z), lanes_cat(z, r * lo), lanes_cat(z, r * hi))


def here():
    dp, tp = lax.axis_index('dp'), lax.axis_index('tp')
    return dp, tp, tp // 2, tp % 2


def source(dz):
    return (here()[2] + 4 - dz) % 4


class Gather:
    def __init__(self, piece, g, send, recv, base, keep=True):
        self.piece, self.g, self.send, self.recv, self.base = piece, g, send, recv, base
        self.dp, self.tp, self.z, self.c = here()
        x, y = self.dp // 2, self.dp % 2
        self.side = ((1 - x) * 2 + y, x * 2 + 1 - y)
        self.partner = (self.dp, 2 * self.z + 1 - self.c)
        self.quarters, self.keep = g.shape[0], keep

    def rdma(self, k, src, dst, dev):
        return pltpu.make_async_remote_copy(src_ref=src, dst_ref=dst, send_sem=self.send.at[self.base + k],
                                            recv_sem=self.recv.at[self.base + k], device_id=dev, device_id_type=MESH)

    def local(self, q):
        return pltpu.make_async_copy(self.piece(q), self.g.at[q, self.tp], self.send.at[self.base + q])

    def own(self, q):
        return self.rdma(4 + q, self.piece(q), self.g.at[q, self.tp], self.partner)

    def line(self, dz):
        return self.rdma(7 + dz, self.piece(self.dp), self.g.at[self.dp, self.tp],
                         (self.dp, 2 * ((self.z + dz) % 4) + self.c))

    def cross(self, dz, n):
        ref = self.g.at[self.dp, 2 * source(dz) + self.c]
        return self.rdma(9 + 2 * dz + n, ref, ref, (self.side[n], self.tp))

    def relay(self, dz, n):
        half = self.g.shape[2] // 2
        ref = self.g.at[self.side[n], 2 * source(dz) + self.c, pl.ds(n * half, half)]
        return self.rdma(15 + 2 * dz + n, ref, ref, (self.side[1 - n], self.tp))

    def over(self, dz):
        ref = self.g.at[:, 2 * source(dz) + self.c]
        return self.rdma(22 + dz, ref, ref, self.partner)

    def peers(self):
        return ([(self.dp, 2 * ((self.z + dz) % 4) + self.c) for dz in (1, 2, 3)]
                + [(p, self.tp) for p in self.side] + [self.partner])

    def start(self):
        for dz in (1, 3, 2):
            self.line(dz).start()
        for q in range(self.quarters):
            self.own(q).start()
            if self.keep:
                self.local(q).start()

    def spread(self, dz):
        self.line(dz).wait_recv()
        for n in range(2):
            self.cross(dz, n).start()

    def pass_on(self, dz):
        for n in range(2):
            self.cross(dz, n).wait_recv()
            self.relay(dz, n).start()

    def hand(self, dz):
        for n in range(2):
            self.relay(dz, n).wait_recv()
        self.over(dz).start()

    def settle_own(self):
        for q in range(self.quarters):
            self.own(q).wait_recv()
            if self.keep:
                self.local(q).wait()

    def settle(self, dz):
        self.over(dz).wait_recv()

    def drain(self):
        for q in range(self.quarters):
            self.own(q).wait_send()
        for dz in (1, 2, 3):
            self.line(dz).wait_send()
            self.over(dz).wait_send()
            for n in range(2):
                self.cross(dz, n).wait_send()
                self.relay(dz, n).wait_send()

    def plan(self, s):
        s = bytes.fromhex(s)
        acts = [(s[0], self.start)]
        for k, f in enumerate((self.spread, self.pass_on, self.hand)):
            acts += [(s[1 + 3 * k + j], functools.partial(f, dz)) for j, dz in enumerate((1, 3, 2))]
        return acts

    def finish(self):
        self.settle_own()
        for dz in (1, 2, 3):
            self.settle(dz)
        self.drain()


class Small:
    def __init__(self, a, g, send, recv):
        self.a, self.g, self.send, self.recv = a, g, send, recv
        self.dp, self.tp, _, _ = here()

    def copy(self, k):
        return pltpu.make_async_remote_copy(src_ref=self.a, dst_ref=self.g.at[self.tp], send_sem=self.send.at[k],
                                            recv_sem=self.recv.at[k], device_id=(self.dp, (self.tp + k) % 8),
                                            device_id_type=MESH)

    def local(self):
        return pltpu.make_async_copy(self.a, self.g.at[self.tp], self.send.at[0])

    def peers(self):
        return [(self.dp, (self.tp + k) % 8) for k in range(1, 8)]

    def start(self):
        self.local().start()
        for k in range(1, 8):
            self.copy(k).start()

    def finish(self):
        self.local().wait()
        for k in range(1, 8):
            self.copy(k).wait()


def entry_barrier(peers):
    sem = pltpu.get_barrier_semaphore()
    for p in peers:
        pl.semaphore_signal(sem, inc=1, device_id=p, device_id_type=MESH)
    pl.semaphore_wait(sem, len(peers))


def at_steps(step, acts):
    for k in sorted({k for k, _ in acts}):
        @pl.when(step == k)
        def _():
            for j, f in acts:
                if j == k:
                    f()


def piece_rows(ref, layer):
    return lambda q: ref.at[layer, pl.ds(q * PC, PC)]


def piece_cols(ref, layer):
    return lambda q: ref.at[layer, :, pl.ds(pl.multiple_of(q * PC, PC) if not isinstance(q, int) else q * PC, PC)]


def p1_body(*refs, geom, mixed, layer, fetch_x, plans):
    n_dp, n_tp, heads, nb = geom
    (u_ref, halo_ref, nw_ref, wbc_ref, cbc_ref, bbc_ref, e3_ref), refs = refs[:7], refs[7:]
    if fetch_x:
        (ax, asm, az, ao), (y_ref, c_ref, ac_ref, send_ref), (gx, gs, gz, go), refs = refs[:4], refs[4:8], refs[8:12], refs[12:]
    else:
        (ax, gx, gs, az, ao), (y_ref, c_ref, ac_ref, send_ref), (gz, go), refs = refs[:5], refs[5:9], refs[9:11], refs[11:]
    (wf, wb, wsem, sm, wdt, cst, st, hcar, xcar, qcar, aoff, ubuf, h_s, la1_s, la2_s, lb1_s, lb2_s, cc_s, cbd_s, row_s, aw_s,
     send, recv), sems = refs[:23], refs[23:]
    p, i = pl.program_id(0), pl.program_id(1)
    np_, ni = pl.num_programs(0), pl.num_programs(1)
    step = p * ni + i
    d_model = u_ref.shape[-1]
    quad = 2 * PC
    dz = p + p // 2 * (1 - 2 * (p % 2))
    zs = source(dz)

    zg = Gather(piece_rows(az, layer), gz, send, recv, 0)
    og = Gather(piece_cols(ao, layer), go, send, recv, SEMS)
    acts = zg.plan(plans[0]) + og.plan(plans[1])
    if fetch_x:
        xg = Gather(piece_rows(ax, layer), gx, send, recv, 2 * SEMS, False)
        small = Small(asm, gs, *sems)
        acts += xg.plan(plans[2])

    def load_w(slot, zsrc):
        return pltpu.make_async_copy(gx.at[:, pl.ds(2 * zsrc, 2)], wf.at[slot], wsem.at[slot])

    def load_own():
        _, tp, _, c = here()
        return ([pltpu.make_async_copy(piece_rows(ax, layer)(q), wf.at[0, q, c], wsem.at[0]) for q in range(n_dp)]
                + [pltpu.make_async_copy(gx.at[q, tp + 1 - 2 * c], wf.at[0, q, 1 - c], wsem.at[0]) for q in range(n_dp)])

    @pl.when(step == 0)
    def _():
        entry_barrier((small.peers() + [(s, here()[1]) for s in zg.side]) if fetch_x else zg.peers())
        if fetch_x:
            small.start()
    at_steps(step, acts)

    @pl.when(step == 0)
    def _():
        if fetch_x:
            small.finish()
            xg.settle_own()
        for v in load_own():
            v.start()
        cp = pltpu.make_async_copy(gs.at[:, pl.ds(layer * SMALL, SMALL)], sm, wsem.at[2])
        cp.start()
        cp.wait()
        kc = d_model // PC
        hp = heads // n_tp
        for t in range(n_tp):
            for k in range(hp):
                r = head_row(hp * t + k, heads)
                for c in range(kc):
                    wdt[r:r + 1, c * PC:(c + 1) * PC] = sm[t, 16 + kc * k + c:17 + kc * k + c, :].astype(BF16)
                cst[r:r + 1, :] = sm[t, 8 + k:9 + k, :]
                cst[heads + r:heads + r + 1, :] = sm[t, 12 + k:13 + k, :]
        aoff[...] = jnp.zeros_like(aoff)
        hh = rms(halo_ref[...], nw_ref[...])
        hcar[...] = hh
        qcar[...] = roll8(round_bf16(dot(hh, wbc_ref[...])))

    first = lax.broadcasted_iota(jnp.int32, (CAR, PC), 0) % 8 == 0

    def conv(cur, prev, taps, bias):
        a, now = conv_block(cur[:SUB], prev, taps, bias, first)
        b, now = conv_block(cur[SUB:], now, taps, bias, first)
        return silu(rows_cat(a, b)), now

    ri = lax.broadcasted_iota(jnp.int32, (BLK, BLK), 0)
    ci = lax.broadcasted_iota(jnp.int32, (BLK, BLK), 1)

    def prologue(b, h):
        j = i * NBS + b
        blk = pl.ds(pl.multiple_of(j * BLK, BLK), BLK)
        h_s[blk, :] = h
        rT = round_bf16(dott(wdt[...], h))
        bc, qcar[...] = conv(round_bf16(dot(h, wbc_ref[...])), qcar[...],
                             [cbc_ref[k:k + 1, :] for k in range(4)], bbc_ref[...])
        bmat, cmat = bc[:, :NST], bc[:, NST:]
        here_rows = slice(b * BLK, (b + 1) * BLK)
        c_ref[here_rows, :] = cmat
        pre = rT + cst[:heads, :BLK]
        dtT = jnp.maximum(pre, 0.0) + jnp.log1p(jnp.exp(-jnp.abs(pre)))
        aT = dtT * cst[heads:, :BLK]
        tr, tc = ri // SUB * SUB + time_of(ri % SUB), ci // SUB * SUB + time_of(ci % SUB)
        acT = dot(aT, jnp.where(tr <= tc, 1.0, 0.0), HI)
        mid, alast = acT[:, SUB - 1:SUB], acT[:, BLK - 1:BLK]
        low = ci[:heads] < SUB
        wT = dtT * jnp.exp2(jnp.where(low, mid, alast) - acT)
        pad = jnp.zeros((BLK - 3 * heads, BLK), BF16)
        aw_s[blk, :] = lanes_cat(rows_cat(*split3(acT), pad).T, rows_cat(*split3(wT), pad).T)
        ac_ref[:, here_rows] = acT + aoff[:, :1]
        aoff[...] = aoff[...] + alast

        def pair_rows(v):
            ev, od = v[:heads // 2], v[heads // 2:]
            l = low[:heads // 2]
            return jnp.where(l, ev, pltpu.roll(od, SUB, 1)), jnp.where(l, pltpu.roll(ev, SUB, 1), od)

        for half, (a, d) in enumerate(zip(pair_rows(acT), pair_rows(dtT))):
            row_s[2 * j + half] = rows_cat(*[v[4 * z:4 * z + 4] for z in range(heads // 8) for v in (a, d)])
        cb = dott(cmat, bmat, HI)
        lowr, tri = ci[:SUB] < SUB, time_of(ri[:SUB]) >= time_of(ci[:SUB] % SUB)
        ca, cd = cb[:SUB], cb[SUB:]
        cbd_s[blk, :] = rows_cat(jnp.where(tri, jnp.where(lowr, ca, pltpu.roll(ca, SUB, 1)), 0.0),
                                 jnp.where(tri, jnp.where(lowr, pltpu.roll(cd, SUB, 1), cd), 0.0))
        bT = bmat.T
        big = pl.ds(pl.multiple_of(j * (NST + SUB), SUB), NST + SUB)
        la1_s[big, :], la2_s[big, :] = kcat6(split3(rows_cat(bT[:, :SUB], cd[:, :SUB])))
        lb1_s[blk, :], lb2_s[blk, :] = kcat6(split3(pltpu.roll(bT, SUB, 1)[:, :SUB]))
        c1, c2, c3 = split3(cmat)
        cc_s[blk, :] = lanes_cat(c1, c2, c1, c3)

    @pl.when(p == 0)
    def _():
        u = u_ref[...].astype(F32)
        h = rms(u if mixed else unmix(u, ubuf), nw_ref[...])
        for b in range(NBS):
            prologue(b, h[b * BLK:(b + 1) * BLK])

    @pl.when(i == 0)
    def _():
        slot = p % 2

        @pl.when(p == 0)
        def _():
            for v in load_own():
                v.wait()

        @pl.when(p > 0)
        def _():
            load_w(slot, zs).wait()
        for q in range(n_dp):
            for k in range(2):
                wb[q * PC:(q + 1) * PC, k * PC:(k + 1) * PC] = wf[slot, q, k].astype(BF16)
        xcar[...] = roll8(round_bf16(dot(hcar[...], wb[...])))
        st[...] = jnp.zeros_like(st)

    @pl.when((i == ni - 1) & (p < np_ - 1))
    def _():
        nd = p + 1
        nd = nd + nd // 2 * (1 - 2 * (nd % 2))
        if fetch_x:
            for d in (1, 2, 3):
                pl.when(nd == d)(functools.partial(xg.settle, d))
        load_w((p + 1) % 2, source(nd)).start()

    lane = lax.broadcasted_iota(jnp.int32, (SUB, LANES), 1)
    lo = jnp.where(lane < HD, 1.0, 0.0).astype(BF16)
    hi = jnp.where(lane < HD, 0.0, 1.0).astype(BF16)
    x0 = [dot(h_s[pl.ds(pl.multiple_of(i * NBS * BLK, BLK), NBS * BLK), :], wb[:, k * PC:(k + 1) * PC]) for k in range(2)]

    def place(b):
        j = i * NBS + b
        return j, pl.ds(pl.multiple_of(j * BLK, BLK), BLK), pl.ds(pl.multiple_of(j * (NST + SUB), SUB), NST + SUB)

    def lanes_of(k):
        return slice(k * PC, (k + 1) * PC), pl.ds(pl.multiple_of((2 * zs + k) * PC, PC), PC)

    def pre(b, k):
        (_, blk, _), (sl, gl) = place(b), lanes_of(k)
        s1, s2, s3 = split3(st[:, sl])
        c12, c13 = cc_s[blk, :2 * NST], cc_s[blk, 2 * NST:]
        inter = dot(c12, rows_cat(s1, s1)) + dot(c12, rows_cat(s2, s2)) + dot(c13, rows_cat(s3, s1))
        n3 = e3_ref.shape[0]
        acx = dot(aw_s[blk, :n3], e3_ref[:, gl])
        wx = dot(aw_s[blk, BLK:BLK + n3], e3_ref[:, gl])
        return x0[k][b * BLK:(b + 1) * BLK], acx, wx, inter

    def mid_(b, k, x0, acx, wx, inter):
        (j, blk, _), (sl, _) = place(b), lanes_of(k)
        t = 2 * zs + k
        x, xcar[:, sl] = conv(round_bf16(x0), xcar[:, sl], [sm[t, r:r + 1, :] for r in range(4)], sm[t, 4:5, :])
        xw = split3(x * wx)
        r = kcat6r([v[:SUB] for v in xw]) + kcat6r([v[SUB:] for v in xw])
        ms, xs = [], []
        for half in range(2):
            rows = slice(half * SUB, (half + 1) * SUB)
            row = row_s[2 * j + half, pl.ds(pl.multiple_of(8 * zs, 8), 8), :]
            cbd = cbd_s[pl.ds(pl.multiple_of(j * BLK + half * SUB, SUB), SUB), :]
            m = []
            for g in range(2):
                seg = acx[rows, g * LANES:(g + 1) * LANES] - row[2 * k + g:2 * k + g + 1]
                m.append(jnp.exp2(jnp.minimum(seg, 0.0)) * cbd * row[4 + 2 * k + g:5 + 2 * k + g])
            ms.append(split3(lanes_cat(*m)))
            xs.append([block_diag(v, lo, hi) for v in split3(x[rows])])
        return x, acx, inter, r, ms, xs

    def fin(b, k, x, acx, inter, r, ms, xs):
        (j, blk, big), (sl, _) = place(b), lanes_of(k)
        ra = dot(la1_s[big, :], r[0]) + dot(la2_s[big, :], r[1])
        rb = dot(lb1_s[blk, :], r[2]) + dot(lb2_s[blk, :], r[3])
        am, al = acx[SUB - 1:SUB], acx[BLK - 1:BLK]
        st[:, sl] = st[:, sl] * jnp.exp2(al) + ra[:NST] * jnp.exp2(al - am) + rb
        skip = sm[2 * zs + k, 6:7, :]
        for half in range(2):
            rows = slice(half * SUB, (half + 1) * SUB)
            (m1, m2, m3), (x1, x2, x3) = ms[half], xs[half]
            r1 = dot(rows_cat(m1, m2, m3), x1)
            r2 = dot(rows_cat(m1, m2), x2)
            y = r1[:SUB] + r1[SUB:2 * SUB] + r1[2 * SUB:] + r2[:SUB] + r2[SUB:] + dot(m1, x3)
            y = y + inter[rows] * jnp.exp2(acx[rows])
            if half:
                y = y + ra[NST:] * jnp.exp2(acx[rows] - am)
            y_ref[b * BLK + half * SUB:b * BLK + (half + 1) * SUB, sl] = y + skip * x[rows]

    units = [(b, k) for b in range(NBS) for k in range(2)]
    m = mid_(*units[0], *pre(*units[0]))
    for a, nxt in zip(units, units[1:] + [None]):
        if nxt:
            v = pre(*nxt)
        fin(*a, *m)
        if nxt:
            m = mid_(*nxt, *v)

    @pl.when(i == ni - 1)
    def _():
        send_ref[...] = st[...]

    @pl.when(step == np_ * ni - 1)
    def _():
        zg.finish()
        og.finish()
        if fetch_x:
            xg.drain()


def p1(u, base, halo, nw, wbc, cbc, bbc, e3, comm, n, n_dp, n_tp, mixed, layer, fetch_x, plans, cid):
    d_model, heads = u.shape[1], PC // HD * n_tp
    width, nb, rows = PC * n_tp, n // BLK, BLK * NBS
    ni = nb // NBS
    fixed = lambda shp: pl.BlockSpec(shp, lambda p, i: (0,) * len(shp), pipeline_mode=pl.Buffered(1))
    once = lambda p, i: jnp.where(p == 0, i, ni - 1)
    col = lambda p: source(p + p // 2 * (1 - 2 * (p % 2)))
    hbm = pl.BlockSpec(memory_space=pl.ANY)
    gathered = lambda r: jax.ShapeDtypeStruct((n_dp, n_tp, r, PC), F32)
    outs = [jax.ShapeDtypeStruct((n, width), F32), jax.ShapeDtypeStruct((n, NST), F32),
            jax.ShapeDtypeStruct((heads, n), F32), jax.ShapeDtypeStruct((NST, width), F32)]
    more = ([gathered(PC), jax.ShapeDtypeStruct((n_tp,) + comm[1].shape, F32)] if fetch_x else []) + [gathered(PC)] * 2
    vm = pltpu.VMEM
    dma = lambda k: [pltpu.SemaphoreType.DMA((k,))] * 2
    return pl.pallas_call(
        functools.partial(p1_body, geom=(n_dp, n_tp, heads, nb), mixed=mixed, layer=layer, fetch_x=fetch_x, plans=plans),
        name="p1", grid=(4, ni),
        in_specs=[pl.BlockSpec((rows, d_model), lambda p, i: (base() + once(p, i), 0)),
                  fixed((CAR, d_model)), fixed((1, d_model)), fixed((d_model, PC)), fixed((4, PC)), fixed((1, PC)),
                  fixed((3 * heads, width))] + [hbm] * len(comm),
        out_specs=[pl.BlockSpec((rows, 2 * PC), lambda p, i: (i, col(p))),
                   pl.BlockSpec((rows, NST), lambda p, i: (once(p, i), 0)),
                   pl.BlockSpec((heads, rows), lambda p, i: (0, once(p, i))),
                   pl.BlockSpec((NST, 2 * PC), lambda p, i: (0, col(p)))] + [hbm] * len(more),
        out_shape=outs + more,
        scratch_shapes=[
            vm((2, n_dp, 2, PC, PC), F32), vm((d_model, 2 * PC), BF16), pltpu.SemaphoreType.DMA((3,)),
            vm((n_tp, SMALL, PC), F32), vm((heads, d_model), BF16), vm((2 * heads, PC), F32), vm((NST, 2 * PC), F32),
            vm((CAR, d_model), BF16), vm((CAR, 2 * PC), F32), vm((CAR, PC), F32), vm((heads, LANES), F32),
            vm((d_model // LANES * rows, LANES), F32), vm((n, d_model), BF16),
            vm((nb * (NST + SUB), 4 * SUB), BF16), vm((nb * (NST + SUB), 2 * SUB), BF16),
            vm((n, 4 * SUB), BF16), vm((n, 2 * SUB), BF16), vm((n, 4 * NST), BF16), vm((n, LANES), F32),
            vm((2 * nb, 2 * heads // 2, LANES), F32), vm((n, 2 * BLK), BF16)]
        + dma(3 * SEMS) + (dma(8) if fetch_x else []),
        compiler_params=pltpu.CompilerParams(dimension_semantics=("arbitrary", "arbitrary"), vmem_limit_bytes=VMEM_CAP,
                                             collective_id=cid, has_side_effects=True),
        cost_estimate=pl.CostEstimate(flops=n * 70 * 10 ** 6, bytes_accessed=n * 12000, transcendentals=0),
    )(u, halo, nw, wbc, cbc, bbc, e3, *comm)


def p2_body(*refs, geom, mix_in, layer, fetch_x, plans):
    n_dp, n_tp, heads = geom
    (u_ref, nw_ref, wz_ref, wo_ref, sm_ref, y_ref, c_ref, ac_ref, s_ref, e3_ref), refs = refs[:10], refs[10:]
    if fetch_x:
        (ax, o_ref, f_ref, gx), refs = refs[:4], refs[4:]
    else:
        (o_ref, r_ref), refs = refs[:2], refs[2:]
    (wzb, wob, s3, ubuf, send, recv), refs = refs[:6], refs[6:]
    i = pl.program_id(0)
    width = PC * n_tp
    if fetch_x:
        xg = Gather(piece_rows(ax, layer + 1), gx, send, recv, 0, False)

        @pl.when(i == 0)
        def _():
            entry_barrier(xg.peers())
        at_steps(i, xg.plan(plans))
    else:
        fbuf, = refs
        dp, tp, z, c = here()

        def swap(k):
            return pltpu.make_async_remote_copy(
                src_ref=fbuf.at[k % 2], dst_ref=r_ref.at[pl.ds(pl.multiple_of(k * BLK2, BLK2), BLK2)],
                send_sem=send.at[k % 2], recv_sem=recv.at[0], device_id=(dp, 2 * z + 1 - c), device_id_type=MESH)

        @pl.when(i == 0)
        def _():
            entry_barrier([(dp, 2 * z + 1 - c)])

        @pl.when(i > 1)
        def _():
            swap(i - 2).wait_send()

        @pl.when(i > 0)
        def _():
            swap(i - 1).start()

    @pl.when(i == 0)
    def _():
        for d in range(n_dp):
            for t in range(n_tp):
                a, b = slice(d * PC, (d + 1) * PC), slice(t * PC, (t + 1) * PC)
                wzb[a, b] = wz_ref[d, t].astype(BF16)
                wob[b, a] = wo_ref[d, t].astype(BF16)
        a, b, c_ = split3(s_ref[...])
        for k, (v, w) in enumerate(((a, a), (b, b), (c_, a))):
            s3[k] = rows_cat(v, w)

    u = u_ref[...].astype(F32)
    u = u if mix_in else unmix(u, ubuf)
    h = rms(u, nw_ref[...])
    c1, c2, c3 = split3(c_ref[...])
    c12, c13 = lanes_cat(c1, c2), lanes_cat(c1, c3)
    eT = rows_cat(*split3(jnp.exp2(ac_ref[...]))).T
    vs, ss = [], 0.0
    for t in range(n_tp):
        sl = slice(t * PC, (t + 1) * PC)
        z_ = round_bf16(dot(h, wzb[:, sl]))
        cor = dot(c12, s3[0, :, sl]) + dot(c12, s3[1, :, sl]) + dot(c13, s3[2, :, sl])
        v = (y_ref[:, sl] + cor * dot(eT, e3_ref[:, sl])) * silu(z_)
        ss = ss + jnp.sum(v * v, axis=-1, keepdims=True)
        vs.append(v)
    sc = lax.rsqrt(ss / width + EPS)
    g = lanes_cat(*[(v * sc * sm_ref[t, 5:6, :]).astype(BF16) for t, v in enumerate(vs)])
    un = round_bf16(u + dot(g, wob[...]))
    if fetch_x:
        o_ref[...] = un.astype(BF16)
        f_ref[...] = un[BLK2 - CAR:]
    else:
        un = unmix(un, ubuf)
        fbuf[i % 2] = un
        o_ref[...] = un.astype(BF16)

    @pl.when(i == pl.num_programs(0) - 1)
    def _():
        if fetch_x:
            xg.finish()
        else:
            swap(i).start()
            for k in range(2):
                swap(i - 1 + k).wait_send()
            whole = pltpu.make_async_copy(r_ref, r_ref, recv.at[0])
            whole.wait()


def p2(u, base, nw, wz, wo, sm, y, c, ac, s, e3, comm, n, n_dp, n_tp, mix_in, layer, fetch_x, plans, cid):
    d_model, heads = u.shape[1], PC // HD * n_tp
    width = PC * n_tp
    fixed = lambda shp: pl.BlockSpec(shp, lambda i: (0,) * len(shp), pipeline_mode=pl.Buffered(1))
    hbm = pl.BlockSpec(memory_space=pl.ANY)
    rows = lambda w: pl.BlockSpec((BLK2, w), lambda i: (i, 0))
    shape = lambda *s: jax.ShapeDtypeStruct(s, F32)
    vm = pltpu.VMEM
    outs = [jax.ShapeDtypeStruct((n, d_model), BF16)]
    specs = [rows(d_model)]
    if fetch_x:
        outs += [shape(CAR, d_model), shape(n_dp, n_tp, PC, PC)]
        specs += [pl.BlockSpec((CAR, d_model), lambda i: (0, 0)), hbm]
    else:
        outs += [shape(n, d_model)]
        specs += [hbm]
    return pl.pallas_call(
        functools.partial(p2_body, geom=(n_dp, n_tp, heads), mix_in=mix_in, layer=layer, fetch_x=fetch_x, plans=plans),
        name="p2", grid=(n // BLK2,),
        in_specs=[pl.BlockSpec((BLK2, d_model), lambda i: (base() + i, 0)), fixed((1, d_model)),
                  fixed((n_dp, n_tp, PC, PC)), fixed((n_dp, n_tp, PC, PC)),
                  pl.BlockSpec((n_tp, SMALL, PC), lambda i: (0, layer, 0), pipeline_mode=pl.Buffered(1)),
                  rows(width), rows(NST), pl.BlockSpec((heads, BLK2), lambda i: (0, i)),
                  fixed((NST, width)), fixed((3 * heads, width))] + [hbm] * len(comm),
        out_specs=specs, out_shape=outs,
        scratch_shapes=[vm((d_model, width), BF16), vm((width, d_model), BF16), vm((3, 2 * NST, width), BF16),
                        vm((d_model // LANES * BLK2, LANES), F32)]
        + [pltpu.SemaphoreType.DMA((SEMS,))] * 2 + ([] if fetch_x else [vm((2, BLK2, d_model), F32)]),
        compiler_params=pltpu.CompilerParams(dimension_semantics=("arbitrary",), vmem_limit_bytes=VMEM_CAP,
                                             collective_id=cid, has_side_effects=True),
        cost_estimate=pl.CostEstimate(flops=n * 30 * 10 ** 6, bytes_accessed=n * 12000, transcendentals=0),
    )(u, nw, wz, wo, sm, y, c, ac, s, e3, *comm)


def finish_body(own_ref, other_ref, o_ref):
    mine = pl.program_id(0) == here()[3]

    @pl.when(mine)
    def _():
        o_ref[...] = own_ref[...]

    @pl.when(jnp.logical_not(mine))
    def _():
        o_ref[...] = other_ref[...].astype(BF16)


def finish(own, other):
    n, d_model = own.shape
    rows = 512
    ni = n // rows
    pick = lambda w: (lambda j, i: (jnp.where((j == here()[3]) == w, i, ni - 1), 0))
    return pl.pallas_call(
        finish_body, name="finish", grid=(2, ni),
        in_specs=[pl.BlockSpec((rows, d_model), pick(True)), pl.BlockSpec((rows, d_model), pick(False))],
        out_specs=pl.BlockSpec((rows, d_model), lambda j, i: (j * ni + i, 0)),
        out_shape=jax.ShapeDtypeStruct((2 * n, d_model), BF16),
        compiler_params=pltpu.CompilerParams(dimension_semantics=("arbitrary", "arbitrary")),
        cost_estimate=pl.CostEstimate(flops=n * d_model, bytes_accessed=n * d_model * 8, transcendentals=0),
    )(own, other)


def small_rows(conv, bias, gate, skip, dtb, al, wdt):
    f = lambda v: v.astype(F32)
    hp = skip.shape[0]
    wide = lambda v: jnp.broadcast_to(v[:, None], (hp, PC))
    return rows_cat(f(conv), f(bias)[None], f(gate)[None], jnp.repeat(skip, HD)[None], jnp.zeros((1, PC), F32),
                    wide(dtb), wide(-jnp.exp(al) * LOG2E), f(wdt).T.reshape(-1, PC))


PLAN_X = "00020305030506040608"
PLAN_Z0 = "04090a0c0b0c0e0c0e10"
PLAN_O0 = "0a0e1012101214121416"
PLAN_Z1 = "00020305030507050709"
PLAN_O1 = "0407090b090b0d0b0d10"
PLAN_X1 = "00020305030506040608"


def solution(mesh):
    n_tp, n_dp = mesh.shape['tp'], mesh.shape['dp']
    rep, col, vec = P(), P(None, None, 'tp'), P(None, 'tp')
    in_specs = (P('dp'), rep, col, col, rep, col, col, rep, vec, rep, vec, vec, vec, vec, P(None, 'tp', None))

    def device_forward(hidden, norm_w, w_z, w_x, w_bc, w_dt, conv_x, conv_bc, bias_x, bias_bc, dt_bias, a_log, d_skip, gate_w, w_out):
        u = hidden[0]
        steps, d_model = u.shape
        n = steps // 2
        core = lax.axis_index('tp') % 2
        e3 = expand_mat(dt_bias.shape[1] * n_tp)
        up = [(2 * k, 2 * k + 1) for k in range(n_tp // 2)]
        ax, az, ao = w_x.astype(F32), w_z.astype(F32), w_out.astype(F32)
        small = rows_cat(*[small_rows(conv_x[l], bias_x[l], gate_w[l], d_skip[l], dt_bias[l], a_log[l], w_dt[l]) for l in range(2)])
        tail = u[n - SUB:n].astype(F32).reshape(8, 8, d_model).transpose(1, 0, 2).reshape(SUB, d_model)[SUB - CAR:]
        halo = jnp.where(core == 1, tail, 0.0)
        half = lambda blk: (lambda: lax.axis_index('tp') % 2 * (n // blk))
        none = lambda: 0
        row = lambda v: v.astype(F32)[None]
        common = (n, n_dp, n_tp)
        bc = lambda l: (row(norm_w[l]), w_bc[l], conv_bc[l].astype(F32), row(bias_bc[l]), e3)

        y, c, ac, s, gx, gs, gz, go = p1(u, half(BLK * NBS), halo, *bc(0), (ax, small, az, ao), *common, False, 0, True,
                                         (PLAN_Z0, PLAN_O0, PLAN_X), 1)
        s = lax.ppermute(s, 'tp', up)
        u, f, gx = p2(u, half(BLK2), row(norm_w[0]), gz, go, gs, y, c, ac, s, e3, (ax,), *common, False, 0, True, PLAN_X1, 2)
        halo = lax.ppermute(f, 'tp', up)
        y, c, ac, s, gz, go = p1(u, none, halo, *bc(1), (ax, gx, gs, az, ao), *common, True, 1, False, (PLAN_Z1, PLAN_O1), 3)
        s = lax.ppermute(s, 'tp', up)
        own, other = p2(u, none, row(norm_w[1]), gz, go, gs, y, c, ac, s, e3, (), *common, True, 1, False, None, 4)
        return finish(own, other)[None]

    return jax.shard_map(device_forward, mesh=mesh, in_specs=in_specs, out_specs=P('dp'), check_vma=False)
```

```python
import functools
import jax
import jax.numpy as jnp
import numpy as np
from jax import lax
from jax.experimental import pallas as pl
from jax.experimental.pallas import tpu as pltpu
from jax.sharding import PartitionSpec as P

EPS = 1e-5
LOG2E = 1.4426950408889634
HI = lax.Precision.HIGHEST
F32 = jnp.float32
BF16 = jnp.bfloat16
MESH = pl.DeviceIdType.MESH
LANES = 128
BLK = 128
SUB = 64
BLK2 = 256
NBS = 4
PC = 256
HD = 64
NST = 128
CAR = 24
SMALL = 32
SEMS = 26
VMEM_CAP = 60 << 20


def silu(v):
    return v / (1.0 + jnp.exp2(v * -LOG2E))


def split3(v):
    a = v.astype(BF16)
    r = v - a.astype(F32)
    b = r.astype(BF16)
    return a, b, (r - b.astype(F32)).astype(BF16)


def round_bf16(v):
    return v.astype(BF16).astype(F32)


def rms(u, nw):
    return (u * lax.rsqrt(jnp.mean(u * u, axis=-1, keepdims=True) + EPS) * nw).astype(BF16)


def dot(a, b, prec=None):
    return jnp.dot(a, b, preferred_element_type=F32, precision=prec)


def dott(a, b, prec=None):
    return lax.dot_general(a, b, (((1,), (1,)), ((), ())), preferred_element_type=F32, precision=prec)


def rows_cat(*v):
    return jnp.concatenate(v, axis=0)


def lanes_cat(*v):
    return jnp.concatenate(v, axis=1)


def time_of(r):
    return 8 * (r % 8) + r // 8


def roll8(v):
    c = v.shape[-1]
    return pltpu.roll(v.reshape(CAR // 8, 8, c), 1, 1).reshape(CAR, c)


def conv_block(cur, prev, taps, bias, first):
    now = roll8(cur[SUB - CAR:])
    sh = jnp.where(first, prev, now)
    out = bias + cur * taps[-1]
    for k in range(1, 4):
        out = out + rows_cat(sh[CAR - 8 * k:], cur[:SUB - 8 * k]) * taps[3 - k]
    return out, now


def unmix(v, buf):
    n, c = v.shape
    for j in range(c // LANES):
        buf[n * j:n * (j + 1), :] = v[:, LANES * j:LANES * (j + 1)]
    cols = [rows_cat(*[buf[pl.ds(n * j + b + k, 8, stride=8), :] for b in range(0, n, SUB) for k in range(8)])
            for j in range(c // LANES)]
    return lanes_cat(*cols)


def head_row(h, heads):
    return (h % 2) * (heads // 2) + h // 2


def expand_mat(heads):
    order = sorted(range(heads), key=lambda h: head_row(h, heads))
    one = np.repeat(np.eye(heads)[order], HD, axis=1)
    return jnp.asarray(np.tile(one, (3, 1)), BF16)


def kcat6(parts):
    a, b, c = parts
    return lanes_cat(a, b, c, a), lanes_cat(b, a)


def kcat6r(parts):
    a, b, c = parts
    return rows_cat(a, a, a, b), rows_cat(b, c)


def block_diag(x, lo, hi):
    z = jnp.zeros((x.shape[0], LANES), BF16)
    l, r = x[:, :LANES], x[:, LANES:]
    return rows_cat(lanes_cat(l * lo, z), lanes_cat(l * hi, z), lanes_cat(z, r * lo), lanes_cat(z, r * hi))


def here():
    dp, tp = lax.axis_index('dp'), lax.axis_index('tp')
    return dp, tp, tp // 2, tp % 2


def source(dz):
    return (here()[2] + 4 - dz) % 4


class Gather:
    def __init__(self, piece, g, send, recv, base, keep=True):
        self.piece, self.g, self.send, self.recv, self.base = piece, g, send, recv, base
        self.dp, self.tp, self.z, self.c = here()
        x, y = self.dp // 2, self.dp % 2
        self.side = ((1 - x) * 2 + y, x * 2 + 1 - y)
        self.partner = (self.dp, 2 * self.z + 1 - self.c)
        self.quarters, self.keep = g.shape[0], keep

    def rdma(self, k, src, dst, dev):
        return pltpu.make_async_remote_copy(src_ref=src, dst_ref=dst, send_sem=self.send.at[self.base + k],
                                            recv_sem=self.recv.at[self.base + k], device_id=dev, device_id_type=MESH)

    def local(self, q):
        return pltpu.make_async_copy(self.piece(q), self.g.at[q, self.tp], self.send.at[self.base + q])

    def own(self, q):
        return self.rdma(4 + q, self.piece(q), self.g.at[q, self.tp], self.partner)

    def line(self, dz):
        return self.rdma(7 + dz, self.piece(self.dp), self.g.at[self.dp, self.tp],
                         (self.dp, 2 * ((self.z + dz) % 4) + self.c))

    def cross(self, dz, n):
        ref = self.g.at[self.dp, 2 * source(dz) + self.c]
        return self.rdma(9 + 2 * dz + n, ref, ref, (self.side[n], self.tp))

    def relay(self, dz, n):
        half = self.g.shape[2] // 2
        ref = self.g.at[self.side[n], 2 * source(dz) + self.c, pl.ds(n * half, half)]
        return self.rdma(15 + 2 * dz + n, ref, ref, (self.side[1 - n], self.tp))

    def over(self, dz):
        ref = self.g.at[:, 2 * source(dz) + self.c]
        return self.rdma(22 + dz, ref, ref, self.partner)

    def peers(self):
        return ([(self.dp, 2 * ((self.z + dz) % 4) + self.c) for dz in (1, 2, 3)]
                + [(p, self.tp) for p in self.side] + [self.partner])

    def start(self):
        for q in range(self.quarters):
            self.own(q).start()
        for dz in (1, 3, 2):
            self.line(dz).start()
        if self.keep:
            for q in range(self.quarters):
                self.local(q).start()

    def spread(self, dz):
        self.line(dz).wait_recv()
        for n in range(2):
            self.cross(dz, n).start()

    def pass_on(self, dz):
        for n in range(2):
            self.cross(dz, n).wait_recv()
            self.relay(dz, n).start()

    def hand(self, dz):
        for n in range(2):
            self.relay(dz, n).wait_recv()
        self.over(dz).start()

    def settle_own(self):
        for q in range(self.quarters):
            self.own(q).wait_recv()
            if self.keep:
                self.local(q).wait()

    def settle(self, dz):
        self.over(dz).wait_recv()

    def drain(self):
        for q in range(self.quarters):
            self.own(q).wait_send()
        for dz in (1, 2, 3):
            self.line(dz).wait_send()
            self.over(dz).wait_send()
            for n in range(2):
                self.cross(dz, n).wait_send()
                self.relay(dz, n).wait_send()

    def plan(self, s):
        s = bytes.fromhex(s)
        acts = [(s[0], self.start)]
        for k, f in enumerate((self.spread, self.pass_on, self.hand)):
            acts += [(s[1 + 3 * k + j], functools.partial(f, dz)) for j, dz in enumerate((1, 3, 2))]
        return acts

    def finish(self):
        self.settle_own()
        for dz in (1, 2, 3):
            self.settle(dz)
        self.drain()


class Small:
    def __init__(self, a, g, send, recv):
        self.a, self.g, self.send, self.recv = a, g, send, recv
        self.dp, self.tp, _, _ = here()

    def copy(self, k):
        return pltpu.make_async_remote_copy(src_ref=self.a, dst_ref=self.g.at[self.tp], send_sem=self.send.at[k],
                                            recv_sem=self.recv.at[k], device_id=(self.dp, (self.tp + k) % 8),
                                            device_id_type=MESH)

    def local(self):
        return pltpu.make_async_copy(self.a, self.g.at[self.tp], self.send.at[0])

    def peers(self):
        return [(self.dp, (self.tp + k) % 8) for k in range(1, 8)]

    def start(self):
        self.local().start()
        for k in range(1, 8):
            self.copy(k).start()

    def finish(self):
        self.local().wait()
        for k in range(1, 8):
            self.copy(k).wait()


def entry_barrier(peers):
    sem = pltpu.get_barrier_semaphore()
    for p in peers:
        pl.semaphore_signal(sem, inc=1, device_id=p, device_id_type=MESH)
    pl.semaphore_wait(sem, len(peers))


def at_steps(step, acts):
    for k in sorted({k for k, _ in acts}):
        @pl.when(step == k)
        def _():
            for j, f in acts:
                if j == k:
                    f()


def piece_rows(ref, layer):
    return lambda q: ref.at[layer, pl.ds(q * PC, PC)]


def piece_cols(ref, layer):
    return lambda q: ref.at[layer, :, pl.ds(pl.multiple_of(q * PC, PC) if not isinstance(q, int) else q * PC, PC)]


def p1_body(*refs, geom, mixed, layer, fetch_x, plans):
    n_dp, n_tp, heads, nb, nbs, sp = geom
    (u_ref, halo_ref, nw_ref, wbc_ref, cbc_ref, bbc_ref, e3_ref), refs = refs[:7], refs[7:]
    nw, cbc, bbc = nw_ref[...].astype(F32), cbc_ref[...].astype(F32), bbc_ref[...].astype(F32)
    if fetch_x:
        (ax, asm, az, ao), (y_ref, c_ref, ac_ref, send_ref), (gx, gs, gz, go), refs = refs[:4], refs[4:8], refs[8:12], refs[12:]
    else:
        (ax, gx, gs, az, ao), (y_ref, c_ref, ac_ref, send_ref), (gz, go), refs = refs[:5], refs[5:9], refs[9:11], refs[11:]
    (wf, wb, wsem, sm, wdt, cst, st, hcar, xcar, qcar, aoff, ubuf, h_s, la1_s, la2_s, lb1_s, lb2_s, cc_s, cbd_s, row_s, aw_s,
     send, recv), sems = refs[:23], refs[23:]
    p, i = pl.program_id(0), pl.program_id(1)
    np_, ni = pl.num_programs(0), pl.num_programs(1)
    step = p * ni + i
    d_model = u_ref.shape[-1]
    by_z = sp < n_tp
    zs = source(p + p // 2 * (1 - 2 * (p % 2))) if by_z else 0

    zg = Gather(piece_rows(az, layer), gz, send, recv, 0)
    og = Gather(piece_cols(ao, layer), go, send, recv, SEMS)
    acts = zg.plan(plans[0]) + og.plan(plans[1])
    if fetch_x:
        xg = Gather(piece_rows(ax, layer), gx, send, recv, 2 * SEMS, False)
        small = Small(asm, gs, *sems)
        acts += xg.plan(plans[2])

    def load_w(slot, zsrc):
        return pltpu.make_async_copy(gx.at[:, pl.ds(2 * zsrc, sp)], wf.at[slot], wsem.at[slot])

    def load_own():
        _, tp, _, c = here()
        return ([pltpu.make_async_copy(piece_rows(ax, layer)(q), wf.at[0, q, c], wsem.at[0]) for q in range(n_dp)]
                + [pltpu.make_async_copy(gx.at[q, tp + 1 - 2 * c], wf.at[0, q, 1 - c], wsem.at[0]) for q in range(n_dp)])

    @pl.when(step == 0)
    def _():
        entry_barrier((small.peers() + [(s, here()[1]) for s in zg.side]) if fetch_x else zg.peers())
        if fetch_x:
            small.start()
    at_steps(step, acts)

    @pl.when(step == 0)
    def _():
        if fetch_x:
            small.finish()
            xg.settle_own()
        if by_z:
            for v in load_own():
                v.start()
        else:
            load_w(0, 0).start()
        cp = pltpu.make_async_copy(gs.at[:, pl.ds(layer * SMALL, SMALL)], sm, wsem.at[2])
        cp.start()
        cp.wait()
        kc = d_model // PC
        hp = heads // n_tp
        for t in range(n_tp):
            for k in range(hp):
                r = head_row(hp * t + k, heads)
                for c in range(kc):
                    wdt[r:r + 1, c * PC:(c + 1) * PC] = sm[t, 16 + kc * k + c:17 + kc * k + c, :].astype(BF16)
                cst[r:r + 1, :] = sm[t, 8 + k:9 + k, :]
                cst[heads + r:heads + r + 1, :] = sm[t, 12 + k:13 + k, :]
        aoff[...] = jnp.zeros_like(aoff)
        hh = rms(halo_ref[...], nw)
        hcar[...] = hh
        qcar[...] = roll8(round_bf16(dot(hh, wbc_ref[...])))

    first = lax.broadcasted_iota(jnp.int32, (CAR, PC), 0) % 8 == 0

    def conv(cur, prev, taps, bias):
        a, now = conv_block(cur[:SUB], prev, taps, bias, first)
        b, now = conv_block(cur[SUB:], now, taps, bias, first)
        return silu(rows_cat(a, b)), now

    ri = lax.broadcasted_iota(jnp.int32, (BLK, BLK), 0)
    ci = lax.broadcasted_iota(jnp.int32, (BLK, BLK), 1)

    def prologue(b, h):
        j = i * nbs + b
        blk = pl.ds(pl.multiple_of(j * BLK, BLK), BLK)
        h_s[blk, :] = h
        rT = round_bf16(dott(wdt[...], h))
        bc, qcar[...] = conv(round_bf16(dot(h, wbc_ref[...])), qcar[...],
                             [cbc[k:k + 1] for k in range(4)], bbc)
        bmat, cmat = bc[:, :NST], bc[:, NST:]
        here_rows = slice(b * BLK, (b + 1) * BLK)
        c_ref[here_rows, :] = cmat
        pre = rT + cst[:heads, :BLK]
        dtT = jnp.maximum(pre, 0.0) + jnp.log1p(jnp.exp(-jnp.abs(pre)))
        aT = dtT * cst[heads:, :BLK]
        tr, tc = ri // SUB * SUB + time_of(ri % SUB), ci // SUB * SUB + time_of(ci % SUB)
        acT = dot(aT, jnp.where(tr <= tc, 1.0, 0.0), HI)
        mid, alast = acT[:, SUB - 1:SUB], acT[:, BLK - 1:BLK]
        low = ci[:heads] < SUB
        wT = dtT * jnp.exp2(jnp.where(low, mid, alast) - acT)
        pad = jnp.zeros((BLK - 3 * heads, BLK), BF16)
        aw_s[blk, :] = lanes_cat(rows_cat(*split3(acT), pad).T, rows_cat(*split3(wT), pad).T)
        ac_ref[:, here_rows] = acT + aoff[:, :1]
        aoff[...] = aoff[...] + alast

        def pair_rows(v):
            ev, od = v[:heads // 2], v[heads // 2:]
            l = low[:heads // 2]
            return jnp.where(l, ev, pltpu.roll(od, SUB, 1)), jnp.where(l, pltpu.roll(ev, SUB, 1), od)

        for half, (a, d) in enumerate(zip(pair_rows(acT), pair_rows(dtT))):
            row_s[2 * j + half] = rows_cat(*[v[4 * z:4 * z + 4] for z in range(heads // 8) for v in (a, d)])
        cb = dott(cmat, bmat, HI)
        lowr, tri = ci[:SUB] < SUB, time_of(ri[:SUB]) >= time_of(ci[:SUB] % SUB)
        ca, cd = cb[:SUB], cb[SUB:]
        cbd_s[blk, :] = rows_cat(jnp.where(tri, jnp.where(lowr, ca, pltpu.roll(ca, SUB, 1)), 0.0),
                                 jnp.where(tri, jnp.where(lowr, pltpu.roll(cd, SUB, 1), cd), 0.0))
        bT = bmat.T
        big = pl.ds(pl.multiple_of(j * (NST + SUB), SUB), NST + SUB)
        la1_s[big, :], la2_s[big, :] = kcat6(split3(rows_cat(bT[:, :SUB], cd[:, :SUB])))
        lb1_s[blk, :], lb2_s[blk, :] = kcat6(split3(pltpu.roll(bT, SUB, 1)[:, :SUB]))
        c1, c2, c3 = split3(cmat)
        cc_s[blk, :] = lanes_cat(c1, c2, c1, c3)

    def all_prologues():
        u = u_ref[...].astype(F32)
        h = rms(u if mixed else unmix(u, ubuf), nw)
        for b in range(nbs):
            prologue(b, h[b * BLK:(b + 1) * BLK])

    if by_z:
        pl.when(p == 0)(all_prologues)

    @pl.when(i == 0)
    def _():
        slot = p % 2 if by_z else 0

        @pl.when(p == 0)
        def _():
            for v in load_own() if by_z else [load_w(0, 0)]:
                v.wait()

        @pl.when(p > 0)
        def _():
            load_w(slot, zs).wait()
        for q in range(n_dp):
            for k in range(sp):
                wb[q * PC:(q + 1) * PC, k * PC:(k + 1) * PC] = wf[slot, q, k].astype(BF16)
        xcar[...] = roll8(round_bf16(dot(hcar[...], wb[...])))
        st[...] = jnp.zeros_like(st)

    @pl.when((i == ni - 1) & (p < np_ - 1))
    def _():
        nd = p + 1
        nd = nd + nd // 2 * (1 - 2 * (nd % 2))
        if fetch_x:
            for d in (1, 2, 3):
                pl.when(nd == d)(functools.partial(xg.settle, d))
        load_w((p + 1) % 2, source(nd)).start()

    if not by_z:
        all_prologues()
    lane = lax.broadcasted_iota(jnp.int32, (SUB, LANES), 1)
    lo = jnp.where(lane < HD, 1.0, 0.0).astype(BF16)
    hi = jnp.where(lane < HD, 0.0, 1.0).astype(BF16)
    x0 = [dot(h_s[pl.ds(pl.multiple_of(i * nbs * BLK, BLK), nbs * BLK), :], wb[:, k * PC:(k + 1) * PC]) for k in range(sp)]

    def place(b):
        j = i * nbs + b
        return j, pl.ds(pl.multiple_of(j * BLK, BLK), BLK), pl.ds(pl.multiple_of(j * (NST + SUB), SUB), NST + SUB)

    def lanes_of(k):
        return slice(k * PC, (k + 1) * PC), pl.ds(pl.multiple_of((2 * zs + k) * PC, PC), PC)

    def pre(b, k):
        (_, blk, _), (sl, gl) = place(b), lanes_of(k)
        s1, s2, s3 = split3(st[:, sl])
        c12, c13 = cc_s[blk, :2 * NST], cc_s[blk, 2 * NST:]
        inter = dot(c12, rows_cat(s1, s1)) + dot(c12, rows_cat(s2, s2)) + dot(c13, rows_cat(s3, s1))
        n3 = e3_ref.shape[0]
        acx = dot(aw_s[blk, :n3], e3_ref[:, gl])
        wx = dot(aw_s[blk, BLK:BLK + n3], e3_ref[:, gl])
        return x0[k][b * BLK:(b + 1) * BLK], acx, wx, inter

    def mid_(b, k, x0, acx, wx, inter):
        (j, blk, _), (sl, _) = place(b), lanes_of(k)
        t = 2 * zs + k
        x, xcar[:, sl] = conv(round_bf16(x0), xcar[:, sl], [sm[t, r:r + 1, :] for r in range(4)], sm[t, 4:5, :])
        xw = split3(x * wx)
        r = kcat6r([v[:SUB] for v in xw]) + kcat6r([v[SUB:] for v in xw])
        ms, xs = [], []
        for half in range(2):
            rows = slice(half * SUB, (half + 1) * SUB)
            row = row_s[2 * j + half, pl.ds(pl.multiple_of(8 * (zs + k // 2), 8), 8), :]
            cbd = cbd_s[pl.ds(pl.multiple_of(j * BLK + half * SUB, SUB), SUB), :]
            m = []
            for g in range(2):
                seg = acx[rows, g * LANES:(g + 1) * LANES] - row[2 * (k % 2) + g:2 * (k % 2) + g + 1]
                m.append(jnp.exp2(jnp.minimum(seg, 0.0)) * cbd * row[4 + 2 * (k % 2) + g:5 + 2 * (k % 2) + g])
            ms.append(split3(lanes_cat(*m)))
            xs.append([block_diag(v, lo, hi) for v in split3(x[rows])])
        return x, acx, inter, r, ms, xs

    def fin(b, k, x, acx, inter, r, ms, xs):
        (j, blk, big), (sl, _) = place(b), lanes_of(k)
        ra = dot(la1_s[big, :], r[0]) + dot(la2_s[big, :], r[1])
        rb = dot(lb1_s[blk, :], r[2]) + dot(lb2_s[blk, :], r[3])
        am, al = acx[SUB - 1:SUB], acx[BLK - 1:BLK]
        st[:, sl] = st[:, sl] * jnp.exp2(al) + ra[:NST] * jnp.exp2(al - am) + rb
        skip = sm[2 * zs + k, 6:7, :]
        for half in range(2):
            rows = slice(half * SUB, (half + 1) * SUB)
            (m1, m2, m3), (x1, x2, x3) = ms[half], xs[half]
            r1 = dot(rows_cat(m1, m2, m3), x1)
            r2 = dot(rows_cat(m1, m2), x2)
            y = r1[:SUB] + r1[SUB:2 * SUB] + r1[2 * SUB:] + r2[:SUB] + r2[SUB:] + dot(m1, x3)
            y = y + inter[rows] * jnp.exp2(acx[rows])
            if half:
                y = y + ra[NST:] * jnp.exp2(acx[rows] - am)
            y_ref[b * BLK + half * SUB:b * BLK + (half + 1) * SUB, sl] = y + skip * x[rows]

    units = [(b, k) for b in range(nbs) for k in range(sp)]
    m = mid_(*units[0], *pre(*units[0]))
    for a, nxt in zip(units, units[1:] + [None]):
        if nxt:
            v = pre(*nxt)
        fin(*a, *m)
        if nxt:
            m = mid_(*nxt, *v)

    @pl.when(i == ni - 1)
    def _():
        send_ref[...] = st[...]

    @pl.when(step == np_ * ni - 1)
    def _():
        zg.finish()
        og.finish()
        if fetch_x:
            xg.drain()


def p1(u, base, halo, nw, wbc, cbc, bbc, e3, comm, n, n_dp, n_tp, mixed, layer, fetch_x, plans, cid):
    d_model, heads = u.shape[-1], PC // HD * n_tp
    sp, nbs = (2, NBS) if fetch_x else (n_tp, 1)
    width, nb, rows = PC * n_tp, n // BLK, BLK * nbs
    ni = nb // nbs
    fixed = lambda shp: pl.BlockSpec(shp, lambda p, i: (0,) * len(shp), pipeline_mode=pl.Buffered(1))
    own_layer = lambda *shp: pl.BlockSpec((None,) + shp, lambda p, i: (layer, 0, 0), pipeline_mode=pl.Buffered(1))
    once = lambda p, i: jnp.where(p == 0, i, ni - 1)
    col = (lambda p: source(p + p // 2 * (1 - 2 * (p % 2)))) if fetch_x else (lambda p: 0)
    hbm = pl.BlockSpec(memory_space=pl.ANY)
    gathered = lambda r: jax.ShapeDtypeStruct((n_dp, n_tp, r, PC), F32)
    outs = [jax.ShapeDtypeStruct((n, width), F32), jax.ShapeDtypeStruct((n, NST), F32),
            jax.ShapeDtypeStruct((heads, n), F32), jax.ShapeDtypeStruct((NST, width), F32)]
    more = ([gathered(PC), jax.ShapeDtypeStruct((n_tp,) + comm[1].shape, F32)] if fetch_x else []) + [gathered(PC)] * 2
    vm = pltpu.VMEM
    dma = lambda k: [pltpu.SemaphoreType.DMA((k,))] * 2
    return pl.pallas_call(
        functools.partial(p1_body, geom=(n_dp, n_tp, heads, nb, nbs, sp), mixed=mixed, layer=layer, fetch_x=fetch_x, plans=plans),
        name="p1", grid=(n_tp // sp, ni),
        in_specs=[pl.BlockSpec((rows, d_model), lambda p, i: (base() + once(p, i), 0)),
                  fixed((CAR, d_model)), own_layer(1, d_model), own_layer(d_model, PC), own_layer(4, PC), own_layer(1, PC),
                  fixed((3 * heads, width))] + [hbm] * len(comm),
        out_specs=[pl.BlockSpec((rows, sp * PC), lambda p, i: (i, col(p))),
                   pl.BlockSpec((rows, NST), lambda p, i: (once(p, i), 0)),
                   pl.BlockSpec((heads, rows), lambda p, i: (0, once(p, i))),
                   pl.BlockSpec((NST, sp * PC), lambda p, i: (0, col(p)))] + [hbm] * len(more),
        out_shape=outs + more,
        scratch_shapes=[
            vm((2 if fetch_x else 1, n_dp, sp, PC, PC), F32), vm((d_model, sp * PC), BF16), pltpu.SemaphoreType.DMA((3,)),
            vm((n_tp, SMALL, PC), F32), vm((heads, d_model), BF16), vm((2 * heads, PC), F32), vm((NST, sp * PC), F32),
            vm((CAR, d_model), BF16), vm((CAR, sp * PC), F32), vm((CAR, PC), F32), vm((heads, LANES), F32),
            vm((d_model // LANES * rows, LANES), F32), vm((n, d_model), BF16),
            vm((nb * (NST + SUB), 4 * SUB), BF16), vm((nb * (NST + SUB), 2 * SUB), BF16),
            vm((n, 4 * SUB), BF16), vm((n, 2 * SUB), BF16), vm((n, 4 * NST), BF16), vm((n, LANES), F32),
            vm((2 * nb, 2 * heads // 2, LANES), F32), vm((n, 2 * BLK), BF16)]
        + dma(3 * SEMS) + (dma(8) if fetch_x else []),
        compiler_params=pltpu.CompilerParams(dimension_semantics=("arbitrary", "arbitrary"), vmem_limit_bytes=VMEM_CAP,
                                             collective_id=cid, has_side_effects=True),
        cost_estimate=pl.CostEstimate(flops=n * 70 * 10 ** 6, bytes_accessed=n * 12000, transcendentals=0),
    )(u, halo, nw, wbc, cbc, bbc, e3, *comm)


def p2_body(*refs, geom, mix_in, layer, fetch_x, plans):
    n_dp, n_tp, heads = geom
    (u_ref, nw_ref, wz_ref, wo_ref, sm_ref, y_ref, c_ref, ac_ref, s_ref, e3_ref), refs = refs[:10], refs[10:]
    if fetch_x:
        (ax, o_ref, f_ref, gx), refs = refs[:4], refs[4:]
    else:
        (o_ref, r_ref), refs = refs[:2], refs[2:]
    (wzb, wob, s3, ubuf, send, recv), refs = refs[:6], refs[6:]
    i = pl.program_id(0)
    width = PC * n_tp
    if fetch_x:
        xg = Gather(piece_rows(ax, layer + 1), gx, send, recv, 0)

        @pl.when(i == 0)
        def _():
            entry_barrier(xg.peers())
        at_steps(i, xg.plan(plans))
    else:
        fbuf, = refs
        dp, tp, z, c = here()

        def swap(k):
            return pltpu.make_async_remote_copy(
                src_ref=fbuf.at[k % 2], dst_ref=r_ref.at[pl.ds(pl.multiple_of(k * BLK2, BLK2), BLK2)],
                send_sem=send.at[k % 2], recv_sem=recv.at[0], device_id=(dp, 2 * z + 1 - c), device_id_type=MESH)

        @pl.when(i == 0)
        def _():
            entry_barrier([(dp, 2 * z + 1 - c)])

        @pl.when(i > 1)
        def _():
            swap(i - 2).wait_send()

        @pl.when(i > 0)
        def _():
            swap(i - 1).start()

    @pl.when(i == 0)
    def _():
        for d in range(n_dp):
            for t in range(n_tp):
                a, b = slice(d * PC, (d + 1) * PC), slice(t * PC, (t + 1) * PC)
                wzb[a, b] = wz_ref[d, t].astype(BF16)
                wob[b, a] = wo_ref[d, t].astype(BF16)
        a, b, c_ = split3(s_ref[...])
        for k, (v, w) in enumerate(((a, a), (b, b), (c_, a))):
            s3[k] = rows_cat(v, w)

    u = u_ref[...].astype(F32)
    u = u if mix_in else unmix(u, ubuf)
    h = rms(u, nw_ref[...].astype(F32))
    c1, c2, c3 = split3(c_ref[...])
    c12, c13 = lanes_cat(c1, c2), lanes_cat(c1, c3)
    eT = rows_cat(*split3(jnp.exp2(ac_ref[...]))).T
    vs, ss = [], 0.0
    for t in range(n_tp):
        sl = slice(t * PC, (t + 1) * PC)
        z_ = round_bf16(dot(h, wzb[:, sl]))
        cor = dot(c12, s3[0, :, sl]) + dot(c12, s3[1, :, sl]) + dot(c13, s3[2, :, sl])
        v = (y_ref[:, sl] + cor * dot(eT, e3_ref[:, sl])) * silu(z_)
        ss = ss + jnp.sum(v * v, axis=-1, keepdims=True)
        vs.append(v)
    sc = lax.rsqrt(ss / width + EPS)
    g = lanes_cat(*[(v * sc * sm_ref[t, 5:6, :]).astype(BF16) for t, v in enumerate(vs)])
    un = round_bf16(u + dot(g, wob[...]))
    if fetch_x:
        o_ref[...] = un.astype(BF16)
        f_ref[...] = un[BLK2 - CAR:]
    else:
        un = unmix(un, ubuf)
        fbuf[i % 2] = un
        o_ref[...] = un.astype(BF16)

    @pl.when(i == pl.num_programs(0) - 1)
    def _():
        if fetch_x:
            xg.finish()
        else:
            swap(i).start()
            for k in range(2):
                swap(i - 1 + k).wait_send()
            whole = pltpu.make_async_copy(r_ref, r_ref, recv.at[0])
            whole.wait()


def p2(u, base, nw, wz, wo, sm, y, c, ac, s, e3, comm, n, n_dp, n_tp, mix_in, layer, fetch_x, plans, cid):
    d_model, heads = u.shape[-1], PC // HD * n_tp
    width = PC * n_tp
    fixed = lambda shp: pl.BlockSpec(shp, lambda i: (0,) * len(shp), pipeline_mode=pl.Buffered(1))
    hbm = pl.BlockSpec(memory_space=pl.ANY)
    rows = lambda w: pl.BlockSpec((BLK2, w), lambda i: (i, 0))
    shape = lambda *s: jax.ShapeDtypeStruct(s, F32)
    vm = pltpu.VMEM
    outs = [jax.ShapeDtypeStruct((n, d_model), BF16)]
    specs = [rows(d_model)]
    if fetch_x:
        outs += [shape(CAR, d_model), shape(n_dp, n_tp, PC, PC)]
        specs += [pl.BlockSpec((CAR, d_model), lambda i: (0, 0)), hbm]
    else:
        outs += [shape(n, d_model)]
        specs += [hbm]
    return pl.pallas_call(
        functools.partial(p2_body, geom=(n_dp, n_tp, heads), mix_in=mix_in, layer=layer, fetch_x=fetch_x, plans=plans),
        name="p2", grid=(n // BLK2,),
        in_specs=[pl.BlockSpec((BLK2, d_model), lambda i: (base() + i, 0)),
                  pl.BlockSpec((None, 1, d_model), lambda i: (layer, 0, 0)),
                  fixed((n_dp, n_tp, PC, PC)), fixed((n_dp, n_tp, PC, PC)),
                  pl.BlockSpec((n_tp, SMALL, PC), lambda i: (0, layer, 0), pipeline_mode=pl.Buffered(1)),
                  rows(width), rows(NST), pl.BlockSpec((heads, BLK2), lambda i: (0, i)),
                  fixed((NST, width)), fixed((3 * heads, width))] + [hbm] * len(comm),
        out_specs=specs, out_shape=outs,
        scratch_shapes=[vm((d_model, width), BF16), vm((width, d_model), BF16), vm((3, 2 * NST, width), BF16),
                        vm((d_model // LANES * BLK2, LANES), F32)]
        + [pltpu.SemaphoreType.DMA((SEMS,))] * 2 + ([] if fetch_x else [vm((2, BLK2, d_model), F32)]),
        compiler_params=pltpu.CompilerParams(dimension_semantics=("arbitrary",), vmem_limit_bytes=VMEM_CAP,
                                             collective_id=cid, has_side_effects=True),
        cost_estimate=pl.CostEstimate(flops=n * 30 * 10 ** 6, bytes_accessed=n * 12000, transcendentals=0),
    )(u, nw, wz, wo, sm, y, c, ac, s, e3, *comm)


def finish_body(own_ref, other_ref, o_ref):
    mine = pl.program_id(0) == here()[3]

    @pl.when(mine)
    def _():
        o_ref[...] = own_ref[...]

    @pl.when(jnp.logical_not(mine))
    def _():
        o_ref[...] = other_ref[...].astype(BF16)


def finish(own, other):
    n, d_model = own.shape
    rows = n // 3
    ni = n // rows
    pick = lambda w: (lambda j, i: (jnp.where((j == here()[3]) == w, i, ni - 1), 0))
    return pl.pallas_call(
        finish_body, name="finish", grid=(2, ni),
        in_specs=[pl.BlockSpec((rows, d_model), pick(True)), pl.BlockSpec((rows, d_model), pick(False))],
        out_specs=pl.BlockSpec((rows, d_model), lambda j, i: (j * ni + i, 0)),
        out_shape=jax.ShapeDtypeStruct((2 * n, d_model), BF16),
        compiler_params=pltpu.CompilerParams(dimension_semantics=("arbitrary", "arbitrary")),
        cost_estimate=pl.CostEstimate(flops=n * d_model, bytes_accessed=n * d_model * 8, transcendentals=0),
    )(own, other)


def small_rows(conv, bias, gate, skip, dtb, al, wdt):
    f = lambda v: v.astype(F32)
    n, hp = skip.shape
    wide = lambda v: jnp.broadcast_to(v[:, :, None], (n, hp, PC))
    one = lambda v: v.reshape(n, 1, PC)
    skip = jnp.broadcast_to(skip[:, :, None], (n, hp, HD))
    v = [f(conv), one(f(bias)), one(f(gate)), one(skip), jnp.zeros((n, 1, PC), F32), wide(dtb), wide(-jnp.exp(al) * LOG2E),
         f(wdt).transpose(0, 2, 1).reshape(n, -1, PC)]
    return jnp.concatenate(v, axis=1).reshape(-1, PC)


PLAN_X = "00020405030607040809"
PLAN_Z0 = "04090a0c0b0c0e0d0e10"
PLAN_O0 = "090d0f110f1113111315"
PLAN_Z1 = "0002040604060906080b"
PLAN_O1 = "06090b0e0b0e100d1013"
PLAN_X1 = "0003050705070907090a"


def solution(mesh):
    n_tp, n_dp = mesh.shape['tp'], mesh.shape['dp']
    rep, col, vec = P(), P(None, None, 'tp'), P(None, 'tp')
    in_specs = (P('dp'), rep, col, col, rep, col, col, rep, vec, rep, vec, vec, vec, vec, P(None, 'tp', None))

    def device_forward(hidden, norm_w, w_z, w_x, w_bc, w_dt, conv_x, conv_bc, bias_x, bias_bc, dt_bias, a_log, d_skip, gate_w, w_out):
        u = hidden[0]
        steps, d_model = u.shape
        n = steps // 2
        core = lax.axis_index('tp') % 2
        e3 = expand_mat(dt_bias.shape[1] * n_tp)
        up = [(2 * k, 2 * k + 1) for k in range(n_tp // 2)]
        ax, az, ao = w_x.astype(F32), w_z.astype(F32), w_out.astype(F32)
        small = small_rows(conv_x, bias_x, gate_w, d_skip, dt_bias, a_log, w_dt)
        tail = u[n - SUB:n].astype(F32).reshape(8, 8, d_model).transpose(1, 0, 2).reshape(SUB, d_model)[SUB - CAR:]
        halo = jnp.where(core == 1, tail, 0.0)
        half = lambda blk: (lambda: lax.axis_index('tp') % 2 * (n // blk))
        none = lambda: 0
        row = lambda v: v.reshape(v.shape[0], 1, v.shape[1])
        common = (n, n_dp, n_tp)
        nw = row(norm_w)
        bc = (nw, w_bc, conv_bc, row(bias_bc), e3)

        y, c, ac, s, gx, gs, gz, go = p1(u, half(BLK * NBS), halo, *bc, (ax, small, az, ao), *common, False, 0, True,
                                         (PLAN_Z0, PLAN_O0, PLAN_X), 1)
        s = lax.ppermute(s, 'tp', up)
        u, f, gx = p2(u, half(BLK2), nw, gz, go, gs, y, c, ac, s, e3, (ax,), *common, False, 0, True, PLAN_X1, 2)
        halo = lax.ppermute(f, 'tp', up)
        y, c, ac, s, gz, go = p1(u, none, halo, *bc, (ax, gx, gs, az, ao), *common, True, 1, False, (PLAN_Z1, PLAN_O1), 3)
        s = lax.ppermute(s, 'tp', up)
        own, other = p2(u, none, nw, gz, go, gs, y, c, ac, s, e3, (), *common, True, 1, False, None, 4)
        return finish(own, other)[None]

    return jax.shard_map(device_forward, mesh=mesh, in_specs=in_specs, out_specs=P('dp'), check_vma=False)
```

```python
import functools
import jax
import jax.numpy as jnp
import numpy as np
from jax import lax
from jax.experimental import pallas as pl
from jax.experimental.pallas import tpu as pltpu
from jax.sharding import PartitionSpec as P

EPS = 1e-5
LOG2E = 1.4426950408889634
HI = lax.Precision.HIGHEST
F32 = jnp.float32
BF16 = jnp.bfloat16
MESH = pl.DeviceIdType.MESH
LANES = 128
BLK = 128
SUB = 64
BLK2 = 256
NBS = 4
PC = 256
HD = 64
NST = 128
CAR = 24
SMALL = 32
ORDER = (1, 3, 2)
EARLY = 6
SEMS = 26
VMEM_CAP = 60 << 20


def silu(v):
    return v / (1.0 + jnp.exp2(v * -LOG2E))


def split3(v):
    a = v.astype(BF16)
    r = v - a.astype(F32)
    b = r.astype(BF16)
    return a, b, (r - b.astype(F32)).astype(BF16)


def round_bf16(v):
    return v.astype(BF16).astype(F32)


def rms(u, nw):
    return (u * lax.rsqrt(jnp.mean(u * u, axis=-1, keepdims=True) + EPS) * nw).astype(BF16)


def dot(a, b, prec=None):
    return jnp.dot(a, b, preferred_element_type=F32, precision=prec)


def dott(a, b, prec=None):
    return lax.dot_general(a, b, (((1,), (1,)), ((), ())), preferred_element_type=F32, precision=prec)


def rows_cat(*v):
    return jnp.concatenate(v, axis=0)


def lanes_cat(*v):
    return jnp.concatenate(v, axis=1)


def time_of(r):
    return 8 * (r % 8) + r // 8


def roll8(v):
    c = v.shape[-1]
    return pltpu.roll(v.reshape(CAR // 8, 8, c), 1, 1).reshape(CAR, c)


def conv_block(cur, prev, taps, bias, first):
    now = roll8(cur[SUB - CAR:])
    sh = jnp.where(first, prev, now)
    out = bias + cur * taps[-1]
    for k in range(1, 4):
        out = out + rows_cat(sh[CAR - 8 * k:], cur[:SUB - 8 * k]) * taps[3 - k]
    return out, now


def unmix(v, buf):
    n, c = v.shape
    for j in range(c // LANES):
        buf[n * j:n * (j + 1), :] = v[:, LANES * j:LANES * (j + 1)]
    cols = [rows_cat(*[buf[pl.ds(n * j + b + k, 8, stride=8), :] for b in range(0, n, SUB) for k in range(8)])
            for j in range(c // LANES)]
    return lanes_cat(*cols)


def head_row(h, heads):
    return (h % 2) * (heads // 2) + h // 2


def expand_mat(heads):
    order = sorted(range(heads), key=lambda h: head_row(h, heads))
    one = np.repeat(np.eye(heads)[order], HD, axis=1)
    return jnp.asarray(np.tile(one, (3, 1)), BF16)


def kcat6(parts):
    a, b, c = parts
    return lanes_cat(a, b, c, a), lanes_cat(b, a)


def kcat6r(parts):
    a, b, c = parts
    return rows_cat(a, a, a, b), rows_cat(b, c)


def block_diag(x, lo, hi):
    z = jnp.zeros((x.shape[0], LANES), BF16)
    l, r = x[:, :LANES], x[:, LANES:]
    return rows_cat(lanes_cat(l * lo, z), lanes_cat(l * hi, z), lanes_cat(z, r * lo), lanes_cat(z, r * hi))


def here():
    dp, tp = lax.axis_index('dp'), lax.axis_index('tp')
    return dp, tp, tp // 2, tp % 2


def source(dz):
    return (here()[2] + 4 - dz) % 4


class Gather:
    def __init__(self, piece, g, send, recv, base, keep=True):
        self.piece, self.g, self.send, self.recv, self.base = piece, g, send, recv, base
        self.dp, self.tp, self.z, self.c = here()
        x, y = self.dp // 2, self.dp % 2
        self.side = ((1 - x) * 2 + y, x * 2 + 1 - y)
        self.partner = (self.dp, 2 * self.z + 1 - self.c)
        self.quarters, self.keep = g.shape[0], keep

    def rdma(self, k, src, dst, dev):
        return pltpu.make_async_remote_copy(src_ref=src, dst_ref=dst, send_sem=self.send.at[self.base + k],
                                            recv_sem=self.recv.at[self.base + k], device_id=dev, device_id_type=MESH)

    def local(self, q):
        return pltpu.make_async_copy(self.piece(q), self.g.at[q, self.tp], self.send.at[self.base + q])

    def own(self, q):
        return self.rdma(4 + q, self.piece(q), self.g.at[q, self.tp], self.partner)

    def line(self, dz):
        return self.rdma(7 + dz, self.piece(self.dp), self.g.at[self.dp, self.tp],
                         (self.dp, 2 * ((self.z + dz) % 4) + self.c))

    def cross(self, dz, n):
        ref = self.g.at[self.dp, 2 * source(dz) + self.c]
        return self.rdma(9 + 2 * dz + n, ref, ref, (self.side[n], self.tp))

    def relay(self, dz, n):
        half = self.g.shape[2] // 2
        ref = self.g.at[self.side[n], 2 * source(dz) + self.c, pl.ds(n * half, half)]
        return self.rdma(15 + 2 * dz + n, ref, ref, (self.side[1 - n], self.tp))

    def over(self, dz):
        ref = self.g.at[:, 2 * source(dz) + self.c]
        return self.rdma(22 + dz, ref, ref, self.partner)

    def peers(self):
        return ([(self.dp, 2 * ((self.z + dz) % 4) + self.c) for dz in ORDER]
                + [(p, self.tp) for p in self.side] + [self.partner])

    def start(self):
        for q in range(self.quarters):
            self.own(q).start()
        for dz in ORDER:
            self.line(dz).start()
        if self.keep:
            for q in range(self.quarters):
                self.local(q).start()

    def spread(self, dz):
        self.line(dz).wait_recv()
        for n in range(2):
            self.cross(dz, n).start()

    def pass_on(self, dz):
        for n in range(2):
            self.cross(dz, n).wait_recv()
            self.relay(dz, n).start()

    def hand(self, dz):
        for n in range(2):
            self.relay(dz, n).wait_recv()
        self.over(dz).start()

    def settle_own(self):
        for q in range(self.quarters):
            self.own(q).wait_recv()
            if self.keep:
                self.local(q).wait()

    def settle(self, dz):
        self.over(dz).wait_recv()

    def drain(self):
        for q in range(self.quarters):
            self.own(q).wait_send()
        for dz in ORDER:
            self.line(dz).wait_send()
            self.over(dz).wait_send()
            for n in range(2):
                self.cross(dz, n).wait_send()
                self.relay(dz, n).wait_send()

    def plan(self, s):
        s = bytes.fromhex(s)
        acts = [(s[0], self.start)]
        for k, f in enumerate((self.spread, self.pass_on, self.hand)):
            acts += [(s[1 + 3 * k + j], functools.partial(f, dz)) for j, dz in enumerate(ORDER)]
        return acts

    def finish(self):
        self.settle_own()
        for dz in ORDER:
            self.settle(dz)
        self.drain()


class Small:
    def __init__(self, a, g, send, recv):
        self.a, self.g, self.send, self.recv = a, g, send, recv
        self.dp, self.tp, _, _ = here()

    def copy(self, k):
        return pltpu.make_async_remote_copy(src_ref=self.a, dst_ref=self.g.at[self.tp], send_sem=self.send.at[k],
                                            recv_sem=self.recv.at[k], device_id=(self.dp, (self.tp + k) % 8),
                                            device_id_type=MESH)

    def local(self):
        return pltpu.make_async_copy(self.a, self.g.at[self.tp], self.send.at[0])

    def peers(self):
        return [(self.dp, (self.tp + k) % 8) for k in range(1, 8)]

    def start(self):
        self.local().start()
        for k in range(1, 8):
            self.copy(k).start()

    def finish(self):
        self.local().wait()
        for k in range(1, 8):
            self.copy(k).wait()


def entry_barrier(peers):
    sem = pltpu.get_barrier_semaphore()
    for p in peers:
        pl.semaphore_signal(sem, inc=1, device_id=p, device_id_type=MESH)
    pl.semaphore_wait(sem, len(peers))


def at_steps(step, acts):
    for k in sorted({k for k, _ in acts}):
        @pl.when(step == k)
        def _():
            for j, f in acts:
                if j == k:
                    f()


def piece_rows(ref, layer):
    return lambda q: ref.at[layer, pl.ds(q * PC, PC)]


def piece_cols(ref, layer):
    return lambda q: ref.at[layer, :, pl.ds(pl.multiple_of(q * PC, PC) if not isinstance(q, int) else q * PC, PC)]


def p1_body(*refs, geom, mixed, layer, fetch_x, plans):
    n_dp, n_tp, heads, nb, nbs, sp = geom
    (u_ref, halo_ref, nw_ref, wbc_ref, cbc_ref, bbc_ref, e3_ref), refs = refs[:7], refs[7:]
    row = slice(layer, layer + 1)
    nw, cbc, bbc = nw_ref[row].astype(F32), cbc_ref[...].astype(F32), bbc_ref[row].astype(F32)
    if fetch_x:
        (ax, asm, az, ao), (y_ref, c_ref, ac_ref, s_in), (gx, gs, gz, go), refs = refs[:4], refs[4:8], refs[8:12], refs[12:]
    else:
        (ax, gx, gs, az, ao), (y_ref, c_ref, ac_ref, s_in), (gz, go), refs = refs[:5], refs[5:9], refs[9:11], refs[11:]
    (wf, wb, wsem, sm, wdt, cst, st, hcar, xcar, qcar, aoff, ubuf, h_s, la1_s, la2_s, lb1_s, lb2_s, cc_s, cbd_s, row_s, aw_s,
     sbuf, hsem, send, recv), sems = refs[:25], refs[25:]
    p, i = pl.program_id(0), pl.program_id(1)
    np_, ni = pl.num_programs(0), pl.num_programs(1)
    step = p * ni + i
    d_model = u_ref.shape[-1]
    by_z = sp < n_tp
    zs_of = (lambda p: source(p + p // 2 * (1 - 2 * (p % 2)))) if by_z else (lambda p: 0)
    zs = zs_of(p)
    upper = here()[3] == 1

    def state_out(p):
        dp, tp, _, c = here()
        cols = pl.ds(pl.multiple_of(2 * zs_of(p) * PC, PC), sp * PC)
        return pltpu.make_async_remote_copy(src_ref=sbuf, dst_ref=s_in.at[:, cols], send_sem=hsem.at[0], recv_sem=hsem.at[1],
                                            device_id=(dp, tp + 1 - 2 * c), device_id_type=MESH)

    zg = Gather(piece_rows(az, layer), gz, send, recv, 0)
    og = Gather(piece_cols(ao, layer), go, send, recv, SEMS)
    acts = zg.plan(plans[0]) + og.plan(plans[1])
    if fetch_x:
        xg = Gather(piece_rows(ax, layer), gx, send, recv, 2 * SEMS, False)
        small = Small(asm, gs, *sems)
        acts += xg.plan(plans[2])

    def load_w(slot, zsrc):
        return pltpu.make_async_copy(gx.at[:, pl.ds(2 * zsrc, sp)], wf.at[slot], wsem.at[slot])

    def load_own():
        _, tp, _, c = here()
        return ([pltpu.make_async_copy(piece_rows(ax, layer)(q), wf.at[0, q, c], wsem.at[0]) for q in range(n_dp)]
                + [pltpu.make_async_copy(gx.at[q, tp + 1 - 2 * c], wf.at[0, q, 1 - c], wsem.at[0]) for q in range(n_dp)])

    @pl.when(step == 0)
    def _():
        entry_barrier((small.peers() + [(s, here()[1]) for s in zg.side]) if fetch_x else zg.peers())
        if fetch_x:
            small.start()
    at_steps(step, acts)

    @pl.when(step == 0)
    def _():
        if fetch_x:
            small.finish()
            xg.settle_own()
        if by_z:
            for v in load_own():
                v.start()
        else:
            load_w(0, 0).start()
        cp = pltpu.make_async_copy(gs.at[:, pl.ds(layer * SMALL, SMALL)], sm, wsem.at[2])
        cp.start()
        cp.wait()
        kc = d_model // PC
        hp = heads // n_tp
        for t in range(n_tp):
            for k in range(hp):
                r = head_row(hp * t + k, heads)
                for c in range(kc):
                    wdt[r:r + 1, c * PC:(c + 1) * PC] = sm[t, 16 + kc * k + c:17 + kc * k + c, :].astype(BF16)
                cst[r:r + 1, :] = sm[t, 8 + k:9 + k, :]
                cst[heads + r:heads + r + 1, :] = sm[t, 12 + k:13 + k, :]
        aoff[...] = jnp.zeros_like(aoff)
        hh = rms(halo_ref[...], nw)
        hcar[...] = hh
        qcar[...] = roll8(round_bf16(dot(hh, wbc_ref[...])))

    first = lax.broadcasted_iota(jnp.int32, (CAR, PC), 0) % 8 == 0

    def conv(cur, prev, taps, bias):
        a, now = conv_block(cur[:SUB], prev, taps, bias, first)
        b, now = conv_block(cur[SUB:], now, taps, bias, first)
        return silu(rows_cat(a, b)), now

    ri = lax.broadcasted_iota(jnp.int32, (BLK, BLK), 0)
    ci = lax.broadcasted_iota(jnp.int32, (BLK, BLK), 1)

    def prologue(h, b, hook):
        q0 = dot(h, wbc_ref[...])
        rT = round_bf16(dott(wdt[...], h))
        hook(h, 2)
        bc, qcar[...] = conv(round_bf16(q0), qcar[...],
                             [cbc[k:k + 1] for k in range(4)], bbc)
        bmat, cmat = bc[:, :NST], bc[:, NST:]
        here_rows = slice(b * BLK, (b + 1) * BLK)
        c_ref[here_rows, :] = cmat
        pre = rT + cst[:heads, :BLK]
        dtT = jnp.maximum(pre, 0.0) + jnp.log1p(jnp.exp(-jnp.abs(pre)))
        aT = dtT * cst[heads:, :BLK]
        tr, tc = ri // SUB * SUB + time_of(ri % SUB), ci // SUB * SUB + time_of(ci % SUB)
        acT = dot(aT, jnp.where(tr <= tc, 1.0, 0.0), HI)
        mid, alast = acT[:, SUB - 1:SUB], acT[:, BLK - 1:BLK]
        low = ci[:heads] < SUB
        wT = dtT * jnp.exp2(jnp.where(low, mid, alast) - acT)
        pad = jnp.zeros((BLK - 3 * heads, BLK), BF16)
        a3, w3 = rows_cat(*split3(acT), pad).T, rows_cat(*split3(wT), pad).T
        ac_ref[:, here_rows] = acT + aoff[:, :1]
        aoff[...] = aoff[...] + alast

        def pair_rows(v):
            ev, od = v[:heads // 2], v[heads // 2:]
            l = low[:heads // 2]
            return jnp.where(l, ev, pltpu.roll(od, SUB, 1)), jnp.where(l, pltpu.roll(ev, SUB, 1), od)

        rows = [rows_cat(*[w for zz in zip(*[jnp.split(v, n_tp // 2) for v in ad]) for w in zz])
                for ad in zip(pair_rows(acT), pair_rows(dtT))]
        hook(h, 4)
        cb = dott(cmat, bmat, HI)
        hook(h, EARLY)
        lowr, tri = ci[:SUB] < SUB, time_of(ri[:SUB]) >= time_of(ci[:SUB] % SUB)
        ca, cd = cb[:SUB], cb[SUB:]
        cbd = [jnp.where(tri, jnp.where(lowr, ca, pltpu.roll(ca, SUB, 1)), 0.0),
               jnp.where(tri, jnp.where(lowr, pltpu.roll(cd, SUB, 1), cd), 0.0)]
        bT = bmat.T
        la = kcat6(split3(rows_cat(bT[:, :SUB], cd[:, :SUB])))
        lb = kcat6(split3(pltpu.roll(bT, SUB, 1)[:, :SUB]))
        c1, c2, c3 = split3(cmat)
        return h, a3, w3, rows, cbd, la, lb, (lanes_cat(c1, c2), lanes_cat(c1, c3))

    def spots(b):
        j = i * nbs + b
        at = lambda r: pl.ds(pl.multiple_of(j * r, SUB), r)
        return j, at(BLK), at(NST + SUB)

    def keep(b, vals):
        h, a3, w3, rows, cbd, la, lb, cc = vals
        j, blk, big = spots(b)
        h_s[blk, :] = h
        aw_s[blk, :] = lanes_cat(a3, w3)
        for half in range(2):
            row_s[2 * j + half] = rows[half]
        cbd_s[blk, :] = rows_cat(*cbd)
        la1_s[big, :], la2_s[big, :] = la
        lb1_s[blk, :], lb2_s[blk, :] = lb
        cc_s[blk, :] = lanes_cat(*cc)

    def kept(b):
        j, blk, big = spots(b)
        eight = pl.ds(pl.multiple_of(8 * zs, 8), 8)
        return (None, aw_s[blk, :BLK], aw_s[blk, BLK:], [row_s[2 * j + half, eight, :] for half in range(2)],
                [cbd_s[pl.ds(pl.multiple_of(j * BLK + half * SUB, SUB), SUB), :] for half in range(2)],
                (la1_s[big, :], la2_s[big, :]), (lb1_s[blk, :], lb2_s[blk, :]), (cc_s[blk, :2 * NST], cc_s[blk, 2 * NST:]))


    def all_prologues(hook):
        u = u_ref[...].astype(F32)
        h = rms(u if mixed else unmix(u, ubuf), nw)
        return [prologue(h[b * BLK:(b + 1) * BLK], b, hook) for b in range(nbs)]

    if by_z:
        @pl.when(p == 0)
        def _():
            for b, v in enumerate(all_prologues(lambda h, k: None)):
                keep(b, v)

    @pl.when(i == 0)
    def _():
        slot = p % 2 if by_z else 0

        @pl.when(p == 0)
        def _():
            for v in load_own() if by_z else [load_w(0, 0)]:
                v.wait()

        @pl.when(p > 0)
        def _():
            load_w(slot, zs).wait()
        for q in range(n_dp):
            for k in range(sp):
                wb[q * PC:(q + 1) * PC, k * PC:(k + 1) * PC] = wf[slot, q, k].astype(BF16)
        @pl.when((p > 0) & jnp.logical_not(upper))
        def _():
            state_out(p - 1).start()
        xcar[...] = roll8(round_bf16(dot(hcar[...], wb[...])))
        st[...] = jnp.zeros_like(st)

    @pl.when((i == ni - 1) & (p < np_ - 1))
    def _():
        nd = p + 1
        nd = nd + nd // 2 * (1 - 2 * (nd % 2))
        if fetch_x:
            for d in ORDER:
                pl.when(nd == d)(functools.partial(xg.settle, d))
        load_w((p + 1) % 2, source(nd)).start()

    lane = lax.broadcasted_iota(jnp.int32, (SUB, LANES), 1)
    lo = jnp.where(lane < HD, 1.0, 0.0).astype(BF16)
    hi = jnp.where(lane < HD, 0.0, 1.0).astype(BF16)
    x0 = {}

    def proj(hs, upto):
        for k in range(len(x0), min(sp, upto)):
            x0[k] = dot(hs, wb[:, k * PC:(k + 1) * PC])

    if by_z:
        vals = [kept(b) for b in range(nbs)]
        hs = h_s[pl.ds(pl.multiple_of(i * nbs * BLK, BLK), nbs * BLK), :]
        proj(hs, sp)
    else:
        vals = all_prologues(proj)
        hs = vals[0][0]

    def lanes_of(k):
        return slice(k * PC, (k + 1) * PC), pl.ds(pl.multiple_of((2 * zs + k) * PC, PC), PC)

    def pre(b, k):
        (sl, gl), (_, a3, w3, _, _, _, _, (c12, c13)) = lanes_of(k), vals[b]
        s1, s2, s3 = split3(st[:, sl])
        inter = dot(c12, rows_cat(s1, s1)) + dot(c12, rows_cat(s2, s2)) + dot(c13, rows_cat(s3, s1))
        n3 = e3_ref.shape[0]
        acx = dot(a3[:, :n3], e3_ref[:, gl])
        wx = dot(w3[:, :n3], e3_ref[:, gl])
        proj(hs, k + EARLY + 1)
        return x0[k][b * BLK:(b + 1) * BLK], acx, wx, inter

    def mid_(b, k, x0, acx, wx, inter):
        (sl, _), (_, _, _, rws, cbds, _, _, _) = lanes_of(k), vals[b]
        t = 2 * zs + k
        base = 0 if by_z else k // 2 * 8
        x, xcar[:, sl] = conv(round_bf16(x0), xcar[:, sl], [sm[t, r:r + 1, :] for r in range(4)], sm[t, 4:5, :])
        xw = split3(x * wx)
        r = kcat6r([v[:SUB] for v in xw]) + kcat6r([v[SUB:] for v in xw])
        ms, xs = [], []
        for half in range(2):
            rows = slice(half * SUB, (half + 1) * SUB)
            row, cbd = rws[half][base:base + 8], cbds[half]
            m = []
            for g in range(2):
                seg = acx[rows, g * LANES:(g + 1) * LANES] - row[2 * (k % 2) + g:2 * (k % 2) + g + 1]
                m.append(jnp.exp2(jnp.minimum(seg, 0.0)) * cbd * row[4 + 2 * (k % 2) + g:5 + 2 * (k % 2) + g])
            ms.append(split3(lanes_cat(*m)))
            xs.append([block_diag(v, lo, hi) for v in split3(x[rows])])
        return x, acx, inter, r, ms, xs

    def fin(b, k, x, acx, inter, r, ms, xs):
        (sl, _), (_, _, _, _, _, la, lb, _) = lanes_of(k), vals[b]
        ra = dot(la[0], r[0]) + dot(la[1], r[1])
        rb = dot(lb[0], r[2]) + dot(lb[1], r[3])
        am, al = acx[SUB - 1:SUB], acx[BLK - 1:BLK]
        st[:, sl] = st[:, sl] * jnp.exp2(al) + ra[:NST] * jnp.exp2(al - am) + rb
        skip = sm[2 * zs + k, 6:7, :]
        for half in range(2):
            rows = slice(half * SUB, (half + 1) * SUB)
            (m1, m2, m3), (x1, x2, x3) = ms[half], xs[half]
            r1 = dot(rows_cat(m1, m2, m3), x1)
            r2 = dot(rows_cat(m1, m2), x2)
            y = r1[:SUB] + r1[SUB:2 * SUB] + r1[2 * SUB:] + r2[:SUB] + r2[SUB:] + dot(m1, x3)
            y = y + inter[rows] * jnp.exp2(acx[rows])
            if half:
                y = y + ra[NST:] * jnp.exp2(acx[rows] - am)
            y_ref[b * BLK + half * SUB:b * BLK + (half + 1) * SUB, sl] = y + skip * x[rows]

    units = [(b, k) for b in range(nbs) for k in range(sp)]
    m = mid_(*units[0], *pre(*units[0]))
    for a, nxt in zip(units, units[1:] + [None]):
        if nxt:
            v = pre(*nxt)
        fin(*a, *m)
        if nxt:
            m = mid_(*nxt, *v)

    @pl.when(i == ni - 1)
    def _():
        @pl.when((p > 0) & jnp.logical_not(upper))
        def _():
            state_out(p - 1).wait_send()
        sbuf[...] = st[...]

    @pl.when(step == np_ * ni - 1)
    def _():
        zg.finish()
        og.finish()
        if fetch_x:
            xg.drain()

        @pl.when(jnp.logical_not(upper))
        def _():
            state_out(p).start()
            state_out(p).wait_send()

        @pl.when(upper)
        def _():
            pltpu.make_async_copy(s_in, s_in, hsem.at[1]).wait()


def p1(u, base, halo, nw, wbc, cbc, bbc, e3, comm, n, n_dp, n_tp, mixed, layer, fetch_x, plans, cid):
    d_model, heads = u.shape[-1], PC // HD * n_tp
    sp, nbs = (2, NBS) if fetch_x else (n_tp, 1)
    width, nb, rows = PC * n_tp, n // BLK, BLK * nbs
    ni = nb // nbs
    fixed = lambda shp: pl.BlockSpec(shp, lambda p, i: (0,) * len(shp), pipeline_mode=pl.Buffered(1))
    own_layer = lambda *shp: pl.BlockSpec((None,) + shp, lambda p, i: (layer, 0, 0), pipeline_mode=pl.Buffered(1))
    once = lambda p, i: jnp.where(p == 0, i, ni - 1)
    col = (lambda p: source(p + p // 2 * (1 - 2 * (p % 2)))) if fetch_x else (lambda p: 0)
    hbm = pl.BlockSpec(memory_space=pl.ANY)
    gathered = lambda r: jax.ShapeDtypeStruct((n_dp, n_tp, r, PC), F32)
    outs = [jax.ShapeDtypeStruct((n, width), F32), jax.ShapeDtypeStruct((n, NST), F32),
            jax.ShapeDtypeStruct((heads, n), F32), jax.ShapeDtypeStruct((NST, width), F32)]
    more = ([gathered(PC), jax.ShapeDtypeStruct((n_tp,) + comm[1].shape, F32)] if fetch_x else []) + [gathered(PC)] * 2
    vm = pltpu.VMEM
    dma = lambda k: [pltpu.SemaphoreType.DMA((k,))] * 2
    return pl.pallas_call(
        functools.partial(p1_body, geom=(n_dp, n_tp, heads, nb, nbs, sp), mixed=mixed, layer=layer, fetch_x=fetch_x, plans=plans),
        name="p1", grid=(n_tp // sp, ni),
        in_specs=[pl.BlockSpec((rows, d_model), lambda p, i: (base() + once(p, i), 0)),
                  fixed((CAR, d_model)), fixed((2, d_model)), own_layer(d_model, PC), own_layer(4, PC), fixed((2, PC)),
                  fixed((3 * heads, width))] + [hbm] * len(comm),
        out_specs=[pl.BlockSpec((rows, sp * PC), lambda p, i: (i, col(p))),
                   pl.BlockSpec((rows, NST), lambda p, i: (once(p, i), 0)),
                   pl.BlockSpec((heads, rows), lambda p, i: (0, once(p, i))),
                   hbm] + [hbm] * len(more),
        out_shape=outs + more,
        scratch_shapes=[
            vm((2 if fetch_x else 1, n_dp, sp, PC, PC), F32), vm((d_model, sp * PC), BF16), pltpu.SemaphoreType.DMA((3,)),
            vm((n_tp, SMALL, PC), F32), vm((heads, d_model), BF16), vm((2 * heads, PC), F32), vm((NST, sp * PC), F32),
            vm((CAR, d_model), BF16), vm((CAR, sp * PC), F32), vm((CAR, PC), F32), vm((heads, LANES), F32),
            vm((d_model // LANES * rows, LANES), F32), vm((n, d_model), BF16),
            vm((nb * (NST + SUB), 4 * SUB), BF16), vm((nb * (NST + SUB), 2 * SUB), BF16),
            vm((n, 4 * SUB), BF16), vm((n, 2 * SUB), BF16), vm((n, 4 * NST), BF16), vm((n, LANES), F32),
            vm((2 * nb, 2 * heads // 2, LANES), F32), vm((n, 2 * BLK), BF16), vm((NST, sp * PC), F32), pltpu.SemaphoreType.DMA((2,))]
        + dma(3 * SEMS) + (dma(8) if fetch_x else []),
        compiler_params=pltpu.CompilerParams(dimension_semantics=("arbitrary", "arbitrary"), vmem_limit_bytes=VMEM_CAP,
                                             collective_id=cid, has_side_effects=True),
        cost_estimate=pl.CostEstimate(flops=n * 70 * 10 ** 6, bytes_accessed=n * 12000, transcendentals=0),
    )(u, halo, nw, wbc, cbc, bbc, e3, *comm)


def p2_body(*refs, geom, mix_in, layer, fetch_x, plans):
    n_dp, n_tp, heads = geom
    (u_ref, nw_ref, wz_ref, wo_ref, sm_ref, y_ref, c_ref, ac_ref, s_ref, e3_ref), refs = refs[:10], refs[10:]
    if fetch_x:
        (ax, o_ref, f_ref, gx), refs = refs[:4], refs[4:]
    else:
        (o_ref, r_ref), refs = refs[:2], refs[2:]
    (wzb, wob, s3, ubuf, send, recv), refs = refs[:6], refs[6:]
    i = pl.program_id(0)
    width = PC * n_tp
    if fetch_x:
        xg = Gather(piece_rows(ax, layer + 1), gx, send, recv, 0)

        @pl.when(i == 0)
        def _():
            entry_barrier(xg.peers())
        at_steps(i, xg.plan(plans))
    else:
        fbuf, = refs
        dp, tp, z, c = here()

        def swap(k):
            return pltpu.make_async_remote_copy(
                src_ref=fbuf.at[k % 2], dst_ref=r_ref.at[pl.ds(pl.multiple_of(k * BLK2, BLK2), BLK2)],
                send_sem=send.at[k % 2], recv_sem=recv.at[0], device_id=(dp, 2 * z + 1 - c), device_id_type=MESH)

        @pl.when(i == 0)
        def _():
            entry_barrier([(dp, 2 * z + 1 - c)])

        @pl.when(i > 1)
        def _():
            swap(i - 2).wait_send()

        @pl.when(i > 0)
        def _():
            swap(i - 1).start()

    @pl.when(i == 0)
    def _():
        for d in range(n_dp):
            for t in range(n_tp):
                a, b = slice(d * PC, (d + 1) * PC), slice(t * PC, (t + 1) * PC)
                wzb[a, b] = wz_ref[d, t].astype(BF16)
                wob[b, a] = wo_ref[d, t].astype(BF16)
        a, b, c_ = split3(jnp.where(here()[3] == 1, s_ref[...], 0.0))
        for k, (v, w) in enumerate(((a, a), (b, b), (c_, a))):
            s3[k] = rows_cat(v, w)

    u = u_ref[...].astype(F32)
    u = u if mix_in else unmix(u, ubuf)
    h = rms(u, nw_ref[layer:layer + 1].astype(F32))
    c1, c2, c3 = split3(c_ref[...])
    c12, c13 = lanes_cat(c1, c2), lanes_cat(c1, c3)
    eT = rows_cat(*split3(jnp.exp2(ac_ref[...]))).T
    vs, ss = [], 0.0
    for t in range(n_tp):
        sl = slice(t * PC, (t + 1) * PC)
        z_ = round_bf16(dot(h, wzb[:, sl]))
        cor = dot(c12, s3[0, :, sl]) + dot(c12, s3[1, :, sl]) + dot(c13, s3[2, :, sl])
        v = (y_ref[:, sl] + cor * dot(eT, e3_ref[:, sl])) * silu(z_)
        ss = ss + jnp.sum(v * v, axis=-1, keepdims=True)
        vs.append(v)
    sc = lax.rsqrt(ss / width + EPS)
    g = lanes_cat(*[(v * sc * sm_ref[t, 5:6, :]).astype(BF16) for t, v in enumerate(vs)])
    un = round_bf16(u + dot(g, wob[...]))
    if fetch_x:
        o_ref[...] = un.astype(BF16)
        f_ref[...] = un[BLK2 - CAR:]
    else:
        un = unmix(un, ubuf)
        fbuf[i % 2] = un
        o_ref[...] = un.astype(BF16)

    @pl.when(i == pl.num_programs(0) - 1)
    def _():
        if fetch_x:
            xg.finish()
        else:
            swap(i).start()
            for k in range(2):
                swap(i - 1 + k).wait_send()
            whole = pltpu.make_async_copy(r_ref, r_ref, recv.at[0])
            whole.wait()


def p2(u, base, nw, wz, wo, sm, y, c, ac, s, e3, comm, n, n_dp, n_tp, mix_in, layer, fetch_x, plans, cid):
    d_model, heads = u.shape[-1], PC // HD * n_tp
    width = PC * n_tp
    fixed = lambda shp: pl.BlockSpec(shp, lambda i: (0,) * len(shp), pipeline_mode=pl.Buffered(1))
    hbm = pl.BlockSpec(memory_space=pl.ANY)
    rows = lambda w: pl.BlockSpec((BLK2, w), lambda i: (i, 0))
    shape = lambda *s: jax.ShapeDtypeStruct(s, F32)
    vm = pltpu.VMEM
    outs = [jax.ShapeDtypeStruct((n, d_model), BF16)]
    specs = [rows(d_model)]
    if fetch_x:
        outs += [shape(CAR, d_model), shape(n_dp, n_tp, PC, PC)]
        specs += [pl.BlockSpec((CAR, d_model), lambda i: (0, 0)), hbm]
    else:
        outs += [shape(n, d_model)]
        specs += [hbm]
    return pl.pallas_call(
        functools.partial(p2_body, geom=(n_dp, n_tp, heads), mix_in=mix_in, layer=layer, fetch_x=fetch_x, plans=plans),
        name="p2", grid=(n // BLK2,),
        in_specs=[pl.BlockSpec((BLK2, d_model), lambda i: (base() + i, 0)),
                  fixed((2, d_model)),
                  fixed((n_dp, n_tp, PC, PC)), fixed((n_dp, n_tp, PC, PC)),
                  pl.BlockSpec((n_tp, SMALL, PC), lambda i: (0, layer, 0), pipeline_mode=pl.Buffered(1)),
                  rows(width), rows(NST), pl.BlockSpec((heads, BLK2), lambda i: (0, i)),
                  fixed((NST, width)), fixed((3 * heads, width))] + [hbm] * len(comm),
        out_specs=specs, out_shape=outs,
        scratch_shapes=[vm((d_model, width), BF16), vm((width, d_model), BF16), vm((3, 2 * NST, width), BF16),
                        vm((d_model // LANES * BLK2, LANES), F32)]
        + [pltpu.SemaphoreType.DMA((SEMS,))] * 2 + ([] if fetch_x else [vm((2, BLK2, d_model), F32)]),
        compiler_params=pltpu.CompilerParams(dimension_semantics=("arbitrary",), vmem_limit_bytes=VMEM_CAP,
                                             collective_id=cid, has_side_effects=True),
        cost_estimate=pl.CostEstimate(flops=n * 30 * 10 ** 6, bytes_accessed=n * 12000, transcendentals=0),
    )(u, nw, wz, wo, sm, y, c, ac, s, e3, *comm)


def finish_body(own_ref, other_ref, o_ref):
    mine = pl.program_id(0) == here()[3]

    @pl.when(mine)
    def _():
        o_ref[...] = own_ref[...]

    @pl.when(jnp.logical_not(mine))
    def _():
        o_ref[...] = other_ref[...].astype(BF16)


def finish(own, other):
    n, d_model = own.shape
    rows = n // 3
    ni = n // rows
    pick = lambda w: (lambda j, i: (jnp.where((j == here()[3]) == w, i, ni - 1), 0))
    return pl.pallas_call(
        finish_body, name="finish", grid=(2, ni),
        in_specs=[pl.BlockSpec((rows, d_model), pick(True)), pl.BlockSpec((rows, d_model), pick(False))],
        out_specs=pl.BlockSpec((rows, d_model), lambda j, i: (j * ni + i, 0)),
        out_shape=jax.ShapeDtypeStruct((2 * n, d_model), BF16),
        compiler_params=pltpu.CompilerParams(dimension_semantics=("arbitrary", "arbitrary")),
        cost_estimate=pl.CostEstimate(flops=n * d_model, bytes_accessed=n * d_model * 8, transcendentals=0),
    )(own, other)


def small_rows(conv, bias, gate, skip, dtb, al, wdt):
    f = lambda v: v.astype(F32)
    n, hp = skip.shape
    wide = lambda v: jnp.broadcast_to(v[:, :, None], (n, hp, PC))
    one = lambda v: v.reshape(n, 1, PC)
    skip = jnp.broadcast_to(skip[:, :, None], (n, hp, HD))
    v = [f(conv), one(f(bias)), one(f(gate)), one(skip), jnp.zeros((n, 1, PC), F32), wide(dtb), wide(-jnp.exp(al) * LOG2E),
         f(wdt).transpose(0, 2, 1).reshape(n, -1, PC)]
    return jnp.concatenate(v, axis=1).reshape(-1, PC)


PLAN_X = "00020405030607040809"
PLAN_Z0 = "04090a0c0b0c0e0d0e10"
PLAN_O0 = "090d0f110f1113111315"
PLAN_Z1 = "0002040604060906080b"
PLAN_O1 = "06090b0e0b0e100d1013"
PLAN_X1 = "0003050705070907090a"


def solution(mesh):
    n_tp, n_dp = mesh.shape['tp'], mesh.shape['dp']
    rep, col, vec = P(), P(None, None, 'tp'), P(None, 'tp')
    in_specs = (P('dp'), rep, col, col, rep, col, col, rep, vec, rep, vec, vec, vec, vec, P(None, 'tp', None))

    def device_forward(hidden, norm_w, w_z, w_x, w_bc, w_dt, conv_x, conv_bc, bias_x, bias_bc, dt_bias, a_log, d_skip, gate_w, w_out):
        u = hidden[0]
        steps, d_model = u.shape
        n = steps // 2
        core = lax.axis_index('tp') % 2
        e3 = expand_mat(dt_bias.shape[1] * n_tp)
        up = [(2 * k, 2 * k + 1) for k in range(n_tp // 2)]
        ax, az, ao = w_x.astype(F32), w_z.astype(F32), w_out.astype(F32)
        small = small_rows(conv_x, bias_x, gate_w, d_skip, dt_bias, a_log, w_dt)
        tail = u[n - SUB:n].astype(F32).reshape(8, 8, d_model).transpose(1, 0, 2).reshape(SUB, d_model)[SUB - CAR:]
        halo = jnp.where(core == 1, tail, 0.0)
        half = lambda blk: (lambda: lax.axis_index('tp') % 2 * (n // blk))
        none = lambda: 0
        common = (n, n_dp, n_tp)
        bc = (norm_w, w_bc, conv_bc, bias_bc, e3)

        y, c, ac, s, gx, gs, gz, go = p1(u, half(BLK * NBS), halo, *bc, (ax, small, az, ao), *common, False, 0, True,
                                         (PLAN_Z0, PLAN_O0, PLAN_X), 1)
        u, f, gx = p2(u, half(BLK2), norm_w, gz, go, gs, y, c, ac, s, e3, (ax,), *common, False, 0, True, PLAN_X1, 2)
        halo = lax.ppermute(f, 'tp', up)
        y, c, ac, s, gz, go = p1(u, none, halo, *bc, (ax, gx, gs, az, ao), *common, True, 1, False, (PLAN_Z1, PLAN_O1), 3)
        own, other = p2(u, none, norm_w, gz, go, gs, y, c, ac, s, e3, (), *common, True, 1, False, None, 4)
        return finish(own, other)[None]

    return jax.shard_map(device_forward, mesh=mesh, in_specs=in_specs, out_specs=P('dp'), check_vma=False)
```

```python
import functools
import jax
import jax.numpy as jnp
import numpy as np
from jax import lax
from jax.experimental import pallas as pl
from jax.experimental.pallas import tpu as pltpu
from jax.sharding import PartitionSpec as P

EPS = 1e-5
LOG2E = 1.4426950408889634
HI = lax.Precision.HIGHEST
F32 = jnp.float32
BF16 = jnp.bfloat16
MESH = pl.DeviceIdType.MESH
LANES = 128
BLK = 128
SUB = 64
BLK2 = 256
NBS = 4
PC = 256
HD = 64
NST = 128
CAR = 24
SMALL = 32
ORDER = (1, 3, 2)
EARLY = 6
SEMS = 26
VMEM_CAP = 60 << 20


def silu(v):
    return v / (1.0 + jnp.exp2(v * -LOG2E))


def split3(v):
    a = v.astype(BF16)
    r = v - a.astype(F32)
    b = r.astype(BF16)
    return a, b, (r - b.astype(F32)).astype(BF16)


def round_bf16(v):
    return v.astype(BF16).astype(F32)


def rms(u, nw):
    return (u * lax.rsqrt(jnp.mean(u * u, axis=-1, keepdims=True) + EPS) * nw).astype(BF16)


def dot(a, b, prec=None):
    return jnp.dot(a, b, preferred_element_type=F32, precision=prec)


def dott(a, b, prec=None):
    return lax.dot_general(a, b, (((1,), (1,)), ((), ())), preferred_element_type=F32, precision=prec)


def rows_cat(*v):
    return jnp.concatenate(v, axis=0)


def lanes_cat(*v):
    return jnp.concatenate(v, axis=1)


def time_of(r):
    return 8 * (r % 8) + r // 8


def roll8(v):
    c = v.shape[-1]
    return pltpu.roll(v.reshape(CAR // 8, 8, c), 1, 1).reshape(CAR, c)


def conv_block(cur, prev, taps, bias, first):
    now = roll8(cur[SUB - CAR:])
    sh = jnp.where(first, prev, now)
    out = bias + cur * taps[-1]
    for k in range(1, 4):
        out = out + rows_cat(sh[CAR - 8 * k:], cur[:SUB - 8 * k]) * taps[3 - k]
    return out, now


def unmix(v, buf):
    n, c = v.shape
    for j in range(c // LANES):
        buf[n * j:n * (j + 1), :] = v[:, LANES * j:LANES * (j + 1)]
    cols = [rows_cat(*[buf[pl.ds(n * j + b + k, 8, stride=8), :] for b in range(0, n, SUB) for k in range(8)])
            for j in range(c // LANES)]
    return lanes_cat(*cols)


def head_row(h, heads):
    return (h % 2) * (heads // 2) + h // 2


def expand_mat(heads):
    order = sorted(range(heads), key=lambda h: head_row(h, heads))
    one = np.repeat(np.eye(heads)[order], HD, axis=1)
    return jnp.asarray(np.tile(one, (3, 1)), BF16)


def per_channel(v, t, heads):
    n, per = v.shape[0], PC // HD
    low = lax.broadcasted_iota(jnp.int32, (n, LANES), 1) < HD
    wide = [jnp.broadcast_to(v[:, r:r + 1], (n, LANES)) for r in [head_row(h, heads) for h in range(per * t, per * (t + 1))]]
    return lanes_cat(*[jnp.where(low, a, b) for a, b in zip(wide[::2], wide[1::2])])


def kcat6(parts):
    a, b, c = parts
    return lanes_cat(a, b, c, a), lanes_cat(b, a)


def kcat6r(parts):
    a, b, c = parts
    return rows_cat(a, a, a, b), rows_cat(b, c)


def block_diag(x, lo, hi):
    z = jnp.zeros((x.shape[0], LANES), BF16)
    l, r = x[:, :LANES], x[:, LANES:]
    return rows_cat(lanes_cat(l * lo, z), lanes_cat(l * hi, z), lanes_cat(z, r * lo), lanes_cat(z, r * hi))


def here():
    dp, tp = lax.axis_index('dp'), lax.axis_index('tp')
    return dp, tp, tp // 2, tp % 2


def source(dz):
    return (here()[2] + 4 - dz) % 4


class Gather:
    def __init__(self, piece, g, send, recv, base, keep=True):
        self.piece, self.g, self.send, self.recv, self.base = piece, g, send, recv, base
        self.dp, self.tp, self.z, self.c = here()
        x, y = self.dp // 2, self.dp % 2
        self.side = ((1 - x) * 2 + y, x * 2 + 1 - y)
        self.partner = (self.dp, 2 * self.z + 1 - self.c)
        self.quarters, self.keep = g.shape[0], keep

    def rdma(self, k, src, dst, dev):
        return pltpu.make_async_remote_copy(src_ref=src, dst_ref=dst, send_sem=self.send.at[self.base + k],
                                            recv_sem=self.recv.at[self.base + k], device_id=dev, device_id_type=MESH)

    def local(self, q):
        return pltpu.make_async_copy(self.piece(q), self.g.at[q, self.tp], self.send.at[self.base + q])

    def own(self, q):
        return self.rdma(4 + q, self.piece(q), self.g.at[q, self.tp], self.partner)

    def line(self, dz):
        return self.rdma(7 + dz, self.piece(self.dp), self.g.at[self.dp, self.tp],
                         (self.dp, 2 * ((self.z + dz) % 4) + self.c))

    def cross(self, dz, n):
        ref = self.g.at[self.dp, 2 * source(dz) + self.c]
        return self.rdma(9 + 2 * dz + n, ref, ref, (self.side[n], self.tp))

    def relay(self, dz, n):
        half = self.g.shape[2] // 2
        ref = self.g.at[self.side[n], 2 * source(dz) + self.c, pl.ds(n * half, half)]
        return self.rdma(15 + 2 * dz + n, ref, ref, (self.side[1 - n], self.tp))

    def over(self, dz):
        ref = self.g.at[:, 2 * source(dz) + self.c]
        return self.rdma(22 + dz, ref, ref, self.partner)

    def peers(self):
        return ([(self.dp, 2 * ((self.z + dz) % 4) + self.c) for dz in ORDER]
                + [(p, self.tp) for p in self.side] + [self.partner])

    def start(self):
        for q in range(self.quarters):
            self.own(q).start()
        for dz in ORDER:
            self.line(dz).start()
        if self.keep:
            for q in range(self.quarters):
                self.local(q).start()

    def spread(self, dz):
        self.line(dz).wait_recv()
        for n in range(2):
            self.cross(dz, n).start()

    def pass_on(self, dz):
        for n in range(2):
            self.cross(dz, n).wait_recv()
            self.relay(dz, n).start()

    def hand(self, dz):
        for n in range(2):
            self.relay(dz, n).wait_recv()
        self.over(dz).start()

    def settle_own(self):
        for q in range(self.quarters):
            self.own(q).wait_recv()
            if self.keep:
                self.local(q).wait()

    def settle(self, dz):
        self.over(dz).wait_recv()

    def drain(self):
        for q in range(self.quarters):
            self.own(q).wait_send()
        for dz in ORDER:
            self.line(dz).wait_send()
            self.over(dz).wait_send()
            for n in range(2):
                self.cross(dz, n).wait_send()
                self.relay(dz, n).wait_send()

    def plan(self, s):
        s = bytes.fromhex(s)
        acts = [(s[0], self.start)]
        for k, f in enumerate((self.spread, self.pass_on, self.hand)):
            acts += [(s[1 + 3 * k + j], functools.partial(f, dz)) for j, dz in enumerate(ORDER)]
        return acts

    def finish(self):
        self.settle_own()
        for dz in ORDER:
            self.settle(dz)
        self.drain()


class Small:
    def __init__(self, a, g, send, recv):
        self.a, self.g, self.send, self.recv = a, g, send, recv
        self.dp, self.tp, _, _ = here()

    def copy(self, k):
        return pltpu.make_async_remote_copy(src_ref=self.a, dst_ref=self.g.at[self.tp], send_sem=self.send.at[k],
                                            recv_sem=self.recv.at[k], device_id=(self.dp, (self.tp + k) % 8),
                                            device_id_type=MESH)

    def local(self):
        return pltpu.make_async_copy(self.a, self.g.at[self.tp], self.send.at[0])

    def peers(self):
        return [(self.dp, (self.tp + k) % 8) for k in range(1, 8)]

    def start(self):
        self.local().start()
        for k in range(1, 8):
            self.copy(k).start()

    def finish(self):
        self.local().wait()
        for k in range(1, 8):
            self.copy(k).wait()


def entry_barrier(peers):
    sem = pltpu.get_barrier_semaphore()
    for p in peers:
        pl.semaphore_signal(sem, inc=1, device_id=p, device_id_type=MESH)
    pl.semaphore_wait(sem, len(peers))


def at_steps(step, acts):
    for k in sorted({k for k, _ in acts}):
        @pl.when(step == k)
        def _():
            for j, f in acts:
                if j == k:
                    f()


def piece_rows(ref, layer):
    return lambda q: ref.at[layer, pl.ds(q * PC, PC)]


def piece_cols(ref, layer):
    return lambda q: ref.at[layer, :, pl.ds(pl.multiple_of(q * PC, PC) if not isinstance(q, int) else q * PC, PC)]


def p1_body(*refs, geom, mixed, layer, fetch_x, plans):
    n_dp, n_tp, heads, nb, nbs, sp = geom
    (u_ref, halo_ref, nw_ref, wbc_ref, cbc_ref, bbc_ref, e3_ref), refs = refs[:7], refs[7:]
    row = slice(layer, layer + 1)
    nw, cbc, bbc = nw_ref[row].astype(F32), cbc_ref[...].astype(F32), bbc_ref[row].astype(F32)
    if fetch_x:
        (ax, asm, az, ao), (y_ref, c_ref, ac_ref, s_in), (gx, gs, gy, gz, go), refs = refs[:4], refs[4:8], refs[8:13], refs[13:]
    else:
        (ax, gx, gs, az, ao), (y_ref, c_ref, ac_ref, s_in), (gz, go), refs = refs[:5], refs[5:9], refs[9:11], refs[11:]
    (wf, wb, wsem, sm, wdt, cst, st, hcar, xcar, qcar, aoff, ubuf, h_s, la1_s, la2_s, lb1_s, lb2_s, cc_s, cbd_s, row_s, aw_s,
     sbuf, hsem, send, recv), sems = refs[:25], refs[25:]
    p, i = pl.program_id(0), pl.program_id(1)
    np_, ni = pl.num_programs(0), pl.num_programs(1)
    step = p * ni + i
    d_model = u_ref.shape[-1]
    by_z = sp < n_tp
    zs_of = (lambda p: source(p + p // 2 * (1 - 2 * (p % 2)))) if by_z else (lambda p: 0)
    zs = zs_of(p)
    upper = here()[3] == 1

    def state_out(p):
        dp, tp, _, c = here()
        cols = pl.ds(pl.multiple_of(2 * zs_of(p) * PC, PC), sp * PC)
        return pltpu.make_async_remote_copy(src_ref=sbuf, dst_ref=s_in.at[:, cols], send_sem=hsem.at[0], recv_sem=hsem.at[1],
                                            device_id=(dp, tp + 1 - 2 * c), device_id_type=MESH)

    zg = Gather(piece_rows(az, layer), gz, send, recv, 0)
    og = Gather(piece_cols(ao, layer), go, send, recv, SEMS)
    acts = zg.plan(plans[0]) + og.plan(plans[1])
    if fetch_x:
        xg = Gather(piece_rows(ax, layer), gx, send, recv, 2 * SEMS, False)
        small = Small(asm, gs, *sems)
        yg = Gather(piece_rows(ax, layer + 1), gy, send, recv, 3 * SEMS)
        acts += xg.plan(plans[2]) + yg.plan(plans[3])

    def load_w(slot, zsrc):
        return pltpu.make_async_copy(gx.at[:, pl.ds(2 * zsrc, sp)], wf.at[slot], wsem.at[slot])

    def load_own():
        _, tp, _, c = here()
        return ([pltpu.make_async_copy(piece_rows(ax, layer)(q), wf.at[0, q, c], wsem.at[0]) for q in range(n_dp)]
                + [pltpu.make_async_copy(gx.at[q, tp + 1 - 2 * c], wf.at[0, q, 1 - c], wsem.at[0]) for q in range(n_dp)])

    @pl.when(step == 0)
    def _():
        entry_barrier((small.peers() + [(s, here()[1]) for s in zg.side]) if fetch_x else zg.peers())
        if fetch_x:
            small.start()
    at_steps(step, acts)

    @pl.when(step == 0)
    def _():
        if fetch_x:
            small.finish()
            xg.settle_own()
        if by_z:
            for v in load_own():
                v.start()
        else:
            load_w(0, 0).start()
        cp = pltpu.make_async_copy(gs.at[:, pl.ds(layer * SMALL, SMALL)], sm, wsem.at[2])
        cp.start()
        cp.wait()
        kc = d_model // PC
        hp = heads // n_tp
        for t in range(n_tp):
            for k in range(hp):
                r = head_row(hp * t + k, heads)
                for c in range(kc):
                    wdt[r:r + 1, c * PC:(c + 1) * PC] = sm[t, 16 + kc * k + c:17 + kc * k + c, :].astype(BF16)
                cst[r:r + 1, :] = sm[t, 8 + k:9 + k, :]
                cst[heads + r:heads + r + 1, :] = sm[t, 12 + k:13 + k, :]
        aoff[...] = jnp.zeros_like(aoff)
        hh = rms(halo_ref[...], nw)
        hcar[...] = hh
        qcar[...] = roll8(round_bf16(dot(hh, wbc_ref[...])))

    first = lax.broadcasted_iota(jnp.int32, (CAR, PC), 0) % 8 == 0

    def conv(cur, prev, taps, bias):
        a, now = conv_block(cur[:SUB], prev, taps, bias, first)
        b, now = conv_block(cur[SUB:], now, taps, bias, first)
        return silu(rows_cat(a, b)), now

    ri = lax.broadcasted_iota(jnp.int32, (BLK, BLK), 0)
    ci = lax.broadcasted_iota(jnp.int32, (BLK, BLK), 1)

    def prologue(h, b, hook):
        q0 = dot(h, wbc_ref[...])
        rT = round_bf16(dott(wdt[...], h))
        hook(h, 2)
        bc, qcar[...] = conv(round_bf16(q0), qcar[...],
                             [cbc[k:k + 1] for k in range(4)], bbc)
        bmat, cmat = bc[:, :NST], bc[:, NST:]
        here_rows = slice(b * BLK, (b + 1) * BLK)
        c_ref[here_rows, :] = cmat
        pre = rT + cst[:heads, :BLK]
        dtT = jnp.maximum(pre, 0.0) + jnp.log1p(jnp.exp(-jnp.abs(pre)))
        aT = dtT * cst[heads:, :BLK]
        tr, tc = ri // SUB * SUB + time_of(ri % SUB), ci // SUB * SUB + time_of(ci % SUB)
        acT = dot(aT, jnp.where(tr <= tc, 1.0, 0.0), HI)
        mid, alast = acT[:, SUB - 1:SUB], acT[:, BLK - 1:BLK]
        low = ci[:heads] < SUB
        wT = dtT * jnp.exp2(jnp.where(low, mid, alast) - acT)
        pad = jnp.zeros((BLK - 3 * heads, BLK), BF16)
        a3, w3 = (rows_cat(*split3(acT), pad).T, rows_cat(*split3(wT), pad).T) if by_z else (acT.T, wT.T)
        ac_ref[:, here_rows] = acT + aoff[:, :1]
        aoff[...] = aoff[...] + alast

        def pair_rows(v):
            ev, od = v[:heads // 2], v[heads // 2:]
            l = low[:heads // 2]
            return jnp.where(l, ev, pltpu.roll(od, SUB, 1)), jnp.where(l, pltpu.roll(ev, SUB, 1), od)

        rows = [rows_cat(*[w for zz in zip(*[jnp.split(v, n_tp // 2) for v in ad]) for w in zz])
                for ad in zip(pair_rows(acT), pair_rows(dtT))]
        hook(h, 4)
        cb = dott(cmat, bmat, HI)
        hook(h, EARLY)
        lowr, tri = ci[:SUB] < SUB, time_of(ri[:SUB]) >= time_of(ci[:SUB] % SUB)
        ca, cd = cb[:SUB], cb[SUB:]
        cbd = [jnp.where(tri, jnp.where(lowr, ca, pltpu.roll(ca, SUB, 1)), 0.0),
               jnp.where(tri, jnp.where(lowr, pltpu.roll(cd, SUB, 1), cd), 0.0)]
        bT = bmat.T
        la = kcat6(split3(rows_cat(bT[:, :SUB], cd[:, :SUB])))
        lb = kcat6(split3(pltpu.roll(bT, SUB, 1)[:, :SUB]))
        c1, c2, c3 = split3(cmat)
        return h, a3, w3, rows, cbd, la, lb, (lanes_cat(c1, c2), lanes_cat(c1, c3))

    def spots(b):
        j = i * nbs + b
        at = lambda r: pl.ds(pl.multiple_of(j * r, SUB), r)
        return j, at(BLK), at(NST + SUB)

    def keep(b, vals):
        h, a3, w3, rows, cbd, la, lb, cc = vals
        j, blk, big = spots(b)
        h_s[blk, :] = h
        aw_s[blk, :] = lanes_cat(a3, w3)
        for half in range(2):
            row_s[2 * j + half] = rows[half]
        cbd_s[blk, :] = rows_cat(*cbd)
        la1_s[big, :], la2_s[big, :] = la
        lb1_s[blk, :], lb2_s[blk, :] = lb
        cc_s[blk, :] = lanes_cat(*cc)

    def kept(b):
        j, blk, big = spots(b)
        eight = pl.ds(pl.multiple_of(8 * zs, 8), 8)
        return (None, aw_s[blk, :BLK], aw_s[blk, BLK:], [row_s[2 * j + half, eight, :] for half in range(2)],
                [cbd_s[pl.ds(pl.multiple_of(j * BLK + half * SUB, SUB), SUB), :] for half in range(2)],
                (la1_s[big, :], la2_s[big, :]), (lb1_s[blk, :], lb2_s[blk, :]), (cc_s[blk, :2 * NST], cc_s[blk, 2 * NST:]))


    def all_prologues(hook):
        u = u_ref[...].astype(F32)
        h = rms(u if mixed else unmix(u, ubuf), nw)
        return [prologue(h[b * BLK:(b + 1) * BLK], b, hook) for b in range(nbs)]

    if by_z:
        @pl.when(p == 0)
        def _():
            for b, v in enumerate(all_prologues(lambda h, k: None)):
                keep(b, v)

    @pl.when(i == 0)
    def _():
        slot = p % 2 if by_z else 0

        @pl.when(p == 0)
        def _():
            for v in load_own() if by_z else [load_w(0, 0)]:
                v.wait()

        @pl.when(p > 0)
        def _():
            load_w(slot, zs).wait()
        for q in range(n_dp):
            for k in range(sp):
                wb[q * PC:(q + 1) * PC, k * PC:(k + 1) * PC] = wf[slot, q, k].astype(BF16)
        @pl.when((p > 0) & jnp.logical_not(upper))
        def _():
            state_out(p - 1).start()
        xcar[...] = roll8(round_bf16(dot(hcar[...], wb[...])))
        st[...] = jnp.zeros_like(st)

    @pl.when((i == ni - 1) & (p < np_ - 1))
    def _():
        nd = p + 1
        nd = nd + nd // 2 * (1 - 2 * (nd % 2))
        if fetch_x:
            for d in ORDER:
                pl.when(nd == d)(functools.partial(xg.settle, d))
        load_w((p + 1) % 2, source(nd)).start()

    lane = lax.broadcasted_iota(jnp.int32, (SUB, LANES), 1)
    lo = jnp.where(lane < HD, 1.0, 0.0).astype(BF16)
    hi = jnp.where(lane < HD, 0.0, 1.0).astype(BF16)
    x0 = {}

    def proj(hs, upto):
        for k in range(len(x0), min(sp, upto)):
            x0[k] = dot(hs, wb[:, k * PC:(k + 1) * PC])

    if by_z:
        vals = [kept(b) for b in range(nbs)]
        hs = h_s[pl.ds(pl.multiple_of(i * nbs * BLK, BLK), nbs * BLK), :]
        proj(hs, sp)
    else:
        vals = all_prologues(proj)
        hs = vals[0][0]

    def lanes_of(k):
        return slice(k * PC, (k + 1) * PC), pl.ds(pl.multiple_of((2 * zs + k) * PC, PC), PC)

    def pre(b, k):
        (sl, gl), (_, a3, w3, _, _, _, _, (c12, c13)) = lanes_of(k), vals[b]
        s1, s2, s3 = split3(st[:, sl])
        inter = dot(c12, rows_cat(s1, s1)) + dot(c12, rows_cat(s2, s2)) + dot(c13, rows_cat(s3, s1))
        n3 = e3_ref.shape[0]
        wide = lambda v: dot(v[:, :n3], e3_ref[:, gl]) if by_z else per_channel(v, k, heads)
        acx, wx = wide(a3), wide(w3)
        proj(hs, k + EARLY + 1)
        return x0[k][b * BLK:(b + 1) * BLK], acx, wx, inter

    def mid_(b, k, x0, acx, wx, inter):
        (sl, _), (_, _, _, rws, cbds, _, _, _) = lanes_of(k), vals[b]
        t = 2 * zs + k
        base = 0 if by_z else k // 2 * 8
        x, xcar[:, sl] = conv(round_bf16(x0), xcar[:, sl], [sm[t, r:r + 1, :] for r in range(4)], sm[t, 4:5, :])
        xw = split3(x * wx)
        r = kcat6r([v[:SUB] for v in xw]) + kcat6r([v[SUB:] for v in xw])
        ms, xs = [], []
        for half in range(2):
            rows = slice(half * SUB, (half + 1) * SUB)
            row, cbd = rws[half][base:base + 8], cbds[half]
            m = []
            for g in range(2):
                seg = acx[rows, g * LANES:(g + 1) * LANES] - row[2 * (k % 2) + g:2 * (k % 2) + g + 1]
                m.append(jnp.exp2(jnp.minimum(seg, 0.0)) * cbd * row[4 + 2 * (k % 2) + g:5 + 2 * (k % 2) + g])
            ms.append(split3(lanes_cat(*m)))
            xs.append([block_diag(v, lo, hi) for v in split3(x[rows])])
        return x, acx, inter, r, ms, xs

    def fin(b, k, x, acx, inter, r, ms, xs):
        (sl, _), (_, _, _, _, _, la, lb, _) = lanes_of(k), vals[b]
        ra = dot(la[0], r[0]) + dot(la[1], r[1])
        rb = dot(lb[0], r[2]) + dot(lb[1], r[3])
        am, al = acx[SUB - 1:SUB], acx[BLK - 1:BLK]
        st[:, sl] = st[:, sl] * jnp.exp2(al) + ra[:NST] * jnp.exp2(al - am) + rb
        skip = sm[2 * zs + k, 6:7, :]
        for half in range(2):
            rows = slice(half * SUB, (half + 1) * SUB)
            (m1, m2, m3), (x1, x2, x3) = ms[half], xs[half]
            r1 = dot(rows_cat(m1, m2, m3), x1)
            r2 = dot(rows_cat(m1, m2), x2)
            y = r1[:SUB] + r1[SUB:2 * SUB] + r1[2 * SUB:] + r2[:SUB] + r2[SUB:] + dot(m1, x3)
            y = y + inter[rows] * jnp.exp2(acx[rows])
            if half:
                y = y + ra[NST:] * jnp.exp2(acx[rows] - am)
            y_ref[b * BLK + half * SUB:b * BLK + (half + 1) * SUB, sl] = y + skip * x[rows]

    units = [(b, k) for b in range(nbs) for k in range(sp)]
    m = mid_(*units[0], *pre(*units[0]))
    for a, nxt in zip(units, units[1:] + [None]):
        if nxt:
            v = pre(*nxt)
        fin(*a, *m)
        if nxt:
            m = mid_(*nxt, *v)

    @pl.when(i == ni - 1)
    def _():
        @pl.when((p > 0) & jnp.logical_not(upper))
        def _():
            state_out(p - 1).wait_send()
        sbuf[...] = st[...]

    @pl.when(step == np_ * ni - 1)
    def _():
        zg.finish()
        og.finish()
        if fetch_x:
            xg.drain()
            yg.finish()

        @pl.when(jnp.logical_not(upper))
        def _():
            state_out(p).start()
            state_out(p).wait_send()

        @pl.when(upper)
        def _():
            pltpu.make_async_copy(s_in, s_in, hsem.at[1]).wait()


def p1(u, base, halo, nw, wbc, cbc, bbc, e3, comm, n, n_dp, n_tp, mixed, layer, fetch_x, plans, cid):
    d_model, heads = u.shape[-1], PC // HD * n_tp
    sp, nbs = (2, NBS) if fetch_x else (n_tp, 1)
    width, nb, rows = PC * n_tp, n // BLK, BLK * nbs
    ni = nb // nbs
    fixed = lambda shp: pl.BlockSpec(shp, lambda p, i: (0,) * len(shp), pipeline_mode=pl.Buffered(1))
    own_layer = lambda *shp: pl.BlockSpec((None,) + shp, lambda p, i: (layer, 0, 0), pipeline_mode=pl.Buffered(1))
    once = lambda p, i: jnp.where(p == 0, i, ni - 1)
    col = (lambda p: source(p + p // 2 * (1 - 2 * (p % 2)))) if fetch_x else (lambda p: 0)
    hbm = pl.BlockSpec(memory_space=pl.ANY)
    gathered = lambda r: jax.ShapeDtypeStruct((n_dp, n_tp, r, PC), F32)
    outs = [jax.ShapeDtypeStruct((n, width), F32), jax.ShapeDtypeStruct((n, NST), F32),
            jax.ShapeDtypeStruct((heads, n), F32), jax.ShapeDtypeStruct((NST, width), F32)]
    more = ([gathered(PC), jax.ShapeDtypeStruct((n_tp,) + comm[1].shape, F32), gathered(PC)] if fetch_x else []) + [gathered(PC)] * 2
    vm = pltpu.VMEM
    dma = lambda k: [pltpu.SemaphoreType.DMA((k,))] * 2
    return pl.pallas_call(
        functools.partial(p1_body, geom=(n_dp, n_tp, heads, nb, nbs, sp), mixed=mixed, layer=layer, fetch_x=fetch_x, plans=plans),
        name="p1", grid=(n_tp // sp, ni),
        in_specs=[pl.BlockSpec((rows, d_model), lambda p, i: (base() + once(p, i), 0)),
                  fixed((CAR, d_model)), fixed((2, d_model)), own_layer(d_model, PC), own_layer(4, PC), fixed((2, PC)),
                  fixed((3 * heads, width))] + [hbm] * len(comm),
        out_specs=[pl.BlockSpec((rows, sp * PC), lambda p, i: (i, col(p))),
                   pl.BlockSpec((rows, NST), lambda p, i: (once(p, i), 0)),
                   pl.BlockSpec((heads, rows), lambda p, i: (0, once(p, i))),
                   hbm] + [hbm] * len(more),
        out_shape=outs + more,
        scratch_shapes=[
            vm((2 if fetch_x else 1, n_dp, sp, PC, PC), F32), vm((d_model, sp * PC), BF16), pltpu.SemaphoreType.DMA((3,)),
            vm((n_tp, SMALL, PC), F32), vm((heads, d_model), BF16), vm((2 * heads, PC), F32), vm((NST, sp * PC), F32),
            vm((CAR, d_model), BF16), vm((CAR, sp * PC), F32), vm((CAR, PC), F32), vm((heads, LANES), F32),
            vm((d_model // LANES * rows, LANES), F32), vm((n, d_model), BF16),
            vm((nb * (NST + SUB), 4 * SUB), BF16), vm((nb * (NST + SUB), 2 * SUB), BF16),
            vm((n, 4 * SUB), BF16), vm((n, 2 * SUB), BF16), vm((n, 4 * NST), BF16), vm((n, LANES), F32),
            vm((2 * nb, 2 * heads // 2, LANES), F32), vm((n, 2 * BLK), BF16), vm((NST, sp * PC), F32), pltpu.SemaphoreType.DMA((2,))]
        + dma(4 * SEMS) + (dma(8) if fetch_x else []),
        compiler_params=pltpu.CompilerParams(dimension_semantics=("arbitrary", "arbitrary"), vmem_limit_bytes=VMEM_CAP,
                                             collective_id=cid, has_side_effects=True),
        cost_estimate=pl.CostEstimate(flops=n * 70 * 10 ** 6, bytes_accessed=n * 12000, transcendentals=0),
    )(u, halo, nw, wbc, cbc, bbc, e3, *comm)


def p2_body(*refs, geom, layer, last):
    n_dp, n_tp, heads = geom
    (u_ref, nw_ref, wz_ref, wo_ref, sm_ref, y_ref, c_ref, ac_ref, s_ref, e3_ref), refs = refs[:10], refs[10:]
    (o_ref, f_ref, wzb, wob, s3, ubuf), refs = refs[:6], refs[6:]
    i = pl.program_id(0)
    width = PC * n_tp
    if last:
        fbuf, send, recv = refs
        dp, tp, _, c = here()
        partner = (dp, tp + 1 - 2 * c)

        def swap(k):
            return pltpu.make_async_remote_copy(
                src_ref=fbuf.at[k % 2], dst_ref=f_ref.at[pl.ds(pl.multiple_of(k * BLK2, BLK2), BLK2)],
                send_sem=send.at[k % 2], recv_sem=recv, device_id=partner, device_id_type=MESH)

        @pl.when(i == 0)
        def _():
            entry_barrier([partner])

        @pl.when(i > 1)
        def _():
            swap(i - 2).wait_send()

        @pl.when(i > 0)
        def _():
            swap(i - 1).start()

    @pl.when(i == 0)
    def _():
        for d in range(n_dp):
            for t in range(n_tp):
                a, b = slice(d * PC, (d + 1) * PC), slice(t * PC, (t + 1) * PC)
                wzb[a, b] = wz_ref[d, t].astype(BF16)
                wob[b, a] = wo_ref[d, t].astype(BF16)
        a, b, c_ = split3(jnp.where(here()[3] == 1, s_ref[...], 0.0))
        for k, (v, w) in enumerate(((a, a), (b, b), (c_, a))):
            s3[k] = rows_cat(v, w)

    u = u_ref[...].astype(F32)
    u = u if last else unmix(u, ubuf)
    h = rms(u, nw_ref[layer:layer + 1].astype(F32))
    c1, c2, c3 = split3(c_ref[...])
    c12, c13 = lanes_cat(c1, c2), lanes_cat(c1, c3)
    eT = rows_cat(*split3(jnp.exp2(ac_ref[...]))).T
    vs, ss = [], 0.0
    for t in range(n_tp):
        sl = slice(t * PC, (t + 1) * PC)
        z_ = round_bf16(dot(h, wzb[:, sl]))
        cor = dot(c12, s3[0, :, sl]) + dot(c12, s3[1, :, sl]) + dot(c13, s3[2, :, sl])
        v = (y_ref[:, sl] + cor * dot(eT, e3_ref[:, sl])) * silu(z_)
        ss = ss + jnp.sum(v * v, axis=-1, keepdims=True)
        vs.append(v)
    sc = lax.rsqrt(ss / width + EPS)
    g = lanes_cat(*[(v * sc * sm_ref[t, 5:6, :]).astype(BF16) for t, v in enumerate(vs)])
    un = round_bf16(u + dot(g, wob[...]))
    if not last:
        o_ref[...] = un.astype(BF16)
        f_ref[...] = un[BLK2 - CAR:]
    else:
        un = unmix(un, ubuf)
        fbuf[i % 2] = un
        o_ref[...] = un.astype(BF16)

        @pl.when(i == pl.num_programs(0) - 1)
        def _():
            swap(i).start()
            for k in range(2):
                swap(i - 1 + k).wait_send()
            pltpu.make_async_copy(f_ref, f_ref, recv).wait()


def p2(u, base, nw, wz, wo, sm, y, c, ac, s, e3, n, n_dp, n_tp, layer, last, cid):
    d_model, heads = u.shape[-1], PC // HD * n_tp
    width = PC * n_tp
    fixed = lambda shp: pl.BlockSpec(shp, lambda i: (0,) * len(shp), pipeline_mode=pl.Buffered(1))
    hbm = pl.BlockSpec(memory_space=pl.ANY)
    rows = lambda w: pl.BlockSpec((BLK2, w), lambda i: (i, 0))
    shape = lambda *s: jax.ShapeDtypeStruct(s, F32)
    vm = pltpu.VMEM
    outs = [jax.ShapeDtypeStruct((n, d_model), BF16)]
    specs = [rows(d_model)]
    if last:
        outs += [shape(n, d_model)]
        specs += [hbm]
    else:
        outs += [shape(CAR, d_model)]
        specs += [pl.BlockSpec((CAR, d_model), lambda i: (0, 0))]
    return pl.pallas_call(
        functools.partial(p2_body, geom=(n_dp, n_tp, heads), layer=layer, last=last),
        name="p2", grid=(n // BLK2,),
        in_specs=[pl.BlockSpec((BLK2, d_model), lambda i: (base() + i, 0)),
                  fixed((2, d_model)),
                  fixed((n_dp, n_tp, PC, PC)), fixed((n_dp, n_tp, PC, PC)),
                  pl.BlockSpec((n_tp, SMALL, PC), lambda i: (0, layer, 0), pipeline_mode=pl.Buffered(1)),
                  rows(width), rows(NST), pl.BlockSpec((heads, BLK2), lambda i: (0, i)),
                  fixed((NST, width)), fixed((3 * heads, width))],
        out_specs=specs, out_shape=outs,
        scratch_shapes=[vm((d_model, width), BF16), vm((width, d_model), BF16), vm((3, 2 * NST, width), BF16),
                        vm((d_model // LANES * BLK2, LANES), F32)]
        + ([vm((2, BLK2, d_model), F32), pltpu.SemaphoreType.DMA((2,)), pltpu.SemaphoreType.DMA] if last else []),
        compiler_params=pltpu.CompilerParams(dimension_semantics=("arbitrary",), vmem_limit_bytes=VMEM_CAP,
                                             collective_id=cid, has_side_effects=last),
        cost_estimate=pl.CostEstimate(flops=n * 30 * 10 ** 6, bytes_accessed=n * 12000, transcendentals=0),
    )(u, nw, wz, wo, sm, y, c, ac, s, e3)


def finish_body(own_ref, other_ref, o_ref):
    mine = pl.program_id(0) == here()[3]

    @pl.when(mine)
    def _():
        o_ref[...] = own_ref[...]

    @pl.when(jnp.logical_not(mine))
    def _():
        o_ref[...] = other_ref[...].astype(BF16)


def finish(own, other):
    n, d_model = own.shape
    rows = n // 3
    ni = n // rows
    pick = lambda w: (lambda j, i: (jnp.where((j == here()[3]) == w, i, ni - 1), 0))
    return pl.pallas_call(
        finish_body, name="finish", grid=(2, ni),
        in_specs=[pl.BlockSpec((rows, d_model), pick(True)), pl.BlockSpec((rows, d_model), pick(False))],
        out_specs=pl.BlockSpec((rows, d_model), lambda j, i: (j * ni + i, 0)),
        out_shape=jax.ShapeDtypeStruct((2 * n, d_model), BF16),
        compiler_params=pltpu.CompilerParams(dimension_semantics=("arbitrary", "arbitrary")),
        cost_estimate=pl.CostEstimate(flops=n * d_model, bytes_accessed=n * d_model * 8, transcendentals=0),
    )(own, other)


def small_rows(conv, bias, gate, skip, dtb, al, wdt):
    f = lambda v: v.astype(F32)
    n, hp = skip.shape
    wide = lambda v: jnp.broadcast_to(v[:, :, None], (n, hp, PC))
    one = lambda v: v.reshape(n, 1, PC)
    skip = jnp.broadcast_to(skip[:, :, None], (n, hp, HD))
    v = [f(conv), one(f(bias)), one(f(gate)), one(skip), jnp.zeros((n, 1, PC), F32), wide(dtb), wide(-jnp.exp(al) * LOG2E),
         f(wdt).transpose(0, 2, 1).reshape(n, -1, PC)]
    return jnp.concatenate(v, axis=1).reshape(-1, PC)


PLAN_X = "00020405030607040809"
PLAN_Z0 = "04080a0b0a0b0d0b0d0f"
PLAN_O0 = "080c0e100e1012101214"
PLAN_Y = "0d101113121315141516"
PLAN_Z1 = "0002040604060906080b"
PLAN_O1 = "06090b0e0b0e100d1013"


def solution(mesh):
    n_tp, n_dp = mesh.shape['tp'], mesh.shape['dp']
    rep, col, vec = P(), P(None, None, 'tp'), P(None, 'tp')
    in_specs = (P('dp'), rep, col, col, rep, col, col, rep, vec, rep, vec, vec, vec, vec, P(None, 'tp', None))

    def device_forward(hidden, norm_w, w_z, w_x, w_bc, w_dt, conv_x, conv_bc, bias_x, bias_bc, dt_bias, a_log, d_skip, gate_w, w_out):
        u = hidden[0]
        steps, d_model = u.shape
        n = steps // 2
        core = lax.axis_index('tp') % 2
        e3 = expand_mat(dt_bias.shape[1] * n_tp)
        up = [(2 * k, 2 * k + 1) for k in range(n_tp // 2)]
        ax, az, ao = w_x.astype(F32), w_z.astype(F32), w_out.astype(F32)
        small = small_rows(conv_x, bias_x, gate_w, d_skip, dt_bias, a_log, w_dt)
        tail = u[n - SUB:n].astype(F32).reshape(8, 8, d_model).transpose(1, 0, 2).reshape(SUB, d_model)[SUB - CAR:]
        halo = jnp.where(core == 1, tail, 0.0)
        half = lambda blk: (lambda: lax.axis_index('tp') % 2 * (n // blk))
        none = lambda: 0
        common = (n, n_dp, n_tp)
        bc = (norm_w, w_bc, conv_bc, bias_bc, e3)

        y, c, ac, s, _, gs, gx, gz, go = p1(u, half(BLK * NBS), halo, *bc, (ax, small, az, ao), *common, False, 0, True,
                                         (PLAN_Z0, PLAN_O0, PLAN_X, PLAN_Y), 1)
        u, f = p2(u, half(BLK2), norm_w, gz, go, gs, y, c, ac, s, e3, *common, 0, False, None)
        halo = lax.ppermute(f, 'tp', up)
        y, c, ac, s, gz, go = p1(u, none, halo, *bc, (ax, gx, gs, az, ao), *common, True, 1, False, (PLAN_Z1, PLAN_O1), 2)
        own, other = p2(u, none, norm_w, gz, go, gs, y, c, ac, s, e3, *common, 1, True, 3)
        return finish(own, other)[None]

    return jax.shard_map(device_forward, mesh=mesh, in_specs=in_specs, out_specs=P('dp'), check_vma=False)
```

```python
import functools
import jax
import jax.numpy as jnp
import numpy as np
from jax import lax
from jax.experimental import pallas as pl
from jax.experimental.pallas import tpu as pltpu
from jax.sharding import PartitionSpec as P

EPS = 1e-5
LOG2E = 1.4426950408889634
HI = lax.Precision.HIGHEST
F32 = jnp.float32
BF16 = jnp.bfloat16
MESH = pl.DeviceIdType.MESH
LANES = 128
BLK = 128
SUB = 64
BLK2 = 256
NBS = 4
PC = 256
HD = 64
NST = 128
CAR = 24
SMALL = 32
ORDER = (1, 3, 2)
EARLY = 6
SEMS = 26
VMEM_CAP = 60 << 20


def silu(v):
    return v / (1.0 + jnp.exp2(v * -LOG2E))


def split3(v):
    a = v.astype(BF16)
    r = v - a.astype(F32)
    b = r.astype(BF16)
    return a, b, (r - b.astype(F32)).astype(BF16)


def round_bf16(v):
    return v.astype(BF16).astype(F32)


def rms(u, nw):
    return (u * lax.rsqrt(jnp.mean(u * u, axis=-1, keepdims=True) + EPS) * nw).astype(BF16)


def dot(a, b, prec=None):
    return jnp.dot(a, b, preferred_element_type=F32, precision=prec)


def dott(a, b, prec=None):
    return lax.dot_general(a, b, (((1,), (1,)), ((), ())), preferred_element_type=F32, precision=prec)


def rows_cat(*v):
    return jnp.concatenate(v, axis=0)


def lanes_cat(*v):
    return jnp.concatenate(v, axis=1)


def time_of(r):
    return 8 * (r % 8) + r // 8


def roll8(v):
    c = v.shape[-1]
    return pltpu.roll(v.reshape(CAR // 8, 8, c), 1, 1).reshape(CAR, c)


def conv_block(cur, prev, taps, bias, first):
    now = roll8(cur[SUB - CAR:])
    sh = jnp.where(first, prev, now)
    out = bias + cur * taps[-1]
    for k in range(1, 4):
        out = out + rows_cat(sh[CAR - 8 * k:], cur[:SUB - 8 * k]) * taps[3 - k]
    return out, now


def unmix(v, buf):
    n, c = v.shape
    for j in range(c // LANES):
        buf[n * j:n * (j + 1), :] = v[:, LANES * j:LANES * (j + 1)]
    cols = [rows_cat(*[buf[pl.ds(n * j + b + k, 8, stride=8), :] for b in range(0, n, SUB) for k in range(8)])
            for j in range(c // LANES)]
    return lanes_cat(*cols)


def head_row(h, heads):
    return (h % 2) * (heads // 2) + h // 2


def expand_mat(heads):
    order = sorted(range(heads), key=lambda h: head_row(h, heads))
    one = np.repeat(np.eye(heads)[order], HD, axis=1)
    return jnp.asarray(np.tile(one, (3, 1)), BF16)


def kcat6(parts):
    a, b, c = parts
    return lanes_cat(a, b, c, a), lanes_cat(b, a)


def kcat6r(parts):
    a, b, c = parts
    return rows_cat(a, a, a, b), rows_cat(b, c)


def block_diag(x, lo, hi):
    z = jnp.zeros((x.shape[0], LANES), BF16)
    l, r = x[:, :LANES], x[:, LANES:]
    return rows_cat(lanes_cat(l * lo, z), lanes_cat(l * hi, z), lanes_cat(z, r * lo), lanes_cat(z, r * hi))


def here():
    dp, tp = lax.axis_index('dp'), lax.axis_index('tp')
    return dp, tp, tp // 2, tp % 2


def source(dz):
    return (here()[2] + 4 - dz) % 4


class Gather:
    def __init__(self, piece, g, send, recv, base):
        self.piece, self.g, self.send, self.recv, self.base = piece, g, send, recv, base
        self.dp, self.tp, self.z, self.c = here()
        x, y = self.dp // 2, self.dp % 2
        self.side = ((1 - x) * 2 + y, x * 2 + 1 - y)
        self.partner = (self.dp, 2 * self.z + 1 - self.c)
        self.quarters = g.shape[0]

    def rdma(self, k, src, dst, dev):
        return pltpu.make_async_remote_copy(src_ref=src, dst_ref=dst, send_sem=self.send.at[self.base + k],
                                            recv_sem=self.recv.at[self.base + k], device_id=dev, device_id_type=MESH)

    def own(self, q):
        return self.rdma(4 + q, self.piece(q), self.g.at[q, self.tp], self.partner)

    def line(self, dz):
        return self.rdma(7 + dz, self.piece(self.dp), self.g.at[self.dp, self.tp],
                         (self.dp, 2 * ((self.z + dz) % 4) + self.c))

    def cross(self, dz, n):
        ref = self.g.at[self.dp, 2 * source(dz) + self.c]
        return self.rdma(9 + 2 * dz + n, ref, ref, (self.side[n], self.tp))

    def relay(self, dz, n):
        half = self.g.shape[2] // 2
        ref = self.g.at[self.side[n], 2 * source(dz) + self.c, pl.ds(n * half, half)]
        return self.rdma(15 + 2 * dz + n, ref, ref, (self.side[1 - n], self.tp))

    def over(self, dz):
        ref = self.g.at[:, 2 * source(dz) + self.c]
        return self.rdma(22 + dz, ref, ref, self.partner)

    def peers(self):
        return ([(self.dp, 2 * ((self.z + dz) % 4) + self.c) for dz in ORDER]
                + [(p, self.tp) for p in self.side] + [self.partner])

    def start(self):
        for q in range(self.quarters):
            self.own(q).start()
        for dz in ORDER:
            self.line(dz).start()

    def spread(self, dz):
        self.line(dz).wait_recv()
        for n in range(2):
            self.cross(dz, n).start()

    def pass_on(self, dz):
        for n in range(2):
            self.cross(dz, n).wait_recv()
            self.relay(dz, n).start()

    def hand(self, dz):
        for n in range(2):
            self.relay(dz, n).wait_recv()
        self.over(dz).start()

    def settle_own(self):
        for q in range(self.quarters):
            self.own(q).wait_recv()

    def settle(self, dz):
        self.over(dz).wait_recv()

    def drain(self):
        for q in range(self.quarters):
            self.own(q).wait_send()
        for dz in ORDER:
            self.line(dz).wait_send()
            self.over(dz).wait_send()
            for n in range(2):
                self.cross(dz, n).wait_send()
                self.relay(dz, n).wait_send()

    def plan(self, s):
        s = bytes.fromhex(s)
        acts = [(s[0], self.start)]
        for k, f in enumerate((self.spread, self.pass_on, self.hand)):
            acts += [(s[1 + 3 * k + j], functools.partial(f, dz)) for j, dz in enumerate(ORDER)]
        return acts

    def finish(self):
        self.settle_own()
        for dz in ORDER:
            self.settle(dz)
        self.drain()


class Small:
    def __init__(self, a, g, send, recv):
        self.a, self.g, self.send, self.recv = a, g, send, recv
        self.dp, self.tp, _, _ = here()

    def copy(self, k):
        return pltpu.make_async_remote_copy(src_ref=self.a, dst_ref=self.g.at[self.tp], send_sem=self.send.at[k],
                                            recv_sem=self.recv.at[k], device_id=(self.dp, (self.tp + k) % 8),
                                            device_id_type=MESH)

    def local(self):
        return pltpu.make_async_copy(self.a, self.g.at[self.tp], self.send.at[0])

    def peers(self):
        return [(self.dp, (self.tp + k) % 8) for k in range(1, 8)]

    def start(self):
        self.local().start()
        for k in range(1, 8):
            self.copy(k).start()

    def finish(self):
        self.local().wait()
        for k in range(1, 8):
            self.copy(k).wait()


def entry_barrier(peers):
    sem = pltpu.get_barrier_semaphore()
    for p in peers:
        pl.semaphore_signal(sem, inc=1, device_id=p, device_id_type=MESH)
    pl.semaphore_wait(sem, len(peers))


def at_steps(step, acts):
    for k in sorted({k for k, _ in acts}):
        @pl.when(step == k)
        def _():
            for j, f in acts:
                if j == k:
                    f()


def piece_rows(ref, layer):
    return lambda q: ref.at[layer, pl.ds(q * PC, PC)]


def piece_cols(ref, layer):
    return lambda q: ref.at[layer, :, pl.ds(pl.multiple_of(q * PC, PC) if not isinstance(q, int) else q * PC, PC)]


def p1_body(*refs, geom, mixed, layer, fetch_x, plans):
    n_dp, n_tp, heads, nb, nbs, sp = geom
    (u_ref, halo_ref, nw_ref, wbc_ref, cbc_ref, bbc_ref, e3_ref, own_ref), refs = refs[:8], refs[8:]
    row = slice(layer, layer + 1)
    nw, cbc, bbc = nw_ref[row].astype(F32), cbc_ref[...].astype(F32), bbc_ref[row].astype(F32)
    if fetch_x:
        (ax, asm, az, ao), (y_ref, c_ref, ac_ref, s_in), (gx, gs, gy, gz, go), refs = refs[:4], refs[4:8], refs[8:13], refs[13:]
    else:
        (gx, gs, az, ao), (y_ref, c_ref, ac_ref, s_in), (gz, go), refs = refs[:4], refs[4:8], refs[8:10], refs[10:]
    (wf, wb, wsem, sm, wdt, cst, st, hcar, xcar, qcar, aoff, ubuf, h_s, la1_s, la2_s, lb1_s, lb2_s, cc_s, cbd_s, row_s, aw_s,
     sbuf, hsem, send, recv), sems = refs[:25], refs[25:]
    p, i = pl.program_id(0), pl.program_id(1)
    np_, ni = pl.num_programs(0), pl.num_programs(1)
    step = p * ni + i
    d_model = u_ref.shape[-1]
    by_z = sp < n_tp
    zs_of = (lambda p: source(p + p // 2 * (1 - 2 * (p % 2)))) if by_z else (lambda p: 0)
    zs = zs_of(p)
    upper = here()[3] == 1

    def state_out(p):
        dp, tp, _, c = here()
        cols = pl.ds(pl.multiple_of(2 * zs_of(p) * PC, PC), sp * PC)
        return pltpu.make_async_remote_copy(src_ref=sbuf, dst_ref=s_in.at[:, cols], send_sem=hsem.at[0], recv_sem=hsem.at[1],
                                            device_id=(dp, tp + 1 - 2 * c), device_id_type=MESH)

    zg = Gather(piece_rows(az, layer), gz, send, recv, 0)
    og = Gather(piece_cols(ao, layer), go, send, recv, SEMS)
    acts = zg.plan(plans[0]) + og.plan(plans[1])
    if fetch_x:
        xg = Gather(piece_rows(ax, layer), gx, send, recv, 2 * SEMS)
        small = Small(asm, gs, *sems)
        yg = Gather(piece_rows(ax, layer + 1), gy, send, recv, 3 * SEMS)
        acts += xg.plan(plans[2]) + yg.plan(plans[3])

    def load_w(slot, zsrc):
        return pltpu.make_async_copy(gx.at[:, pl.ds(2 * zsrc, sp)], wf.at[slot], wsem.at[slot])

    def load_first():
        _, tp, _, c = here()
        return pltpu.make_async_copy(gx.at[:, tp + 1 - 2 * c], wf.at[0, :, 1 - c], wsem.at[0]) if by_z else load_w(0, 0)

    @pl.when(step == 0)
    def _():
        entry_barrier((small.peers() + [(s, here()[1]) for s in zg.side]) if fetch_x else zg.peers())
        if fetch_x:
            small.start()
    at_steps(step, acts)

    @pl.when(step == 0)
    def _():
        if fetch_x:
            small.finish()
            xg.settle_own()
        load_first().start()
        cp = pltpu.make_async_copy(gs.at[:, pl.ds(layer * SMALL, SMALL)], sm, wsem.at[2])
        cp.start()
        cp.wait()
        kc = d_model // PC
        hp = heads // n_tp
        for t in range(n_tp):
            for k in range(hp):
                r = head_row(hp * t + k, heads)
                for c in range(kc):
                    wdt[r:r + 1, c * PC:(c + 1) * PC] = sm[t, 16 + kc * k + c:17 + kc * k + c, :].astype(BF16)
                cst[r:r + 1, :] = sm[t, 8 + k:9 + k, :]
                cst[heads + r:heads + r + 1, :] = sm[t, 12 + k:13 + k, :]
        aoff[...] = jnp.zeros_like(aoff)
        hh = rms(halo_ref[...], nw)
        hcar[...] = hh
        qcar[...] = roll8(round_bf16(dot(hh, wbc_ref[...])))

    first = lax.broadcasted_iota(jnp.int32, (CAR, PC), 0) % 8 == 0

    def conv(cur, prev, taps, bias):
        a, now = conv_block(cur[:SUB], prev, taps, bias, first)
        b, now = conv_block(cur[SUB:], now, taps, bias, first)
        return silu(rows_cat(a, b)), now

    ri = lax.broadcasted_iota(jnp.int32, (BLK, BLK), 0)
    ci = lax.broadcasted_iota(jnp.int32, (BLK, BLK), 1)

    def prologue(h, b, hook):
        q0 = dot(h, wbc_ref[...])
        rT = round_bf16(dott(wdt[...], h))
        hook(h, 2)
        bc, qcar[...] = conv(round_bf16(q0), qcar[...],
                             [cbc[k:k + 1] for k in range(4)], bbc)
        bmat, cmat = bc[:, :NST], bc[:, NST:]
        here_rows = slice(b * BLK, (b + 1) * BLK)
        c_ref[here_rows, :] = cmat
        pre = rT + cst[:heads, :BLK]
        dtT = jnp.maximum(pre, 0.0) + jnp.log1p(jnp.exp(-jnp.abs(pre)))
        aT = dtT * cst[heads:, :BLK]
        tr, tc = ri // SUB * SUB + time_of(ri % SUB), ci // SUB * SUB + time_of(ci % SUB)
        acT = dot(aT, jnp.where(tr <= tc, 1.0, 0.0), HI)
        mid, alast = acT[:, SUB - 1:SUB], acT[:, BLK - 1:BLK]
        low = ci[:heads] < SUB
        wT = dtT * jnp.exp2(jnp.where(low, mid, alast) - acT)
        pad = jnp.zeros((BLK - 3 * heads, BLK), BF16)
        a3, w3 = rows_cat(*split3(acT), pad).T, rows_cat(*split3(wT), pad).T
        ac_ref[:, here_rows] = acT + aoff[:, :1]
        aoff[...] = aoff[...] + alast

        def pair_rows(v):
            ev, od = v[:heads // 2], v[heads // 2:]
            l = low[:heads // 2]
            return jnp.where(l, ev, pltpu.roll(od, SUB, 1)), jnp.where(l, pltpu.roll(ev, SUB, 1), od)

        rows = [rows_cat(*[w for zz in zip(*[jnp.split(v, n_tp // 2) for v in ad]) for w in zz])
                for ad in zip(pair_rows(acT), pair_rows(dtT))]
        hook(h, 4)
        cb = dott(cmat, bmat, HI)
        hook(h, EARLY)
        lowr, tri = ci[:SUB] < SUB, time_of(ri[:SUB]) >= time_of(ci[:SUB] % SUB)
        ca, cd = cb[:SUB], cb[SUB:]
        cbd = [jnp.where(tri, jnp.where(lowr, ca, pltpu.roll(ca, SUB, 1)), 0.0),
               jnp.where(tri, jnp.where(lowr, pltpu.roll(cd, SUB, 1), cd), 0.0)]
        bT = bmat.T
        la = kcat6(split3(rows_cat(bT[:, :SUB], cd[:, :SUB])))
        lb = kcat6(split3(pltpu.roll(bT, SUB, 1)[:, :SUB]))
        c1, c2, c3 = split3(cmat)
        return h, a3, w3, rows, cbd, la, lb, (lanes_cat(c1, c2), lanes_cat(c1, c3))

    def spots(b):
        j = i * nbs + b
        at = lambda r: pl.ds(pl.multiple_of(j * r, SUB), r)
        return j, at(BLK), at(NST + SUB)

    def keep(b, vals):
        h, a3, w3, rows, cbd, la, lb, cc = vals
        j, blk, big = spots(b)
        h_s[blk, :] = h
        aw_s[blk, :] = lanes_cat(a3, w3)
        for half in range(2):
            row_s[2 * j + half] = rows[half]
        cbd_s[blk, :] = rows_cat(*cbd)
        la1_s[big, :], la2_s[big, :] = la
        lb1_s[blk, :], lb2_s[blk, :] = lb
        cc_s[blk, :] = lanes_cat(*cc)

    def kept(b):
        j, blk, big = spots(b)
        eight = pl.ds(pl.multiple_of(8 * zs, 8), 8)
        return (None, aw_s[blk, :BLK], aw_s[blk, BLK:], [row_s[2 * j + half, eight, :] for half in range(2)],
                [cbd_s[pl.ds(pl.multiple_of(j * BLK + half * SUB, SUB), SUB), :] for half in range(2)],
                (la1_s[big, :], la2_s[big, :]), (lb1_s[blk, :], lb2_s[blk, :]), (cc_s[blk, :2 * NST], cc_s[blk, 2 * NST:]))


    def all_prologues(hook):
        u = u_ref[...].astype(F32)
        h = rms(u if mixed else unmix(u, ubuf), nw)
        return [prologue(h[b * BLK:(b + 1) * BLK], b, hook) for b in range(nbs)]

    if by_z:
        @pl.when(p == 0)
        def _():
            for b, v in enumerate(all_prologues(lambda h, k: None)):
                keep(b, v)

    @pl.when(i == 0)
    def _():
        slot = p % 2 if by_z else 0

        @pl.when(p == 0)
        def _():
            load_first().wait()

        @pl.when(p > 0)
        def _():
            load_w(slot, zs).wait()
        for q in range(n_dp):
            for k in range(sp):
                wb[q * PC:(q + 1) * PC, k * PC:(k + 1) * PC] = wf[slot, q, k].astype(BF16)

        @pl.when(p == 0)
        def _():
            _, tp, _, c = here()
            wb[:, pl.ds(pl.multiple_of((c if by_z else tp) * PC, PC), PC)] = own_ref[...].astype(BF16)

        @pl.when((p > 0) & jnp.logical_not(upper))
        def _():
            state_out(p - 1).start()
        xcar[...] = roll8(round_bf16(dot(hcar[...], wb[...])))
        st[...] = jnp.zeros_like(st)

    @pl.when((i == ni - 1) & (p < np_ - 1))
    def _():
        nd = p + 1
        nd = nd + nd // 2 * (1 - 2 * (nd % 2))
        if fetch_x:
            for d in ORDER:
                pl.when(nd == d)(functools.partial(xg.settle, d))
        load_w((p + 1) % 2, source(nd)).start()

    lane = lax.broadcasted_iota(jnp.int32, (SUB, LANES), 1)
    lo = jnp.where(lane < HD, 1.0, 0.0).astype(BF16)
    hi = jnp.where(lane < HD, 0.0, 1.0).astype(BF16)
    x0 = {}

    def proj(hs, upto):
        for k in range(len(x0), min(sp, upto)):
            x0[k] = dot(hs, wb[:, k * PC:(k + 1) * PC])

    if by_z:
        vals = [kept(b) for b in range(nbs)]
        hs = h_s[pl.ds(pl.multiple_of(i * nbs * BLK, BLK), nbs * BLK), :]
        proj(hs, sp)
    else:
        vals = all_prologues(proj)
        hs = vals[0][0]

    def lanes_of(k):
        return slice(k * PC, (k + 1) * PC), pl.ds(pl.multiple_of((2 * zs + k) * PC, PC), PC)

    def pre(b, k):
        (sl, gl), (_, a3, w3, _, _, _, _, (c12, c13)) = lanes_of(k), vals[b]
        s1, s2, s3 = split3(st[:, sl])
        inter = dot(c12, rows_cat(s1, s1)) + dot(c12, rows_cat(s2, s2)) + dot(c13, rows_cat(s3, s1))
        n3 = e3_ref.shape[0]
        wide = lambda v: dot(v[:, :n3], e3_ref[:, gl])
        acx, wx = wide(a3), wide(w3)
        proj(hs, k + EARLY + 1)
        return x0[k][b * BLK:(b + 1) * BLK], acx, wx, inter

    def mid_(b, k, x0, acx, wx, inter):
        (sl, _), (_, _, _, rws, cbds, _, _, _) = lanes_of(k), vals[b]
        t = 2 * zs + k
        base = 0 if by_z else k // 2 * 8
        x, xcar[:, sl] = conv(round_bf16(x0), xcar[:, sl], [sm[t, r:r + 1, :] for r in range(4)], sm[t, 4:5, :])
        xw = split3(x * wx)
        r = kcat6r([v[:SUB] for v in xw]) + kcat6r([v[SUB:] for v in xw])
        ms, xs = [], []
        for half in range(2):
            rows = slice(half * SUB, (half + 1) * SUB)
            row, cbd = rws[half][base:base + 8], cbds[half]
            m = []
            for g in range(2):
                seg = acx[rows, g * LANES:(g + 1) * LANES] - row[2 * (k % 2) + g:2 * (k % 2) + g + 1]
                m.append(jnp.exp2(jnp.minimum(seg, 0.0)) * cbd * row[4 + 2 * (k % 2) + g:5 + 2 * (k % 2) + g])
            ms.append(split3(lanes_cat(*m)))
            xs.append([block_diag(v, lo, hi) for v in split3(x[rows])])
        return x, acx, inter, r, ms, xs

    def fin(b, k, x, acx, inter, r, ms, xs):
        (sl, _), (_, _, _, _, _, la, lb, _) = lanes_of(k), vals[b]
        ra = dot(la[0], r[0]) + dot(la[1], r[1])
        rb = dot(lb[0], r[2]) + dot(lb[1], r[3])
        am, al = acx[SUB - 1:SUB], acx[BLK - 1:BLK]
        st[:, sl] = st[:, sl] * jnp.exp2(al) + ra[:NST] * jnp.exp2(al - am) + rb
        skip = sm[2 * zs + k, 6:7, :]
        for half in range(2):
            rows = slice(half * SUB, (half + 1) * SUB)
            (m1, m2, m3), (x1, x2, x3) = ms[half], xs[half]
            r1 = dot(rows_cat(m1, m2, m3), x1)
            r2 = dot(rows_cat(m1, m2), x2)
            y = r1[:SUB] + r1[SUB:2 * SUB] + r1[2 * SUB:] + r2[:SUB] + r2[SUB:] + dot(m1, x3)
            y = y + inter[rows] * jnp.exp2(acx[rows])
            if half:
                y = y + ra[NST:] * jnp.exp2(acx[rows] - am)
            y_ref[b * BLK + half * SUB:b * BLK + (half + 1) * SUB, sl] = y + skip * x[rows]

    units = [(b, k) for b in range(nbs) for k in range(sp)]
    m = mid_(*units[0], *pre(*units[0]))
    for a, nxt in zip(units, units[1:] + [None]):
        if nxt:
            v = pre(*nxt)
        fin(*a, *m)
        if nxt:
            m = mid_(*nxt, *v)

    @pl.when(i == ni - 1)
    def _():
        @pl.when((p > 0) & jnp.logical_not(upper))
        def _():
            state_out(p - 1).wait_send()
        sbuf[...] = st[...]

    @pl.when(step == np_ * ni - 1)
    def _():
        zg.finish()
        og.finish()
        if fetch_x:
            xg.drain()
            yg.finish()

        @pl.when(jnp.logical_not(upper))
        def _():
            state_out(p).start()
            state_out(p).wait_send()

        @pl.when(upper)
        def _():
            pltpu.make_async_copy(s_in, s_in, hsem.at[1]).wait()


def p1(u, base, halo, nw, wbc, cbc, bbc, e3, own, comm, n, n_dp, n_tp, mixed, layer, fetch_x, plans, cid):
    d_model, heads = u.shape[-1], PC // HD * n_tp
    sp, nbs = (2, NBS) if fetch_x else (n_tp, 1)
    width, nb, rows = PC * n_tp, n // BLK, BLK * nbs
    ni = nb // nbs
    fixed = lambda shp: pl.BlockSpec(shp, lambda p, i: (0,) * len(shp), pipeline_mode=pl.Buffered(1))
    own_layer = lambda *shp: pl.BlockSpec((None,) + shp, lambda p, i: (layer, 0, 0), pipeline_mode=pl.Buffered(1))
    once = lambda p, i: jnp.where(p == 0, i, ni - 1)
    col = (lambda p: source(p + p // 2 * (1 - 2 * (p % 2)))) if fetch_x else (lambda p: 0)
    hbm = pl.BlockSpec(memory_space=pl.ANY)
    gathered = lambda r: jax.ShapeDtypeStruct((n_dp, n_tp, r, PC), F32)
    outs = [jax.ShapeDtypeStruct((n, width), F32), jax.ShapeDtypeStruct((n, NST), F32),
            jax.ShapeDtypeStruct((heads, n), F32), jax.ShapeDtypeStruct((NST, width), F32)]
    more = ([gathered(PC), jax.ShapeDtypeStruct((n_tp,) + comm[1].shape, F32), gathered(PC)] if fetch_x else []) + [gathered(PC)] * 2
    vm = pltpu.VMEM
    dma = lambda k: [pltpu.SemaphoreType.DMA((k,))] * 2
    return pl.pallas_call(
        functools.partial(p1_body, geom=(n_dp, n_tp, heads, nb, nbs, sp), mixed=mixed, layer=layer, fetch_x=fetch_x, plans=plans),
        name="p1", grid=(n_tp // sp, ni),
        in_specs=[pl.BlockSpec((rows, d_model), lambda p, i: (base() + once(p, i), 0)),
                  fixed((CAR, d_model)), fixed((2, d_model)), own_layer(d_model, PC), own_layer(4, PC), fixed((2, PC)),
                  fixed((3 * heads, width)), own_layer(d_model, PC)] + [hbm] * len(comm),
        out_specs=[pl.BlockSpec((rows, sp * PC), lambda p, i: (i, col(p))),
                   pl.BlockSpec((rows, NST), lambda p, i: (once(p, i), 0)),
                   pl.BlockSpec((heads, rows), lambda p, i: (0, once(p, i))),
                   hbm] + [hbm] * len(more),
        out_shape=outs + more,
        scratch_shapes=[
            vm((2 if fetch_x else 1, n_dp, sp, PC, PC), F32), vm((d_model, sp * PC), BF16), pltpu.SemaphoreType.DMA((3,)),
            vm((n_tp, SMALL, PC), F32), vm((heads, d_model), BF16), vm((2 * heads, PC), F32), vm((NST, sp * PC), F32),
            vm((CAR, d_model), BF16), vm((CAR, sp * PC), F32), vm((CAR, PC), F32), vm((heads, LANES), F32),
            vm((d_model // LANES * rows, LANES), F32), vm((n, d_model), BF16),
            vm((nb * (NST + SUB), 4 * SUB), BF16), vm((nb * (NST + SUB), 2 * SUB), BF16),
            vm((n, 4 * SUB), BF16), vm((n, 2 * SUB), BF16), vm((n, 4 * NST), BF16), vm((n, LANES), F32),
            vm((2 * nb, 2 * heads // 2, LANES), F32), vm((n, 2 * BLK), BF16), vm((NST, sp * PC), F32), pltpu.SemaphoreType.DMA((2,))]
        + dma(4 * SEMS) + (dma(8) if fetch_x else []),
        compiler_params=pltpu.CompilerParams(dimension_semantics=("arbitrary", "arbitrary"), vmem_limit_bytes=VMEM_CAP,
                                             collective_id=cid, has_side_effects=True),
        cost_estimate=pl.CostEstimate(flops=n * 70 * 10 ** 6, bytes_accessed=n * 12000, transcendentals=0),
    )(u, halo, nw, wbc, cbc, bbc, e3, own, *comm)


def p2_body(*refs, geom, layer, last):
    n_dp, n_tp, heads = geom
    (u_ref, nw_ref, wz_ref, wo_ref, ownz_ref, owno_ref, sm_ref, y_ref, c_ref, ac_ref, s_ref, e3_ref), refs = refs[:12], refs[12:]
    (o_ref, f_ref, wzb, wob, s3, ubuf), refs = refs[:6], refs[6:]
    i = pl.program_id(0)
    width = PC * n_tp
    if last:
        fbuf, send, recv = refs
        dp, tp, _, c = here()
        partner = (dp, tp + 1 - 2 * c)

        def swap(k):
            return pltpu.make_async_remote_copy(
                src_ref=fbuf.at[k % 2], dst_ref=f_ref.at[pl.ds(pl.multiple_of(k * BLK2, BLK2), BLK2)],
                send_sem=send.at[k % 2], recv_sem=recv, device_id=partner, device_id_type=MESH)

        @pl.when(i == 0)
        def _():
            entry_barrier([partner])

        @pl.when(i > 1)
        def _():
            swap(i - 2).wait_send()

        @pl.when(i > 0)
        def _():
            swap(i - 1).start()

    @pl.when(i == 0)
    def _():
        for d in range(n_dp):
            for t in range(n_tp):
                a, b = slice(d * PC, (d + 1) * PC), slice(t * PC, (t + 1) * PC)
                wzb[a, b] = wz_ref[d, t].astype(BF16)
                wob[b, a] = wo_ref[d, t].astype(BF16)
        mine = pl.ds(pl.multiple_of(here()[1] * PC, PC), PC)
        wzb[:, mine] = ownz_ref[...].astype(BF16)
        wob[mine, :] = owno_ref[...].astype(BF16)
        a, b, c_ = split3(jnp.where(here()[3] == 1, s_ref[...], 0.0))
        for k, (v, w) in enumerate(((a, a), (b, b), (c_, a))):
            s3[k] = rows_cat(v, w)

    u = u_ref[...].astype(F32)
    u = u if last else unmix(u, ubuf)
    h = rms(u, nw_ref[layer:layer + 1].astype(F32))
    c1, c2, c3 = split3(c_ref[...])
    c12, c13 = lanes_cat(c1, c2), lanes_cat(c1, c3)
    eT = rows_cat(*split3(jnp.exp2(ac_ref[...]))).T
    vs, ss = [], 0.0
    for t in range(n_tp):
        sl = slice(t * PC, (t + 1) * PC)
        z_ = round_bf16(dot(h, wzb[:, sl]))
        cor = dot(c12, s3[0, :, sl]) + dot(c12, s3[1, :, sl]) + dot(c13, s3[2, :, sl])
        v = (y_ref[:, sl] + cor * dot(eT, e3_ref[:, sl])) * silu(z_)
        ss = ss + jnp.sum(v * v, axis=-1, keepdims=True)
        vs.append(v)
    sc = lax.rsqrt(ss / width + EPS)
    g = lanes_cat(*[(v * sc * sm_ref[t, 5:6, :]).astype(BF16) for t, v in enumerate(vs)])
    un = round_bf16(u + dot(g, wob[...]))
    if not last:
        o_ref[...] = un.astype(BF16)
        f_ref[...] = un[BLK2 - CAR:]
    else:
        un = unmix(un, ubuf)
        fbuf[i % 2] = un
        o_ref[...] = un.astype(BF16)

        @pl.when(i == pl.num_programs(0) - 1)
        def _():
            swap(i).start()
            for k in range(2):
                swap(i - 1 + k).wait_send()
            pltpu.make_async_copy(f_ref, f_ref, recv).wait()


def p2(u, base, nw, wz, wo, az, ao, sm, y, c, ac, s, e3, n, n_dp, n_tp, layer, last, cid):
    d_model, heads = u.shape[-1], PC // HD * n_tp
    width = PC * n_tp
    fixed = lambda shp: pl.BlockSpec(shp, lambda i: (0,) * len(shp), pipeline_mode=pl.Buffered(1))
    own_layer = lambda *shp: pl.BlockSpec((None,) + shp, lambda i: (layer, 0, 0), pipeline_mode=pl.Buffered(1))
    hbm = pl.BlockSpec(memory_space=pl.ANY)
    rows = lambda w: pl.BlockSpec((BLK2, w), lambda i: (i, 0))
    shape = lambda *s: jax.ShapeDtypeStruct(s, F32)
    vm = pltpu.VMEM
    outs = [jax.ShapeDtypeStruct((n, d_model), BF16)]
    specs = [rows(d_model)]
    if last:
        outs += [shape(n, d_model)]
        specs += [hbm]
    else:
        outs += [shape(CAR, d_model)]
        specs += [pl.BlockSpec((CAR, d_model), lambda i: (0, 0))]
    return pl.pallas_call(
        functools.partial(p2_body, geom=(n_dp, n_tp, heads), layer=layer, last=last),
        name="p2", grid=(n // BLK2,),
        in_specs=[pl.BlockSpec((BLK2, d_model), lambda i: (base() + i, 0)),
                  fixed((2, d_model)),
                  fixed((n_dp, n_tp, PC, PC)), fixed((n_dp, n_tp, PC, PC)), own_layer(d_model, PC), own_layer(PC, d_model),
                  pl.BlockSpec((n_tp, SMALL, PC), lambda i: (0, layer, 0), pipeline_mode=pl.Buffered(1)),
                  rows(width), rows(NST), pl.BlockSpec((heads, BLK2), lambda i: (0, i)),
                  fixed((NST, width)), fixed((3 * heads, width))],
        out_specs=specs, out_shape=outs,
        scratch_shapes=[vm((d_model, width), BF16), vm((width, d_model), BF16), vm((3, 2 * NST, width), BF16),
                        vm((d_model // LANES * BLK2, LANES), F32)]
        + ([vm((2, BLK2, d_model), F32), pltpu.SemaphoreType.DMA((2,)), pltpu.SemaphoreType.DMA] if last else []),
        compiler_params=pltpu.CompilerParams(dimension_semantics=("arbitrary",), vmem_limit_bytes=VMEM_CAP,
                                             collective_id=cid, has_side_effects=last),
        cost_estimate=pl.CostEstimate(flops=n * 30 * 10 ** 6, bytes_accessed=n * 12000, transcendentals=0),
    )(u, nw, wz, wo, az, ao, sm, y, c, ac, s, e3)


def finish_body(own_ref, other_ref, o_ref):
    mine = pl.program_id(0) == here()[3]

    @pl.when(mine)
    def _():
        o_ref[...] = own_ref[...]

    @pl.when(jnp.logical_not(mine))
    def _():
        o_ref[...] = other_ref[...].astype(BF16)


def finish(own, other):
    n, d_model = own.shape
    rows = n // 3
    ni = n // rows
    pick = lambda w: (lambda j, i: (jnp.where((j == here()[3]) == w, i, ni - 1), 0))
    return pl.pallas_call(
        finish_body, name="finish", grid=(2, ni),
        in_specs=[pl.BlockSpec((rows, d_model), pick(True)), pl.BlockSpec((rows, d_model), pick(False))],
        out_specs=pl.BlockSpec((rows, d_model), lambda j, i: (j * ni + i, 0)),
        out_shape=jax.ShapeDtypeStruct((2 * n, d_model), BF16),
        compiler_params=pltpu.CompilerParams(dimension_semantics=("arbitrary", "arbitrary")),
        cost_estimate=pl.CostEstimate(flops=n * d_model, bytes_accessed=n * d_model * 8, transcendentals=0),
    )(own, other)


def small_rows(conv, bias, gate, skip, dtb, al, wdt):
    f = lambda v: v.astype(F32)
    n, hp = skip.shape
    wide = lambda v: jnp.broadcast_to(v[:, :, None], (n, hp, PC))
    one = lambda v: v.reshape(n, 1, PC)
    skip = jnp.broadcast_to(skip[:, :, None], (n, hp, HD))
    v = [f(conv), one(f(bias)), one(f(gate)), one(skip), jnp.zeros((n, 1, PC), F32), wide(dtb), wide(-jnp.exp(al) * LOG2E),
         f(wdt).transpose(0, 2, 1).reshape(n, -1, PC)]
    return jnp.concatenate(v, axis=1).reshape(-1, PC)


PLAN_X = "00020405030607040809"
PLAN_Z0 = "04080a0b0a0b0d0b0d0f"
PLAN_O0 = "080c0e100e1012101214"
PLAN_Y = "0d101113121315141516"
PLAN_Z1 = "0002040604060906080b"
PLAN_O1 = "06090b0e0b0e100d1013"


def solution(mesh):
    n_tp, n_dp = mesh.shape['tp'], mesh.shape['dp']
    rep, col, vec = P(), P(None, None, 'tp'), P(None, 'tp')
    in_specs = (P('dp'), rep, col, col, rep, col, col, rep, vec, rep, vec, vec, vec, vec, P(None, 'tp', None))

    def device_forward(hidden, norm_w, w_z, w_x, w_bc, w_dt, conv_x, conv_bc, bias_x, bias_bc, dt_bias, a_log, d_skip, gate_w, w_out):
        u = hidden[0]
        steps, d_model = u.shape
        n = steps // 2
        core = lax.axis_index('tp') % 2
        e3 = expand_mat(dt_bias.shape[1] * n_tp)
        up = [(2 * k, 2 * k + 1) for k in range(n_tp // 2)]
        ax, az, ao = w_x.astype(F32), w_z.astype(F32), w_out.astype(F32)
        small = small_rows(conv_x, bias_x, gate_w, d_skip, dt_bias, a_log, w_dt)
        tail = u[n - SUB:n].astype(F32).reshape(8, 8, d_model).transpose(1, 0, 2).reshape(SUB, d_model)[SUB - CAR:]
        halo = jnp.where(core == 1, tail, 0.0)
        half = lambda blk: (lambda: lax.axis_index('tp') % 2 * (n // blk))
        none = lambda: 0
        common = (n, n_dp, n_tp)
        bc = (norm_w, w_bc, conv_bc, bias_bc, e3, ax)

        y, c, ac, s, _, gs, gx, gz, go = p1(u, half(BLK * NBS), halo, *bc, (ax, small, az, ao), *common, False, 0, True,
                                         (PLAN_Z0, PLAN_O0, PLAN_X, PLAN_Y), 1)
        u, f = p2(u, half(BLK2), norm_w, gz, go, az, ao, gs, y, c, ac, s, e3, *common, 0, False, None)
        halo = lax.ppermute(f, 'tp', up)
        y, c, ac, s, gz, go = p1(u, none, halo, *bc, (gx, gs, az, ao), *common, True, 1, False, (PLAN_Z1, PLAN_O1), 2)
        own, other = p2(u, none, norm_w, gz, go, az, ao, gs, y, c, ac, s, e3, *common, 1, True, 3)
        return finish(own, other)[None]

    return jax.shard_map(device_forward, mesh=mesh, in_specs=in_specs, out_specs=P('dp'), check_vma=False)
```

```python
import functools
import jax
import jax.numpy as jnp
import numpy as np
from jax import lax
from jax.experimental import pallas as pl
from jax.experimental.pallas import tpu as pltpu
from jax.sharding import PartitionSpec as P

EPS = 1e-5
LOG2E = 1.4426950408889634
HI = lax.Precision.HIGHEST
F32 = jnp.float32
BF16 = jnp.bfloat16
MESH = pl.DeviceIdType.MESH
LANES = 128
BLK = 128
SUB = 64
BLK2 = 256
NBS = 4
PC = 256
HD = 64
NST = 128
CAR = 24
SMALL = 32
ORDER = (1, 3, 2)
EARLY = 6
SEMS = 26
VMEM_CAP = 60 << 20


def silu(v):
    return v / (1.0 + jnp.exp2(v * -LOG2E))


def split3(v):
    a = v.astype(BF16)
    r = v - a.astype(F32)
    b = r.astype(BF16)
    return a, b, (r - b.astype(F32)).astype(BF16)


def round_bf16(v):
    return v.astype(BF16).astype(F32)


def rms(u, nw):
    return (u * lax.rsqrt(jnp.mean(u * u, axis=-1, keepdims=True) + EPS) * nw).astype(BF16)


def dot(a, b, prec=None):
    return jnp.dot(a, b, preferred_element_type=F32, precision=prec)


def dott(a, b, prec=None):
    return lax.dot_general(a, b, (((1,), (1,)), ((), ())), preferred_element_type=F32, precision=prec)


def rows_cat(*v):
    return jnp.concatenate(v, axis=0)


def lanes_cat(*v):
    return jnp.concatenate(v, axis=1)


def time_of(r):
    return 8 * (r % 8) + r // 8


def roll8(v):
    c = v.shape[-1]
    return pltpu.roll(v.reshape(CAR // 8, 8, c), 1, 1).reshape(CAR, c)


def conv_block(cur, prev, taps, bias, first):
    now = roll8(cur[SUB - CAR:])
    sh = jnp.where(first, prev, now)
    out = bias + cur * taps[-1]
    for k in range(1, 4):
        out = out + rows_cat(sh[CAR - 8 * k:], cur[:SUB - 8 * k]) * taps[3 - k]
    return out, now


def unmix(v, buf):
    n, c = v.shape
    for j in range(c // LANES):
        buf[n * j:n * (j + 1), :] = v[:, LANES * j:LANES * (j + 1)]
    cols = [rows_cat(*[buf[pl.ds(n * j + b + k, 8, stride=8), :] for b in range(0, n, SUB) for k in range(8)])
            for j in range(c // LANES)]
    return lanes_cat(*cols)


def head_row(h, heads):
    return (h % 2) * (heads // 2) + h // 2


def expand_mat(heads):
    order = sorted(range(heads), key=lambda h: head_row(h, heads))
    one = np.repeat(np.eye(heads)[order], HD, axis=1)
    return jnp.asarray(np.tile(one, (3, 1)), BF16)


def kcat6(parts):
    a, b, c = parts
    return lanes_cat(a, b, c, a), lanes_cat(b, a)


def kcat6r(parts):
    a, b, c = parts
    return rows_cat(a, a, a, b), rows_cat(b, c)


def block_diag(x, lo, hi):
    z = jnp.zeros((x.shape[0], LANES), BF16)
    l, r = x[:, :LANES], x[:, LANES:]
    return rows_cat(lanes_cat(l * lo, z), lanes_cat(l * hi, z), lanes_cat(z, r * lo), lanes_cat(z, r * hi))


def here():
    dp, tp = lax.axis_index('dp'), lax.axis_index('tp')
    return dp, tp, tp // 2, tp % 2


def source(dz):
    return (here()[2] + 4 - dz) % 4


class Gather:
    def __init__(self, piece, g, send, recv, base, keep=True):
        self.piece, self.g, self.send, self.recv, self.base = piece, g, send, recv, base
        self.dp, self.tp, self.z, self.c = here()
        x, y = self.dp // 2, self.dp % 2
        self.side = ((1 - x) * 2 + y, x * 2 + 1 - y)
        self.partner = (self.dp, 2 * self.z + 1 - self.c)
        self.quarters, self.keep = g.shape[0], keep

    def rdma(self, k, src, dst, dev):
        return pltpu.make_async_remote_copy(src_ref=src, dst_ref=dst, send_sem=self.send.at[self.base + k],
                                            recv_sem=self.recv.at[self.base + k], device_id=dev, device_id_type=MESH)

    def local(self, q):
        return pltpu.make_async_copy(self.piece(q), self.g.at[q, self.tp], self.send.at[self.base + q])

    def own(self, q):
        return self.rdma(4 + q, self.piece(q), self.g.at[q, self.tp], self.partner)

    def line(self, dz):
        return self.rdma(7 + dz, self.piece(self.dp), self.g.at[self.dp, self.tp],
                         (self.dp, 2 * ((self.z + dz) % 4) + self.c))

    def cross(self, dz, n):
        ref = self.g.at[self.dp, 2 * source(dz) + self.c]
        return self.rdma(9 + 2 * dz + n, ref, ref, (self.side[n], self.tp))

    def relay(self, dz, n):
        half = self.g.shape[2] // 2
        ref = self.g.at[self.side[n], 2 * source(dz) + self.c, pl.ds(n * half, half)]
        return self.rdma(15 + 2 * dz + n, ref, ref, (self.side[1 - n], self.tp))

    def over(self, dz):
        ref = self.g.at[:, 2 * source(dz) + self.c]
        return self.rdma(22 + dz, ref, ref, self.partner)

    def peers(self):
        return ([(self.dp, 2 * ((self.z + dz) % 4) + self.c) for dz in ORDER]
                + [(p, self.tp) for p in self.side] + [self.partner])

    def start(self):
        for q in range(self.quarters):
            self.own(q).start()
        for dz in ORDER:
            self.line(dz).start()
        if self.keep:
            for q in range(self.quarters):
                self.local(q).start()

    def spread(self, dz):
        self.line(dz).wait_recv()
        for n in range(2):
            self.cross(dz, n).start()

    def pass_on(self, dz):
        for n in range(2):
            self.cross(dz, n).wait_recv()
            self.relay(dz, n).start()

    def hand(self, dz):
        for n in range(2):
            self.relay(dz, n).wait_recv()
        self.over(dz).start()

    def settle_own(self):
        for q in range(self.quarters):
            self.own(q).wait_recv()
            if self.keep:
                self.local(q).wait()

    def settle(self, dz):
        self.over(dz).wait_recv()

    def drain(self):
        for q in range(self.quarters):
            self.own(q).wait_send()
        for dz in ORDER:
            self.line(dz).wait_send()
            self.over(dz).wait_send()
            for n in range(2):
                self.cross(dz, n).wait_send()
                self.relay(dz, n).wait_send()

    def plan(self, s):
        s = bytes.fromhex(s)
        acts = [(s[0], self.start)]
        for k, f in enumerate((self.spread, self.pass_on, self.hand)):
            acts += [(s[1 + 3 * k + j], functools.partial(f, dz)) for j, dz in enumerate(ORDER)]
        return acts

    def finish(self):
        self.settle_own()
        for dz in ORDER:
            self.settle(dz)
        self.drain()


class Small:
    def __init__(self, a, g, send, recv):
        self.a, self.g, self.send, self.recv = a, g, send, recv
        self.dp, self.tp, _, _ = here()

    def copy(self, k):
        return pltpu.make_async_remote_copy(src_ref=self.a, dst_ref=self.g.at[self.tp], send_sem=self.send.at[k],
                                            recv_sem=self.recv.at[k], device_id=(self.dp, (self.tp + k) % 8),
                                            device_id_type=MESH)

    def local(self):
        return pltpu.make_async_copy(self.a, self.g.at[self.tp], self.send.at[0])

    def peers(self):
        return [(self.dp, (self.tp + k) % 8) for k in range(1, 8)]

    def start(self):
        self.local().start()
        for k in range(1, 8):
            self.copy(k).start()

    def finish(self):
        self.local().wait()
        for k in range(1, 8):
            self.copy(k).wait()


def entry_barrier(peers):
    sem = pltpu.get_barrier_semaphore()
    for p in peers:
        pl.semaphore_signal(sem, inc=1, device_id=p, device_id_type=MESH)
    pl.semaphore_wait(sem, len(peers))


def at_steps(step, acts):
    for k in sorted({k for k, _ in acts}):
        @pl.when(step == k)
        def _():
            for j, f in acts:
                if j == k:
                    f()


def piece_rows(ref, layer):
    return lambda q: ref.at[layer, pl.ds(q * PC, PC)]


def piece_cols(ref, layer):
    return lambda q: ref.at[layer, :, pl.ds(pl.multiple_of(q * PC, PC) if not isinstance(q, int) else q * PC, PC)]


def p1_body(*refs, geom, mixed, layer, fetch_x, plans):
    n_dp, n_tp, heads, nb, nbs, sp = geom
    (u_ref, halo_ref, nw_ref, wbc_ref, cbc_ref, bbc_ref, e3_ref), refs = refs[:7], refs[7:]
    row = slice(layer, layer + 1)
    nw, cbc, bbc = nw_ref[row].astype(F32), cbc_ref[...].astype(F32), bbc_ref[row].astype(F32)
    if fetch_x:
        (ax, asm, az, ao), (y_ref, c_ref, ac_ref, s_in), (gx, gs, gz, go), refs = refs[:4], refs[4:8], refs[8:12], refs[12:]
    else:
        (ax, gx, gs, az, ao), (y_ref, c_ref, ac_ref, s_in), (gz, go), refs = refs[:5], refs[5:9], refs[9:11], refs[11:]
    (wf, wb, wsem, sm, wdt, cst, st, hcar, xcar, qcar, aoff, ubuf, h_s, la1_s, la2_s, lb1_s, lb2_s, cc_s, cbd_s, row_s, aw_s,
     sbuf, hsem, send, recv), sems = refs[:25], refs[25:]
    p, i = pl.program_id(0), pl.program_id(1)
    np_, ni = pl.num_programs(0), pl.num_programs(1)
    step = p * ni + i
    d_model = u_ref.shape[-1]
    by_z = sp < n_tp
    zs_of = (lambda p: source(p + p // 2 * (1 - 2 * (p % 2)))) if by_z else (lambda p: 0)
    zs = zs_of(p)
    upper = here()[3] == 1

    def state_out(p):
        dp, tp, _, c = here()
        cols = pl.ds(pl.multiple_of(2 * zs_of(p) * PC, PC), sp * PC)
        return pltpu.make_async_remote_copy(src_ref=sbuf, dst_ref=s_in.at[:, cols], send_sem=hsem.at[0], recv_sem=hsem.at[1],
                                            device_id=(dp, tp + 1 - 2 * c), device_id_type=MESH)

    zg = Gather(piece_rows(az, layer), gz, send, recv, 0)
    og = Gather(piece_cols(ao, layer), go, send, recv, SEMS)
    acts = zg.plan(plans[0]) + og.plan(plans[1])
    if fetch_x:
        xg = Gather(piece_rows(ax, layer), gx, send, recv, 2 * SEMS, False)
        small = Small(asm, gs, *sems)
        acts += xg.plan(plans[2])

    def load_w(slot, zsrc):
        return pltpu.make_async_copy(gx.at[:, pl.ds(2 * zsrc, sp)], wf.at[slot], wsem.at[slot])

    def load_own():
        _, tp, _, c = here()
        return ([pltpu.make_async_copy(piece_rows(ax, layer)(q), wf.at[0, q, c], wsem.at[0]) for q in range(n_dp)]
                + [pltpu.make_async_copy(gx.at[q, tp + 1 - 2 * c], wf.at[0, q, 1 - c], wsem.at[0]) for q in range(n_dp)])

    @pl.when(step == 0)
    def _():
        entry_barrier((small.peers() + [(s, here()[1]) for s in zg.side]) if fetch_x else zg.peers())
        if fetch_x:
            small.start()
    at_steps(step, acts)

    @pl.when(step == 0)
    def _():
        if fetch_x:
            small.finish()
            xg.settle_own()
        if by_z:
            for v in load_own():
                v.start()
        else:
            load_w(0, 0).start()
        cp = pltpu.make_async_copy(gs.at[:, pl.ds(layer * SMALL, SMALL)], sm, wsem.at[2])
        cp.start()
        cp.wait()
        kc = d_model // PC
        hp = heads // n_tp
        for t in range(n_tp):
            for k in range(hp):
                r = head_row(hp * t + k, heads)
                for c in range(kc):
                    wdt[r:r + 1, c * PC:(c + 1) * PC] = sm[t, 16 + kc * k + c:17 + kc * k + c, :].astype(BF16)
                cst[r:r + 1, :] = sm[t, 8 + k:9 + k, :]
                cst[heads + r:heads + r + 1, :] = sm[t, 12 + k:13 + k, :]
        aoff[...] = jnp.zeros_like(aoff)
        hh = rms(halo_ref[...], nw)
        hcar[...] = hh
        qcar[...] = roll8(round_bf16(dot(hh, wbc_ref[...])))

    first = lax.broadcasted_iota(jnp.int32, (CAR, PC), 0) % 8 == 0

    def conv(cur, prev, taps, bias):
        a, now = conv_block(cur[:SUB], prev, taps, bias, first)
        b, now = conv_block(cur[SUB:], now, taps, bias, first)
        return silu(rows_cat(a, b)), now

    ri = lax.broadcasted_iota(jnp.int32, (BLK, BLK), 0)
    ci = lax.broadcasted_iota(jnp.int32, (BLK, BLK), 1)

    def prologue(h, b, hook):
        q0 = dot(h, wbc_ref[...])
        rT = round_bf16(dott(wdt[...], h))
        hook(h, 2)
        bc, qcar[...] = conv(round_bf16(q0), qcar[...],
                             [cbc[k:k + 1] for k in range(4)], bbc)
        bmat, cmat = bc[:, :NST], bc[:, NST:]
        here_rows = slice(b * BLK, (b + 1) * BLK)
        c_ref[here_rows, :] = cmat
        pre = rT + cst[:heads, :BLK]
        dtT = jnp.maximum(pre, 0.0) + jnp.log1p(jnp.exp(-jnp.abs(pre)))
        aT = dtT * cst[heads:, :BLK]
        tr, tc = ri // SUB * SUB + time_of(ri % SUB), ci // SUB * SUB + time_of(ci % SUB)
        acT = dot(aT, jnp.where(tr <= tc, 1.0, 0.0), HI)
        mid, alast = acT[:, SUB - 1:SUB], acT[:, BLK - 1:BLK]
        low = ci[:heads] < SUB
        wT = dtT * jnp.exp2(jnp.where(low, mid, alast) - acT)
        pad = jnp.zeros((BLK - 3 * heads, BLK), BF16)
        a3, w3 = rows_cat(*split3(acT), pad).T, rows_cat(*split3(wT), pad).T
        ac_ref[:, here_rows] = acT + aoff[:, :1]
        aoff[...] = aoff[...] + alast

        def pair_rows(v):
            ev, od = v[:heads // 2], v[heads // 2:]
            l = low[:heads // 2]
            return jnp.where(l, ev, pltpu.roll(od, SUB, 1)), jnp.where(l, pltpu.roll(ev, SUB, 1), od)

        rows = [rows_cat(*[w for zz in zip(*[jnp.split(v, n_tp // 2) for v in ad]) for w in zz])
                for ad in zip(pair_rows(acT), pair_rows(dtT))]
        hook(h, 4)
        cb = dott(cmat, bmat, HI)
        hook(h, EARLY)
        lowr, tri = ci[:SUB] < SUB, time_of(ri[:SUB]) >= time_of(ci[:SUB] % SUB)
        ca, cd = cb[:SUB], cb[SUB:]
        cbd = [jnp.where(tri, jnp.where(lowr, ca, pltpu.roll(ca, SUB, 1)), 0.0),
               jnp.where(tri, jnp.where(lowr, pltpu.roll(cd, SUB, 1), cd), 0.0)]
        bT = bmat.T
        la = kcat6(split3(rows_cat(bT[:, :SUB], cd[:, :SUB])))
        lb = kcat6(split3(pltpu.roll(bT, SUB, 1)[:, :SUB]))
        c1, c2, c3 = split3(cmat)
        return h, a3, w3, rows, cbd, la, lb, (lanes_cat(c1, c2), lanes_cat(c1, c3))

    def spots(b):
        j = i * nbs + b
        at = lambda r: pl.ds(pl.multiple_of(j * r, SUB), r)
        return j, at(BLK), at(NST + SUB)

    def keep(b, vals):
        h, a3, w3, rows, cbd, la, lb, cc = vals
        j, blk, big = spots(b)
        h_s[blk, :] = h
        aw_s[blk, :] = lanes_cat(a3, w3)
        for half in range(2):
            row_s[2 * j + half] = rows[half]
        cbd_s[blk, :] = rows_cat(*cbd)
        la1_s[big, :], la2_s[big, :] = la
        lb1_s[blk, :], lb2_s[blk, :] = lb
        cc_s[blk, :] = lanes_cat(*cc)

    def kept(b):
        j, blk, big = spots(b)
        eight = pl.ds(pl.multiple_of(8 * zs, 8), 8)
        return (None, aw_s[blk, :BLK], aw_s[blk, BLK:], [row_s[2 * j + half, eight, :] for half in range(2)],
                [cbd_s[pl.ds(pl.multiple_of(j * BLK + half * SUB, SUB), SUB), :] for half in range(2)],
                (la1_s[big, :], la2_s[big, :]), (lb1_s[blk, :], lb2_s[blk, :]), (cc_s[blk, :2 * NST], cc_s[blk, 2 * NST:]))


    def all_prologues(hook):
        u = u_ref[...].astype(F32)
        h = rms(u if mixed else unmix(u, ubuf), nw)
        return [prologue(h[b * BLK:(b + 1) * BLK], b, hook) for b in range(nbs)]

    if by_z:
        @pl.when(p == 0)
        def _():
            for b, v in enumerate(all_prologues(lambda h, k: None)):
                keep(b, v)

    @pl.when(i == 0)
    def _():
        slot = p % 2 if by_z else 0

        @pl.when(p == 0)
        def _():
            for v in load_own() if by_z else [load_w(0, 0)]:
                v.wait()

        @pl.when(p > 0)
        def _():
            load_w(slot, zs).wait()
        for q in range(n_dp):
            for k in range(sp):
                wb[q * PC:(q + 1) * PC, k * PC:(k + 1) * PC] = wf[slot, q, k].astype(BF16)
        @pl.when((p > 0) & jnp.logical_not(upper))
        def _():
            state_out(p - 1).start()
        xcar[...] = roll8(round_bf16(dot(hcar[...], wb[...])))
        st[...] = jnp.zeros_like(st)

    @pl.when((i == ni - 1) & (p < np_ - 1))
    def _():
        nd = p + 1
        nd = nd + nd // 2 * (1 - 2 * (nd % 2))
        if fetch_x:
            for d in ORDER:
                pl.when(nd == d)(functools.partial(xg.settle, d))
        load_w((p + 1) % 2, source(nd)).start()

    lane = lax.broadcasted_iota(jnp.int32, (SUB, LANES), 1)
    lo = jnp.where(lane < HD, 1.0, 0.0).astype(BF16)
    hi = jnp.where(lane < HD, 0.0, 1.0).astype(BF16)
    x0 = {}

    def proj(hs, upto):
        for k in range(len(x0), min(sp, upto)):
            x0[k] = dot(hs, wb[:, k * PC:(k + 1) * PC])

    if by_z:
        vals = [kept(b) for b in range(nbs)]
        hs = h_s[pl.ds(pl.multiple_of(i * nbs * BLK, BLK), nbs * BLK), :]
        proj(hs, sp)
    else:
        vals = all_prologues(proj)
        hs = vals[0][0]

    def lanes_of(k):
        return slice(k * PC, (k + 1) * PC), pl.ds(pl.multiple_of((2 * zs + k) * PC, PC), PC)

    def pre(b, k):
        (sl, gl), (_, a3, w3, _, _, _, _, (c12, c13)) = lanes_of(k), vals[b]
        s1, s2, s3 = split3(st[:, sl])
        inter = dot(c12, rows_cat(s1, s1)) + dot(c12, rows_cat(s2, s2)) + dot(c13, rows_cat(s3, s1))
        n3 = e3_ref.shape[0]
        acx = dot(a3[:, :n3], e3_ref[:, gl])
        wx = dot(w3[:, :n3], e3_ref[:, gl])
        proj(hs, k + EARLY + 1)
        return x0[k][b * BLK:(b + 1) * BLK], acx, wx, inter

    def mid_(b, k, x0, acx, wx, inter):
        (sl, _), (_, _, _, rws, cbds, _, _, _) = lanes_of(k), vals[b]
        t = 2 * zs + k
        base = 0 if by_z else k // 2 * 8
        x, xcar[:, sl] = conv(round_bf16(x0), xcar[:, sl], [sm[t, r:r + 1, :] for r in range(4)], sm[t, 4:5, :])
        xw = split3(x * wx)
        r = kcat6r([v[:SUB] for v in xw]) + kcat6r([v[SUB:] for v in xw])
        ms, xs = [], []
        for half in range(2):
            rows = slice(half * SUB, (half + 1) * SUB)
            row, cbd = rws[half][base:base + 8], cbds[half]
            m = []
            for g in range(2):
                seg = acx[rows, g * LANES:(g + 1) * LANES] - row[2 * (k % 2) + g:2 * (k % 2) + g + 1]
                m.append(jnp.exp2(jnp.minimum(seg, 0.0)) * cbd * row[4 + 2 * (k % 2) + g:5 + 2 * (k % 2) + g])
            ms.append(split3(lanes_cat(*m)))
            xs.append([block_diag(v, lo, hi) for v in split3(x[rows])])
        return x, acx, inter, r, ms, xs

    def fin(b, k, x, acx, inter, r, ms, xs):
        (sl, _), (_, _, _, _, _, la, lb, _) = lanes_of(k), vals[b]
        ra = dot(la[0], r[0]) + dot(la[1], r[1])
        rb = dot(lb[0], r[2]) + dot(lb[1], r[3])
        am, al = acx[SUB - 1:SUB], acx[BLK - 1:BLK]
        st[:, sl] = st[:, sl] * jnp.exp2(al) + ra[:NST] * jnp.exp2(al - am) + rb
        skip = sm[2 * zs + k, 6:7, :]
        for half in range(2):
            rows = slice(half * SUB, (half + 1) * SUB)
            (m1, m2, m3), (x1, x2, x3) = ms[half], xs[half]
            r1 = dot(rows_cat(m1, m2, m3), x1)
            r2 = dot(rows_cat(m1, m2), x2)
            y = r1[:SUB] + r1[SUB:2 * SUB] + r1[2 * SUB:] + r2[:SUB] + r2[SUB:] + dot(m1, x3)
            y = y + inter[rows] * jnp.exp2(acx[rows])
            if half:
                y = y + ra[NST:] * jnp.exp2(acx[rows] - am)
            y_ref[b * BLK + half * SUB:b * BLK + (half + 1) * SUB, sl] = y + skip * x[rows]

    units = [(b, k) for b in range(nbs) for k in range(sp)]
    m = mid_(*units[0], *pre(*units[0]))
    for a, nxt in zip(units, units[1:] + [None]):
        if nxt:
            v = pre(*nxt)
        fin(*a, *m)
        if nxt:
            m = mid_(*nxt, *v)

    @pl.when(i == ni - 1)
    def _():
        @pl.when((p > 0) & jnp.logical_not(upper))
        def _():
            state_out(p - 1).wait_send()
        sbuf[...] = st[...]

    @pl.when(step == np_ * ni - 1)
    def _():
        zg.finish()
        og.finish()
        if fetch_x:
            xg.drain()

        @pl.when(jnp.logical_not(upper))
        def _():
            state_out(p).start()
            state_out(p).wait_send()

        @pl.when(upper)
        def _():
            pltpu.make_async_copy(s_in, s_in, hsem.at[1]).wait()


def p1(u, base, halo, nw, wbc, cbc, bbc, e3, comm, n, n_dp, n_tp, mixed, layer, fetch_x, plans, cid):
    d_model, heads = u.shape[-1], PC // HD * n_tp
    sp, nbs = (2, NBS) if fetch_x else (n_tp, 1)
    width, nb, rows = PC * n_tp, n // BLK, BLK * nbs
    ni = nb // nbs
    fixed = lambda shp: pl.BlockSpec(shp, lambda p, i: (0,) * len(shp), pipeline_mode=pl.Buffered(1))
    own_layer = lambda *shp: pl.BlockSpec((None,) + shp, lambda p, i: (layer, 0, 0), pipeline_mode=pl.Buffered(1))
    once = lambda p, i: jnp.where(p == 0, i, ni - 1)
    col = (lambda p: source(p + p // 2 * (1 - 2 * (p % 2)))) if fetch_x else (lambda p: 0)
    hbm = pl.BlockSpec(memory_space=pl.ANY)
    gathered = lambda r: jax.ShapeDtypeStruct((n_dp, n_tp, r, PC), F32)
    outs = [jax.ShapeDtypeStruct((n, width), F32), jax.ShapeDtypeStruct((n, NST), F32),
            jax.ShapeDtypeStruct((heads, n), F32), jax.ShapeDtypeStruct((NST, width), F32)]
    more = ([gathered(PC), jax.ShapeDtypeStruct((n_tp,) + comm[1].shape, F32)] if fetch_x else []) + [gathered(PC)] * 2
    vm = pltpu.VMEM
    dma = lambda k: [pltpu.SemaphoreType.DMA((k,))] * 2
    return pl.pallas_call(
        functools.partial(p1_body, geom=(n_dp, n_tp, heads, nb, nbs, sp), mixed=mixed, layer=layer, fetch_x=fetch_x, plans=plans),
        name="p1", grid=(n_tp // sp, ni),
        in_specs=[pl.BlockSpec((rows, d_model), lambda p, i: (base() + once(p, i), 0)),
                  fixed((CAR, d_model)), fixed((2, d_model)), own_layer(d_model, PC), own_layer(4, PC), fixed((2, PC)),
                  fixed((3 * heads, width))] + [hbm] * len(comm),
        out_specs=[pl.BlockSpec((rows, sp * PC), lambda p, i: (i, col(p))),
                   pl.BlockSpec((rows, NST), lambda p, i: (once(p, i), 0)),
                   pl.BlockSpec((heads, rows), lambda p, i: (0, once(p, i))),
                   hbm] + [hbm] * len(more),
        out_shape=outs + more,
        scratch_shapes=[
            vm((2 if fetch_x else 1, n_dp, sp, PC, PC), F32), vm((d_model, sp * PC), BF16), pltpu.SemaphoreType.DMA((3,)),
            vm((n_tp, SMALL, PC), F32), vm((heads, d_model), BF16), vm((2 * heads, PC), F32), vm((NST, sp * PC), F32),
            vm((CAR, d_model), BF16), vm((CAR, sp * PC), F32), vm((CAR, PC), F32), vm((heads, LANES), F32),
            vm((d_model // LANES * rows, LANES), F32), vm((n, d_model), BF16),
            vm((nb * (NST + SUB), 4 * SUB), BF16), vm((nb * (NST + SUB), 2 * SUB), BF16),
            vm((n, 4 * SUB), BF16), vm((n, 2 * SUB), BF16), vm((n, 4 * NST), BF16), vm((n, LANES), F32),
            vm((2 * nb, 2 * heads // 2, LANES), F32), vm((n, 2 * BLK), BF16), vm((NST, sp * PC), F32), pltpu.SemaphoreType.DMA((2,))]
        + dma(3 * SEMS) + (dma(8) if fetch_x else []),
        compiler_params=pltpu.CompilerParams(dimension_semantics=("arbitrary", "arbitrary"), vmem_limit_bytes=VMEM_CAP,
                                             collective_id=cid, has_side_effects=True),
        cost_estimate=pl.CostEstimate(flops=n * 70 * 10 ** 6, bytes_accessed=n * 12000, transcendentals=0),
    )(u, halo, nw, wbc, cbc, bbc, e3, *comm)


def p2_body(*refs, geom, mix_in, layer, fetch_x, plans):
    n_dp, n_tp, heads = geom
    (u_ref, nw_ref, wz_ref, wo_ref, sm_ref, y_ref, c_ref, ac_ref, s_ref, e3_ref), refs = refs[:10], refs[10:]
    if fetch_x:
        (ax, o_ref, f_ref, gx), refs = refs[:4], refs[4:]
    else:
        (o_ref, r_ref), refs = refs[:2], refs[2:]
    (wzb, wob, s3, ubuf, send, recv), refs = refs[:6], refs[6:]
    i = pl.program_id(0)
    width = PC * n_tp
    if fetch_x:
        xg = Gather(piece_rows(ax, layer + 1), gx, send, recv, 0)

        @pl.when(i == 0)
        def _():
            entry_barrier(xg.peers())
        at_steps(i, xg.plan(plans))
    else:
        fbuf, = refs
        dp, tp, z, c = here()

        def swap(k):
            return pltpu.make_async_remote_copy(
                src_ref=fbuf.at[k % 2], dst_ref=r_ref.at[pl.ds(pl.multiple_of(k * BLK2, BLK2), BLK2)],
                send_sem=send.at[k % 2], recv_sem=recv.at[0], device_id=(dp, 2 * z + 1 - c), device_id_type=MESH)

        @pl.when(i == 0)
        def _():
            entry_barrier([(dp, 2 * z + 1 - c)])

        @pl.when(i > 1)
        def _():
            swap(i - 2).wait_send()

        @pl.when(i > 0)
        def _():
            swap(i - 1).start()

    @pl.when(i == 0)
    def _():
        for d in range(n_dp):
            for t in range(n_tp):
                a, b = slice(d * PC, (d + 1) * PC), slice(t * PC, (t + 1) * PC)
                wzb[a, b] = wz_ref[d, t].astype(BF16)
                wob[b, a] = wo_ref[d, t].astype(BF16)
        a, b, c_ = split3(jnp.where(here()[3] == 1, s_ref[...], 0.0))
        for k, (v, w) in enumerate(((a, a), (b, b), (c_, a))):
            s3[k] = rows_cat(v, w)

    u = u_ref[...].astype(F32)
    u = u if mix_in else unmix(u, ubuf)
    h = rms(u, nw_ref[layer:layer + 1].astype(F32))
    c1, c2, c3 = split3(c_ref[...])
    c12, c13 = lanes_cat(c1, c2), lanes_cat(c1, c3)
    eT = rows_cat(*split3(jnp.exp2(ac_ref[...]))).T
    vs, ss = [], 0.0
    for t in range(n_tp):
        sl = slice(t * PC, (t + 1) * PC)
        z_ = round_bf16(dot(h, wzb[:, sl]))
        cor = dot(c12, s3[0, :, sl]) + dot(c12, s3[1, :, sl]) + dot(c13, s3[2, :, sl])
        v = (y_ref[:, sl] + cor * dot(eT, e3_ref[:, sl])) * silu(z_)
        ss = ss + jnp.sum(v * v, axis=-1, keepdims=True)
        vs.append(v)
    sc = lax.rsqrt(ss / width + EPS)
    g = lanes_cat(*[(v * sc * sm_ref[t, 5:6, :]).astype(BF16) for t, v in enumerate(vs)])
    un = round_bf16(u + dot(g, wob[...]))
    if fetch_x:
        o_ref[...] = un.astype(BF16)
        f_ref[...] = un[BLK2 - CAR:]
    else:
        un = unmix(un, ubuf)
        fbuf[i % 2] = un
        o_ref[...] = un.astype(BF16)

    @pl.when(i == pl.num_programs(0) - 1)
    def _():
        if fetch_x:
            xg.finish()
        else:
            swap(i).start()
            for k in range(2):
                swap(i - 1 + k).wait_send()
            whole = pltpu.make_async_copy(r_ref, r_ref, recv.at[0])
            whole.wait()


def p2(u, base, nw, wz, wo, sm, y, c, ac, s, e3, comm, n, n_dp, n_tp, mix_in, layer, fetch_x, plans, cid):
    d_model, heads = u.shape[-1], PC // HD * n_tp
    width = PC * n_tp
    fixed = lambda shp: pl.BlockSpec(shp, lambda i: (0,) * len(shp), pipeline_mode=pl.Buffered(1))
    hbm = pl.BlockSpec(memory_space=pl.ANY)
    rows = lambda w: pl.BlockSpec((BLK2, w), lambda i: (i, 0))
    shape = lambda *s: jax.ShapeDtypeStruct(s, F32)
    vm = pltpu.VMEM
    outs = [jax.ShapeDtypeStruct((n, d_model), BF16)]
    specs = [rows(d_model)]
    if fetch_x:
        outs += [shape(CAR, d_model), shape(n_dp, n_tp, PC, PC)]
        specs += [pl.BlockSpec((CAR, d_model), lambda i: (0, 0)), hbm]
    else:
        outs += [shape(n, d_model)]
        specs += [hbm]
    return pl.pallas_call(
        functools.partial(p2_body, geom=(n_dp, n_tp, heads), mix_in=mix_in, layer=layer, fetch_x=fetch_x, plans=plans),
        name="p2", grid=(n // BLK2,),
        in_specs=[pl.BlockSpec((BLK2, d_model), lambda i: (base() + i, 0)),
                  fixed((2, d_model)),
                  fixed((n_dp, n_tp, PC, PC)), fixed((n_dp, n_tp, PC, PC)),
                  pl.BlockSpec((n_tp, SMALL, PC), lambda i: (0, layer, 0), pipeline_mode=pl.Buffered(1)),
                  rows(width), rows(NST), pl.BlockSpec((heads, BLK2), lambda i: (0, i)),
                  fixed((NST, width)), fixed((3 * heads, width))] + [hbm] * len(comm),
        out_specs=specs, out_shape=outs,
        scratch_shapes=[vm((d_model, width), BF16), vm((width, d_model), BF16), vm((3, 2 * NST, width), BF16),
                        vm((d_model // LANES * BLK2, LANES), F32)]
        + [pltpu.SemaphoreType.DMA((SEMS,))] * 2 + ([] if fetch_x else [vm((2, BLK2, d_model), F32)]),
        compiler_params=pltpu.CompilerParams(dimension_semantics=("arbitrary",), vmem_limit_bytes=VMEM_CAP,
                                             collective_id=cid, has_side_effects=True),
        cost_estimate=pl.CostEstimate(flops=n * 30 * 10 ** 6, bytes_accessed=n * 12000, transcendentals=0),
    )(u, nw, wz, wo, sm, y, c, ac, s, e3, *comm)


def finish_body(own_ref, other_ref, o_ref):
    mine = pl.program_id(0) == here()[3]

    @pl.when(mine)
    def _():
        o_ref[...] = own_ref[...]

    @pl.when(jnp.logical_not(mine))
    def _():
        o_ref[...] = other_ref[...].astype(BF16)


def finish(own, other):
    n, d_model = own.shape
    rows = n // 3
    ni = n // rows
    pick = lambda w: (lambda j, i: (jnp.where((j == here()[3]) == w, i, ni - 1), 0))
    return pl.pallas_call(
        finish_body, name="finish", grid=(2, ni),
        in_specs=[pl.BlockSpec((rows, d_model), pick(True)), pl.BlockSpec((rows, d_model), pick(False))],
        out_specs=pl.BlockSpec((rows, d_model), lambda j, i: (j * ni + i, 0)),
        out_shape=jax.ShapeDtypeStruct((2 * n, d_model), BF16),
        compiler_params=pltpu.CompilerParams(dimension_semantics=("arbitrary", "arbitrary")),
        cost_estimate=pl.CostEstimate(flops=n * d_model, bytes_accessed=n * d_model * 8, transcendentals=0),
    )(own, other)


def small_rows(conv, bias, gate, skip, dtb, al, wdt):
    f = lambda v: v.astype(F32)
    n, hp = skip.shape
    wide = lambda v: jnp.broadcast_to(v[:, :, None], (n, hp, PC))
    one = lambda v: v.reshape(n, 1, PC)
    skip = jnp.broadcast_to(skip[:, :, None], (n, hp, HD))
    v = [f(conv), one(f(bias)), one(f(gate)), one(skip), jnp.zeros((n, 1, PC), F32), wide(dtb), wide(-jnp.exp(al) * LOG2E),
         f(wdt).transpose(0, 2, 1).reshape(n, -1, PC)]
    return jnp.concatenate(v, axis=1).reshape(-1, PC)


PLAN_X = "00010305030507040709"
PLAN_Z0 = "0407080b0a0b0e0d0e11"
PLAN_O0 = "080c0e110f1113121315"
PLAN_Z1 = "0003050806080b090b0e"
PLAN_O1 = "000a0c0f0d0f12101214"
PLAN_X1 = "0003050806080a080a0b"


def solution(mesh):
    n_tp, n_dp = mesh.shape['tp'], mesh.shape['dp']
    rep, col, vec = P(), P(None, None, 'tp'), P(None, 'tp')
    in_specs = (P('dp'), rep, col, col, rep, col, col, rep, vec, rep, vec, vec, vec, vec, P(None, 'tp', None))

    def device_forward(hidden, norm_w, w_z, w_x, w_bc, w_dt, conv_x, conv_bc, bias_x, bias_bc, dt_bias, a_log, d_skip, gate_w, w_out):
        u = hidden[0]
        steps, d_model = u.shape
        n = steps // 2
        core = lax.axis_index('tp') % 2
        e3 = expand_mat(dt_bias.shape[1] * n_tp)
        up = [(2 * k, 2 * k + 1) for k in range(n_tp // 2)]
        ax, az, ao = w_x.astype(F32), w_z.astype(F32), w_out.astype(F32)
        small = small_rows(conv_x, bias_x, gate_w, d_skip, dt_bias, a_log, w_dt)
        tail = u[n - SUB:n].astype(F32).reshape(8, 8, d_model).transpose(1, 0, 2).reshape(SUB, d_model)[SUB - CAR:]
        halo = jnp.where(core == 1, tail, 0.0)
        half = lambda blk: (lambda: lax.axis_index('tp') % 2 * (n // blk))
        none = lambda: 0
        common = (n, n_dp, n_tp)
        bc = (norm_w, w_bc, conv_bc, bias_bc, e3)

        y, c, ac, s, gx, gs, gz, go = p1(u, half(BLK * NBS), halo, *bc, (ax, small, az, ao), *common, False, 0, True,
                                         (PLAN_Z0, PLAN_O0, PLAN_X), 1)
        u, f, gx = p2(u, half(BLK2), norm_w, gz, go, gs, y, c, ac, s, e3, (ax,), *common, False, 0, True, PLAN_X1, 2)
        halo = lax.ppermute(f, 'tp', up)
        y, c, ac, s, gz, go = p1(u, none, halo, *bc, (ax, gx, gs, az, ao), *common, True, 1, False, (PLAN_Z1, PLAN_O1), 3)
        own, other = p2(u, none, norm_w, gz, go, gs, y, c, ac, s, e3, (), *common, True, 1, False, None, 4)
        return finish(own, other)[None]

    return jax.shard_map(device_forward, mesh=mesh, in_specs=in_specs, out_specs=P('dp'), check_vma=False)
```

```python
import functools
import jax
import jax.numpy as jnp
import numpy as np
from jax import lax
from jax.experimental import pallas as pl
from jax.experimental.pallas import tpu as pltpu
from jax.sharding import PartitionSpec as P

EPS = 1e-5
LOG2E = 1.4426950408889634
HI = lax.Precision.HIGHEST
F32 = jnp.float32
BF16 = jnp.bfloat16
MESH = pl.DeviceIdType.MESH
LANES = 128
BLK = 128
SUB = 64
BLK2 = 256
NBS = 4
PC = 256
HD = 64
NST = 128
CAR = 24
SMALL = 32
ORDER = (1, 3, 2)
EARLY = 6
SEMS = 26
VMEM_CAP = 60 << 20


def silu(v):
    return v / (1.0 + jnp.exp2(v * -LOG2E))


def split3(v):
    a = v.astype(BF16)
    r = v - a.astype(F32)
    b = r.astype(BF16)
    return a, b, (r - b.astype(F32)).astype(BF16)


def round_bf16(v):
    return v.astype(BF16).astype(F32)


def rms(u, nw):
    return (u * lax.rsqrt(jnp.mean(u * u, axis=-1, keepdims=True) + EPS) * nw).astype(BF16)


def dot(a, b, prec=None):
    return jnp.dot(a, b, preferred_element_type=F32, precision=prec)


def dott(a, b, prec=None):
    return lax.dot_general(a, b, (((1,), (1,)), ((), ())), preferred_element_type=F32, precision=prec)


def rows_cat(*v):
    return jnp.concatenate(v, axis=0)


def lanes_cat(*v):
    return jnp.concatenate(v, axis=1)


def time_of(r):
    return 8 * (r % 8) + r // 8


def roll8(v):
    c = v.shape[-1]
    return pltpu.roll(v.reshape(CAR // 8, 8, c), 1, 1).reshape(CAR, c)


def conv_block(cur, prev, taps, bias, first):
    now = roll8(cur[SUB - CAR:])
    sh = jnp.where(first, prev, now)
    out = bias + cur * taps[-1]
    for k in range(1, 4):
        out = out + rows_cat(sh[CAR - 8 * k:], cur[:SUB - 8 * k]) * taps[3 - k]
    return out, now


def unmix(v, buf):
    n, c = v.shape
    for j in range(c // LANES):
        buf[n * j:n * (j + 1), :] = v[:, LANES * j:LANES * (j + 1)]
    cols = [rows_cat(*[buf[pl.ds(n * j + b + k, 8, stride=8), :] for b in range(0, n, SUB) for k in range(8)])
            for j in range(c // LANES)]
    return lanes_cat(*cols)


def head_row(h, heads):
    return (h % 2) * (heads // 2) + h // 2


def expand_mat(heads):
    order = sorted(range(heads), key=lambda h: head_row(h, heads))
    one = np.repeat(np.eye(heads)[order], HD, axis=1)
    return jnp.asarray(np.tile(one, (3, 1)), BF16)


def kcat6(parts):
    a, b, c = parts
    return lanes_cat(a, b, c, a), lanes_cat(b, a)


def kcat6r(parts):
    a, b, c = parts
    return rows_cat(a, a, a, b), rows_cat(b, c)


def block_diag(x, lo, hi):
    z = jnp.zeros((x.shape[0], LANES), BF16)
    l, r = x[:, :LANES], x[:, LANES:]
    return rows_cat(lanes_cat(l * lo, z), lanes_cat(l * hi, z), lanes_cat(z, r * lo), lanes_cat(z, r * hi))


def here():
    dp, tp = lax.axis_index('dp'), lax.axis_index('tp')
    return dp, tp, tp // 2, tp % 2


def source(dz):
    return (here()[2] + 4 - dz) % 4


class Gather:
    def __init__(self, piece, g, send, recv, base, keep=True):
        self.piece, self.g, self.send, self.recv, self.base = piece, g, send, recv, base
        self.dp, self.tp, self.z, self.c = here()
        x, y = self.dp // 2, self.dp % 2
        self.side = ((1 - x) * 2 + y, x * 2 + 1 - y)
        self.partner = (self.dp, 2 * self.z + 1 - self.c)
        self.quarters, self.keep = g.shape[0], keep

    def rdma(self, k, src, dst, dev):
        return pltpu.make_async_remote_copy(src_ref=src, dst_ref=dst, send_sem=self.send.at[self.base + k],
                                            recv_sem=self.recv.at[self.base + k], device_id=dev, device_id_type=MESH)

    def local(self, q):
        return pltpu.make_async_copy(self.piece(q), self.g.at[q, self.tp], self.send.at[self.base + q])

    def own(self, q):
        return self.rdma(4 + q, self.piece(q), self.g.at[q, self.tp], self.partner)

    def line(self, dz):
        return self.rdma(7 + dz, self.piece(self.dp), self.g.at[self.dp, self.tp],
                         (self.dp, 2 * ((self.z + dz) % 4) + self.c))

    def cross(self, dz, n):
        ref = self.g.at[self.dp, 2 * source(dz) + self.c]
        return self.rdma(9 + 2 * dz + n, ref, ref, (self.side[n], self.tp))

    def relay(self, dz, n):
        half = self.g.shape[2] // 2
        ref = self.g.at[self.side[n], 2 * source(dz) + self.c, pl.ds(n * half, half)]
        return self.rdma(15 + 2 * dz + n, ref, ref, (self.side[1 - n], self.tp))

    def over(self, dz):
        ref = self.g.at[:, 2 * source(dz) + self.c]
        return self.rdma(22 + dz, ref, ref, self.partner)

    def peers(self):
        return ([(self.dp, 2 * ((self.z + dz) % 4) + self.c) for dz in ORDER]
                + [(p, self.tp) for p in self.side] + [self.partner])

    def start(self):
        for q in range(self.quarters):
            self.own(q).start()
        for dz in ORDER:
            self.line(dz).start()
        if self.keep:
            for q in range(self.quarters):
                self.local(q).start()

    def spread(self, dz):
        self.line(dz).wait_recv()
        for n in range(2):
            self.cross(dz, n).start()

    def pass_on(self, dz):
        for n in range(2):
            self.cross(dz, n).wait_recv()
            self.relay(dz, n).start()

    def hand(self, dz):
        for n in range(2):
            self.relay(dz, n).wait_recv()
        self.over(dz).start()

    def settle_own(self):
        for q in range(self.quarters):
            self.own(q).wait_recv()
            if self.keep:
                self.local(q).wait()

    def settle(self, dz):
        self.over(dz).wait_recv()

    def drain(self):
        for q in range(self.quarters):
            self.own(q).wait_send()
        for dz in ORDER:
            self.line(dz).wait_send()
            self.over(dz).wait_send()
            for n in range(2):
                self.cross(dz, n).wait_send()
                self.relay(dz, n).wait_send()

    def plan(self, s):
        s = bytes.fromhex(s)
        acts = [(s[0], self.start)]
        for k, f in enumerate((self.spread, self.pass_on, self.hand)):
            acts += [(s[1 + 3 * k + j], functools.partial(f, dz)) for j, dz in enumerate(ORDER)]
        return acts

    def finish(self):
        self.settle_own()
        for dz in ORDER:
            self.settle(dz)
        self.drain()


class Small:
    def __init__(self, a, g, send, recv):
        self.a, self.g, self.send, self.recv = a, g, send, recv
        self.dp, self.tp, _, _ = here()

    def copy(self, k):
        return pltpu.make_async_remote_copy(src_ref=self.a, dst_ref=self.g.at[self.tp], send_sem=self.send.at[k],
                                            recv_sem=self.recv.at[k], device_id=(self.dp, (self.tp + k) % 8),
                                            device_id_type=MESH)

    def local(self):
        return pltpu.make_async_copy(self.a, self.g.at[self.tp], self.send.at[0])

    def peers(self):
        return [(self.dp, (self.tp + k) % 8) for k in range(1, 8)]

    def start(self):
        self.local().start()
        for k in range(1, 8):
            self.copy(k).start()

    def finish(self):
        self.local().wait()
        for k in range(1, 8):
            self.copy(k).wait()


def entry_barrier(peers):
    sem = pltpu.get_barrier_semaphore()
    for p in peers:
        pl.semaphore_signal(sem, inc=1, device_id=p, device_id_type=MESH)
    pl.semaphore_wait(sem, len(peers))


def at_steps(step, acts):
    for k in sorted({k for k, _ in acts}):
        @pl.when(step == k)
        def _():
            for j, f in acts:
                if j == k:
                    f()


def piece_rows(ref, layer):
    return lambda q: ref.at[layer, pl.ds(q * PC, PC)]


def piece_cols(ref, layer):
    return lambda q: ref.at[layer, :, pl.ds(pl.multiple_of(q * PC, PC) if not isinstance(q, int) else q * PC, PC)]


def p1_body(*refs, geom, mixed, layer, fetch_x, plans):
    n_dp, n_tp, heads, nb, nbs, sp = geom
    (u_ref, halo_ref, nw_ref, wbc_ref, cbc_ref, bbc_ref, e3_ref), refs = refs[:7], refs[7:]
    row = slice(layer, layer + 1)
    nw, cbc, bbc = nw_ref[row].astype(F32), cbc_ref[...].astype(F32), bbc_ref[row].astype(F32)
    if fetch_x:
        (ax, asm, az, ao), (y_ref, c_ref, ac_ref, s_in), (gx, gs, gz, go), refs = refs[:4], refs[4:8], refs[8:12], refs[12:]
    else:
        (ax, gx, gs, az, ao), (y_ref, c_ref, ac_ref, s_in), (gz, go), refs = refs[:5], refs[5:9], refs[9:11], refs[11:]
    (wf, wb, wsem, sm, wdt, cst, st, hcar, xcar, qcar, aoff, ubuf, h_s, la1_s, la2_s, lb1_s, lb2_s, cc_s, cbd_s, row_s, aw_s,
     sbuf, hsem, send, recv), sems = refs[:25], refs[25:]
    p, i = pl.program_id(0), pl.program_id(1)
    np_, ni = pl.num_programs(0), pl.num_programs(1)
    step = p * ni + i
    d_model = u_ref.shape[-1]
    by_z = sp < n_tp
    zs_of = (lambda p: source(p + p // 2 * (1 - 2 * (p % 2)))) if by_z else (lambda p: 0)
    zs = zs_of(p)
    upper = here()[3] == 1

    def state_out(p):
        dp, tp, _, c = here()
        cols = pl.ds(pl.multiple_of(2 * zs_of(p) * PC, PC), sp * PC)
        return pltpu.make_async_remote_copy(src_ref=sbuf, dst_ref=s_in.at[:, cols], send_sem=hsem.at[0], recv_sem=hsem.at[1],
                                            device_id=(dp, tp + 1 - 2 * c), device_id_type=MESH)

    zg = Gather(piece_rows(az, layer), gz, send, recv, 0)
    og = Gather(piece_cols(ao, layer), go, send, recv, SEMS)
    acts = zg.plan(plans[0]) + og.plan(plans[1])
    if fetch_x:
        xg = Gather(piece_rows(ax, layer), gx, send, recv, 2 * SEMS, False)
        small = Small(asm, gs, *sems)
        acts += xg.plan(plans[2])

    def load_w(slot, zsrc):
        return pltpu.make_async_copy(gx.at[:, pl.ds(2 * zsrc, sp)], wf.at[slot], wsem.at[slot])

    def load_own():
        _, tp, _, c = here()
        return ([pltpu.make_async_copy(piece_rows(ax, layer)(q), wf.at[0, q, c], wsem.at[0]) for q in range(n_dp)]
                + [pltpu.make_async_copy(gx.at[q, tp + 1 - 2 * c], wf.at[0, q, 1 - c], wsem.at[0]) for q in range(n_dp)])

    @pl.when(step == 0)
    def _():
        if not by_z:
            load_w(0, 0).start()
        entry_barrier((small.peers() + [(s, here()[1]) for s in zg.side]) if fetch_x else zg.peers())
        if fetch_x:
            small.start()
    at_steps(step, acts)

    @pl.when(step == 0)
    def _():
        if fetch_x:
            small.finish()
            xg.settle_own()
        if by_z:
            for v in load_own():
                v.start()
        cp = pltpu.make_async_copy(gs.at[:, pl.ds(layer * SMALL, SMALL)], sm, wsem.at[2])
        cp.start()
        cp.wait()
        kc = d_model // PC
        hp = heads // n_tp
        for t in range(n_tp):
            for k in range(hp):
                r = head_row(hp * t + k, heads)
                for c in range(kc):
                    wdt[r:r + 1, c * PC:(c + 1) * PC] = sm[t, 16 + kc * k + c:17 + kc * k + c, :].astype(BF16)
                cst[r:r + 1, :] = sm[t, 8 + k:9 + k, :]
                cst[heads + r:heads + r + 1, :] = sm[t, 12 + k:13 + k, :]
        aoff[...] = jnp.zeros_like(aoff)
        hh = rms(halo_ref[...], nw)
        hcar[...] = hh
        qcar[...] = roll8(round_bf16(dot(hh, wbc_ref[...])))

    first = lax.broadcasted_iota(jnp.int32, (CAR, PC), 0) % 8 == 0

    def conv(cur, prev, taps, bias):
        a, now = conv_block(cur[:SUB], prev, taps, bias, first)
        b, now = conv_block(cur[SUB:], now, taps, bias, first)
        return silu(rows_cat(a, b)), now

    ri = lax.broadcasted_iota(jnp.int32, (BLK, BLK), 0)
    ci = lax.broadcasted_iota(jnp.int32, (BLK, BLK), 1)

    def prologue(h, b, hook):
        q0 = dot(h, wbc_ref[...])
        rT = round_bf16(dott(wdt[...], h))
        hook(h, 2)
        bc, qcar[...] = conv(round_bf16(q0), qcar[...],
                             [cbc[k:k + 1] for k in range(4)], bbc)
        bmat, cmat = bc[:, :NST], bc[:, NST:]
        here_rows = slice(b * BLK, (b + 1) * BLK)
        c_ref[here_rows, :] = cmat
        pre = rT + cst[:heads, :BLK]
        dtT = jnp.maximum(pre, 0.0) + jnp.log1p(jnp.exp(-jnp.abs(pre)))
        aT = dtT * cst[heads:, :BLK]
        tr, tc = ri // SUB * SUB + time_of(ri % SUB), ci // SUB * SUB + time_of(ci % SUB)
        acT = dot(aT, jnp.where(tr <= tc, 1.0, 0.0), HI)
        mid, alast = acT[:, SUB - 1:SUB], acT[:, BLK - 1:BLK]
        low = ci[:heads] < SUB
        wT = dtT * jnp.exp2(jnp.where(low, mid, alast) - acT)
        pad = jnp.zeros((BLK - 3 * heads, BLK), BF16)
        a3, w3 = rows_cat(*split3(acT), pad).T, rows_cat(*split3(wT), pad).T
        ac_ref[:, here_rows] = acT + aoff[:, :1]
        aoff[...] = aoff[...] + alast

        def pair_rows(v):
            ev, od = v[:heads // 2], v[heads // 2:]
            l = low[:heads // 2]
            return jnp.where(l, ev, pltpu.roll(od, SUB, 1)), jnp.where(l, pltpu.roll(ev, SUB, 1), od)

        rows = [rows_cat(*[w for zz in zip(*[jnp.split(v, n_tp // 2) for v in ad]) for w in zz])
                for ad in zip(pair_rows(acT), pair_rows(dtT))]
        hook(h, 4)
        cb = dott(cmat, bmat, HI)
        hook(h, EARLY)
        lowr, tri = ci[:SUB] < SUB, time_of(ri[:SUB]) >= time_of(ci[:SUB] % SUB)
        ca, cd = cb[:SUB], cb[SUB:]
        cbd = [jnp.where(tri, jnp.where(lowr, ca, pltpu.roll(ca, SUB, 1)), 0.0),
               jnp.where(tri, jnp.where(lowr, pltpu.roll(cd, SUB, 1), cd), 0.0)]
        bT = bmat.T
        la = kcat6(split3(rows_cat(bT[:, :SUB], cd[:, :SUB])))
        lb = kcat6(split3(pltpu.roll(bT, SUB, 1)[:, :SUB]))
        c1, c2, c3 = split3(cmat)
        return h, a3, w3, rows, cbd, la, lb, (lanes_cat(c1, c2), lanes_cat(c1, c3))

    def spots(b):
        j = i * nbs + b
        at = lambda r: pl.ds(pl.multiple_of(j * r, SUB), r)
        return j, at(BLK), at(NST + SUB)

    def keep(b, vals):
        h, a3, w3, rows, cbd, la, lb, cc = vals
        j, blk, big = spots(b)
        h_s[blk, :] = h
        aw_s[blk, :] = lanes_cat(a3, w3)
        for half in range(2):
            row_s[2 * j + half] = rows[half]
        cbd_s[blk, :] = rows_cat(*cbd)
        la1_s[big, :], la2_s[big, :] = la
        lb1_s[blk, :], lb2_s[blk, :] = lb
        cc_s[blk, :] = lanes_cat(*cc)

    def kept(b):
        j, blk, big = spots(b)
        eight = pl.ds(pl.multiple_of(8 * zs, 8), 8)
        return (None, aw_s[blk, :BLK], aw_s[blk, BLK:], [row_s[2 * j + half, eight, :] for half in range(2)],
                [cbd_s[pl.ds(pl.multiple_of(j * BLK + half * SUB, SUB), SUB), :] for half in range(2)],
                (la1_s[big, :], la2_s[big, :]), (lb1_s[blk, :], lb2_s[blk, :]), (cc_s[blk, :2 * NST], cc_s[blk, 2 * NST:]))


    def all_prologues(hook):
        u = u_ref[...].astype(F32)
        h = rms(u if mixed else unmix(u, ubuf), nw)
        return [prologue(h[b * BLK:(b + 1) * BLK], b, hook) for b in range(nbs)]

    if by_z:
        @pl.when(p == 0)
        def _():
            for b, v in enumerate(all_prologues(lambda h, k: None)):
                keep(b, v)

    @pl.when(i == 0)
    def _():
        slot = p % 2 if by_z else 0

        @pl.when(p == 0)
        def _():
            for v in load_own() if by_z else [load_w(0, 0)]:
                v.wait()

        @pl.when(p > 0)
        def _():
            load_w(slot, zs).wait()
        for q in range(n_dp):
            for k in range(sp):
                wb[q * PC:(q + 1) * PC, k * PC:(k + 1) * PC] = wf[slot, q, k].astype(BF16)
        @pl.when((p > 0) & jnp.logical_not(upper))
        def _():
            state_out(p - 1).start()
        xcar[...] = roll8(round_bf16(dot(hcar[...], wb[...])))
        st[...] = jnp.zeros_like(st)

    @pl.when((i == ni - 1) & (p < np_ - 1))
    def _():
        nd = p + 1
        nd = nd + nd // 2 * (1 - 2 * (nd % 2))
        if fetch_x:
            for d in ORDER:
                pl.when(nd == d)(functools.partial(xg.settle, d))
        load_w((p + 1) % 2, source(nd)).start()

    lane = lax.broadcasted_iota(jnp.int32, (SUB, LANES), 1)
    lo = jnp.where(lane < HD, 1.0, 0.0).astype(BF16)
    hi = jnp.where(lane < HD, 0.0, 1.0).astype(BF16)
    x0 = {}

    def proj(hs, upto):
        for k in range(len(x0), min(sp, upto)):
            x0[k] = dot(hs, wb[:, k * PC:(k + 1) * PC])

    if by_z:
        vals = [kept(b) for b in range(nbs)]
        hs = h_s[pl.ds(pl.multiple_of(i * nbs * BLK, BLK), nbs * BLK), :]
        proj(hs, sp)
    else:
        vals = all_prologues(proj)
        hs = vals[0][0]

    def lanes_of(k):
        return slice(k * PC, (k + 1) * PC), pl.ds(pl.multiple_of((2 * zs + k) * PC, PC), PC)

    def pre(b, k):
        (sl, gl), (_, a3, w3, _, _, _, _, (c12, c13)) = lanes_of(k), vals[b]
        s1, s2, s3 = split3(st[:, sl])
        inter = dot(c12, rows_cat(s1, s1)) + dot(c12, rows_cat(s2, s2)) + dot(c13, rows_cat(s3, s1))
        n3 = e3_ref.shape[0]
        acx = dot(a3[:, :n3], e3_ref[:, gl])
        wx = dot(w3[:, :n3], e3_ref[:, gl])
        proj(hs, k + EARLY + 1)
        return x0[k][b * BLK:(b + 1) * BLK], acx, wx, inter

    def mid_(b, k, x0, acx, wx, inter):
        (sl, _), (_, _, _, rws, cbds, _, _, _) = lanes_of(k), vals[b]
        t = 2 * zs + k
        base = 0 if by_z else k // 2 * 8
        x, xcar[:, sl] = conv(round_bf16(x0), xcar[:, sl], [sm[t, r:r + 1, :] for r in range(4)], sm[t, 4:5, :])
        xw = split3(x * wx)
        r = kcat6r([v[:SUB] for v in xw]) + kcat6r([v[SUB:] for v in xw])
        ms, xs = [], []
        for half in range(2):
            rows = slice(half * SUB, (half + 1) * SUB)
            row, cbd = rws[half][base:base + 8], cbds[half]
            m = []
            for g in range(2):
                seg = acx[rows, g * LANES:(g + 1) * LANES] - row[2 * (k % 2) + g:2 * (k % 2) + g + 1]
                m.append(jnp.exp2(jnp.minimum(seg, 0.0)) * cbd * row[4 + 2 * (k % 2) + g:5 + 2 * (k % 2) + g])
            ms.append(split3(lanes_cat(*m)))
            xs.append([block_diag(v, lo, hi) for v in split3(x[rows])])
        return x, acx, inter, r, ms, xs

    def fin(b, k, x, acx, inter, r, ms, xs):
        (sl, _), (_, _, _, _, _, la, lb, _) = lanes_of(k), vals[b]
        ra = dot(la[0], r[0]) + dot(la[1], r[1])
        rb = dot(lb[0], r[2]) + dot(lb[1], r[3])
        am, al = acx[SUB - 1:SUB], acx[BLK - 1:BLK]
        st[:, sl] = st[:, sl] * jnp.exp2(al) + ra[:NST] * jnp.exp2(al - am) + rb
        skip = sm[2 * zs + k, 6:7, :]
        for half in range(2):
            rows = slice(half * SUB, (half + 1) * SUB)
            (m1, m2, m3), (x1, x2, x3) = ms[half], xs[half]
            r1 = dot(rows_cat(m1, m2, m3), x1)
            r2 = dot(rows_cat(m1, m2), x2)
            y = r1[:SUB] + r1[SUB:2 * SUB] + r1[2 * SUB:] + r2[:SUB] + r2[SUB:] + dot(m1, x3)
            y = y + inter[rows] * jnp.exp2(acx[rows])
            if half:
                y = y + ra[NST:] * jnp.exp2(acx[rows] - am)
            y_ref[b * BLK + half * SUB:b * BLK + (half + 1) * SUB, sl] = y + skip * x[rows]

    units = [(b, k) for b in range(nbs) for k in range(sp)]
    m = mid_(*units[0], *pre(*units[0]))
    for a, nxt in zip(units, units[1:] + [None]):
        if nxt:
            v = pre(*nxt)
        fin(*a, *m)
        if nxt:
            m = mid_(*nxt, *v)

    @pl.when(i == ni - 1)
    def _():
        @pl.when((p > 0) & jnp.logical_not(upper))
        def _():
            state_out(p - 1).wait_send()
        sbuf[...] = st[...]

    @pl.when(step == np_ * ni - 1)
    def _():
        zg.finish()
        og.finish()
        if fetch_x:
            xg.drain()

        @pl.when(jnp.logical_not(upper))
        def _():
            state_out(p).start()
            state_out(p).wait_send()

        @pl.when(upper)
        def _():
            pltpu.make_async_copy(s_in, s_in, hsem.at[1]).wait()


def p1(u, base, halo, nw, wbc, cbc, bbc, e3, comm, n, n_dp, n_tp, mixed, layer, fetch_x, plans, cid):
    d_model, heads = u.shape[-1], PC // HD * n_tp
    sp, nbs = (2, NBS) if fetch_x else (n_tp, 1)
    width, nb, rows = PC * n_tp, n // BLK, BLK * nbs
    ni = nb // nbs
    fixed = lambda shp: pl.BlockSpec(shp, lambda p, i: (0,) * len(shp), pipeline_mode=pl.Buffered(1))
    own_layer = lambda *shp: pl.BlockSpec((None,) + shp, lambda p, i: (layer, 0, 0), pipeline_mode=pl.Buffered(1))
    once = lambda p, i: jnp.where(p == 0, i, ni - 1)
    col = (lambda p: source(p + p // 2 * (1 - 2 * (p % 2)))) if fetch_x else (lambda p: 0)
    hbm = pl.BlockSpec(memory_space=pl.ANY)
    gathered = lambda r: jax.ShapeDtypeStruct((n_dp, n_tp, r, PC), F32)
    outs = [jax.ShapeDtypeStruct((n, width), F32), jax.ShapeDtypeStruct((n, NST), F32),
            jax.ShapeDtypeStruct((heads, n), F32), jax.ShapeDtypeStruct((NST, width), F32)]
    more = ([gathered(PC), jax.ShapeDtypeStruct((n_tp,) + comm[1].shape, F32)] if fetch_x else []) + [gathered(PC)] * 2
    vm = pltpu.VMEM
    dma = lambda k: [pltpu.SemaphoreType.DMA((k,))] * 2
    return pl.pallas_call(
        functools.partial(p1_body, geom=(n_dp, n_tp, heads, nb, nbs, sp), mixed=mixed, layer=layer, fetch_x=fetch_x, plans=plans),
        name="p1", grid=(n_tp // sp, ni),
        in_specs=[pl.BlockSpec((rows, d_model), lambda p, i: (base() + once(p, i), 0)),
                  fixed((CAR, d_model)), fixed((2, d_model)), own_layer(d_model, PC), own_layer(4, PC), fixed((2, PC)),
                  fixed((3 * heads, width))] + [hbm] * len(comm),
        out_specs=[pl.BlockSpec((rows, sp * PC), lambda p, i: (i, col(p))),
                   pl.BlockSpec((rows, NST), lambda p, i: (once(p, i), 0)),
                   pl.BlockSpec((heads, rows), lambda p, i: (0, once(p, i))),
                   hbm] + [hbm] * len(more),
        out_shape=outs + more,
        scratch_shapes=[
            vm((2 if fetch_x else 1, n_dp, sp, PC, PC), F32), vm((d_model, sp * PC), BF16), pltpu.SemaphoreType.DMA((3,)),
            vm((n_tp, SMALL, PC), F32), vm((heads, d_model), BF16), vm((2 * heads, PC), F32), vm((NST, sp * PC), F32),
            vm((CAR, d_model), BF16), vm((CAR, sp * PC), F32), vm((CAR, PC), F32), vm((heads, LANES), F32),
            vm((d_model // LANES * rows, LANES), F32), vm((n, d_model), BF16),
            vm((nb * (NST + SUB), 4 * SUB), BF16), vm((nb * (NST + SUB), 2 * SUB), BF16),
            vm((n, 4 * SUB), BF16), vm((n, 2 * SUB), BF16), vm((n, 4 * NST), BF16), vm((n, LANES), F32),
            vm((2 * nb, 2 * heads // 2, LANES), F32), vm((n, 2 * BLK), BF16), vm((NST, sp * PC), F32), pltpu.SemaphoreType.DMA((2,))]
        + dma(3 * SEMS) + (dma(8) if fetch_x else []),
        compiler_params=pltpu.CompilerParams(dimension_semantics=("arbitrary", "arbitrary"), vmem_limit_bytes=VMEM_CAP,
                                             collective_id=cid, has_side_effects=True),
        cost_estimate=pl.CostEstimate(flops=n * 70 * 10 ** 6, bytes_accessed=n * 12000, transcendentals=0),
    )(u, halo, nw, wbc, cbc, bbc, e3, *comm)


def p2_body(*refs, geom, mix_in, layer, fetch_x, plans):
    n_dp, n_tp, heads = geom
    (u_ref, nw_ref, wz_ref, wo_ref, sm_ref, y_ref, c_ref, ac_ref, s_ref, e3_ref), refs = refs[:10], refs[10:]
    if fetch_x:
        (ax, o_ref, f_ref, gx), refs = refs[:4], refs[4:]
    else:
        (o_ref, r_ref), refs = refs[:2], refs[2:]
    (wzb, wob, wof, wsem, s3, ubuf, send, recv), refs = refs[:8], refs[8:]
    i = pl.program_id(0)
    width = PC * n_tp
    if fetch_x:
        xg = Gather(piece_rows(ax, layer + 1), gx, send, recv, 0)

        @pl.when(i == 0)
        def _():
            entry_barrier(xg.peers())
        at_steps(i, xg.plan(plans))
    else:
        fbuf, = refs
        dp, tp, z, c = here()

        def swap(k):
            return pltpu.make_async_remote_copy(
                src_ref=fbuf.at[k % 2], dst_ref=r_ref.at[pl.ds(pl.multiple_of(k * BLK2, BLK2), BLK2)],
                send_sem=send.at[k % 2], recv_sem=recv.at[0], device_id=(dp, 2 * z + 1 - c), device_id_type=MESH)

        @pl.when(i == 0)
        def _():
            entry_barrier([(dp, 2 * z + 1 - c)])

        @pl.when(i > 1)
        def _():
            swap(i - 2).wait_send()

        @pl.when(i > 0)
        def _():
            swap(i - 1).start()

    @pl.when(i == 0)
    def _():
        pltpu.make_async_copy(wo_ref, wof, wsem).start()
        for d in range(n_dp):
            for t in range(n_tp):
                wzb[d * PC:(d + 1) * PC, t * PC:(t + 1) * PC] = wz_ref[d, t].astype(BF16)
        a, b, c_ = split3(jnp.where(here()[3] == 1, s_ref[...], 0.0))
        for k, (v, w) in enumerate(((a, a), (b, b), (c_, a))):
            s3[k] = rows_cat(v, w)

    u = u_ref[...].astype(F32)
    u = u if mix_in else unmix(u, ubuf)
    h = rms(u, nw_ref[layer:layer + 1].astype(F32))
    c1, c2, c3 = split3(c_ref[...])
    c12, c13 = lanes_cat(c1, c2), lanes_cat(c1, c3)
    eT = rows_cat(*split3(jnp.exp2(ac_ref[...]))).T
    vs, ss = [], 0.0
    for t in range(n_tp):
        sl = slice(t * PC, (t + 1) * PC)
        z_ = round_bf16(dot(h, wzb[:, sl]))
        cor = dot(c12, s3[0, :, sl]) + dot(c12, s3[1, :, sl]) + dot(c13, s3[2, :, sl])
        v = (y_ref[:, sl] + cor * dot(eT, e3_ref[:, sl])) * silu(z_)
        ss = ss + jnp.sum(v * v, axis=-1, keepdims=True)
        vs.append(v)
    sc = lax.rsqrt(ss / width + EPS)
    g = lanes_cat(*[(v * sc * sm_ref[t, 5:6, :]).astype(BF16) for t, v in enumerate(vs)])

    @pl.when(i == 0)
    def _():
        pltpu.make_async_copy(wo_ref, wof, wsem).wait()
        for d in range(n_dp):
            for t in range(n_tp):
                wob[t * PC:(t + 1) * PC, d * PC:(d + 1) * PC] = wof[d, t].astype(BF16)

    un = round_bf16(u + dot(g, wob[...]))
    if fetch_x:
        o_ref[...] = un.astype(BF16)
        f_ref[...] = un[BLK2 - CAR:]
    else:
        un = unmix(un, ubuf)
        fbuf[i % 2] = un
        o_ref[...] = un.astype(BF16)

    @pl.when(i == pl.num_programs(0) - 1)
    def _():
        if fetch_x:
            xg.finish()
        else:
            swap(i).start()
            for k in range(2):
                swap(i - 1 + k).wait_send()
            whole = pltpu.make_async_copy(r_ref, r_ref, recv.at[0])
            whole.wait()


def p2(u, base, nw, wz, wo, sm, y, c, ac, s, e3, comm, n, n_dp, n_tp, mix_in, layer, fetch_x, plans, cid):
    d_model, heads = u.shape[-1], PC // HD * n_tp
    width = PC * n_tp
    fixed = lambda shp: pl.BlockSpec(shp, lambda i: (0,) * len(shp), pipeline_mode=pl.Buffered(1))
    hbm = pl.BlockSpec(memory_space=pl.ANY)
    rows = lambda w: pl.BlockSpec((BLK2, w), lambda i: (i, 0))
    shape = lambda *s: jax.ShapeDtypeStruct(s, F32)
    vm = pltpu.VMEM
    outs = [jax.ShapeDtypeStruct((n, d_model), BF16)]
    specs = [rows(d_model)]
    if fetch_x:
        outs += [shape(CAR, d_model), shape(n_dp, n_tp, PC, PC)]
        specs += [pl.BlockSpec((CAR, d_model), lambda i: (0, 0)), hbm]
    else:
        outs += [shape(n, d_model)]
        specs += [hbm]
    return pl.pallas_call(
        functools.partial(p2_body, geom=(n_dp, n_tp, heads), mix_in=mix_in, layer=layer, fetch_x=fetch_x, plans=plans),
        name="p2", grid=(n // BLK2,),
        in_specs=[pl.BlockSpec((BLK2, d_model), lambda i: (base() + i, 0)),
                  fixed((2, d_model)),
                  fixed((n_dp, n_tp, PC, PC)), hbm,
                  pl.BlockSpec((n_tp, SMALL, PC), lambda i: (0, layer, 0), pipeline_mode=pl.Buffered(1)),
                  rows(width), rows(NST), pl.BlockSpec((heads, BLK2), lambda i: (0, i)),
                  fixed((NST, width)), fixed((3 * heads, width))] + [hbm] * len(comm),
        out_specs=specs, out_shape=outs,
        scratch_shapes=[vm((d_model, width), BF16), vm((width, d_model), BF16), vm((n_dp, n_tp, PC, PC), F32),
                        pltpu.SemaphoreType.DMA, vm((3, 2 * NST, width), BF16),
                        vm((d_model // LANES * BLK2, LANES), F32)]
        + [pltpu.SemaphoreType.DMA((SEMS,))] * 2 + ([] if fetch_x else [vm((2, BLK2, d_model), F32)]),
        compiler_params=pltpu.CompilerParams(dimension_semantics=("arbitrary",), vmem_limit_bytes=VMEM_CAP,
                                             collective_id=cid, has_side_effects=True),
        cost_estimate=pl.CostEstimate(flops=n * 30 * 10 ** 6, bytes_accessed=n * 12000, transcendentals=0),
    )(u, nw, wz, wo, sm, y, c, ac, s, e3, *comm)


def finish_body(own_ref, other_ref, o_ref):
    mine = pl.program_id(0) == here()[3]

    @pl.when(mine)
    def _():
        o_ref[...] = own_ref[...]

    @pl.when(jnp.logical_not(mine))
    def _():
        o_ref[...] = other_ref[...].astype(BF16)


def finish(own, other):
    n, d_model = own.shape
    rows = n // 3
    ni = n // rows
    pick = lambda w: (lambda j, i: (jnp.where((j == here()[3]) == w, i, ni - 1), 0))
    return pl.pallas_call(
        finish_body, name="finish", grid=(2, ni),
        in_specs=[pl.BlockSpec((rows, d_model), pick(True)), pl.BlockSpec((rows, d_model), pick(False))],
        out_specs=pl.BlockSpec((rows, d_model), lambda j, i: (j * ni + i, 0)),
        out_shape=jax.ShapeDtypeStruct((2 * n, d_model), BF16),
        compiler_params=pltpu.CompilerParams(dimension_semantics=("arbitrary", "arbitrary")),
        cost_estimate=pl.CostEstimate(flops=n * d_model, bytes_accessed=n * d_model * 8, transcendentals=0),
    )(own, other)


def small_rows(conv, bias, gate, skip, dtb, al, wdt):
    f = lambda v: v.astype(F32)
    n, hp = skip.shape
    wide = lambda v: jnp.broadcast_to(v[:, :, None], (n, hp, PC))
    one = lambda v: v.reshape(n, 1, PC)
    skip = jnp.broadcast_to(skip[:, :, None], (n, hp, HD))
    v = [f(conv), one(f(bias)), one(f(gate)), one(skip), jnp.zeros((n, 1, PC), F32), wide(dtb), wide(-jnp.exp(al) * LOG2E),
         f(wdt).transpose(0, 2, 1).reshape(n, -1, PC)]
    return jnp.concatenate(v, axis=1).reshape(-1, PC)


PLAN_X = "00010305030507040709"
PLAN_Z0 = "0407080b0a0b0e0d0e11"
PLAN_O0 = "080c0e110f1113121315"
PLAN_Z1 = "0003050806080b090b0e"
PLAN_O1 = "000a0c0f0d0f12101214"
PLAN_X1 = "0003050806080a080a0b"


def solution(mesh):
    n_tp, n_dp = mesh.shape['tp'], mesh.shape['dp']
    rep, col, vec = P(), P(None, None, 'tp'), P(None, 'tp')
    in_specs = (P('dp'), rep, col, col, rep, col, col, rep, vec, rep, vec, vec, vec, vec, P(None, 'tp', None))

    def device_forward(hidden, norm_w, w_z, w_x, w_bc, w_dt, conv_x, conv_bc, bias_x, bias_bc, dt_bias, a_log, d_skip, gate_w, w_out):
        u = hidden[0]
        steps, d_model = u.shape
        n = steps // 2
        core = lax.axis_index('tp') % 2
        e3 = expand_mat(dt_bias.shape[1] * n_tp)
        up = [(2 * k, 2 * k + 1) for k in range(n_tp // 2)]
        ax, az, ao = w_x.astype(F32), w_z.astype(F32), w_out.astype(F32)
        small = small_rows(conv_x, bias_x, gate_w, d_skip, dt_bias, a_log, w_dt)
        tail = u[n - SUB:n].astype(F32).reshape(8, 8, d_model).transpose(1, 0, 2).reshape(SUB, d_model)[SUB - CAR:]
        halo = jnp.where(core == 1, tail, 0.0)
        half = lambda blk: (lambda: lax.axis_index('tp') % 2 * (n // blk))
        none = lambda: 0
        common = (n, n_dp, n_tp)
        bc = (norm_w, w_bc, conv_bc, bias_bc, e3)

        y, c, ac, s, gx, gs, gz, go = p1(u, half(BLK * NBS), halo, *bc, (ax, small, az, ao), *common, False, 0, True,
                                         (PLAN_Z0, PLAN_O0, PLAN_X), 1)
        u, f, gx = p2(u, half(BLK2), norm_w, gz, go, gs, y, c, ac, s, e3, (ax,), *common, False, 0, True, PLAN_X1, 2)
        halo = lax.ppermute(f, 'tp', up)
        y, c, ac, s, gz, go = p1(u, none, halo, *bc, (ax, gx, gs, az, ao), *common, True, 1, False, (PLAN_Z1, PLAN_O1), 3)
        own, other = p2(u, none, norm_w, gz, go, gs, y, c, ac, s, e3, (), *common, True, 1, False, None, 4)
        return finish(own, other)[None]

    return jax.shard_map(device_forward, mesh=mesh, in_specs=in_specs, out_specs=P('dp'), check_vma=False)
```
